32 devices in a mesh: expert: 16 (over z, y, x), wshard: 2 (over core).
Axes of the slice: x: 2, y: 2, z: 4, core: 2. Of those that a mesh axis runs over, the one named last changes fastest.
Arguments:
- layer_input: bfloat16 [4096, 2048], P(('expert', 'wshard')), may hold values from -40 to 40
- attn_gain: bfloat16 [2048], P(('expert', 'wshard')), may hold values from 0.5 to 4
- w_query: bfloat16 [2048, 3072], P(('expert', 'wshard')), may hold values from -1 to 1
- w_latent: bfloat16 [2048, 576], P(('expert', 'wshard')), may hold values from -1 to 1
- kv_gain: bfloat16 [512], P(('expert', 'wshard')), may hold values from 0.5 to 1.5
- w_expand: bfloat16 [512, 4096], P(('expert', 'wshard')), may hold values from -2 to 2
- w_output: bfloat16 [2048, 2048], P(('expert', 'wshard')), may hold values from -2 to 2
- ffn_gain: bfloat16 [2048], P(('expert', 'wshard')), may hold values from 0.5 to 4
- w_router: bfloat16 [2048, 16], P(('expert', 'wshard')), may hold values from -3 to 3
- shared_gate: bfloat16 [2048, 2816], P(('expert', 'wshard')), may hold values from -0.125 to 0.125
- shared_up: bfloat16 [2048, 2816], P(('expert', 'wshard')), may hold values from -0.125 to 0.125
- shared_down: bfloat16 [2816, 2048], P(('expert', 'wshard')), may hold values from -0.109375 to 0.109375
- expert_gate: bfloat16 [16, 2048, 1408], P('expert', None, 'wshard'), may hold values from -0.125 to 0.125
- expert_up: bfloat16 [16, 2048, 1408], P('expert', None, 'wshard'), may hold values from -0.125 to 0.125
- expert_down: bfloat16 [16, 1408, 2048], P('expert', 'wshard'), may hold values from -0.875 to 0.875
- routes: int32 [4096, 6], P(('expert', 'wshard')), may hold values from 0 to 15, all different within a row; in each aligned block of 128 rows (0 to 127, 128 to 255, ...) at most 96 rows name the same one
- segments: int32 [4096], P(('expert', 'wshard')), may hold values from 0 to 7, never falling along the last dimension, each value on 1 to 1024 neighbouring positions
- cotangent: bfloat16 [4096, 2048], P(('expert', 'wshard')), may hold values from -6 to 6
Outputs:
- layer_output: float32 [4096, 2048], P(('expert', 'wshard'))
- grad_x: float32 [4096, 2048], P(('expert', 'wshard'))
- grad_attn_gain: float32 [2048], P(('expert', 'wshard'))
- grad_w_query: float32 [2048, 3072], P(('expert', 'wshard'))
- grad_w_latent: float32 [2048, 576], P(('expert', 'wshard'))
- grad_kv_gain: float32 [512], P(('expert', 'wshard'))
- grad_w_expand: float32 [512, 4096], P(('expert', 'wshard'))
- grad_w_output: float32 [2048, 2048], P(('expert', 'wshard'))
- grad_ffn_gain: float32 [2048], P(('expert', 'wshard'))
- grad_w_router: float32 [2048, 16], P(('expert', 'wshard'))
- grad_shared_gate: float32 [2048, 2816], P(('expert', 'wshard'))
- grad_shared_up: float32 [2048, 2816], P(('expert', 'wshard'))
- grad_shared_down: float32 [2816, 2048], P(('expert', 'wshard'))
- grad_expert_gate: float32 [16, 2048, 1408], P('expert', None, 'wshard')
- grad_expert_up: float32 [16, 2048, 1408], P('expert', None, 'wshard')
- grad_expert_down: float32 [16, 1408, 2048], P('expert', 'wshard')
The draws below stay inside these ranges and needn't reach their ends.
Inputs may be any that keep to these rules, and one draw needn't show every extreme that they name: `routes`: each row names 6 different experts. Among the 128 rows of one device (aligned blocks) no expert is named by more than 96 rows, a bound that some block reaches. `segments`: document numbers never fall along the tokens; each document holds 1 to 1024 consecutive tokens and one holds exactly 1024.
All inputs are finite; a program needn't handle non-finite values.
Results may differ from the reference program's by a relative error of at most 0.025.
The reference program's roundings to bfloat16 on the way count: a program that leaves them out, or rounds other values in their place, can miss the bound.
Values may be sent and summed in bfloat16 or wider, within the bound.
A program may use at most 448 MiB of HBM per device.

```python
import math
import jax
import jax.numpy as jnp
import numpy as np
from jax import lax

D = 2048
HEADS = 16
NOPE = 128
ROPE = 64
VDIM = 128
RANK = 512
EFF = 1408
TOP = 6
TOK_DEV = 128
DOC_MAX = 1024
SFF = 2816
EXPERTS = 16
TOKENS = 4096
CAP = 96
N_EXPERT = 16
N_WSHARD = 2


def gain_values(key, count):
    values = 1.0 + 0.1 * jnp.clip(jax.random.normal(key, (count,), jnp.float32), -4.0, 4.0)
    return values.astype(jnp.bfloat16)


def draw_attn_gain(key, part):
    return gain_values(jax.random.fold_in(key, 11), D)


def draw_ffn_gain(key, part):
    return gain_values(jax.random.fold_in(key, 23), D)


def base_weight(key, shape, fan_in):
    return jnp.clip(jax.random.normal(key, shape, jnp.float32), -4.0, 4.0) * fan_in ** (-0.5)


def draw_layer_input(key, part):
    values = jnp.clip(jax.random.normal(jax.random.fold_in(key, 201), (TOKENS, D), jnp.float32), -6.0, 6.0)
    return values.astype(jnp.bfloat16)


def draw_w_query(key, part):
    values = base_weight(jax.random.fold_in(key, 211), (D, HEADS, NOPE + ROPE), D)
    return values.reshape(D, HEADS * (NOPE + ROPE)).astype(jnp.bfloat16)


def draw_w_latent(key, part):
    values = base_weight(jax.random.fold_in(key, 213), (D, RANK + ROPE), D)
    return values.astype(jnp.bfloat16)


def draw_w_expand(key, part):
    values = base_weight(jax.random.fold_in(key, 215), (RANK, HEADS, NOPE + VDIM), RANK)
    return values.reshape(RANK, HEADS * (NOPE + VDIM)).astype(jnp.bfloat16)


def draw_w_router(key, part):
    values = base_weight(jax.random.fold_in(key, 217), (D, EXPERTS), D)
    return values.astype(jnp.bfloat16)


def block_scale(own_key, shape, split, least, high):
    factor_of = 1.0
    for dim, blocks in split:
        steps = jax.random.uniform(jax.random.fold_in(jax.random.fold_in(own_key, 6), dim), (blocks,), jnp.float32, least / len(split), high / len(split))
        factor_of = factor_of * jnp.repeat(jnp.exp(steps), shape[dim] // blocks).reshape((-1,) + (1,) * (len(shape) - 1 - dim))
    return factor_of


def split_up(count, total, bound, lean):
    loads = [(1 << 20) // math.isqrt(rank ** lean) + 1 for rank in range(2, count + 1)]
    surplus, counts = total - bound - (count - 1), [1] * (count - 1)
    while surplus > 0:
        movable = [i for i in range(count - 1) if counts[i] < bound]
        whole, left = sum([loads[i] for i in movable]), surplus
        for i in movable:
            addition = min(bound - counts[i], max(1, left * loads[i] // whole), surplus)
            counts[i] = counts[i] + addition
            surplus = surplus - addition
    return np.array([bound] + counts)


def ragged_sizes(key, amount, total, limit, lean):
    if amount == 2:
        one = jax.random.randint(key, (), max(1, total - limit), min(limit, total - 1) + 1)
        return jnp.stack([one, total - one])
    sizes = jnp.asarray(split_up(amount, total, limit, lean), jnp.int32)
    pairs = (amount - 1) // 2
    donor, receiver = sizes[1:1 + 2 * pairs:2], sizes[2:2 + 2 * pairs:2]
    slack = jnp.minimum(donor - 1, limit - receiver)
    shifted = jax.random.randint(jax.random.fold_in(key, 1), (pairs,), 0, 1 << 20) % (slack + 1)
    sizes = sizes.at[1:1 + 2 * pairs:2].set(donor - shifted).at[2:2 + 2 * pairs:2].set(receiver + shifted)
    return sizes[jax.random.permutation(jax.random.fold_in(key, 2), amount)]


def routed_block(own_key, own, number, rows, count, top, most, slope):
    sequence = jax.random.permutation(own_key, count)
    crowded, usual = portions_of(count, rows * top, most, slope, True), portions_of(count, rows * top, most, slope, False)
    places = jnp.arange(count)

    def named(sizes, offset_by):
        used = int((sizes > 0).sum())
        fixed = max(1, used // 4)
        shifted = fixed + (places - fixed + offset_by * (used - fixed)) % max(1, count - fixed)
        return jnp.zeros((count,), jnp.int32).at[sequence[jnp.where(places < fixed, places, shifted)]].set(jnp.asarray(sizes, jnp.int32))

    sizes = jnp.where(number % 4 == 0, named(crowded, number // 4), named(usual, number - number // 4 - 1))
    mixed = jax.random.permutation(jax.random.fold_in(own, 3), count)
    source_of, receiver = mixed[0:count // 2 * 2:2], mixed[1:count // 2 * 2:2]
    slack = jnp.minimum(sizes[source_of] - 1, most - sizes[receiver]) // 2
    slack = jnp.where((source_of == sequence[0]) | (receiver == sequence[0]) | (sizes[receiver] == 0), 0, jnp.maximum(slack, 0))
    shifted = jax.random.randint(jax.random.fold_in(own, 4), (count // 2,), 0, 1 << 20) % (slack + 1)
    sizes = sizes.at[source_of].add(-shifted).at[receiver].add(shifted)
    items = jnp.searchsorted(jnp.cumsum(sizes), jnp.arange(rows * top), side="right").astype(jnp.int32)
    table = items.reshape(top, rows).T
    table = table[jax.random.permutation(jax.random.fold_in(own, 1), rows)]
    offset_by = jax.random.randint(jax.random.fold_in(own, 2), (rows, 1), 0, top)
    return jnp.take_along_axis(table, (jnp.arange(top)[None, :] + offset_by) % top, axis=1)


def portions_of(number_of, total, bound, skew, full):
    portions = [(1 << 20) // math.isqrt(standing ** skew) + 1 for standing in range(1, number_of + 1)]
    largest = bound if full else min(bound, max(-(-total // number_of), total * portions[0] // sum(portions)))
    least = 1 if total - largest >= number_of - 1 else 0
    counts, spare = [largest] + [least] * (number_of - 1), total - largest - least * (number_of - 1)
    while spare > 0:
        free = [i for i in range(1, number_of) if counts[i] < largest] or [i for i in range(1, number_of) if counts[i] < bound]
        whole, remaining = sum([portions[i] for i in free]), spare
        for i in free:
            extra = min(bound - counts[i], max(1, remaining * portions[i] // whole), spare)
            counts[i] = counts[i] + extra
            spare = spare - extra
    return np.array(counts)


def normal_values(stream_key, extent, scale, reach, split=(), kind=jnp.bfloat16):
    level = block_scale(stream_key, extent, split, -0.22, 0.18) if split else 1.0
    values = jax.random.normal(stream_key, extent, jnp.float32) * scale * level
    return jnp.minimum(jnp.maximum(values, -reach), reach).astype(kind)


def setup_inputs(seed: int = 0) -> dict:
    streams_of = jax.random.split(jax.random.key(seed), 19)
    layer_input = draw_layer_input(jax.random.fold_in(streams_of[18], 71), 0)
    attn_gain = draw_attn_gain(jax.random.fold_in(streams_of[18], 71), 0)
    w_query = draw_w_query(jax.random.fold_in(streams_of[18], 71), 0)
    w_latent = draw_w_latent(jax.random.fold_in(streams_of[18], 71), 0)
    kv_gain = jnp.clip(1.0 + 0.1 * jax.random.normal(streams_of[4], (RANK,), jnp.float32), 0.5, 1.5).astype(jnp.bfloat16)
    w_expand = draw_w_expand(jax.random.fold_in(streams_of[18], 71), 0)
    w_output = normal_values(streams_of[6], (HEADS * VDIM, D), (HEADS * VDIM * 4 // DOC_MAX) ** -0.5, 2.0, ((0, 32),))
    ffn_gain = draw_ffn_gain(jax.random.fold_in(streams_of[18], 71), 0)
    w_router = draw_w_router(jax.random.fold_in(streams_of[18], 71), 0)
    shared_gate = normal_values(streams_of[9], (D, SFF), D ** -0.5, 0.125, ((0, 32),))
    shared_up = normal_values(streams_of[10], (D, SFF), D ** -0.5, 0.125, ((0, 32),))
    shared_down = normal_values(streams_of[11], (SFF, D), SFF ** -0.5, 0.109375, ((0, 32),))
    expert_gate = normal_values(streams_of[12], (EXPERTS, D, EFF), D ** -0.5, 0.125, ((0, 16), (2, 2)))
    expert_up = normal_values(streams_of[13], (EXPERTS, D, EFF), D ** -0.5, 0.125, ((0, 16), (2, 2)))
    expert_down = normal_values(streams_of[14], (EXPERTS, EFF, D), (EFF // 32) ** -0.5, 0.875, ((0, 16), (1, 2)))
    routes_keys = jax.random.split(jax.random.fold_in(streams_of[15], 1), TOKENS // TOK_DEV)
    routes_turns = jax.random.permutation(jax.random.fold_in(streams_of[15], 3), TOKENS // TOK_DEV)
    routes = jax.vmap(lambda own, number: routed_block(jax.random.fold_in(streams_of[15], 2), own, number, TOK_DEV, EXPERTS, TOP, CAP, 2))(routes_keys, routes_turns).reshape((TOKENS, TOP))
    segments = jnp.searchsorted(jnp.cumsum(ragged_sizes(streams_of[16], 2 * TOKENS // DOC_MAX, TOKENS, DOC_MAX, 0)), jnp.arange(TOKENS), side="right").astype(jnp.int32)
    cotangent = normal_values(streams_of[17], (TOKENS, D), 1.0, 6.0, ((0, 32),))
    return dict(layer_input=layer_input, attn_gain=attn_gain, w_query=w_query, w_latent=w_latent, kv_gain=kv_gain, w_expand=w_expand, w_output=w_output, ffn_gain=ffn_gain, w_router=w_router, shared_gate=shared_gate, shared_up=shared_up, shared_down=shared_down, expert_gate=expert_gate, expert_up=expert_up, expert_down=expert_down, routes=routes, segments=segments, cotangent=cotangent)


@jax.custom_vjp
def low(v):
    return lax.optimization_barrier(v.astype(jnp.bfloat16)).astype(jnp.float32)

@jax.custom_vjp
def low_back(v):
    return v

def low_keep(v):
    return (low(v), None)

def low_pass(kept, grad):
    return (grad,)

def back_keep(v):
    return (v, None)

def back_low(kept, grad):
    return (low(grad),)
low.defvjp(low_keep, low_pass)
low_back.defvjp(back_keep, back_low)
highest = lax.Precision.HIGHEST
epsilon = 1e-06
query_rows = 512

def matmul(left, right):
    return jnp.dot(left, right, precision=highest, preferred_element_type=jnp.float32)

def rms_norm(vector, scaling):
    return vector * lax.rsqrt(lax.optimization_barrier(jnp.mean(vector * vector, axis=-1, keepdims=True)) + epsilon) * scaling

def rotate(vector, cosine, sine_part):
    half_width = vector.shape[-1] // 2
    front_half = vector[..., :half_width]
    back_half = vector[..., half_width:]
    return jnp.concatenate([front_half * cosine - back_half * sine_part, back_half * cosine + front_half * sine_part], axis=-1)

def softmax_rows(scores):
    row_top = lax.optimization_barrier(jnp.max(scores, axis=-1, keepdims=True))
    exp_scores = jnp.exp(scores - row_top)
    return exp_scores / lax.optimization_barrier(jnp.sum(exp_scores, axis=-1, keepdims=True))

def slot_places(routes):
    device_total = N_EXPERT * N_WSHARD
    blocks = routes.reshape(device_total, TOK_DEV * TOP)
    route_hot = (blocks[:, :, None] == jnp.arange(EXPERTS, dtype=jnp.int32)[None, None, :]).astype(jnp.int32)
    earlier = jnp.cumsum(route_hot, axis=1) - route_hot
    route_slot = lax.optimization_barrier(jnp.sum(earlier * route_hot, axis=2))
    device_ids = jnp.arange(device_total, dtype=jnp.int32)[:, None]
    return (device_ids * (EXPERTS * CAP) + blocks * CAP + route_slot).reshape(-1)

def layer(params, routes, segments, places):
    layer_input, attn_gain, w_query, w_latent, kv_gain, w_expand, w_output, ffn_gain, w_router, shared_gate, shared_up, shared_down, expert_gate, expert_up, expert_down = params
    device_total = N_EXPERT * N_WSHARD
    hidden = low(rms_norm(layer_input, attn_gain))
    rope_half = ROPE // 2
    positions = jnp.arange(TOKENS, dtype=jnp.float32)
    frequency = 10000.0 ** (-jnp.arange(rope_half, dtype=jnp.float32) / rope_half)
    angles = positions[:, None] * frequency[None, :]
    cosine = jnp.cos(angles)
    sine_part = jnp.sin(angles)
    query_lin = low_back(matmul(hidden, w_query)).reshape(TOKENS, HEADS, NOPE + ROPE)
    queries = low(jnp.concatenate([query_lin[..., :NOPE], rotate(query_lin[..., NOPE:], cosine[:, None, :], sine_part[:, None, :])], axis=-1))
    latent = low_back(matmul(hidden, w_latent))
    compressed = low(rms_norm(latent[:, :RANK], kv_gain))
    key_rope = low(rotate(latent[:, RANK:], cosine, sine_part))
    expanded = low_back(low(matmul(compressed, w_expand))).reshape(TOKENS, HEADS, NOPE + VDIM)
    padded_keys = jnp.pad(expanded, ((DOC_MAX, 0), (0, 0), (0, 0)))
    padded_rope = jnp.pad(key_rope, ((DOC_MAX, 0), (0, 0)))
    padded_segments = jnp.pad(segments, (DOC_MAX, 0), constant_values=-1)
    score_scale = (NOPE + ROPE) ** (-0.5)
    window = query_rows + DOC_MAX

    def attend(start):
        block_queries = lax.dynamic_slice_in_dim(queries, start, query_rows, 0)
        query_segments = lax.dynamic_slice_in_dim(segments, start, query_rows, 0)
        block_keys = lax.dynamic_slice_in_dim(padded_keys, start, window, 0)
        block_rope = lax.dynamic_slice_in_dim(padded_rope, start, window, 0)
        key_segments = lax.dynamic_slice_in_dim(padded_segments, start, window, 0)
        raw_scores = jnp.einsum('qhn,khn->hqk', block_queries[..., :NOPE], block_keys[..., :NOPE], precision=highest)
        raw_scores = raw_scores + jnp.einsum('qhr,kr->hqk', block_queries[..., NOPE:], block_rope, precision=highest)
        scaled = low_back(raw_scores) * score_scale
        query_pos = jnp.arange(query_rows, dtype=jnp.int32) + DOC_MAX
        key_pos = jnp.arange(window, dtype=jnp.int32)
        allowed = (query_segments[:, None] == key_segments[None, :]) & (key_pos[None, :] <= query_pos[:, None])
        scaled = jnp.where(allowed[None], scaled, -1e+30)
        attn_probs = softmax_rows(scaled)
        mixed_block = jnp.einsum('hqk,khv->qhv', low(attn_probs), block_keys[..., NOPE:], precision=highest)
        return mixed_block.reshape(query_rows, HEADS * VDIM)
    starts = jnp.arange(TOKENS // query_rows, dtype=jnp.int32) * query_rows
    mixed = lax.map(jax.checkpoint(attend), starts).reshape(TOKENS, HEADS * VDIM)
    mixed = low_back(low(mixed))
    residual_one = layer_input + low_back(matmul(mixed, w_output))
    h_two = low(rms_norm(residual_one, ffn_gain))
    router_probs = softmax_rows(low_back(matmul(h_two, w_router)))
    shared_gate_pre = low_back(matmul(h_two, shared_gate))
    shared_up_pre = low_back(matmul(h_two, shared_up))
    shared_act = low(jax.nn.silu(shared_gate_pre) * shared_up_pre)
    shared_out = low_back(matmul(shared_act, shared_down))
    repeated = jnp.repeat(h_two, TOP, axis=0)
    slot_rows = jnp.zeros((device_total * EXPERTS * CAP, D), jnp.float32).at[places].set(repeated)
    slot_rows = low_back(slot_rows)
    by_expert = slot_rows.reshape(device_total, EXPERTS, CAP, D).transpose(1, 0, 2, 3).reshape(EXPERTS, device_total * CAP, D)

    def expert_apply(inputs):
        rows_in, gate_weight, up_weight, down_weight = inputs
        gate_pre = low_back(matmul(rows_in, gate_weight))
        up_pre = low_back(matmul(rows_in, up_weight))
        activation = low(jax.nn.silu(gate_pre) * up_pre)
        return low_back(low(matmul(activation, down_weight)))
    expert_rows = lax.map(jax.checkpoint(expert_apply), (by_expert, expert_gate, expert_up, expert_down))
    expert_rows = expert_rows.reshape(EXPERTS, device_total, CAP, D).transpose(1, 0, 2, 3).reshape(device_total * EXPERTS * CAP, D)
    picked = expert_rows[places].reshape(TOKENS, TOP, D)
    gate_weights = jnp.take_along_axis(router_probs, routes, axis=1)
    routed = lax.optimization_barrier(jnp.sum(gate_weights[:, :, None] * picked, axis=1))
    return residual_one + shared_out + routed

def reference(layer_input, attn_gain, w_query, w_latent, kv_gain, w_expand, w_output, ffn_gain, w_router, shared_gate, shared_up, shared_down, expert_gate, expert_up, expert_down, routes, segments, cotangent):
    places = slot_places(routes)
    params = tuple((argument.astype(jnp.float32) for argument in (layer_input, attn_gain, w_query, w_latent, kv_gain, w_expand, w_output, ffn_gain, w_router, shared_gate, shared_up, shared_down, expert_gate, expert_up, expert_down)))

    def forward(*values):
        return layer(values, routes, segments, places)
    output, pullback = jax.vjp(forward, *params)
    grads = pullback(cotangent.astype(jnp.float32))
    return (output, grads[0], grads[1], grads[2], grads[3], grads[4], grads[5], grads[6], grads[7], grads[8], grads[9], grads[10], grads[11], grads[12], grads[13], grads[14])
```

```python
import functools

import jax
import jax.numpy as jnp
from jax import lax
from jax.experimental import pallas as pl
from jax.experimental.pallas import tpu as pltpu
from jax.sharding import Mesh, PartitionSpec as P

HEADS = 16
NOPE = 128
ROPE = 64
VDIM = 128
RANK = 512
TOP = 6
DOC_MAX = 1024
QUERY_BLOCK = 256

BF = jnp.bfloat16
F32 = jnp.float32
ALL = ("g", "p", "c")
PLANE = ("p", "c")

epsilon = 1e-06


def rms_norm(vector, scaling):
    return vector * lax.rsqrt(jnp.mean(vector * vector, axis=-1, keepdims=True) + epsilon) * scaling


def rotate(vector, cosine, sine_part):
    half_width = vector.shape[-1] // 2
    front_half = vector[..., :half_width]
    back_half = vector[..., half_width:]
    return jnp.concatenate(
        [front_half * cosine - back_half * sine_part, back_half * cosine + front_half * sine_part],
        axis=-1,
    )


def unrotate(vector, cosine, sine_part):
    return rotate(vector, cosine, -sine_part)


def matmul(left, right):
    return jnp.dot(left, right, preferred_element_type=F32)


def dot_nt(left, right):
    return lax.dot_general(left, right, (((1,), (1,)), ((), ())), preferred_element_type=F32)


def dot_tn(left, right):
    return lax.dot_general(left, right, (((0,), (0,)), ((), ())), preferred_element_type=F32)


def swiglu(gate_pre, up_pre):
    return jax.nn.silu(gate_pre) * up_pre


def softmax_rows(scores):
    row_top = jnp.max(scores, axis=-1, keepdims=True)
    exp_scores = jnp.exp(scores - row_top)
    return exp_scores / jnp.sum(exp_scores, axis=-1, keepdims=True)


def masked_scores(base, low_bound, q_nope, q_rope, k_nope, k_rope, scale):
    rows, span = q_nope.shape[0], k_nope.shape[0]
    key_at = lax.broadcasted_iota(jnp.int32, (rows, span), 1) + base
    query_at = lax.broadcasted_iota(jnp.int32, (rows, span), 0) + (base + DOC_MAX)
    allowed = (key_at >= low_bound) & (key_at <= query_at)
    scores = (dot_nt(q_nope, k_nope) + dot_nt(q_rope, k_rope)) * scale
    return jnp.where(allowed, scores, -1e30)


def attend_kernel(heads, scale, low_ref, qn_ref, qr_ref, ex_ref, kr_ref, out_ref, lse_ref):
    rows = qn_ref.shape[0]
    base = pl.multiple_of(pl.program_id(0) * rows, rows)
    window = pl.ds(base, rows + DOC_MAX)
    k_rope = kr_ref[window, :]
    low_bound = low_ref[...]
    for h in range(heads):
        at = h * (NOPE + VDIM)
        k_nope = ex_ref[window, at : at + NOPE]
        value = ex_ref[window, at + NOPE : at + NOPE + VDIM]
        scores = masked_scores(
            base,
            low_bound,
            qn_ref[:, h * NOPE : (h + 1) * NOPE],
            qr_ref[:, h * ROPE : (h + 1) * ROPE],
            k_nope,
            k_rope,
            scale,
        )
        top = jnp.max(scores, axis=-1, keepdims=True)
        exps = jnp.exp(scores - top)
        total = jnp.sum(exps, axis=-1, keepdims=True)
        probs = (exps / total).astype(BF)
        out_ref[:, h * VDIM : (h + 1) * VDIM] = jnp.dot(
            probs, value, preferred_element_type=F32
        ).astype(BF)
        lse_ref[:, h : h + 1] = top + jnp.log(total)


def attend(low_bound, q_nope, q_rope, expanded, key_rope, scale):
    queries = q_nope.shape[0]
    heads = q_nope.shape[1] // NOPE
    rows = QUERY_BLOCK

    def whole(array):
        return pl.BlockSpec(array.shape, lambda i: (0, 0))

    def blocked(width):
        return pl.BlockSpec((rows, width), lambda i: (i, 0))

    flops = 2 * heads * queries * (rows + DOC_MAX) * (NOPE + ROPE + VDIM)
    return pl.pallas_call(
        functools.partial(attend_kernel, heads, scale),
        grid=(queries // rows,),
        in_specs=[
            blocked(1),
            blocked(heads * NOPE),
            blocked(heads * ROPE),
            whole(expanded),
            whole(key_rope),
        ],
        out_specs=[blocked(heads * VDIM), blocked(heads)],
        out_shape=[
            jax.ShapeDtypeStruct((queries, heads * VDIM), BF),
            jax.ShapeDtypeStruct((queries, heads), F32),
        ],
        cost_estimate=pl.CostEstimate(
            flops=flops, bytes_accessed=4 * expanded.size, transcendentals=flops // 640
        ),
        compiler_params=pltpu.CompilerParams(vmem_limit_bytes=50 * 1024 * 1024),
        name="attend",
    )(low_bound, q_nope, q_rope, expanded, key_rope)


def attend_back_kernel(
    heads, scale, low_ref, qn_ref, qr_ref, ex_ref, kr_ref, lse_ref, gm_ref,
    dqn_ref, dqr_ref, dex_ref, dkr_ref,
):
    rows = qn_ref.shape[0]
    step = pl.program_id(0)
    base = pl.multiple_of(step * rows, rows)
    window = pl.ds(base, rows + DOC_MAX)

    @pl.when(step == 0)
    def _():
        dex_ref[...] = jnp.zeros_like(dex_ref)
        dkr_ref[...] = jnp.zeros_like(dkr_ref)

    k_rope = kr_ref[window, :]
    low_bound = low_ref[...]
    for h in range(heads):
        at = h * (NOPE + VDIM)
        k_nope = ex_ref[window, at : at + NOPE]
        value = ex_ref[window, at + NOPE : at + NOPE + VDIM]
        q_nope = qn_ref[:, h * NOPE : (h + 1) * NOPE]
        q_rope = qr_ref[:, h * ROPE : (h + 1) * ROPE]
        grad_out = gm_ref[:, h * VDIM : (h + 1) * VDIM]
        scores = masked_scores(base, low_bound, q_nope, q_rope, k_nope, k_rope, scale)
        probs = jnp.exp(scores - lse_ref[:, h : h + 1])
        grad_probs = dot_nt(grad_out, value)
        mean_grad = jnp.sum(probs * grad_probs, axis=-1, keepdims=True)
        grad_scores = (probs * (grad_probs - mean_grad) * scale).astype(BF)
        probs_low = probs.astype(BF)
        dqn_ref[:, h * NOPE : (h + 1) * NOPE] = jnp.dot(
            grad_scores, k_nope, preferred_element_type=F32
        )
        dqr_ref[:, h * ROPE : (h + 1) * ROPE] = jnp.dot(
            grad_scores, k_rope, preferred_element_type=F32
        )
        dex_ref[window, at : at + NOPE] += dot_tn(grad_scores, q_nope)
        dex_ref[window, at + NOPE : at + NOPE + VDIM] += dot_tn(probs_low, grad_out)
        dkr_ref[window, :] += dot_tn(grad_scores, q_rope)


def attend_back(low_bound, q_nope, q_rope, expanded, key_rope, lse, grad_mixed, scale):
    queries = q_nope.shape[0]
    heads = q_nope.shape[1] // NOPE
    rows = QUERY_BLOCK

    def whole(shape):
        return pl.BlockSpec(shape, lambda i: (0, 0))

    def blocked(width):
        return pl.BlockSpec((rows, width), lambda i: (i, 0))

    flops = 2 * heads * queries * (rows + DOC_MAX) * (3 * NOPE + 3 * ROPE + 2 * VDIM)
    return pl.pallas_call(
        functools.partial(attend_back_kernel, heads, scale),
        grid=(queries // rows,),
        in_specs=[
            blocked(1),
            blocked(heads * NOPE),
            blocked(heads * ROPE),
            whole(expanded.shape),
            whole(key_rope.shape),
            blocked(heads),
            blocked(heads * VDIM),
        ],
        out_specs=[
            blocked(heads * NOPE),
            blocked(heads * ROPE),
            whole(expanded.shape),
            whole(key_rope.shape),
        ],
        out_shape=[
            jax.ShapeDtypeStruct(q_nope.shape, F32),
            jax.ShapeDtypeStruct(q_rope.shape, F32),
            jax.ShapeDtypeStruct(expanded.shape, F32),
            jax.ShapeDtypeStruct(key_rope.shape, F32),
        ],
        cost_estimate=pl.CostEstimate(
            flops=flops, bytes_accessed=8 * expanded.size, transcendentals=flops // 1664
        ),
        compiler_params=pltpu.CompilerParams(vmem_limit_bytes=56 * 1024 * 1024),
        name="attend_back",
    )(low_bound, q_nope, q_rope, expanded, key_rope, lse, grad_mixed)


def gather_all(x):
    return lax.all_gather(x, ALL, axis=0, tiled=True)


def experts_chunk(h2, cot, weight, slots, expert_w, shared_w):
    w_gate, w_up, w_down = expert_w
    s_both, s_down = shared_w
    blocks, rows, width = h2.shape
    per_block = slots.shape[1]
    hidden_s = s_down.shape[0]
    flat_h2 = h2.reshape(blocks * rows, width)
    flat_cot = cot.reshape(blocks * rows, width)

    def pick(table):
        return (
            jnp.einsum("bst,btd->bsd", slots, table, preferred_element_type=F32)
            .astype(BF)
            .reshape(blocks * per_block, width)
        )

    def place(table):
        return jnp.einsum(
            "bst,bsd->btd",
            slots,
            table.astype(BF).reshape(blocks, per_block, width),
            preferred_element_type=F32,
        ).reshape(blocks * rows, width)

    cot_rows = pick(cot)
    back_act = dot_nt(cot_rows, w_down)
    shared_back = dot_nt(flat_cot, s_down)
    row_weight = jnp.sum(slots.astype(F32) * weight[:, None, :], axis=2).reshape(-1, 1)
    rows_in = pick(h2)
    gate_pre = matmul(rows_in, w_gate)
    up_pre = matmul(rows_in, w_up)
    act, act_vjp = jax.vjp(swiglu, gate_pre, up_pre)
    act_low = act.astype(BF)
    grad_gate, grad_up = act_vjp(back_act * row_weight)
    grad_gate = grad_gate.astype(BF)
    grad_up = grad_up.astype(BF)
    picked_grad = jnp.sum(act_low.astype(F32) * back_act, axis=1).reshape(blocks, per_block, 1)
    token_grad = jnp.sum(slots.astype(F32) * picked_grad, axis=1)
    grad_rows = dot_nt(grad_gate, w_gate) + dot_nt(grad_up, w_up)

    shared_pre = matmul(flat_h2, s_both)
    s_act, s_vjp = jax.vjp(swiglu, shared_pre[:, :hidden_s], shared_pre[:, hidden_s:])
    s_act = s_act.astype(BF)
    s_grad = jnp.concatenate(s_vjp(shared_back), axis=1).astype(BF)
    grad_h2 = (place(grad_rows) + dot_nt(s_grad, s_both)).astype(BF)

    out_rows = matmul(act_low, w_down) * row_weight
    out = (place(out_rows) + matmul(s_act, s_down)).astype(BF)

    grad_in = (cot_rows.astype(F32) * row_weight).astype(BF)
    grads = (
        dot_tn(rows_in, grad_gate),
        dot_tn(rows_in, grad_up),
        dot_tn(act_low, grad_in),
        dot_tn(flat_h2, s_grad),
        dot_tn(s_act, flat_cot),
    )
    return out, grad_h2, token_grad, grads


def body(
    n_groups, n_plane, layer_input, attn_gain, w_query, w_latent, kv_gain, w_expand, w_output,
    ffn_gain, w_router, shared_gate, shared_up, shared_down, expert_gate, expert_up,
    expert_down, routes, segments, cotangent,
):
    tok, width = layer_input.shape
    devices = n_groups * n_plane
    experts = w_router.shape[1]
    local_heads = HEADS // n_plane
    scale = (NOPE + ROPE) ** (-0.5)
    group = lax.axis_index("g")
    place_in = lax.axis_index(PLANE)
    me = lax.axis_index(ALL)
    expert_id = lax.axis_index(("g", "p"))
    plane_tok = n_plane * tok
    plane_start = group * plane_tok

    rows_w = w_router.shape[0]
    kv_n = kv_gain.shape[0]
    small = jnp.concatenate([attn_gain, ffn_gain, kv_gain, w_router.reshape(-1)])
    small = gather_all(small[None, :])
    gain_one = small[:, :rows_w].reshape(-1).astype(F32)
    gain_two = small[:, rows_w : 2 * rows_w].reshape(-1).astype(F32)
    gain_kv = small[:, 2 * rows_w : 2 * rows_w + kv_n].reshape(-1).astype(F32)
    router_weight = small[:, 2 * rows_w + kv_n :].reshape(width, experts)
    ints = gather_all(jnp.concatenate([routes.reshape(-1), segments])[None, :])
    routes_all = ints[:, : tok * TOP].reshape(devices, tok, TOP)
    segments_all = ints[:, tok * TOP :].reshape(-1)

    x_plane = lax.all_gather(layer_input, PLANE, axis=0, tiled=True).astype(F32)

    def to_heads(weight):
        rows, cols = weight.shape
        split = weight.reshape(rows, n_plane, cols // n_plane)
        mine = lax.all_to_all(split, PLANE, split_axis=1, concat_axis=0)
        mine = mine.reshape(n_plane * rows, cols // n_plane)
        return lax.all_gather(mine, "g", axis=0, tiled=True)

    query_weight = to_heads(w_query).reshape(width, local_heads, NOPE + ROPE)
    wq_nope = query_weight[:, :, :NOPE].reshape(width, local_heads * NOPE)
    wq_rope = query_weight[:, :, NOPE:].reshape(width, local_heads * ROPE)
    expand_weight = to_heads(w_expand)
    latent_weight = gather_all(w_latent)
    output_weight = gather_all(w_output)

    shared_n = shared_down.shape[0]
    s_both = jnp.concatenate(
        [
            shared_gate.reshape(rows_w, devices, shared_n),
            shared_up.reshape(rows_w, devices, shared_n),
        ],
        axis=2,
    )
    s_both = lax.all_to_all(s_both, ALL, split_axis=1, concat_axis=0).reshape(width, 2 * shared_n)

    hidden = rms_norm(x_plane, gain_one).astype(BF)
    rope_half = ROPE // 2
    positions = plane_start + jnp.arange(plane_tok, dtype=jnp.int32)
    frequency = 10000.0 ** (-jnp.arange(rope_half, dtype=F32) / rope_half)
    angles = positions.astype(F32)[:, None] * frequency[None, :]
    cosine = jnp.cos(angles)
    sine_part = jnp.sin(angles)
    cos_h, sin_h = cosine[:, None, :], sine_part[:, None, :]
    latent = matmul(hidden, latent_weight)
    compressed_own = rms_norm(latent[:, :RANK], gain_kv).astype(BF)
    key_rope_own = rotate(latent[:, RANK:], cosine, sine_part).astype(BF)

    def own_rows(table):
        return lax.dynamic_slice_in_dim(table, place_in * tok, tok, 0)

    up_pairs = [(i, i + 1) for i in range(n_groups - 1)]
    down_pairs = [(i + 1, i) for i in range(n_groups - 1)]
    piece = own_rows(jnp.concatenate([compressed_own, key_rope_own], axis=1))
    before = lax.ppermute(piece, "g", up_pairs)
    before = lax.all_gather(before, PLANE, axis=0, tiled=True)
    compressed = jnp.concatenate([before[:, :RANK], compressed_own], axis=0)
    key_rope = jnp.concatenate([before[:, RANK:], key_rope_own], axis=0)
    q_nope = matmul(hidden, wq_nope).astype(BF)
    q_rope = rotate(
        matmul(hidden, wq_rope).reshape(plane_tok, local_heads, ROPE), cos_h, sin_h
    ).reshape(plane_tok, local_heads * ROPE).astype(BF)
    expanded = matmul(compressed, expand_weight).astype(BF)
    plane_segments = lax.dynamic_slice_in_dim(segments_all, plane_start, plane_tok, 0)
    doc_start = jnp.sum(
        (segments_all[None, :] < plane_segments[:, None]).astype(jnp.int32), axis=1, keepdims=True
    )
    low_bound = doc_start - plane_start + DOC_MAX
    mixed_heads, lse = attend(low_bound, q_nope, q_rope, expanded, key_rope, scale)
    mixed = lax.all_to_all(mixed_heads, PLANE, split_axis=0, concat_axis=1, tiled=True)

    input_float = layer_input.astype(F32)
    residual_one = input_float + matmul(mixed, output_weight)
    h_two_f, norm_two_back = jax.vjp(rms_norm, residual_one, gain_two)
    h_two = h_two_f.astype(BF)
    router_probs = softmax_rows(matmul(h_two, router_weight))

    expert_w = (expert_gate[0], expert_up[0], expert_down[0])
    shared_w = (s_both, shared_down)
    slot_limit = 2 * tok * TOP // experts

    def scatter_all(x):
        return lax.psum_scatter(x, ALL, scatter_dimension=0, tiled=True)

    def on_rows(h2, probs, cot_gathered, routes_here):
        rows = h2.shape[0]
        h2_all = gather_all(h2).reshape(devices, rows, width)
        probs_all = gather_all(probs.T[None])
        weight_all = lax.dynamic_index_in_dim(probs_all, expert_id, 1, keepdims=False)
        slot_count = min(slot_limit, rows)
        member = jnp.any(routes_here == expert_id, axis=2)
        member_int = member.astype(jnp.int32)
        rank = jnp.cumsum(member_int, axis=1) - member_int
        slots = (
            (rank[:, None, :] == jnp.arange(slot_count, dtype=jnp.int32)[None, :, None])
            & member[:, None, :]
        ).astype(BF)
        out, grad_h2, token_grad, grads = experts_chunk(
            h2_all, cot_gathered, weight_all, slots, expert_w, shared_w
        )
        table = (jnp.arange(experts, dtype=jnp.int32) == expert_id).astype(F32)
        picked = scatter_all((token_grad[:, None, :] * table[None, :, None]).reshape(devices, -1))
        picked = picked.reshape(experts, rows).T
        return scatter_all(out), scatter_all(grad_h2), picked, grads

    parts = max(1, devices * tok // 4096)
    if parts == 1:
        cot_all = gather_all(cotangent).reshape(devices, tok, width)
        out_own, grad_h2_own, grad_router_probs, grads = on_rows(
            h_two, router_probs, cot_all, routes_all
        )
    else:
        rows = tok // parts

        def step(total, inputs):
            h2, probs, cot, routes_here = inputs
            cot_part = gather_all(cot).reshape(devices, rows, width)
            out, grad_h2, picked, grads = on_rows(h2, probs, cot_part, routes_here)
            total = tuple(a + b for a, b in zip(total, grads))
            return total, (out, grad_h2, picked)

        shapes = expert_w + shared_w
        grads, (out_own, grad_h2_own, grad_router_probs) = lax.scan(
            step,
            tuple(jnp.zeros(s.shape, F32) for s in shapes),
            (
                h_two.reshape(parts, rows, width),
                router_probs.reshape(parts, rows, experts),
                cotangent.reshape(parts, rows, width),
                routes_all.reshape(devices, parts, rows, TOP).transpose(1, 0, 2, 3),
            ),
        )
        out_own = out_own.reshape(tok, width)
        grad_h2_own = grad_h2_own.reshape(tok, width)
        grad_router_probs = grad_router_probs.reshape(tok, experts)
    g_gate, g_up, g_down, g_both, g_sdown = grads
    grad_logits = router_probs * (
        grad_router_probs - jnp.sum(router_probs * grad_router_probs, axis=1, keepdims=True)
    )
    grad_logits = grad_logits.astype(BF)
    grad_router = dot_tn(h_two, grad_logits)
    grad_h_two = grad_h2_own.astype(F32) + dot_nt(grad_logits, router_weight)
    output = residual_one + out_own.astype(F32)

    grad_x_one, grad_gain_two = norm_two_back(grad_h_two)
    grad_x_one = grad_x_one + cotangent.astype(F32)
    grad_attn_out = grad_x_one.astype(BF)
    grad_mixed = dot_nt(grad_attn_out, output_weight).astype(BF)
    grad_mixed = lax.all_to_all(grad_mixed, PLANE, split_axis=1, concat_axis=0, tiled=True)
    dqn, dqr, dex, dkr = attend_back(
        low_bound, q_nope, q_rope, expanded, key_rope, lse, grad_mixed, scale
    )

    def own_columns(table):
        rows = table.shape[0]
        split = table.reshape(rows, n_groups, n_plane, rows_w)
        mine = lax.dynamic_index_in_dim(split, place_in, 2, keepdims=False)
        return mine.reshape(rows, n_groups * rows_w)

    def scatter_groups(partial):
        return lax.psum_scatter(partial.astype(BF), "g", scatter_dimension=0, tiled=True)

    mixed_split = mixed.reshape(tok, n_groups, n_plane, rows_w).transpose(0, 2, 1, 3)
    mixed_cols = lax.all_to_all(mixed_split, PLANE, split_axis=1, concat_axis=0)
    mixed_cols = mixed_cols.reshape(plane_tok, n_groups * rows_w)
    plane_grad = lax.all_gather(grad_attn_out, PLANE, axis=0, tiled=True)
    grad_output_weight = scatter_groups(dot_tn(mixed_cols, plane_grad)).astype(F32)

    grad_expanded = dex.astype(BF)
    grad_expand = dot_tn(compressed, grad_expanded)
    grad_comp = dot_nt(grad_expanded, expand_weight)
    key_grads = jnp.concatenate([grad_comp, dkr], axis=1).astype(BF)
    key_grads = key_grads.reshape(2, n_plane, tok, RANK + ROPE).transpose(1, 0, 2, 3)
    key_grads = lax.psum_scatter(key_grads, PLANE, scatter_dimension=0, tiled=False)
    later = lax.ppermute(key_grads[0], "g", down_pairs).astype(F32)
    key_grad = key_grads[1].astype(F32) + later
    latent_own = own_rows(latent)
    kv_norm_back = jax.vjp(rms_norm, latent_own[:, :RANK], gain_kv)[1]
    grad_comp_in, grad_gain_kv = kv_norm_back(key_grad[:, :RANK])
    grad_rope_in = unrotate(key_grad[:, RANK:], own_rows(cosine), own_rows(sine_part))
    grad_latent = jnp.concatenate([grad_comp_in, grad_rope_in], axis=1).astype(BF)

    gq_nope = dqn.astype(BF)
    gq_rope = (
        unrotate(dqr.reshape(plane_tok, local_heads, ROPE), cos_h, sin_h)
        .reshape(plane_tok, local_heads * ROPE)
        .astype(BF)
    )
    grad_hidden_q = (dot_nt(gq_nope, wq_nope) + dot_nt(gq_rope, wq_rope)).astype(BF)
    grad_hidden = lax.psum_scatter(grad_hidden_q, PLANE, scatter_dimension=0, tiled=True)
    g_query = jnp.concatenate(
        [
            dot_tn(hidden, gq_nope).reshape(width, local_heads, NOPE),
            dot_tn(hidden, gq_rope).reshape(width, local_heads, ROPE),
        ],
        axis=2,
    ).reshape(width, local_heads * (NOPE + ROPE))

    def from_heads(partial):
        mine = scatter_groups(partial)
        rows, cols = mine.shape
        split = mine.reshape(n_plane, rows // n_plane, cols)
        full = lax.all_to_all(split, PLANE, split_axis=0, concat_axis=1)
        return full.reshape(rows // n_plane, n_plane * cols).astype(F32)

    grad_query_weight = from_heads(g_query)
    grad_expand_weight = from_heads(grad_expand)

    latent_grads = lax.all_gather(grad_latent, PLANE, axis=0, tiled=True)
    grad_latent_weight = scatter_groups(dot_tn(own_columns(hidden), latent_grads)).astype(F32)

    grad_hidden = grad_hidden.astype(F32) + dot_nt(grad_latent, latent_weight)
    norm_one_back = jax.vjp(rms_norm, input_float, gain_one)[1]
    grad_x_norm, grad_gain_one = norm_one_back(grad_hidden)
    grad_input = grad_x_one + grad_x_norm

    small_grads = jnp.concatenate(
        [
            grad_gain_one.reshape(devices, rows_w),
            grad_gain_two.reshape(devices, rows_w),
            grad_gain_kv.reshape(devices, kv_n),
            grad_router.reshape(devices, rows_w * experts),
        ],
        axis=1,
    )
    small_grads = scatter_all(small_grads)[0]
    g_shared = lax.all_to_all(
        g_both.reshape(devices, rows_w, 2 * shared_n), ALL, split_axis=0, concat_axis=1
    )
    grad_shared_gate = g_shared[:, :, :shared_n].reshape(rows_w, devices * shared_n)
    grad_shared_up = g_shared[:, :, shared_n:].reshape(rows_w, devices * shared_n)
    return (
        output,
        grad_input,
        small_grads[:rows_w],
        grad_query_weight,
        grad_latent_weight,
        small_grads[2 * rows_w : 2 * rows_w + kv_n],
        grad_expand_weight,
        grad_output_weight,
        small_grads[rows_w : 2 * rows_w],
        small_grads[2 * rows_w + kv_n :].reshape(rows_w, experts),
        grad_shared_gate,
        grad_shared_up,
        g_sdown,
        g_gate[None],
        g_up[None],
        g_down[None],
    )


def solution(mesh):
    n_expert, n_shard = mesh.shape["expert"], mesh.shape["wshard"]
    devices = n_expert * n_shard

    def program(*args):
        tok = args[0].shape[0] // devices
        n_plane = DOC_MAX // tok
        n_groups = devices // n_plane
        inner = Mesh(mesh.devices.reshape(n_groups, n_plane // n_shard, n_shard), ALL)
        rows, vector = P(ALL, None), P(ALL)
        wide, tall = P(("g", "p"), None, "c"), P(("g", "p"), "c", None)
        step = jax.shard_map(
            functools.partial(body, n_groups, n_plane),
            mesh=inner,
            in_specs=(
                rows, vector, rows, rows, vector, rows, rows, vector, rows, rows, rows, rows,
                wide, wide, tall, rows, vector, rows,
            ),
            out_specs=(
                rows, rows, vector, rows, rows, vector, rows, rows, vector, rows, rows, rows,
                rows, wide, wide, tall,
            ),
            check_vma=False,
        )
        return step(*args)

    return program
```

```python
import functools

import jax
import jax.numpy as jnp
from jax import lax
from jax.experimental import pallas as pl
from jax.experimental.pallas import tpu as pltpu
from jax.sharding import Mesh, PartitionSpec as P

HEADS = 16
NOPE = 128
ROPE = 64
VDIM = 128
RANK = 512
TOP = 6
DOC_MAX = 1024
QUERY_BLOCK = 256

BF = jnp.bfloat16
F32 = jnp.float32
ALL = ("g", "p", "c")
PLANE = ("p", "c")

epsilon = 1e-06


def rms_norm(vector, scaling):
    return vector * lax.rsqrt(jnp.mean(vector * vector, axis=-1, keepdims=True) + epsilon) * scaling


def rotate(vector, cosine, sine_part):
    half_width = vector.shape[-1] // 2
    front_half = vector[..., :half_width]
    back_half = vector[..., half_width:]
    return jnp.concatenate(
        [front_half * cosine - back_half * sine_part, back_half * cosine + front_half * sine_part],
        axis=-1,
    )


def unrotate(vector, cosine, sine_part):
    return rotate(vector, cosine, -sine_part)


def matmul(left, right):
    return jnp.dot(left, right, preferred_element_type=F32)


def dot_nt(left, right):
    return lax.dot_general(left, right, (((1,), (1,)), ((), ())), preferred_element_type=F32)


def dot_tn(left, right):
    return lax.dot_general(left, right, (((0,), (0,)), ((), ())), preferred_element_type=F32)


def swiglu(gate_pre, up_pre):
    return jax.nn.silu(gate_pre) * up_pre


def softmax_rows(scores):
    row_top = jnp.max(scores, axis=-1, keepdims=True)
    exp_scores = jnp.exp(scores - row_top)
    return exp_scores / jnp.sum(exp_scores, axis=-1, keepdims=True)


def masked_scores(base, low_bound, q_nope, q_rope, k_nope, k_rope, scale):
    rows, span = q_nope.shape[0], k_nope.shape[0]
    key_at = lax.broadcasted_iota(jnp.int32, (rows, span), 1) + base
    query_at = lax.broadcasted_iota(jnp.int32, (rows, span), 0) + (base + DOC_MAX)
    allowed = (key_at >= low_bound) & (key_at <= query_at)
    scores = (dot_nt(q_nope, k_nope) + dot_nt(q_rope, k_rope)) * scale
    return jnp.where(allowed, scores, -1e30)


def attend_kernel(heads, scale, low_ref, qn_ref, qr_ref, ex_ref, kr_ref, out_ref, lse_ref):
    rows = qn_ref.shape[0]
    base = pl.multiple_of(pl.program_id(0) * rows, rows)
    window = pl.ds(base, rows + DOC_MAX)
    k_rope = kr_ref[window, :]
    low_bound = low_ref[...]
    for h in range(heads):
        at = h * (NOPE + VDIM)
        k_nope = ex_ref[window, at : at + NOPE]
        value = ex_ref[window, at + NOPE : at + NOPE + VDIM]
        scores = masked_scores(
            base,
            low_bound,
            qn_ref[:, h * NOPE : (h + 1) * NOPE],
            qr_ref[:, h * ROPE : (h + 1) * ROPE],
            k_nope,
            k_rope,
            scale,
        )
        top = jnp.max(scores, axis=-1, keepdims=True)
        exps = jnp.exp(scores - top)
        total = jnp.sum(exps, axis=-1, keepdims=True)
        probs = (exps / total).astype(BF)
        out_ref[:, h * VDIM : (h + 1) * VDIM] = jnp.dot(
            probs, value, preferred_element_type=F32
        ).astype(BF)
        lse_ref[:, h : h + 1] = top + jnp.log(total)


def attend(low_bound, q_nope, q_rope, expanded, key_rope, scale):
    queries = q_nope.shape[0]
    heads = q_nope.shape[1] // NOPE
    rows = QUERY_BLOCK

    def whole(array):
        return pl.BlockSpec(array.shape, lambda i: (0, 0))

    def blocked(width):
        return pl.BlockSpec((rows, width), lambda i: (i, 0))

    flops = 2 * heads * queries * (rows + DOC_MAX) * (NOPE + ROPE + VDIM)
    return pl.pallas_call(
        functools.partial(attend_kernel, heads, scale),
        grid=(queries // rows,),
        in_specs=[
            blocked(1),
            blocked(heads * NOPE),
            blocked(heads * ROPE),
            whole(expanded),
            whole(key_rope),
        ],
        out_specs=[blocked(heads * VDIM), blocked(heads)],
        out_shape=[
            jax.ShapeDtypeStruct((queries, heads * VDIM), BF),
            jax.ShapeDtypeStruct((queries, heads), F32),
        ],
        cost_estimate=pl.CostEstimate(
            flops=flops, bytes_accessed=4 * expanded.size, transcendentals=flops // 640
        ),
        compiler_params=pltpu.CompilerParams(vmem_limit_bytes=50 * 1024 * 1024),
        name="attend",
    )(low_bound, q_nope, q_rope, expanded, key_rope)


def attend_back_kernel(
    heads, scale, low_ref, qn_ref, qr_ref, ex_ref, kr_ref, lse_ref, gm_ref,
    dqn_ref, dqr_ref, dex_ref, dkr_ref,
):
    rows = qn_ref.shape[0]
    step = pl.program_id(0)
    base = pl.multiple_of(step * rows, rows)
    window = pl.ds(base, rows + DOC_MAX)

    @pl.when(step == 0)
    def _():
        dex_ref[...] = jnp.zeros_like(dex_ref)
        dkr_ref[...] = jnp.zeros_like(dkr_ref)

    k_rope = kr_ref[window, :]
    low_bound = low_ref[...]
    for h in range(heads):
        at = h * (NOPE + VDIM)
        k_nope = ex_ref[window, at : at + NOPE]
        value = ex_ref[window, at + NOPE : at + NOPE + VDIM]
        q_nope = qn_ref[:, h * NOPE : (h + 1) * NOPE]
        q_rope = qr_ref[:, h * ROPE : (h + 1) * ROPE]
        grad_out = gm_ref[:, h * VDIM : (h + 1) * VDIM]
        scores = masked_scores(base, low_bound, q_nope, q_rope, k_nope, k_rope, scale)
        probs = jnp.exp(scores - lse_ref[:, h : h + 1])
        grad_probs = dot_nt(grad_out, value)
        mean_grad = jnp.sum(probs * grad_probs, axis=-1, keepdims=True)
        grad_scores = (probs * (grad_probs - mean_grad) * scale).astype(BF)
        probs_low = probs.astype(BF)
        dqn_ref[:, h * NOPE : (h + 1) * NOPE] = jnp.dot(
            grad_scores, k_nope, preferred_element_type=F32
        )
        dqr_ref[:, h * ROPE : (h + 1) * ROPE] = jnp.dot(
            grad_scores, k_rope, preferred_element_type=F32
        )
        dex_ref[window, at : at + NOPE] += dot_tn(grad_scores, q_nope)
        dex_ref[window, at + NOPE : at + NOPE + VDIM] += dot_tn(probs_low, grad_out)
        dkr_ref[window, :] += dot_tn(grad_scores, q_rope)


def attend_back(low_bound, q_nope, q_rope, expanded, key_rope, lse, grad_mixed, scale):
    queries = q_nope.shape[0]
    heads = q_nope.shape[1] // NOPE
    rows = QUERY_BLOCK

    def whole(shape):
        return pl.BlockSpec(shape, lambda i: (0, 0))

    def blocked(width):
        return pl.BlockSpec((rows, width), lambda i: (i, 0))

    flops = 2 * heads * queries * (rows + DOC_MAX) * (3 * NOPE + 3 * ROPE + 2 * VDIM)
    return pl.pallas_call(
        functools.partial(attend_back_kernel, heads, scale),
        grid=(queries // rows,),
        in_specs=[
            blocked(1),
            blocked(heads * NOPE),
            blocked(heads * ROPE),
            whole(expanded.shape),
            whole(key_rope.shape),
            blocked(heads),
            blocked(heads * VDIM),
        ],
        out_specs=[
            blocked(heads * NOPE),
            blocked(heads * ROPE),
            whole(expanded.shape),
            whole(key_rope.shape),
        ],
        out_shape=[
            jax.ShapeDtypeStruct(q_nope.shape, F32),
            jax.ShapeDtypeStruct(q_rope.shape, F32),
            jax.ShapeDtypeStruct(expanded.shape, F32),
            jax.ShapeDtypeStruct(key_rope.shape, F32),
        ],
        cost_estimate=pl.CostEstimate(
            flops=flops, bytes_accessed=8 * expanded.size, transcendentals=flops // 1664
        ),
        compiler_params=pltpu.CompilerParams(vmem_limit_bytes=56 * 1024 * 1024),
        name="attend_back",
    )(low_bound, q_nope, q_rope, expanded, key_rope, lse, grad_mixed)


MESH = pl.DeviceIdType.MESH


class Wires:
    def __init__(self, n_groups, n_plane, send, recv):
        self.n_groups, self.n_plane, self.send, self.recv = n_groups, n_plane, send, recv
        self.cores = 2
        self.g, self.p, self.c = lax.axis_index("g"), lax.axis_index("p"), lax.axis_index("c")
        self.j = self.p * self.cores + self.c
        self.used = 0

    def at_plane(self, j):
        return {"g": self.g, "p": j // self.cores, "c": j % self.cores}

    def at_chip(self, p):
        return {"g": self.g, "p": p, "c": self.c}

    def at_group(self, g):
        return {"g": g, "p": self.p, "c": self.c}

    def partner(self):
        return {"g": self.g, "p": self.p, "c": 1 - self.c}

    def plane_peer(self, d):
        return lax.rem(self.j + d, self.n_plane)

    def group_peer(self, d):
        return lax.rem(self.g + d, self.n_groups)

    def start(self, src, dst, device):
        copy = pltpu.make_async_remote_copy(
            src_ref=src,
            dst_ref=dst,
            send_sem=self.send.at[self.used],
            recv_sem=self.recv.at[self.used],
            device_id=device,
            device_id_type=MESH,
        )
        self.used += 1
        copy.start()
        return copy

    def meet(self):
        barrier = pltpu.get_barrier_semaphore()
        for d in range(1, self.n_plane):
            pl.semaphore_signal(
                barrier, inc=1, device_id=self.at_plane(self.plane_peer(d)), device_id_type=MESH
            )
        for d in range(1, self.n_groups):
            pl.semaphore_signal(
                barrier, inc=1, device_id=self.at_group(self.group_peer(d)), device_id_type=MESH
            )
        pl.semaphore_wait(barrier, self.n_plane - 1 + self.n_groups - 1)


def sum_rows(dst, sources):
    rows = dst.shape[0]
    tile = 32 if rows % 32 == 0 else rows

    def step(i, carry):
        at = pl.ds(pl.multiple_of(i * tile, tile), tile)
        total = sources[0][at, :].astype(F32)
        for source in sources[1:]:
            total = total + source[at, :].astype(F32)
        dst[at, :] = total.astype(dst.dtype)
        return carry

    lax.fori_loop(0, rows // tile, step, 0)


def wait_all(copies):
    for copy in copies:
        copy.wait()


def wait_received(copies):
    for copy in copies:
        copy.wait_recv()


def wait_sent(copies):
    for copy in copies:
        copy.wait_send()


def plane_gather(w, src, out):
    chips = w.n_plane // w.cores
    first = [
        w.start(src, out.at[w.j], w.at_chip(lax.rem(w.p + d, chips))) for d in range(1, chips)
    ]
    second = [w.start(src, out.at[w.j], w.partner())]
    out[w.j] = src[...]
    yield
    for d in range(1, chips):
        first[d - 1].wait_recv()
        at = lax.rem(w.p + chips - d, chips) * w.cores + w.c
        second.append(w.start(out.at[at], out.at[at], w.partner()))
    yield
    wait_sent(first)
    wait_all(second)


def shift_gather(w, src, mid, out):
    copy = w.start(src, mid, w.at_group(lax.rem(w.g + 1, w.n_groups)))
    yield
    copy.wait()
    yield from plane_gather(w, mid, out)


def whole_gather(w, src, out):
    first = [
        w.start(src, out.at[w.g, w.j], w.at_group(w.group_peer(d))) for d in range(1, w.n_groups)
    ]
    out[w.g, w.j] = src[...]
    yield
    wait_received(first)
    second = [
        w.start(out.at[:, w.j], out.at[:, w.j], w.at_plane(w.plane_peer(d)))
        for d in range(1, w.n_plane)
    ]
    yield
    wait_sent(first)
    wait_all(second)


def plane_swap_gather(w, src, out):
    first = []
    for d in range(1, w.n_plane):
        to = w.plane_peer(d)
        first.append(w.start(src.at[to], out.at[w.g, w.j], w.at_plane(to)))
    out[w.g, w.j] = src[w.j]
    yield
    wait_received(first)
    second = [
        w.start(out.at[w.g], out.at[w.g], w.at_group(w.group_peer(d)))
        for d in range(1, w.n_groups)
    ]
    yield
    wait_sent(first)
    wait_all(second)


def plane_swap(w, src, out):
    copies = []
    for d in range(1, w.n_plane):
        to = w.plane_peer(d)
        copies.append(w.start(src.at[to], out.at[w.j], w.at_plane(to)))
    out[w.j] = src[w.j]
    yield
    wait_all(copies)


def plane_sum(w, src, out, from_core, pairs, from_chips):
    chips = w.n_plane // w.cores
    first = []
    for d in range(chips):
        p = lax.rem(w.p + d, chips)
        first.append(w.start(src.at[p * w.cores + 1 - w.c], from_core.at[d], w.partner()))
    yield
    second = []
    for d in list(range(1, chips)) + [0]:
        p = lax.rem(w.p + d, chips)
        first[d].wait_recv()
        sum_rows(pairs.at[d], [src.at[p * w.cores + w.c], from_core.at[d]])
        if d:
            second.append(w.start(pairs.at[d], from_chips.at[d - 1], w.at_chip(p)))
    yield
    wait_received(second)
    sum_rows(out, [pairs.at[0]] + [from_chips.at[d] for d in range(chips - 1)])
    wait_sent(first)
    wait_sent(second)


def whole_sum(w, src, out, from_plane, total, parts):
    first = []
    for d in range(1, w.n_plane):
        to = w.plane_peer(d)
        first.append(w.start(src.at[:, to], from_plane.at[d - 1], w.at_plane(to)))
    yield
    wait_received(first)

    def step(i, carry):
        sum_rows(
            total.at[i], [src.at[i, w.j]] + [from_plane.at[d, i] for d in range(w.n_plane - 1)]
        )
        return carry

    lax.fori_loop(0, w.n_groups, step, 0)
    wait_sent(first)
    yield from group_sum(w, total, out, parts)


def group_sum(w, src, out, parts):
    copies = []
    for d in range(1, w.n_groups):
        to = w.group_peer(d)
        copies.append(w.start(src.at[to], parts.at[d - 1], w.at_group(to)))
    yield
    wait_received(copies)
    sum_rows(out, [src.at[w.g]] + [parts.at[d] for d in range(w.n_groups - 1)])
    wait_sent(copies)


def group_sum_swap(w, src, out, total, parts):
    copies = []
    for d in range(1, w.n_groups):
        to = w.group_peer(d)
        copies.append(w.start(src.at[to], parts.at[d - 1], w.at_group(to)))
    yield
    wait_received(copies)

    def step(i, carry):
        sum_rows(total.at[i], [src.at[w.g, i]] + [parts.at[d, i] for d in range(w.n_groups - 1)])
        return carry

    lax.fori_loop(0, w.n_plane, step, 0)
    second = []
    for d in range(1, w.n_plane):
        to = w.plane_peer(d)
        second.append(w.start(total.at[to], out.at[w.j], w.at_plane(to)))
    out[w.j] = total[w.j]
    yield
    wait_sent(copies)
    wait_all(second)


ROUTINES = {
    "plane_gather": plane_gather,
    "shift_gather": shift_gather,
    "whole_gather": whole_gather,
    "plane_swap_gather": plane_swap_gather,
    "plane_swap": plane_swap,
    "plane_sum": plane_sum,
    "group_sum": group_sum,
    "whole_sum": whole_sum,
    "group_sum_swap": group_sum_swap,
}


def exchange_kernel(n_groups, n_plane, kinds, extra, *refs):
    count = len(kinds)
    sources, outs = refs[:count], refs[count : 2 * count]
    scratch = list(refs[2 * count : -2])
    w = Wires(n_groups, n_plane, refs[-2], refs[-1])
    w.meet()
    running = []
    for kind, source, out, number in zip(kinds, sources, outs, extra):
        mine, scratch = scratch[:number], scratch[number:]
        if kind == "shift_gather":
            running.append(shift_gather(w, source, mine[0], out))
        else:
            running.append(ROUTINES[kind](w, source, out, *mine))
    while running:
        still = []
        for routine in running:
            try:
                next(routine)
                still.append(routine)
            except StopIteration:
                pass
        running = still


def exchange(n_groups, n_plane, number, *items):
    kinds = [kind for kind, _ in items]
    arrays = [array for _, array in items]
    shapes, scratch, extra = [], [], []
    chips = n_plane // 2
    for kind, array in items:
        shape, dtype = array.shape, array.dtype
        own = []
        if kind in ("plane_gather", "shift_gather"):
            out = (n_plane,) + shape
            if kind == "shift_gather":
                own = [shape]
        elif kind == "whole_gather":
            out = (n_groups, n_plane) + shape
        elif kind == "plane_swap_gather":
            out = (n_groups,) + shape
        elif kind == "plane_swap":
            out = shape
        elif kind == "plane_sum":
            out = shape[1:]
            own = [(chips,) + out, (chips,) + out, (chips - 1,) + out]
        elif kind == "group_sum":
            out = shape[1:]
            own = [(n_groups - 1,) + out]
        elif kind == "whole_sum":
            out = shape[2:]
            own = [(n_plane - 1, n_groups) + out, (n_groups,) + out, (n_groups - 1,) + out]
        elif kind == "group_sum_swap":
            out = shape[1:]
            own = [out, (n_groups - 1,) + out]
        if kind in ("plane_sum", "group_sum", "whole_sum"):
            shapes.append(jax.ShapeDtypeStruct(out, F32))
        else:
            shapes.append(jax.ShapeDtypeStruct(out, dtype))
        scratch += [pltpu.VMEM(s, dtype) for s in own]
        extra.append(len(own))
    copies = 64 + 32 * len(items)
    vmem = pl.BlockSpec(memory_space=pltpu.VMEM)
    return pl.pallas_call(
        functools.partial(exchange_kernel, n_groups, n_plane, kinds, extra),
        out_shape=shapes,
        in_specs=[vmem] * len(items),
        out_specs=[vmem] * len(items),
        scratch_shapes=scratch
        + [pltpu.SemaphoreType.DMA((copies,)), pltpu.SemaphoreType.DMA((copies,))],
        compiler_params=pltpu.CompilerParams(
            collective_id=number,
            has_side_effects=True,
            vmem_limit_bytes=60 * 1024 * 1024,
        ),
        name="exchange_%d" % number,
    )(*arrays)


def gather_all(x):
    return lax.all_gather(x, ALL, axis=0, tiled=True)


def experts_chunk(h2, cot, expert_id, slots, expert_w, shared_w, router_weight):
    w_gate, w_up, w_down = expert_w
    s_both, s_down = shared_w
    blocks, rows, width = h2.shape
    per_block = slots.shape[1]
    hidden_s = s_down.shape[0]
    flat_h2 = h2.reshape(blocks * rows, width)
    flat_cot = cot.reshape(blocks * rows, width)

    def pick(table):
        return (
            jnp.einsum("bst,btd->bsd", slots, table, preferred_element_type=F32)
            .astype(BF)
            .reshape(blocks * per_block, width)
        )

    def place(table):
        return jnp.einsum(
            "bst,bsd->btd",
            slots,
            table.astype(BF).reshape(blocks, per_block, width),
            preferred_element_type=F32,
        ).reshape(blocks * rows, width)

    cot_rows = pick(cot)
    back_act = dot_nt(cot_rows, w_down)
    shared_back = dot_nt(flat_cot, s_down)
    shared_pre = matmul(flat_h2, jnp.concatenate([s_both, router_weight], axis=1))
    probs = softmax_rows(shared_pre[:, 2 * hidden_s :])
    chosen = jnp.arange(probs.shape[1], dtype=jnp.int32) == expert_id
    weight = jnp.sum(jnp.where(chosen, probs, 0.0), axis=1).reshape(blocks, 1, rows)
    row_weight = jnp.sum(slots.astype(F32) * weight, axis=2).reshape(-1, 1)
    rows_in = pick(h2)
    gate_pre = matmul(rows_in, w_gate)
    up_pre = matmul(rows_in, w_up)
    act, act_vjp = jax.vjp(swiglu, gate_pre, up_pre)
    act_low = act.astype(BF)
    grad_gate, grad_up = act_vjp(back_act * row_weight)
    grad_gate = grad_gate.astype(BF)
    grad_up = grad_up.astype(BF)
    grad_rows = dot_nt(grad_gate, w_gate) + dot_nt(grad_up, w_up)
    s_act, s_vjp = jax.vjp(swiglu, shared_pre[:, :hidden_s], shared_pre[:, hidden_s : 2 * hidden_s])
    s_act = s_act.astype(BF)
    s_grad = jnp.concatenate(s_vjp(shared_back), axis=1).astype(BF)
    grad_h2 = (place(grad_rows) + dot_nt(s_grad, s_both)).astype(BF)

    grad_h2, act_low, back_act, grad_gate, grad_up, s_act, s_grad = lax.optimization_barrier(
        (grad_h2, act_low, back_act, grad_gate, grad_up, s_act, s_grad)
    )
    picked_grad = jnp.sum(act_low.astype(F32) * back_act, axis=1).reshape(blocks, per_block, 1)
    token_grad = jnp.sum(slots.astype(F32) * picked_grad, axis=1)
    out_rows = matmul(act_low, w_down) * row_weight
    out = (place(out_rows) + matmul(s_act, s_down)).astype(BF)

    grad_in = (cot_rows.astype(F32) * row_weight).astype(BF)
    grads = (
        dot_tn(rows_in, grad_gate),
        dot_tn(rows_in, grad_up),
        dot_tn(act_low, grad_in),
        dot_tn(flat_h2, s_grad),
        dot_tn(s_act, flat_cot),
    )
    return out, grad_h2, token_grad, grads


def body(
    n_groups, n_plane, layer_input, attn_gain, w_query, w_latent, kv_gain, w_expand, w_output,
    ffn_gain, w_router, shared_gate, shared_up, shared_down, expert_gate, expert_up,
    expert_down, routes, segments, cotangent,
):
    tok, width = layer_input.shape
    devices = n_groups * n_plane
    experts = w_router.shape[1]
    local_heads = HEADS // n_plane
    scale = (NOPE + ROPE) ** (-0.5)
    group = lax.axis_index("g")
    place_in = lax.axis_index(PLANE)
    me = lax.axis_index(ALL)
    expert_id = lax.axis_index(("g", "p"))
    plane_tok = n_plane * tok
    plane_start = group * plane_tok

    rows_w = w_router.shape[0]
    kv_n = kv_gain.shape[0]
    small = jnp.concatenate(
        [
            attn_gain,
            ffn_gain,
            kv_gain,
            w_router.reshape(-1),
            routes.reshape(-1).astype(BF),
            segments.astype(BF),
        ]
    )
    small = jnp.pad(small, (0, -small.shape[0] % 4096)).reshape(-1, 128)
    head_cols = local_heads * (NOPE + ROPE)
    kv_cols = local_heads * (NOPE + VDIM)
    fold = kv_n * kv_cols // rows_w
    pair = jnp.concatenate(
        [
            w_query.reshape(rows_w, n_plane, head_cols).transpose(1, 0, 2),
            w_expand.reshape(kv_n, n_plane, kv_cols // fold, fold)
            .transpose(1, 0, 2, 3)
            .reshape(n_plane, rows_w, fold),
        ],
        axis=2,
    )
    swap = functools.partial(exchange, n_groups, n_plane)
    x_plane, small, latent_weight, pair = swap(
        0,
        ("plane_gather", layer_input),
        ("whole_gather", small),
        ("whole_gather", w_latent),
        ("plane_swap_gather", pair),
    )
    x_plane = x_plane.reshape(plane_tok, width).astype(F32)
    latent_weight = latent_weight.reshape(width, RANK + ROPE)
    pair = pair.reshape(width, head_cols + fold)
    small = small.reshape(devices, -1)
    cuts = [rows_w, 2 * rows_w, 2 * rows_w + kv_n, 2 * rows_w + kv_n + rows_w * experts]
    cuts = cuts + [cuts[-1] + tok * TOP, cuts[-1] + tok * TOP + tok]
    gain_one = small[:, : cuts[0]].reshape(-1).astype(F32)
    gain_two = small[:, cuts[0] : cuts[1]].reshape(-1).astype(F32)
    gain_kv = small[:, cuts[1] : cuts[2]].reshape(-1).astype(F32)
    router_weight = small[:, cuts[2] : cuts[3]].reshape(width, experts)
    routes_all = small[:, cuts[3] : cuts[4]].astype(jnp.int32).reshape(devices, tok, TOP)
    segments_all = small[:, cuts[4] : cuts[5]].astype(jnp.int32).reshape(-1)

    query_weight = pair[:, :head_cols].reshape(width, local_heads, NOPE + ROPE)
    wq_nope = query_weight[:, :, :NOPE].reshape(width, local_heads * NOPE)
    wq_rope = query_weight[:, :, NOPE:].reshape(width, local_heads * ROPE)
    expand_weight = pair[:, head_cols:].reshape(RANK, kv_cols)
    output_weight = gather_all(w_output)

    shared_n = shared_down.shape[0]
    s_both = jnp.concatenate(
        [
            shared_gate.reshape(rows_w, devices, shared_n),
            shared_up.reshape(rows_w, devices, shared_n),
        ],
        axis=2,
    )
    s_both = lax.all_to_all(s_both, ALL, split_axis=1, concat_axis=0).reshape(width, 2 * shared_n)

    hidden = rms_norm(x_plane, gain_one).astype(BF)
    rope_half = ROPE // 2
    positions = plane_start + jnp.arange(plane_tok, dtype=jnp.int32)
    frequency = 10000.0 ** (-jnp.arange(rope_half, dtype=F32) / rope_half)
    angles = positions.astype(F32)[:, None] * frequency[None, :]
    cosine = jnp.cos(angles)
    sine_part = jnp.sin(angles)
    cos_h, sin_h = cosine[:, None, :], sine_part[:, None, :]
    latent = matmul(hidden, latent_weight)
    compressed_own = rms_norm(latent[:, :RANK], gain_kv).astype(BF)
    key_rope_own = rotate(latent[:, RANK:], cosine, sine_part).astype(BF)

    def own_rows(table):
        return lax.dynamic_slice_in_dim(table, place_in * tok, tok, 0)

    down_pairs = [(i + 1, i) for i in range(n_groups - 1)]
    piece = own_rows(jnp.concatenate([compressed_own, key_rope_own], axis=1))
    before = swap(1, ("shift_gather", piece))[0].reshape(plane_tok, RANK + ROPE)
    compressed = jnp.concatenate([before[:, :RANK], compressed_own], axis=0)
    key_rope = jnp.concatenate([before[:, RANK:], key_rope_own], axis=0)
    q_nope = matmul(hidden, wq_nope).astype(BF)
    q_rope = rotate(
        matmul(hidden, wq_rope).reshape(plane_tok, local_heads, ROPE), cos_h, sin_h
    ).reshape(plane_tok, local_heads * ROPE).astype(BF)
    expanded = matmul(compressed, expand_weight).astype(BF)
    plane_segments = lax.dynamic_slice_in_dim(segments_all, plane_start, plane_tok, 0)
    doc_start = jnp.sum(
        (segments_all[None, :] < plane_segments[:, None]).astype(jnp.int32), axis=1, keepdims=True
    )
    low_bound = doc_start - plane_start + DOC_MAX
    mixed_heads, lse = attend(low_bound, q_nope, q_rope, expanded, key_rope, scale)
    mixed = swap(2, ("plane_swap", mixed_heads.reshape(n_plane, tok, local_heads * VDIM)))[0]
    mixed = mixed.transpose(1, 0, 2).reshape(tok, width)

    input_float = layer_input.astype(F32)
    residual_one = input_float + matmul(mixed, output_weight)
    h_two_f, norm_two_back = jax.vjp(rms_norm, residual_one, gain_two)
    h_two = h_two_f.astype(BF)
    router_probs = softmax_rows(matmul(h_two, router_weight))

    expert_w = (expert_gate[0], expert_up[0], expert_down[0])
    shared_w = (s_both, shared_down)
    slot_limit = 2 * tok * TOP // experts

    def scatter_all(x):
        return lax.psum_scatter(x, ALL, scatter_dimension=0, tiled=True)

    def on_rows(h2, cot_gathered, routes_here):
        rows = h2.shape[0]
        h2_all = gather_all(h2).reshape(devices, rows, width)
        slot_count = min(slot_limit, rows)
        member = jnp.any(routes_here == expert_id, axis=2)
        member_int = member.astype(jnp.int32)
        rank = jnp.cumsum(member_int, axis=1) - member_int
        slots = (
            (rank[:, None, :] == jnp.arange(slot_count, dtype=jnp.int32)[None, :, None])
            & member[:, None, :]
        ).astype(BF)
        out, grad_h2, token_grad, grads = experts_chunk(
            h2_all, cot_gathered, expert_id, slots, expert_w, shared_w, router_weight
        )
        picked = lax.all_to_all(token_grad, ALL, split_axis=0, concat_axis=0, tiled=True)
        picked = jnp.sum(picked.reshape(experts, devices // experts, rows), axis=1).T
        grad_h2, out, grads, picked = lax.optimization_barrier(
            (scatter_all(grad_h2), out, grads, picked)
        )
        return scatter_all(out), grad_h2, picked, grads

    parts = max(1, devices * tok // 4096)
    if parts == 1:
        cot_all = gather_all(cotangent).reshape(devices, tok, width)
        out_own, grad_h2_own, grad_router_probs, grads = on_rows(
            h_two, cot_all, routes_all
        )
    else:
        rows = tok // parts

        def step(total, inputs):
            h2, cot, routes_here = inputs
            cot_part = gather_all(cot).reshape(devices, rows, width)
            out, grad_h2, picked, grads = on_rows(h2, cot_part, routes_here)
            total = tuple(a + b for a, b in zip(total, grads))
            return total, (out, grad_h2, picked)

        shapes = expert_w + shared_w
        grads, (out_own, grad_h2_own, grad_router_probs) = lax.scan(
            step,
            tuple(jnp.zeros(s.shape, F32) for s in shapes),
            (
                h_two.reshape(parts, rows, width),
                cotangent.reshape(parts, rows, width),
                routes_all.reshape(devices, parts, rows, TOP).transpose(1, 0, 2, 3),
            ),
        )
        out_own = out_own.reshape(tok, width)
        grad_h2_own = grad_h2_own.reshape(tok, width)
        grad_router_probs = grad_router_probs.reshape(tok, experts)
    g_gate, g_up, g_down, g_both, g_sdown = grads
    grad_logits = router_probs * (
        grad_router_probs - jnp.sum(router_probs * grad_router_probs, axis=1, keepdims=True)
    )
    grad_logits = grad_logits.astype(BF)
    grad_router = dot_tn(h_two, grad_logits)
    grad_h_two = grad_h2_own.astype(F32) + dot_nt(grad_logits, router_weight)
    output = residual_one + out_own.astype(F32)

    grad_x_one, grad_gain_two = norm_two_back(grad_h_two)
    grad_x_one = grad_x_one + cotangent.astype(F32)
    grad_attn_out = grad_x_one.astype(BF)
    plane_grad = swap(3, ("plane_gather", grad_attn_out))[0].reshape(plane_tok, width)
    head_rows = local_heads * VDIM
    own_output = lax.dynamic_slice_in_dim(output_weight, place_in * head_rows, head_rows, 0)
    grad_mixed = dot_nt(plane_grad, own_output).astype(BF)
    dqn, dqr, dex, dkr = attend_back(
        low_bound, q_nope, q_rope, expanded, key_rope, lse, grad_mixed, scale
    )

    def own_columns(table):
        rows = table.shape[0]
        split = table.reshape(rows, n_groups, n_plane, rows_w)
        mine = lax.dynamic_index_in_dim(split, place_in, 2, keepdims=False)
        return mine.reshape(rows, n_groups * rows_w)

    mixed_split = mixed.reshape(tok, n_groups, n_plane, rows_w).transpose(0, 2, 1, 3)
    mixed_cols = lax.all_to_all(mixed_split, PLANE, split_axis=1, concat_axis=0)
    mixed_cols = mixed_cols.reshape(plane_tok, n_groups * rows_w)
    g_output = dot_tn(mixed_cols, plane_grad).astype(BF).reshape(n_groups, rows_w, width)

    grad_expanded = dex.astype(BF)
    grad_expand = dot_tn(compressed, grad_expanded)
    grad_comp = dot_nt(grad_expanded, expand_weight)
    key_grads = jnp.concatenate([grad_comp, dkr], axis=1).astype(BF)
    key_grads = (
        key_grads.reshape(2, n_plane, tok, RANK + ROPE)
        .transpose(1, 0, 2, 3)
        .reshape(n_plane, 2 * tok, RANK + ROPE)
    )

    gq_nope = dqn.astype(BF)
    gq_rope = (
        unrotate(dqr.reshape(plane_tok, local_heads, ROPE), cos_h, sin_h)
        .reshape(plane_tok, local_heads * ROPE)
        .astype(BF)
    )
    grad_hidden = (dot_nt(gq_nope, wq_nope) + dot_nt(gq_rope, wq_rope)).astype(BF)
    key_grads, grad_hidden, grad_output_weight = swap(
        4,
        ("plane_sum", key_grads),
        ("plane_sum", grad_hidden.reshape(n_plane, tok, width)),
        ("group_sum", g_output),
    )
    later = lax.ppermute(key_grads[:tok].astype(BF), "g", down_pairs).astype(F32)
    key_grad = key_grads[tok:] + later
    latent_own = own_rows(latent)
    kv_norm_back = jax.vjp(rms_norm, latent_own[:, :RANK], gain_kv)[1]
    grad_comp_in, grad_gain_kv = kv_norm_back(key_grad[:, :RANK])
    grad_rope_in = unrotate(key_grad[:, RANK:], own_rows(cosine), own_rows(sine_part))
    grad_latent = jnp.concatenate([grad_comp_in, grad_rope_in], axis=1).astype(BF)

    g_query = jnp.concatenate(
        [
            dot_tn(hidden, gq_nope).reshape(width, local_heads, NOPE),
            dot_tn(hidden, gq_rope).reshape(width, local_heads, ROPE),
        ],
        axis=2,
    ).reshape(width, local_heads * (NOPE + ROPE))

    g_query = g_query.astype(BF).reshape(n_groups, n_plane, rows_w, head_cols)
    g_expand = grad_expand.astype(BF).reshape(n_groups, n_plane, kv_n, kv_cols)
    g_query, g_expand, latent_grads = swap(
        5,
        ("group_sum_swap", g_query),
        ("group_sum_swap", g_expand),
        ("plane_gather", grad_latent),
    )
    grad_query_weight = g_query.transpose(1, 0, 2).reshape(rows_w, -1).astype(F32)
    grad_expand_weight = g_expand.transpose(1, 0, 2).reshape(kv_n, -1).astype(F32)

    latent_grads = latent_grads.reshape(plane_tok, RANK + ROPE)
    g_latent = dot_tn(own_columns(hidden), latent_grads).astype(BF)
    grad_hidden = grad_hidden + dot_nt(grad_latent, latent_weight)
    norm_one_back = jax.vjp(rms_norm, input_float, gain_one)[1]
    grad_x_norm, grad_gain_one = norm_one_back(grad_hidden)
    grad_input = grad_x_one + grad_x_norm

    small_grads = jnp.concatenate(
        [
            p.reshape(devices, -1)
            for p in (grad_gain_one, grad_gain_two, grad_gain_kv, grad_router)
        ],
        axis=1,
    )
    small_grads = jnp.pad(small_grads, ((0, 0), (0, -small_grads.shape[1] % 1024)))
    grad_latent_weight, small_grads = swap(
        6,
        ("group_sum", g_latent.reshape(n_groups, rows_w, RANK + ROPE)),
        ("whole_sum", small_grads.reshape(n_groups, n_plane, -1, 128)),
    )
    small_grads = small_grads.reshape(-1)
    g_shared = lax.all_to_all(
        g_both.reshape(devices, rows_w, 2 * shared_n), ALL, split_axis=0, concat_axis=1
    )
    grad_shared_gate = g_shared[:, :, :shared_n].reshape(rows_w, devices * shared_n)
    grad_shared_up = g_shared[:, :, shared_n:].reshape(rows_w, devices * shared_n)
    return (
        output,
        grad_input,
        small_grads[: cuts[0]],
        grad_query_weight,
        grad_latent_weight,
        small_grads[cuts[1] : cuts[2]],
        grad_expand_weight,
        grad_output_weight,
        small_grads[cuts[0] : cuts[1]],
        small_grads[cuts[2] : cuts[3]].reshape(rows_w, experts),
        grad_shared_gate,
        grad_shared_up,
        g_sdown,
        g_gate[None],
        g_up[None],
        g_down[None],
    )


def solution(mesh):
    n_expert, n_shard = mesh.shape["expert"], mesh.shape["wshard"]
    devices = n_expert * n_shard

    def program(*args):
        tok = args[0].shape[0] // devices
        n_plane = DOC_MAX // tok
        n_groups = devices // n_plane
        inner = Mesh(mesh.devices.reshape(n_groups, n_plane // n_shard, n_shard), ALL)
        rows, vector = P(ALL, None), P(ALL)
        wide, tall = P(("g", "p"), None, "c"), P(("g", "p"), "c", None)
        step = jax.shard_map(
            functools.partial(body, n_groups, n_plane),
            mesh=inner,
            in_specs=(
                rows, vector, rows, rows, vector, rows, rows, vector, rows, rows, rows, rows,
                wide, wide, tall, rows, vector, rows,
            ),
            out_specs=(
                rows, rows, vector, rows, rows, vector, rows, rows, vector, rows, rows, rows,
                rows, wide, wide, tall,
            ),
            check_vma=False,
        )
        return step(*args)

    return program
```

```python
import functools

import jax
import jax.numpy as jnp
from jax import lax
from jax.experimental import pallas as pl
from jax.experimental.pallas import tpu as pltpu
from jax.sharding import Mesh, PartitionSpec as P

HEADS = 16
NOPE = 128
ROPE = 64
VDIM = 128
RANK = 512
TOP = 6
DOC_MAX = 1024
QUERY_BLOCK = 256

BF = jnp.bfloat16
F32 = jnp.float32
ALL = ("g", "p", "c")
PLANE = ("p", "c")

epsilon = 1e-06


def rms_norm(vector, scaling):
    return vector * lax.rsqrt(jnp.mean(vector * vector, axis=-1, keepdims=True) + epsilon) * scaling


def rotate(vector, cosine, sine_part):
    half_width = vector.shape[-1] // 2
    front_half = vector[..., :half_width]
    back_half = vector[..., half_width:]
    return jnp.concatenate(
        [front_half * cosine - back_half * sine_part, back_half * cosine + front_half * sine_part],
        axis=-1,
    )


def unrotate(vector, cosine, sine_part):
    return rotate(vector, cosine, -sine_part)


def matmul(left, right):
    return jnp.dot(left, right, preferred_element_type=F32)


def dot_nt(left, right):
    return lax.dot_general(left, right, (((1,), (1,)), ((), ())), preferred_element_type=F32)


def dot_tn(left, right):
    return lax.dot_general(left, right, (((0,), (0,)), ((), ())), preferred_element_type=F32)


def swiglu(gate_pre, up_pre):
    return jax.nn.silu(gate_pre) * up_pre


def softmax_rows(scores):
    row_top = jnp.max(scores, axis=-1, keepdims=True)
    exp_scores = jnp.exp(scores - row_top)
    return exp_scores / jnp.sum(exp_scores, axis=-1, keepdims=True)


def masked_scores(base, low_bound, q_nope, q_rope, k_nope, k_rope, scale):
    rows, span = q_nope.shape[0], k_nope.shape[0]
    key_at = lax.broadcasted_iota(jnp.int32, (rows, span), 1) + base
    query_at = lax.broadcasted_iota(jnp.int32, (rows, span), 0) + (base + DOC_MAX)
    allowed = (key_at >= low_bound) & (key_at <= query_at)
    scores = (dot_nt(q_nope, k_nope) + dot_nt(q_rope, k_rope)) * scale
    return jnp.where(allowed, scores, -1e30)


def attend_kernel(heads, scale, low_ref, qn_ref, qr_ref, ex_ref, kr_ref, out_ref, lse_ref):
    rows = qn_ref.shape[0]
    base = pl.multiple_of(pl.program_id(0) * rows, rows)
    window = pl.ds(base, rows + DOC_MAX)
    k_rope = kr_ref[window, :]
    low_bound = low_ref[...]
    for h in range(heads):
        at = h * (NOPE + VDIM)
        k_nope = ex_ref[window, at : at + NOPE]
        value = ex_ref[window, at + NOPE : at + NOPE + VDIM]
        scores = masked_scores(
            base,
            low_bound,
            qn_ref[:, h * NOPE : (h + 1) * NOPE],
            qr_ref[:, h * ROPE : (h + 1) * ROPE],
            k_nope,
            k_rope,
            scale,
        )
        top = jnp.max(scores, axis=-1, keepdims=True)
        exps = jnp.exp(scores - top)
        total = jnp.sum(exps, axis=-1, keepdims=True)
        probs = (exps / total).astype(BF)
        out_ref[:, h * VDIM : (h + 1) * VDIM] = jnp.dot(
            probs, value, preferred_element_type=F32
        ).astype(BF)
        lse_ref[:, h : h + 1] = top + jnp.log(total)


def attend(low_bound, q_nope, q_rope, expanded, key_rope, scale):
    queries = q_nope.shape[0]
    heads = q_nope.shape[1] // NOPE
    rows = QUERY_BLOCK

    def whole(array):
        return pl.BlockSpec(array.shape, lambda i: (0, 0))

    def blocked(width):
        return pl.BlockSpec((rows, width), lambda i: (i, 0))

    flops = 2 * heads * queries * (rows + DOC_MAX) * (NOPE + ROPE + VDIM)
    return pl.pallas_call(
        functools.partial(attend_kernel, heads, scale),
        grid=(queries // rows,),
        in_specs=[
            blocked(1),
            blocked(heads * NOPE),
            blocked(heads * ROPE),
            whole(expanded),
            whole(key_rope),
        ],
        out_specs=[blocked(heads * VDIM), blocked(heads)],
        out_shape=[
            jax.ShapeDtypeStruct((queries, heads * VDIM), BF),
            jax.ShapeDtypeStruct((queries, heads), F32),
        ],
        cost_estimate=pl.CostEstimate(
            flops=flops, bytes_accessed=4 * expanded.size, transcendentals=flops // 640
        ),
        compiler_params=pltpu.CompilerParams(vmem_limit_bytes=50 * 1024 * 1024),
        name="attend",
    )(low_bound, q_nope, q_rope, expanded, key_rope)


def attend_back_kernel(
    heads, scale, low_ref, qn_ref, qr_ref, ex_ref, kr_ref, lse_ref, gm_ref,
    dqn_ref, dqr_ref, dex_ref, dkr_ref,
):
    rows = qn_ref.shape[0]
    step = pl.program_id(0)
    base = pl.multiple_of(step * rows, rows)
    window = pl.ds(base, rows + DOC_MAX)

    @pl.when(step == 0)
    def _():
        dex_ref[...] = jnp.zeros_like(dex_ref)
        dkr_ref[...] = jnp.zeros_like(dkr_ref)

    k_rope = kr_ref[window, :]
    low_bound = low_ref[...]
    for h in range(heads):
        at = h * (NOPE + VDIM)
        k_nope = ex_ref[window, at : at + NOPE]
        value = ex_ref[window, at + NOPE : at + NOPE + VDIM]
        q_nope = qn_ref[:, h * NOPE : (h + 1) * NOPE]
        q_rope = qr_ref[:, h * ROPE : (h + 1) * ROPE]
        grad_out = gm_ref[:, h * VDIM : (h + 1) * VDIM]
        scores = masked_scores(base, low_bound, q_nope, q_rope, k_nope, k_rope, scale)
        probs = jnp.exp(scores - lse_ref[:, h : h + 1])
        grad_probs = dot_nt(grad_out, value)
        mean_grad = jnp.sum(probs * grad_probs, axis=-1, keepdims=True)
        grad_scores = (probs * (grad_probs - mean_grad) * scale).astype(BF)
        probs_low = probs.astype(BF)
        dqn_ref[:, h * NOPE : (h + 1) * NOPE] = jnp.dot(
            grad_scores, k_nope, preferred_element_type=F32
        )
        dqr_ref[:, h * ROPE : (h + 1) * ROPE] = jnp.dot(
            grad_scores, k_rope, preferred_element_type=F32
        )
        dex_ref[window, at : at + NOPE] += dot_tn(grad_scores, q_nope)
        dex_ref[window, at + NOPE : at + NOPE + VDIM] += dot_tn(probs_low, grad_out)
        dkr_ref[window, :] += dot_tn(grad_scores, q_rope)


def attend_back(low_bound, q_nope, q_rope, expanded, key_rope, lse, grad_mixed, scale):
    queries = q_nope.shape[0]
    heads = q_nope.shape[1] // NOPE
    rows = QUERY_BLOCK

    def whole(shape):
        return pl.BlockSpec(shape, lambda i: (0, 0))

    def blocked(width):
        return pl.BlockSpec((rows, width), lambda i: (i, 0))

    flops = 2 * heads * queries * (rows + DOC_MAX) * (3 * NOPE + 3 * ROPE + 2 * VDIM)
    return pl.pallas_call(
        functools.partial(attend_back_kernel, heads, scale),
        grid=(queries // rows,),
        in_specs=[
            blocked(1),
            blocked(heads * NOPE),
            blocked(heads * ROPE),
            whole(expanded.shape),
            whole(key_rope.shape),
            blocked(heads),
            blocked(heads * VDIM),
        ],
        out_specs=[
            blocked(heads * NOPE),
            blocked(heads * ROPE),
            whole(expanded.shape),
            whole(key_rope.shape),
        ],
        out_shape=[
            jax.ShapeDtypeStruct(q_nope.shape, F32),
            jax.ShapeDtypeStruct(q_rope.shape, F32),
            jax.ShapeDtypeStruct(expanded.shape, F32),
            jax.ShapeDtypeStruct(key_rope.shape, F32),
        ],
        cost_estimate=pl.CostEstimate(
            flops=flops, bytes_accessed=8 * expanded.size, transcendentals=flops // 1664
        ),
        compiler_params=pltpu.CompilerParams(vmem_limit_bytes=56 * 1024 * 1024),
        name="attend_back",
    )(low_bound, q_nope, q_rope, expanded, key_rope, lse, grad_mixed)


MESH = pl.DeviceIdType.MESH


class Wires:
    def __init__(self, n_groups, n_plane, send, recv):
        self.n_groups, self.n_plane, self.send, self.recv = n_groups, n_plane, send, recv
        self.cores = 2
        self.g, self.p, self.c = lax.axis_index("g"), lax.axis_index("p"), lax.axis_index("c")
        self.j = self.p * self.cores + self.c
        self.used = 0

    def at_plane(self, j):
        return {"g": self.g, "p": j // self.cores, "c": j % self.cores}

    def at_chip(self, p):
        return {"g": self.g, "p": p, "c": self.c}

    def at_group(self, g):
        return {"g": g, "p": self.p, "c": self.c}

    def partner(self):
        return {"g": self.g, "p": self.p, "c": 1 - self.c}

    def plane_peer(self, d):
        return lax.rem(self.j + d, self.n_plane)

    def group_peer(self, d):
        return lax.rem(self.g + d, self.n_groups)

    def start(self, src, dst, device):
        copy = pltpu.make_async_remote_copy(
            src_ref=src,
            dst_ref=dst,
            send_sem=self.send.at[self.used],
            recv_sem=self.recv.at[self.used],
            device_id=device,
            device_id_type=MESH,
        )
        self.used += 1
        copy.start()
        return copy

    def meet(self):
        barrier = pltpu.get_barrier_semaphore()
        for d in range(1, self.n_plane):
            pl.semaphore_signal(
                barrier, inc=1, device_id=self.at_plane(self.plane_peer(d)), device_id_type=MESH
            )
        for d in range(1, self.n_groups):
            pl.semaphore_signal(
                barrier, inc=1, device_id=self.at_group(self.group_peer(d)), device_id_type=MESH
            )
        pl.semaphore_wait(barrier, self.n_plane - 1 + self.n_groups - 1)


def sum_rows(dst, sources):
    rows = dst.shape[0]
    tile = 32 if rows % 32 == 0 else rows

    def step(i, carry):
        at = pl.ds(pl.multiple_of(i * tile, tile), tile)
        total = sources[0][at, :].astype(F32)
        for source in sources[1:]:
            total = total + source[at, :].astype(F32)
        dst[at, :] = total.astype(dst.dtype)
        return carry

    lax.fori_loop(0, rows // tile, step, 0)


def wait_all(copies):
    for copy in copies:
        copy.wait()


def wait_received(copies):
    for copy in copies:
        copy.wait_recv()


def wait_sent(copies):
    for copy in copies:
        copy.wait_send()


def plane_gather(w, src, out):
    chips = w.n_plane // w.cores
    first = [
        w.start(src, out.at[w.j], w.at_chip(lax.rem(w.p + d, chips))) for d in range(1, chips)
    ]
    second = [w.start(src, out.at[w.j], w.partner())]
    out[w.j] = src[...]
    yield
    for d in range(1, chips):
        first[d - 1].wait_recv()
        at = lax.rem(w.p + chips - d, chips) * w.cores + w.c
        second.append(w.start(out.at[at], out.at[at], w.partner()))
    yield
    wait_sent(first)
    wait_all(second)


def shift_gather(w, src, mid, out):
    copy = w.start(src, mid, w.at_group(lax.rem(w.g + 1, w.n_groups)))
    yield
    copy.wait()
    yield from plane_gather(w, mid, out)


def whole_gather(w, src, out):
    first = [
        w.start(src, out.at[w.g, w.j], w.at_group(w.group_peer(d))) for d in range(1, w.n_groups)
    ]
    out[w.g, w.j] = src[...]
    yield
    wait_received(first)
    second = [
        w.start(out.at[:, w.j], out.at[:, w.j], w.at_plane(w.plane_peer(d)))
        for d in range(1, w.n_plane)
    ]
    yield
    wait_sent(first)
    wait_all(second)


def plane_swap_gather(w, src, out):
    first = []
    for d in range(1, w.n_plane):
        to = w.plane_peer(d)
        first.append(w.start(src.at[to], out.at[w.g, w.j], w.at_plane(to)))
    out[w.g, w.j] = src[w.j]
    yield
    wait_received(first)
    second = [
        w.start(out.at[w.g], out.at[w.g], w.at_group(w.group_peer(d)))
        for d in range(1, w.n_groups)
    ]
    yield
    wait_sent(first)
    wait_all(second)


def plane_swap(w, src, out):
    copies = []
    for d in range(1, w.n_plane):
        to = w.plane_peer(d)
        copies.append(w.start(src.at[to], out.at[w.j], w.at_plane(to)))
    out[w.j] = src[w.j]
    yield
    wait_all(copies)


def plane_sum(w, src, out, from_core, pairs, from_chips):
    chips = w.n_plane // w.cores
    first = []
    for d in range(chips):
        p = lax.rem(w.p + d, chips)
        first.append(w.start(src.at[p * w.cores + 1 - w.c], from_core.at[d], w.partner()))
    yield
    second = []
    for d in list(range(1, chips)) + [0]:
        p = lax.rem(w.p + d, chips)
        first[d].wait_recv()
        sum_rows(pairs.at[d], [src.at[p * w.cores + w.c], from_core.at[d]])
        if d:
            second.append(w.start(pairs.at[d], from_chips.at[d - 1], w.at_chip(p)))
    yield
    wait_received(second)
    sum_rows(out, [pairs.at[0]] + [from_chips.at[d] for d in range(chips - 1)])
    wait_sent(first)
    wait_sent(second)


def whole_sum(w, src, out, from_plane, total, parts):
    first = []
    for d in range(1, w.n_plane):
        to = w.plane_peer(d)
        first.append(w.start(src.at[:, to], from_plane.at[d - 1], w.at_plane(to)))
    yield
    wait_received(first)

    def step(i, carry):
        sum_rows(
            total.at[i], [src.at[i, w.j]] + [from_plane.at[d, i] for d in range(w.n_plane - 1)]
        )
        return carry

    lax.fori_loop(0, w.n_groups, step, 0)
    wait_sent(first)
    yield from group_sum(w, total, out, parts)


def whole_swap(w, src, out, mid):
    first = []
    for d in range(1, w.n_plane):
        to = w.plane_peer(d)
        first.append(w.start(src.at[:, to], mid.at[w.j], w.at_plane(to)))
    mid[w.j] = src[:, w.j]
    yield
    wait_received(first)
    second = []
    for d in range(1, w.n_groups):
        to = w.group_peer(d)
        second.append(w.start(mid.at[:, to], out.at[w.g], w.at_group(to)))
    out[w.g] = mid[:, w.g]
    yield
    wait_sent(first)
    wait_all(second)


def group_sum(w, src, out, parts):
    copies = []
    for d in range(1, w.n_groups):
        to = w.group_peer(d)
        copies.append(w.start(src.at[to], parts.at[d - 1], w.at_group(to)))
    yield
    wait_received(copies)
    sum_rows(out, [src.at[w.g]] + [parts.at[d] for d in range(w.n_groups - 1)])
    wait_sent(copies)


def group_sum_swap(w, src, out, total, parts):
    copies = []
    for d in range(1, w.n_groups):
        to = w.group_peer(d)
        copies.append(w.start(src.at[to], parts.at[d - 1], w.at_group(to)))
    yield
    wait_received(copies)

    def step(i, carry):
        sum_rows(total.at[i], [src.at[w.g, i]] + [parts.at[d, i] for d in range(w.n_groups - 1)])
        return carry

    lax.fori_loop(0, w.n_plane, step, 0)
    second = []
    for d in range(1, w.n_plane):
        to = w.plane_peer(d)
        second.append(w.start(total.at[to], out.at[w.j], w.at_plane(to)))
    out[w.j] = total[w.j]
    yield
    wait_sent(copies)
    wait_all(second)


ROUTINES = {
    "plane_gather": plane_gather,
    "shift_gather": shift_gather,
    "whole_gather": whole_gather,
    "plane_swap_gather": plane_swap_gather,
    "plane_swap": plane_swap,
    "plane_sum": plane_sum,
    "group_sum": group_sum,
    "whole_sum": whole_sum,
    "whole_swap": whole_swap,
    "group_sum_swap": group_sum_swap,
}


def exchange_kernel(n_groups, n_plane, kinds, extra, *refs):
    count = len(kinds)
    sources, outs = refs[:count], refs[count : 2 * count]
    scratch = list(refs[2 * count : -2])
    w = Wires(n_groups, n_plane, refs[-2], refs[-1])
    w.meet()
    running = []
    for kind, source, out, number in zip(kinds, sources, outs, extra):
        mine, scratch = scratch[:number], scratch[number:]
        if kind == "shift_gather":
            running.append(shift_gather(w, source, mine[0], out))
        else:
            running.append(ROUTINES[kind](w, source, out, *mine))
    while running:
        still = []
        for routine in running:
            try:
                next(routine)
                still.append(routine)
            except StopIteration:
                pass
        running = still


def exchange(n_groups, n_plane, number, *items):
    kinds = [kind for kind, _ in items]
    arrays = [array for _, array in items]
    shapes, scratch, extra = [], [], []
    chips = n_plane // 2
    for kind, array in items:
        shape, dtype = array.shape, array.dtype
        own = []
        if kind in ("plane_gather", "shift_gather"):
            out = (n_plane,) + shape
            if kind == "shift_gather":
                own = [shape]
        elif kind == "whole_gather":
            out = (n_groups, n_plane) + shape
        elif kind == "plane_swap_gather":
            out = (n_groups,) + shape
        elif kind == "plane_swap":
            out = shape
        elif kind == "plane_sum":
            out = shape[1:]
            own = [(chips,) + out, (chips,) + out, (chips - 1,) + out]
        elif kind == "group_sum":
            out = shape[1:]
            own = [(n_groups - 1,) + out]
        elif kind == "whole_swap":
            out = shape
            own = [(n_plane, n_groups) + shape[2:]]
        elif kind == "whole_sum":
            out = shape[2:]
            own = [(n_plane - 1, n_groups) + out, (n_groups,) + out, (n_groups - 1,) + out]
        elif kind == "group_sum_swap":
            out = shape[1:]
            own = [out, (n_groups - 1,) + out]
        if kind in ("plane_sum", "group_sum", "whole_sum"):
            shapes.append(jax.ShapeDtypeStruct(out, F32))
        else:
            shapes.append(jax.ShapeDtypeStruct(out, dtype))
        scratch += [pltpu.VMEM(s, dtype) for s in own]
        extra.append(len(own))
    copies = 64 + 32 * len(items)
    vmem = pl.BlockSpec(memory_space=pltpu.VMEM)
    return pl.pallas_call(
        functools.partial(exchange_kernel, n_groups, n_plane, kinds, extra),
        out_shape=shapes,
        in_specs=[vmem] * len(items),
        out_specs=[vmem] * len(items),
        scratch_shapes=scratch
        + [pltpu.SemaphoreType.DMA((copies,)), pltpu.SemaphoreType.DMA((copies,))],
        compiler_params=pltpu.CompilerParams(
            collective_id=number,
            has_side_effects=True,
            vmem_limit_bytes=60 * 1024 * 1024,
        ),
        name="exchange_%d" % number,
    )(*arrays)


def gather_all(x):
    return lax.all_gather(x, ALL, axis=0, tiled=True)


def moe_kernel(
    first_logit, experts, slot_count, id_ref, h2_ref, cot_ref, place_ref, wg_ref, wu_ref, wd_ref,
    sc_ref, sd_ref,
    gh2_ref, rows_ref, gin_ref, act_ref, gg_ref, gu_ref, rw_ref, pg_ref, sact_ref, sgrad_ref,
):
    blocks = h2_ref.shape[0] // 128
    step = pl.program_id(0)
    half = sc_ref.shape[1] // 2
    h2, cot = h2_ref[...], cot_ref[...]

    pre = jnp.dot(h2, sc_ref[...], preferred_element_type=F32)
    back = dot_nt(cot, sd_ref[...])
    gate, up = pre[:, :half], pre[:, half:]
    lane = lax.broadcasted_iota(jnp.int32, gate.shape, 1)
    logits = jnp.where((lane >= first_logit) & (lane < first_logit + experts), gate, -1e30)
    exps = jnp.exp(logits - jnp.max(logits, axis=1, keepdims=True))
    chosen = jnp.where(lane == first_logit + id_ref[0], exps, 0.0)
    weight = jnp.sum(chosen, axis=1, keepdims=True) / jnp.sum(exps, axis=1, keepdims=True)
    act, grad_gate, grad_up = swiglu_both(gate, up, back)
    sact_ref[...] = act.astype(BF)
    shared_grad = jnp.concatenate([grad_gate.astype(BF), grad_up.astype(BF)], axis=1)
    sgrad_ref[...] = shared_grad

    hots, weights = [], []
    for b in range(blocks):
        place = place_ref[pl.ds(step * blocks + b, 1), :]
        hot = lax.broadcasted_iota(jnp.int32, (slot_count, 128), 0) == place
        hots.append(hot.astype(F32).astype(BF))
        tokens = slice(b * 128, (b + 1) * 128)
        slots = slice(b * slot_count, (b + 1) * slot_count)
        rows_ref[slots, :] = jnp.dot(hots[b], h2[tokens], preferred_element_type=F32).astype(BF)
        gin_ref[slots, :] = jnp.dot(hots[b], cot[tokens], preferred_element_type=F32).astype(BF)
        spread = jnp.broadcast_to(weight[tokens], (128, 128))
        weights.append(
            jnp.dot(
                hot.astype(F32),
                spread,
                preferred_element_type=F32,
                precision=lax.Precision.HIGHEST,
            )[:, :1]
        )
    row_weight = jnp.concatenate(weights, axis=0)
    rw_ref[...] = row_weight
    rows = rows_ref[...]
    picked_cot = gin_ref[...]
    back = dot_nt(picked_cot, wd_ref[...])
    gin_ref[...] = (picked_cot.astype(F32) * row_weight).astype(BF)
    gate = jnp.dot(rows, wg_ref[...], preferred_element_type=F32)
    up = jnp.dot(rows, wu_ref[...], preferred_element_type=F32)
    act, grad_gate, grad_up = swiglu_both(gate, up, back * row_weight)
    act_low, grad_gate, grad_up = act.astype(BF), grad_gate.astype(BF), grad_up.astype(BF)
    act_ref[...] = act_low
    gg_ref[...] = grad_gate
    gu_ref[...] = grad_up
    pg_ref[...] = jnp.sum(act_low.astype(F32) * back, axis=1, keepdims=True)
    grad_rows = (dot_nt(grad_gate, wg_ref[...]) + dot_nt(grad_up, wu_ref[...])).astype(BF)
    for b in range(blocks):
        tokens = slice(b * 128, (b + 1) * 128)
        slots = slice(b * slot_count, (b + 1) * slot_count)
        total = dot_tn(hots[b], grad_rows[slots]) + dot_nt(shared_grad[tokens], sc_ref[...])
        gh2_ref[tokens, :] = total.astype(BF)


def swiglu_both(gate, up, grad):
    sigmoid = 1.0 / (1.0 + jnp.exp(-gate))
    silu = gate * sigmoid
    return silu * up, grad * up * (sigmoid * (1.0 + gate * (1.0 - sigmoid))), grad * silu


def out_kernel(slot_count, act_ref, rw_ref, place_ref, sact_ref, wd_ref, sd_ref, out_ref):
    blocks = out_ref.shape[0] // 128
    step = pl.program_id(0)
    rows = (jnp.dot(act_ref[...], wd_ref[...], preferred_element_type=F32) * rw_ref[...]).astype(BF)
    for b in range(blocks):
        place = place_ref[pl.ds(step * blocks + b, 1), :]
        hot = lax.broadcasted_iota(jnp.int32, (slot_count, 128), 0) == place
        tokens = slice(b * 128, (b + 1) * 128)
        slots = slice(b * slot_count, (b + 1) * slot_count)
        total = dot_tn(hot.astype(F32).astype(BF), rows[slots]) + jnp.dot(
            sact_ref[tokens, :], sd_ref[...], preferred_element_type=F32
        )
        out_ref[tokens, :] = total.astype(BF)


def experts_chunk(h2, cot, expert_id, place, slot_count, expert_w, shared_w, router_weight):
    w_gate, w_up, w_down = expert_w
    s_both, s_down = shared_w
    tokens, width = h2.shape
    hidden, hidden_s = w_down.shape[0], s_down.shape[0]
    experts = router_weight.shape[1]
    blocks = 4
    steps = tokens // (128 * blocks)
    step_slots = slot_count * blocks
    all_slots = step_slots * steps
    half = 128
    s_cat = jnp.concatenate(
        [
            s_both[:, :hidden_s],
            router_weight,
            jnp.zeros((width, half - hidden_s - experts), BF),
            s_both[:, hidden_s:],
            jnp.zeros((width, half - hidden_s), BF),
        ],
        axis=1,
    )
    s_tall = jnp.pad(s_down, ((0, half - hidden_s), (0, 0)))

    def whole(array):
        return pl.BlockSpec(array.shape, lambda i: (0, 0), pipeline_mode=pl.Buffered(1))

    def blocked(rows, cols):
        return pl.BlockSpec((rows, cols), lambda i: (i, 0))

    token_rows = blocked(128 * blocks, width)
    shape = jax.ShapeDtypeStruct
    flops = 2 * all_slots * width * hidden * 5 + 2 * tokens * width * (4 * half + 4 * slot_count)
    grad_h2, rows_in, grad_in, act, grad_gate, grad_up, row_weight, picked, s_act, s_grad = (
        pl.pallas_call(
            functools.partial(moe_kernel, hidden_s, experts, slot_count),
            grid=(steps,),
            in_specs=[
                pl.BlockSpec(memory_space=pltpu.SMEM),
                token_rows,
                token_rows,
                whole(place),
                whole(w_gate),
                whole(w_up),
                whole(w_down),
                whole(s_cat),
                whole(s_tall),
            ],
            out_specs=[
                token_rows,
                blocked(step_slots, width),
                blocked(step_slots, width),
                blocked(step_slots, hidden),
                blocked(step_slots, hidden),
                blocked(step_slots, hidden),
                blocked(step_slots, 1),
                blocked(step_slots, 1),
                blocked(128 * blocks, half),
                blocked(128 * blocks, 2 * half),
            ],
            out_shape=[
                shape((tokens, width), BF),
                shape((all_slots, width), BF),
                shape((all_slots, width), BF),
                shape((all_slots, hidden), BF),
                shape((all_slots, hidden), BF),
                shape((all_slots, hidden), BF),
                shape((all_slots, 1), F32),
                shape((all_slots, 1), F32),
                shape((tokens, half), BF),
                shape((tokens, 2 * half), BF),
            ],
            cost_estimate=pl.CostEstimate(
                flops=flops, bytes_accessed=12 * tokens * width, transcendentals=tokens * 1024
            ),
            compiler_params=pltpu.CompilerParams(vmem_limit_bytes=63 * 1024 * 1024),
            name="experts",
        )(expert_id.reshape(1), h2, cot, place, w_gate, w_up, w_down, s_cat, s_tall)
    )

    grad_h2, act, rows_in, grad_in, s_act, s_grad = lax.optimization_barrier(
        (grad_h2, act, rows_in, grad_in, s_act, s_grad)
    )
    hot = jnp.arange(slot_count, dtype=jnp.int32)[None, :, None] == place[:, None, :]
    token_grad = jnp.sum(jnp.where(hot, picked.reshape(-1, slot_count, 1), 0.0), axis=1)
    out = pl.pallas_call(
        functools.partial(out_kernel, slot_count),
        grid=(steps,),
        in_specs=[
            blocked(step_slots, hidden),
            blocked(step_slots, 1),
            whole(place),
            blocked(128 * blocks, half),
            whole(w_down),
            whole(s_tall),
        ],
        out_specs=token_rows,
        out_shape=shape((tokens, width), BF),
        cost_estimate=pl.CostEstimate(
            flops=2 * width * (all_slots * hidden + tokens * (half + slot_count)),
            bytes_accessed=4 * tokens * width,
            transcendentals=0,
        ),
        compiler_params=pltpu.CompilerParams(vmem_limit_bytes=56 * 1024 * 1024),
        name="expert_out",
    )(act, row_weight, place, s_act, w_down, s_tall)
    g_both = dot_tn(h2, s_grad)
    g_both = jnp.concatenate([g_both[:, :hidden_s], g_both[:, half : half + hidden_s]], axis=1)
    grads = (
        dot_tn(rows_in, grad_gate),
        dot_tn(rows_in, grad_up),
        dot_tn(act, grad_in),
        g_both,
        dot_tn(s_act, cot)[:hidden_s],
    )
    return out, grad_h2, token_grad, grads


def body(
    n_groups, n_plane, layer_input, attn_gain, w_query, w_latent, kv_gain, w_expand, w_output,
    ffn_gain, w_router, shared_gate, shared_up, shared_down, expert_gate, expert_up,
    expert_down, routes, segments, cotangent,
):
    tok, width = layer_input.shape
    devices = n_groups * n_plane
    experts = w_router.shape[1]
    local_heads = HEADS // n_plane
    scale = (NOPE + ROPE) ** (-0.5)
    group = lax.axis_index("g")
    place_in = lax.axis_index(PLANE)
    me = lax.axis_index(ALL)
    expert_id = lax.axis_index(("g", "p"))
    plane_tok = n_plane * tok
    plane_start = group * plane_tok

    rows_w = w_router.shape[0]
    kv_n = kv_gain.shape[0]
    small = jnp.concatenate(
        [
            attn_gain,
            ffn_gain,
            kv_gain,
            w_router.reshape(-1),
            routes.reshape(-1).astype(BF),
            segments.astype(BF),
        ]
    )
    small = jnp.pad(small, (0, -small.shape[0] % 4096)).reshape(-1, 128)
    head_cols = local_heads * (NOPE + ROPE)
    kv_cols = local_heads * (NOPE + VDIM)
    fold = kv_n * kv_cols // rows_w
    pair = jnp.concatenate(
        [
            w_query.reshape(rows_w, n_plane, head_cols).transpose(1, 0, 2),
            w_expand.reshape(kv_n, n_plane, kv_cols // fold, fold)
            .transpose(1, 0, 2, 3)
            .reshape(n_plane, rows_w, fold),
        ],
        axis=2,
    )
    swap = functools.partial(exchange, n_groups, n_plane)
    x_plane, small, latent_weight, pair = swap(
        0,
        ("plane_gather", layer_input),
        ("whole_gather", small),
        ("whole_gather", w_latent),
        ("plane_swap_gather", pair),
    )
    x_plane = x_plane.reshape(plane_tok, width).astype(F32)
    latent_weight = latent_weight.reshape(width, RANK + ROPE)
    pair = pair.reshape(width, head_cols + fold)
    small = small.reshape(devices, -1)
    cuts = [rows_w, 2 * rows_w, 2 * rows_w + kv_n, 2 * rows_w + kv_n + rows_w * experts]
    cuts = cuts + [cuts[-1] + tok * TOP, cuts[-1] + tok * TOP + tok]
    gain_one = small[:, : cuts[0]].reshape(-1).astype(F32)
    gain_two = small[:, cuts[0] : cuts[1]].reshape(-1).astype(F32)
    gain_kv = small[:, cuts[1] : cuts[2]].reshape(-1).astype(F32)
    router_weight = small[:, cuts[2] : cuts[3]].reshape(width, experts)
    routes_all = small[:, cuts[3] : cuts[4]].astype(jnp.int32).reshape(devices, tok, TOP)
    segments_all = small[:, cuts[4] : cuts[5]].astype(jnp.int32).reshape(-1)

    query_weight = pair[:, :head_cols].reshape(width, local_heads, NOPE + ROPE)
    wq_nope = query_weight[:, :, :NOPE].reshape(width, local_heads * NOPE)
    wq_rope = query_weight[:, :, NOPE:].reshape(width, local_heads * ROPE)
    expand_weight = pair[:, head_cols:].reshape(RANK, kv_cols)
    output_weight = gather_all(w_output)

    shared_n = shared_down.shape[0]
    s_both = jnp.concatenate(
        [
            shared_gate.reshape(rows_w, devices, shared_n),
            shared_up.reshape(rows_w, devices, shared_n),
        ],
        axis=2,
    )
    s_both = lax.all_to_all(s_both, ALL, split_axis=1, concat_axis=0).reshape(width, 2 * shared_n)

    hidden = rms_norm(x_plane, gain_one).astype(BF)
    rope_half = ROPE // 2
    positions = plane_start + jnp.arange(plane_tok, dtype=jnp.int32)
    frequency = 10000.0 ** (-jnp.arange(rope_half, dtype=F32) / rope_half)
    angles = positions.astype(F32)[:, None] * frequency[None, :]
    cosine = jnp.cos(angles)
    sine_part = jnp.sin(angles)
    cos_h, sin_h = cosine[:, None, :], sine_part[:, None, :]
    latent = matmul(hidden, latent_weight)
    compressed_own = rms_norm(latent[:, :RANK], gain_kv).astype(BF)
    key_rope_own = rotate(latent[:, RANK:], cosine, sine_part).astype(BF)

    def own_rows(table):
        return lax.dynamic_slice_in_dim(table, place_in * tok, tok, 0)

    down_pairs = [(i + 1, i) for i in range(n_groups - 1)]
    piece = own_rows(jnp.concatenate([compressed_own, key_rope_own], axis=1))
    before = swap(1, ("shift_gather", piece))[0].reshape(plane_tok, RANK + ROPE)
    compressed = jnp.concatenate([before[:, :RANK], compressed_own], axis=0)
    key_rope = jnp.concatenate([before[:, RANK:], key_rope_own], axis=0)
    q_nope = matmul(hidden, wq_nope).astype(BF)
    q_rope = rotate(
        matmul(hidden, wq_rope).reshape(plane_tok, local_heads, ROPE), cos_h, sin_h
    ).reshape(plane_tok, local_heads * ROPE).astype(BF)
    expanded = matmul(compressed, expand_weight).astype(BF)
    plane_segments = lax.dynamic_slice_in_dim(segments_all, plane_start, plane_tok, 0)
    doc_start = jnp.sum(
        (segments_all[None, :] < plane_segments[:, None]).astype(jnp.int32), axis=1, keepdims=True
    )
    low_bound = doc_start - plane_start + DOC_MAX
    mixed_heads, lse = attend(low_bound, q_nope, q_rope, expanded, key_rope, scale)
    mixed = swap(2, ("plane_swap", mixed_heads.reshape(n_plane, tok, local_heads * VDIM)))[0]
    mixed = mixed.transpose(1, 0, 2).reshape(tok, width)

    input_float = layer_input.astype(F32)
    residual_one = input_float + matmul(mixed, output_weight)
    h_two_f, norm_two_back = jax.vjp(rms_norm, residual_one, gain_two)
    h_two = h_two_f.astype(BF)
    router_probs = softmax_rows(matmul(h_two, router_weight))

    expert_w = (expert_gate[0], expert_up[0], expert_down[0])
    shared_w = (s_both, shared_down)
    slot_limit = 2 * tok * TOP // experts

    def scatter_all(x):
        return lax.psum_scatter(x, ALL, scatter_dimension=0, tiled=True)

    def on_rows(h2, cot_gathered, routes_here):
        rows = h2.shape[0]
        h2_all = gather_all(h2)
        slot_count = min(slot_limit, rows)
        member = jnp.any(routes_here == expert_id, axis=2)
        member_int = member.astype(jnp.int32)
        rank = jnp.cumsum(member_int, axis=1) - member_int
        merged = 128 // rows
        first_slot = jnp.arange(devices, dtype=jnp.int32) % merged * slot_count
        place = jnp.where(member, rank + first_slot[:, None], -1).reshape(-1, 128)
        out, grad_h2, token_grad, grads = experts_chunk(
            h2_all,
            cot_gathered,
            expert_id,
            place,
            merged * slot_count,
            expert_w,
            shared_w,
            router_weight,
        )
        token_grad = token_grad.reshape(devices, rows)
        picked = lax.all_to_all(token_grad, ALL, split_axis=0, concat_axis=0, tiled=True)
        picked = jnp.sum(picked.reshape(experts, devices // experts, rows), axis=1).T
        grad_h2, out, grads, picked = lax.optimization_barrier(
            (scatter_all(grad_h2), out, grads, picked)
        )
        return scatter_all(out), grad_h2, picked, grads

    parts = max(1, devices * tok // 4096)
    if parts == 1:
        cot_all = gather_all(cotangent)
        out_own, grad_h2_own, grad_router_probs, grads = on_rows(
            h_two, cot_all, routes_all
        )
    else:
        rows = tok // parts

        def step(total, inputs):
            h2, cot, routes_here = inputs
            cot_part = gather_all(cot)
            out, grad_h2, picked, grads = on_rows(h2, cot_part, routes_here)
            total = tuple(a + b for a, b in zip(total, grads))
            return total, (out, grad_h2, picked)

        shapes = expert_w + shared_w
        grads, (out_own, grad_h2_own, grad_router_probs) = lax.scan(
            step,
            tuple(jnp.zeros(s.shape, F32) for s in shapes),
            (
                h_two.reshape(parts, rows, width),
                cotangent.reshape(parts, rows, width),
                routes_all.reshape(devices, parts, rows, TOP).transpose(1, 0, 2, 3),
            ),
        )
        out_own = out_own.reshape(tok, width)
        grad_h2_own = grad_h2_own.reshape(tok, width)
        grad_router_probs = grad_router_probs.reshape(tok, experts)
    g_gate, g_up, g_down, g_both, g_sdown = grads
    grad_logits = router_probs * (
        grad_router_probs - jnp.sum(router_probs * grad_router_probs, axis=1, keepdims=True)
    )
    grad_logits = grad_logits.astype(BF)
    grad_router = dot_tn(h_two, grad_logits)
    grad_h_two = grad_h2_own.astype(F32) + dot_nt(grad_logits, router_weight)
    output = residual_one + out_own.astype(F32)

    grad_x_one, grad_gain_two = norm_two_back(grad_h_two)
    grad_x_one = grad_x_one + cotangent.astype(F32)
    grad_attn_out = grad_x_one.astype(BF)
    plane_grad = swap(3, ("plane_gather", grad_attn_out))[0].reshape(plane_tok, width)
    head_rows = local_heads * VDIM
    own_output = lax.dynamic_slice_in_dim(output_weight, place_in * head_rows, head_rows, 0)
    grad_mixed = dot_nt(plane_grad, own_output).astype(BF)
    dqn, dqr, dex, dkr = attend_back(
        low_bound, q_nope, q_rope, expanded, key_rope, lse, grad_mixed, scale
    )

    g_output = dot_tn(mixed_heads, plane_grad).astype(BF).reshape(n_groups, rows_w, width)

    grad_expanded = dex.astype(BF)
    grad_expand = dot_tn(compressed, grad_expanded)
    grad_comp = dot_nt(grad_expanded, expand_weight)
    key_grads = jnp.concatenate([grad_comp, dkr], axis=1).astype(BF)
    key_grads = (
        key_grads.reshape(2, n_plane, tok, RANK + ROPE)
        .transpose(1, 0, 2, 3)
        .reshape(n_plane, 2 * tok, RANK + ROPE)
    )

    gq_nope = dqn.astype(BF)
    gq_rope = (
        unrotate(dqr.reshape(plane_tok, local_heads, ROPE), cos_h, sin_h)
        .reshape(plane_tok, local_heads * ROPE)
        .astype(BF)
    )
    grad_hidden = (dot_nt(gq_nope, wq_nope) + dot_nt(gq_rope, wq_rope)).astype(BF)
    key_grads, grad_hidden, grad_output_weight, g_shared = swap(
        4,
        ("plane_sum", key_grads),
        ("plane_sum", grad_hidden.reshape(n_plane, tok, width)),
        ("group_sum", g_output),
        ("whole_swap", g_both.astype(BF).reshape(n_groups, n_plane, rows_w, 2 * shared_n)),
    )
    row_pairs = [
        (g * n_plane + j, n_groups * j + g) for g in range(n_groups) for j in range(n_plane)
    ]
    grad_output_weight = lax.ppermute(grad_output_weight, ALL, row_pairs)
    later = lax.ppermute(key_grads[:tok].astype(BF), "g", down_pairs).astype(F32)
    key_grad = key_grads[tok:] + later
    latent_own = own_rows(latent)
    kv_norm_back = jax.vjp(rms_norm, latent_own[:, :RANK], gain_kv)[1]
    grad_comp_in, grad_gain_kv = kv_norm_back(key_grad[:, :RANK])
    grad_rope_in = unrotate(key_grad[:, RANK:], own_rows(cosine), own_rows(sine_part))
    grad_latent = jnp.concatenate([grad_comp_in, grad_rope_in], axis=1).astype(BF)

    g_query = jnp.concatenate(
        [
            dot_tn(hidden, gq_nope).reshape(width, local_heads, NOPE),
            dot_tn(hidden, gq_rope).reshape(width, local_heads, ROPE),
        ],
        axis=2,
    ).reshape(width, local_heads * (NOPE + ROPE))

    g_query = g_query.astype(BF).reshape(n_groups, n_plane, rows_w, head_cols)
    g_expand = grad_expand.astype(BF).reshape(n_groups, n_plane, kv_n, kv_cols)
    g_query, g_expand, latent_grads = swap(
        5,
        ("group_sum_swap", g_query),
        ("group_sum_swap", g_expand),
        ("plane_gather", grad_latent),
    )
    grad_query_weight = g_query.transpose(1, 0, 2).reshape(rows_w, -1).astype(F32)
    grad_expand_weight = g_expand.transpose(1, 0, 2).reshape(kv_n, -1).astype(F32)

    latent_grads = latent_grads.reshape(plane_tok, RANK + ROPE)
    g_latent = dot_tn(hidden, latent_grads).astype(BF)
    g_latent = g_latent.reshape(n_groups, n_plane, rows_w, RANK + ROPE)
    g_latent = lax.dynamic_index_in_dim(g_latent, place_in, 1, keepdims=False)
    grad_hidden = grad_hidden + dot_nt(grad_latent, latent_weight)
    norm_one_back = jax.vjp(rms_norm, input_float, gain_one)[1]
    grad_x_norm, grad_gain_one = norm_one_back(grad_hidden)
    grad_input = grad_x_one + grad_x_norm

    small_grads = jnp.concatenate(
        [
            p.reshape(devices, -1)
            for p in (grad_gain_one, grad_gain_two, grad_gain_kv, grad_router)
        ],
        axis=1,
    )
    small_grads = jnp.pad(small_grads, ((0, 0), (0, -small_grads.shape[1] % 1024)))
    grad_latent_weight, small_grads = swap(
        6,
        ("group_sum", g_latent),
        ("whole_sum", small_grads.reshape(n_groups, n_plane, -1, 128)),
    )
    small_grads = small_grads.reshape(-1)
    g_shared = g_shared.transpose(2, 0, 1, 3).reshape(rows_w, devices, 2 * shared_n).astype(F32)
    grad_shared_gate = g_shared[:, :, :shared_n].reshape(rows_w, devices * shared_n)
    grad_shared_up = g_shared[:, :, shared_n:].reshape(rows_w, devices * shared_n)
    return (
        output,
        grad_input,
        small_grads[: cuts[0]],
        grad_query_weight,
        grad_latent_weight,
        small_grads[cuts[1] : cuts[2]],
        grad_expand_weight,
        grad_output_weight,
        small_grads[cuts[0] : cuts[1]],
        small_grads[cuts[2] : cuts[3]].reshape(rows_w, experts),
        grad_shared_gate,
        grad_shared_up,
        g_sdown,
        g_gate[None],
        g_up[None],
        g_down[None],
    )


def solution(mesh):
    n_expert, n_shard = mesh.shape["expert"], mesh.shape["wshard"]
    devices = n_expert * n_shard

    def program(*args):
        tok = args[0].shape[0] // devices
        n_plane = DOC_MAX // tok
        n_groups = devices // n_plane
        inner = Mesh(mesh.devices.reshape(n_groups, n_plane // n_shard, n_shard), ALL)
        rows, vector = P(ALL, None), P(ALL)
        wide, tall = P(("g", "p"), None, "c"), P(("g", "p"), "c", None)
        step = jax.shard_map(
            functools.partial(body, n_groups, n_plane),
            mesh=inner,
            in_specs=(
                rows, vector, rows, rows, vector, rows, rows, vector, rows, rows, rows, rows,
                wide, wide, tall, rows, vector, rows,
            ),
            out_specs=(
                rows, rows, vector, rows, rows, vector, rows, rows, vector, rows, rows, rows,
                rows, wide, wide, tall,
            ),
            check_vma=False,
        )
        return step(*args)

    return program
```

```python
import functools

import jax
import jax.numpy as jnp
from jax import lax
from jax.experimental import pallas as pl
from jax.experimental.pallas import tpu as pltpu
from jax.sharding import Mesh, PartitionSpec as P

HEADS = 16
NOPE = 128
ROPE = 64
VDIM = 128
RANK = 512
TOP = 6
DOC_MAX = 1024
QUERY_BLOCK = 256

BF = jnp.bfloat16
F32 = jnp.float32
ALL = ("g", "p", "c")
PLANE = ("p", "c")

epsilon = 1e-06


def rms_norm(vector, scaling):
    return vector * lax.rsqrt(jnp.mean(vector * vector, axis=-1, keepdims=True) + epsilon) * scaling


def rotate(vector, cosine, sine_part):
    half_width = vector.shape[-1] // 2
    front_half = vector[..., :half_width]
    back_half = vector[..., half_width:]
    return jnp.concatenate(
        [front_half * cosine - back_half * sine_part, back_half * cosine + front_half * sine_part],
        axis=-1,
    )


def unrotate(vector, cosine, sine_part):
    return rotate(vector, cosine, -sine_part)


def matmul(left, right):
    return jnp.dot(left, right, preferred_element_type=F32)


def dot_nt(left, right):
    return lax.dot_general(left, right, (((1,), (1,)), ((), ())), preferred_element_type=F32)


def dot_tn(left, right):
    return lax.dot_general(left, right, (((0,), (0,)), ((), ())), preferred_element_type=F32)


def swiglu(gate_pre, up_pre):
    return jax.nn.silu(gate_pre) * up_pre


def softmax_rows(scores):
    row_top = jnp.max(scores, axis=-1, keepdims=True)
    exp_scores = jnp.exp(scores - row_top)
    return exp_scores / jnp.sum(exp_scores, axis=-1, keepdims=True)


def masked_scores(base, low_bound, q_nope, q_rope, k_nope, k_rope, scale):
    rows, span = q_nope.shape[0], k_nope.shape[0]
    key_at = lax.broadcasted_iota(jnp.int32, (rows, span), 1) + base
    query_at = lax.broadcasted_iota(jnp.int32, (rows, span), 0) + (base + DOC_MAX)
    allowed = (key_at >= low_bound) & (key_at <= query_at)
    scores = (dot_nt(q_nope, k_nope) + dot_nt(q_rope, k_rope)) * scale
    return jnp.where(allowed, scores, -1e30)


def attend_kernel(heads, scale, low_ref, qn_ref, qr_ref, ex_ref, kr_ref, out_ref, lse_ref):
    rows = qn_ref.shape[0]
    base = pl.multiple_of(pl.program_id(0) * rows, rows)
    window = pl.ds(base, rows + DOC_MAX)
    k_rope = kr_ref[window, :]
    low_bound = low_ref[...]
    for h in range(heads):
        at = h * (NOPE + VDIM)
        k_nope = ex_ref[window, at : at + NOPE]
        value = ex_ref[window, at + NOPE : at + NOPE + VDIM]
        scores = masked_scores(
            base,
            low_bound,
            qn_ref[:, h * NOPE : (h + 1) * NOPE],
            qr_ref[:, h * ROPE : (h + 1) * ROPE],
            k_nope,
            k_rope,
            scale,
        )
        top = jnp.max(scores, axis=-1, keepdims=True)
        exps = jnp.exp(scores - top)
        total = jnp.sum(exps, axis=-1, keepdims=True)
        probs = (exps / total).astype(BF)
        out_ref[:, h * VDIM : (h + 1) * VDIM] = jnp.dot(
            probs, value, preferred_element_type=F32
        ).astype(BF)
        lse_ref[:, h : h + 1] = top + jnp.log(total)


def attend(low_bound, q_nope, q_rope, expanded, key_rope, scale):
    queries = q_nope.shape[0]
    heads = q_nope.shape[1] // NOPE
    rows = QUERY_BLOCK

    def whole(array):
        return pl.BlockSpec(array.shape, lambda i: (0, 0))

    def blocked(width):
        return pl.BlockSpec((rows, width), lambda i: (i, 0))

    flops = 2 * heads * queries * (rows + DOC_MAX) * (NOPE + ROPE + VDIM)
    return pl.pallas_call(
        functools.partial(attend_kernel, heads, scale),
        grid=(queries // rows,),
        in_specs=[
            blocked(1),
            blocked(heads * NOPE),
            blocked(heads * ROPE),
            whole(expanded),
            whole(key_rope),
        ],
        out_specs=[blocked(heads * VDIM), blocked(heads)],
        out_shape=[
            jax.ShapeDtypeStruct((queries, heads * VDIM), BF),
            jax.ShapeDtypeStruct((queries, heads), F32),
        ],
        cost_estimate=pl.CostEstimate(
            flops=flops, bytes_accessed=4 * expanded.size, transcendentals=flops // 640
        ),
        compiler_params=pltpu.CompilerParams(vmem_limit_bytes=50 * 1024 * 1024),
        name="attend",
    )(low_bound, q_nope, q_rope, expanded, key_rope)


def attend_back_kernel(
    heads, scale, low_ref, qn_ref, qr_ref, ex_ref, kr_ref, lse_ref, gm_ref,
    dqn_ref, dqr_ref, dex_ref, dkr_ref,
):
    rows = qn_ref.shape[0]
    step = pl.program_id(0)
    base = pl.multiple_of(step * rows, rows)
    window = pl.ds(base, rows + DOC_MAX)

    @pl.when(step == 0)
    def _():
        dex_ref[...] = jnp.zeros_like(dex_ref)
        dkr_ref[...] = jnp.zeros_like(dkr_ref)

    k_rope = kr_ref[window, :]
    low_bound = low_ref[...]
    for h in range(heads):
        at = h * (NOPE + VDIM)
        k_nope = ex_ref[window, at : at + NOPE]
        value = ex_ref[window, at + NOPE : at + NOPE + VDIM]
        q_nope = qn_ref[:, h * NOPE : (h + 1) * NOPE]
        q_rope = qr_ref[:, h * ROPE : (h + 1) * ROPE]
        grad_out = gm_ref[:, h * VDIM : (h + 1) * VDIM]
        scores = masked_scores(base, low_bound, q_nope, q_rope, k_nope, k_rope, scale)
        probs = jnp.exp(scores - lse_ref[:, h : h + 1])
        grad_probs = dot_nt(grad_out, value)
        mean_grad = jnp.sum(probs * grad_probs, axis=-1, keepdims=True)
        grad_scores = (probs * (grad_probs - mean_grad) * scale).astype(BF)
        probs_low = probs.astype(BF)
        dqn_ref[:, h * NOPE : (h + 1) * NOPE] = jnp.dot(
            grad_scores, k_nope, preferred_element_type=F32
        )
        dqr_ref[:, h * ROPE : (h + 1) * ROPE] = jnp.dot(
            grad_scores, k_rope, preferred_element_type=F32
        )
        dex_ref[window, at : at + NOPE] += dot_tn(grad_scores, q_nope)
        dex_ref[window, at + NOPE : at + NOPE + VDIM] += dot_tn(probs_low, grad_out)
        dkr_ref[window, :] += dot_tn(grad_scores, q_rope)


def attend_back(low_bound, q_nope, q_rope, expanded, key_rope, lse, grad_mixed, scale):
    queries = q_nope.shape[0]
    heads = q_nope.shape[1] // NOPE
    rows = QUERY_BLOCK

    def whole(shape):
        return pl.BlockSpec(shape, lambda i: (0, 0))

    def blocked(width):
        return pl.BlockSpec((rows, width), lambda i: (i, 0))

    flops = 2 * heads * queries * (rows + DOC_MAX) * (3 * NOPE + 3 * ROPE + 2 * VDIM)
    return pl.pallas_call(
        functools.partial(attend_back_kernel, heads, scale),
        grid=(queries // rows,),
        in_specs=[
            blocked(1),
            blocked(heads * NOPE),
            blocked(heads * ROPE),
            whole(expanded.shape),
            whole(key_rope.shape),
            blocked(heads),
            blocked(heads * VDIM),
        ],
        out_specs=[
            blocked(heads * NOPE),
            blocked(heads * ROPE),
            whole(expanded.shape),
            whole(key_rope.shape),
        ],
        out_shape=[
            jax.ShapeDtypeStruct(q_nope.shape, F32),
            jax.ShapeDtypeStruct(q_rope.shape, F32),
            jax.ShapeDtypeStruct(expanded.shape, F32),
            jax.ShapeDtypeStruct(key_rope.shape, F32),
        ],
        cost_estimate=pl.CostEstimate(
            flops=flops, bytes_accessed=8 * expanded.size, transcendentals=flops // 1664
        ),
        compiler_params=pltpu.CompilerParams(vmem_limit_bytes=56 * 1024 * 1024),
        name="attend_back",
    )(low_bound, q_nope, q_rope, expanded, key_rope, lse, grad_mixed)


MESH = pl.DeviceIdType.MESH


class Wires:
    def __init__(self, n_groups, n_plane, send, recv):
        self.n_groups, self.n_plane, self.send, self.recv = n_groups, n_plane, send, recv
        self.cores = 2
        self.g, self.p, self.c = lax.axis_index("g"), lax.axis_index("p"), lax.axis_index("c")
        self.j = self.p * self.cores + self.c
        self.used = 0

    def at_plane(self, j):
        return {"g": self.g, "p": j // self.cores, "c": j % self.cores}

    def at_chip(self, p):
        return {"g": self.g, "p": p, "c": self.c}

    def at_group(self, g):
        return {"g": g, "p": self.p, "c": self.c}

    def partner(self):
        return {"g": self.g, "p": self.p, "c": 1 - self.c}

    def plane_peer(self, d):
        return lax.rem(self.j + d, self.n_plane)

    def group_peer(self, d):
        return lax.rem(self.g + d, self.n_groups)

    def start(self, src, dst, device):
        copy = pltpu.make_async_remote_copy(
            src_ref=src,
            dst_ref=dst,
            send_sem=self.send.at[self.used],
            recv_sem=self.recv.at[self.used],
            device_id=device,
            device_id_type=MESH,
        )
        self.used += 1
        copy.start()
        return copy

    def meet(self):
        barrier = pltpu.get_barrier_semaphore()
        for d in range(1, self.n_plane):
            pl.semaphore_signal(
                barrier, inc=1, device_id=self.at_plane(self.plane_peer(d)), device_id_type=MESH
            )
        for d in range(1, self.n_groups):
            pl.semaphore_signal(
                barrier, inc=1, device_id=self.at_group(self.group_peer(d)), device_id_type=MESH
            )
        pl.semaphore_wait(barrier, self.n_plane - 1 + self.n_groups - 1)


def sum_rows(dst, sources):
    rows = dst.shape[0]
    tile = 32 if rows % 32 == 0 else rows

    def step(i, carry):
        at = pl.ds(pl.multiple_of(i * tile, tile), tile)
        total = sources[0][at, :].astype(F32)
        for source in sources[1:]:
            total = total + source[at, :].astype(F32)
        dst[at, :] = total.astype(dst.dtype)
        return carry

    lax.fori_loop(0, rows // tile, step, 0)


def wait_all(copies):
    for copy in copies:
        copy.wait()


def wait_received(copies):
    for copy in copies:
        copy.wait_recv()


def wait_sent(copies):
    for copy in copies:
        copy.wait_send()


def plane_gather(w, src, out):
    chips = w.n_plane // w.cores
    first = [
        w.start(src, out.at[w.j], w.at_chip(lax.rem(w.p + d, chips))) for d in range(1, chips)
    ]
    second = [w.start(src, out.at[w.j], w.partner())]
    out[w.j] = src[...]
    yield
    for d in range(1, chips):
        first[d - 1].wait_recv()
        at = lax.rem(w.p + chips - d, chips) * w.cores + w.c
        second.append(w.start(out.at[at], out.at[at], w.partner()))
    yield
    wait_sent(first)
    wait_all(second)


def shift_gather(w, src, mid, out):
    copy = w.start(src, mid, w.at_group(lax.rem(w.g + 1, w.n_groups)))
    yield
    copy.wait()
    yield from plane_gather(w, mid, out)


def whole_gather(w, src, out):
    first = [
        w.start(src, out.at[w.g, w.j], w.at_group(w.group_peer(d))) for d in range(1, w.n_groups)
    ]
    out[w.g, w.j] = src[...]
    yield
    wait_received(first)
    second = [
        w.start(out.at[:, w.j], out.at[:, w.j], w.at_plane(w.plane_peer(d)))
        for d in range(1, w.n_plane)
    ]
    yield
    wait_sent(first)
    wait_all(second)


def plane_swap_gather(w, src, out):
    first = []
    for d in range(1, w.n_plane):
        to = w.plane_peer(d)
        first.append(w.start(src.at[to], out.at[w.g, w.j], w.at_plane(to)))
    out[w.g, w.j] = src[w.j]
    yield
    wait_received(first)
    second = [
        w.start(out.at[w.g], out.at[w.g], w.at_group(w.group_peer(d)))
        for d in range(1, w.n_groups)
    ]
    yield
    wait_sent(first)
    wait_all(second)


def plane_swap(w, src, out):
    copies = []
    for d in range(1, w.n_plane):
        to = w.plane_peer(d)
        copies.append(w.start(src.at[to], out.at[w.j], w.at_plane(to)))
    out[w.j] = src[w.j]
    yield
    wait_all(copies)


def plane_sum(w, src, out, from_core, pairs, from_chips):
    chips = w.n_plane // w.cores
    first = []
    for d in range(chips):
        p = lax.rem(w.p + d, chips)
        first.append(w.start(src.at[p * w.cores + 1 - w.c], from_core.at[d], w.partner()))
    yield
    second = []
    for d in list(range(1, chips)) + [0]:
        p = lax.rem(w.p + d, chips)
        first[d].wait_recv()
        sum_rows(pairs.at[d], [src.at[p * w.cores + w.c], from_core.at[d]])
        if d:
            second.append(w.start(pairs.at[d], from_chips.at[d - 1], w.at_chip(p)))
    yield
    wait_received(second)
    sum_rows(out, [pairs.at[0]] + [from_chips.at[d] for d in range(chips - 1)])
    wait_sent(first)
    wait_sent(second)


def whole_sum(w, src, out, from_plane, total, parts):
    first = []
    for d in range(1, w.n_plane):
        to = w.plane_peer(d)
        first.append(w.start(src.at[:, to], from_plane.at[d - 1], w.at_plane(to)))
    yield
    wait_received(first)

    def step(i, carry):
        sum_rows(
            total.at[i], [src.at[i, w.j]] + [from_plane.at[d, i] for d in range(w.n_plane - 1)]
        )
        return carry

    lax.fori_loop(0, w.n_groups, step, 0)
    wait_sent(first)
    yield from group_sum(w, total, out, parts)


def whole_swap(w, src, out, mid):
    first = []
    for d in range(1, w.n_plane):
        to = w.plane_peer(d)
        first.append(w.start(src.at[:, to], mid.at[w.j], w.at_plane(to)))
    mid[w.j] = src[:, w.j]
    yield
    wait_received(first)
    second = []
    for d in range(1, w.n_groups):
        to = w.group_peer(d)
        second.append(w.start(mid.at[:, to], out.at[w.g], w.at_group(to)))
    out[w.g] = mid[:, w.g]
    yield
    wait_sent(first)
    wait_all(second)


def group_sum(w, src, out, parts):
    copies = []
    for d in range(1, w.n_groups):
        to = w.group_peer(d)
        copies.append(w.start(src.at[to], parts.at[d - 1], w.at_group(to)))
    yield
    wait_received(copies)
    sum_rows(out, [src.at[w.g]] + [parts.at[d] for d in range(w.n_groups - 1)])
    wait_sent(copies)


def group_sum_swap(w, src, out, total, parts):
    copies = []
    for d in range(1, w.n_groups):
        to = w.group_peer(d)
        copies.append(w.start(src.at[to], parts.at[d - 1], w.at_group(to)))
    yield
    wait_received(copies)

    def step(i, carry):
        sum_rows(total.at[i], [src.at[w.g, i]] + [parts.at[d, i] for d in range(w.n_groups - 1)])
        return carry

    lax.fori_loop(0, w.n_plane, step, 0)
    second = []
    for d in range(1, w.n_plane):
        to = w.plane_peer(d)
        second.append(w.start(total.at[to], out.at[w.j], w.at_plane(to)))
    out[w.j] = total[w.j]
    yield
    wait_sent(copies)
    wait_all(second)


ROUTINES = {
    "plane_gather": plane_gather,
    "shift_gather": shift_gather,
    "whole_gather": whole_gather,
    "plane_swap_gather": plane_swap_gather,
    "plane_swap": plane_swap,
    "plane_sum": plane_sum,
    "group_sum": group_sum,
    "whole_sum": whole_sum,
    "whole_swap": whole_swap,
    "group_sum_swap": group_sum_swap,
}


def exchange_kernel(n_groups, n_plane, kinds, extra, *refs):
    count = len(kinds)
    sources, outs = refs[:count], refs[count : 2 * count]
    scratch = list(refs[2 * count : -2])
    w = Wires(n_groups, n_plane, refs[-2], refs[-1])
    w.meet()
    running = []
    for kind, source, out, number in zip(kinds, sources, outs, extra):
        mine, scratch = scratch[:number], scratch[number:]
        if kind == "shift_gather":
            running.append(shift_gather(w, source, mine[0], out))
        else:
            running.append(ROUTINES[kind](w, source, out, *mine))
    while running:
        still = []
        for routine in running:
            try:
                next(routine)
                still.append(routine)
            except StopIteration:
                pass
        running = still


def exchange(n_groups, n_plane, number, *items):
    kinds = [kind for kind, _ in items]
    arrays = [array for _, array in items]
    shapes, scratch, extra = [], [], []
    chips = n_plane // 2
    for kind, array in items:
        shape, dtype = array.shape, array.dtype
        own = []
        if kind in ("plane_gather", "shift_gather"):
            out = (n_plane,) + shape
            if kind == "shift_gather":
                own = [shape]
        elif kind == "whole_gather":
            out = (n_groups, n_plane) + shape
        elif kind == "plane_swap_gather":
            out = (n_groups,) + shape
        elif kind == "plane_swap":
            out = shape
        elif kind == "plane_sum":
            out = shape[1:]
            own = [(chips,) + out, (chips,) + out, (chips - 1,) + out]
        elif kind == "group_sum":
            out = shape[1:]
            own = [(n_groups - 1,) + out]
        elif kind == "whole_swap":
            out = shape
            own = [(n_plane, n_groups) + shape[2:]]
        elif kind == "whole_sum":
            out = shape[2:]
            own = [(n_plane - 1, n_groups) + out, (n_groups,) + out, (n_groups - 1,) + out]
        elif kind == "group_sum_swap":
            out = shape[1:]
            own = [out, (n_groups - 1,) + out]
        if kind in ("plane_sum", "group_sum", "whole_sum"):
            shapes.append(jax.ShapeDtypeStruct(out, F32))
        else:
            shapes.append(jax.ShapeDtypeStruct(out, dtype))
        scratch += [pltpu.VMEM(s, dtype) for s in own]
        extra.append(len(own))
    copies = 64 + 32 * len(items)
    vmem = pl.BlockSpec(memory_space=pltpu.VMEM)
    return pl.pallas_call(
        functools.partial(exchange_kernel, n_groups, n_plane, kinds, extra),
        out_shape=shapes,
        in_specs=[vmem] * len(items),
        out_specs=[vmem] * len(items),
        scratch_shapes=scratch
        + [pltpu.SemaphoreType.DMA((copies,)), pltpu.SemaphoreType.DMA((copies,))],
        compiler_params=pltpu.CompilerParams(
            collective_id=number,
            has_side_effects=True,
            vmem_limit_bytes=60 * 1024 * 1024,
        ),
        name="exchange_%d" % number,
    )(*arrays)


def gather_all(x):
    return lax.all_gather(x, ALL, axis=0, tiled=True)


class StreamSum:
    def __init__(self, w, steps, stage, from_core, pairs, from_chips, totals, parts, sems, credit):
        self.w, self.steps = w, steps
        self.stage, self.from_core, self.pairs = stage, from_core, pairs
        self.from_chips, self.totals, self.parts = from_chips, totals, parts
        self.core_sems, self.chip_sems, self.chip_recv, self.group_sems = sems
        self.credit = credit

    @staticmethod
    def distances(step):
        half = lax.rem(step, 2)
        return 1 + 2 * half, 2 - 2 * half

    def core_copy(self, step, i):
        slot = lax.rem(step, 2)
        return pltpu.make_async_remote_copy(
            src_ref=self.stage.at[slot, 2 * i + 1 - self.w.c],
            dst_ref=self.from_core.at[slot, i],
            send_sem=self.core_sems.at[0, slot, i],
            recv_sem=self.core_sems.at[1, slot, i],
            device_id=self.w.partner(),
            device_id_type=MESH,
        )

    def chip_copy(self, step, i):
        slot, distance = lax.rem(step, 2), self.distances(step)[i]
        group_at = step // 2
        return pltpu.make_async_remote_copy(
            src_ref=self.pairs.at[slot, i],
            dst_ref=self.from_chips.at[group_at, distance - 1],
            send_sem=self.chip_sems.at[slot, i],
            recv_sem=self.chip_recv.at[group_at, distance - 1],
            device_id=self.w.at_chip(lax.rem(self.w.p + distance, 4)),
            device_id_type=MESH,
        )

    def chip_arrival(self, group_at, distance):
        return pltpu.make_async_remote_copy(
            src_ref=self.pairs.at[0, 0],
            dst_ref=self.from_chips.at[group_at, distance - 1],
            send_sem=self.chip_sems.at[0, 0],
            recv_sem=self.chip_recv.at[group_at, distance - 1],
            device_id=self.w.at_chip(lax.rem(self.w.p + distance, 4)),
            device_id_type=MESH,
        )

    def group_copy(self, group_at):
        return pltpu.make_async_remote_copy(
            src_ref=self.totals.at[group_at],
            dst_ref=self.parts.at[group_at],
            send_sem=self.group_sems.at[0, group_at],
            recv_sem=self.group_sems.at[1, group_at],
            device_id=self.w.at_group(self.w.group_peer(group_at + 1)),
            device_id_type=MESH,
        )

    def open_stage(self, step):
        @pl.when(step >= 2)
        def _():
            for i in range(2):
                self.core_copy(step, i).wait_send()

    def push(self, step):
        @pl.when(step >= 2)
        def _():
            pl.semaphore_wait(self.credit, 1)

        for i in range(2):
            self.core_copy(step, i).start()

    def merge(self, step):
        slot = lax.rem(step, 2)
        for i in range(2):
            self.core_copy(step, i).wait_recv()
            sends = slot == 0 if i else slot >= 0

            @pl.when(sends & (step >= 2))
            def _():
                self.chip_copy(step, i).wait_send()

            sum_rows(
                self.pairs.at[slot, i],
                [self.stage.at[slot, 2 * i + self.w.c], self.from_core.at[slot, i]],
            )

            @pl.when(sends)
            def _():
                self.chip_copy(step, i).start()

        @pl.when(step + 2 < self.steps)
        def _():
            pl.semaphore_signal(
                self.credit, inc=1, device_id=self.w.partner(), device_id_type=MESH
            )

    def plane_total(self, group_at):
        for distance in (1, 2, 3):
            self.chip_arrival(group_at, distance).wait_recv()
        return [self.pairs.at[1, 1]] + [self.from_chips.at[group_at, d] for d in range(3)]

    def advance(self, step):
        @pl.when(step >= 1)
        def _():
            last = step - 1

            @pl.when((lax.rem(last, 2) == 0) & (last >= 2))
            def _():
                group_at = last // 2 - 1
                sum_rows(self.totals.at[group_at], self.plane_total(group_at))
                self.group_copy(group_at).start()

            self.merge(last)

    def finish(self, out):
        steps = self.steps
        self.merge(steps - 1)
        sources = self.plane_total(steps // 2 - 1)
        groups = steps // 2 - 1
        for d in range(groups):
            self.group_copy(d).wait_recv()
            sources.append(self.parts.at[d])
        sum_rows(out, sources)
        for d in range(groups):
            self.group_copy(d).wait_send()
        for i in range(2):
            self.core_copy(steps - 2, i).wait_send()
            self.core_copy(steps - 1, i).wait_send()
            self.chip_copy(steps - 2, i).wait_send()
        self.chip_copy(steps - 1, 0).wait_send()

    @staticmethod
    def scratch(n_groups, rows, width):
        dma = pltpu.SemaphoreType.DMA
        return [
            pltpu.VMEM((2, 4, rows, width), BF),
            pltpu.VMEM((2, 2, rows, width), BF),
            pltpu.VMEM((2, 2, rows, width), BF),
            pltpu.VMEM((n_groups, 3, rows, width), BF),
            pltpu.VMEM((n_groups - 1, rows, width), BF),
            pltpu.VMEM((n_groups - 1, rows, width), BF),
            dma((2, 2, 2)),
            dma((2, 2)),
            dma((n_groups, 3)),
            dma((2, n_groups - 1)),
            pltpu.SemaphoreType.REGULAR,
        ]


def swiglu_both(gate, up, grad):
    sigmoid = 1.0 / (1.0 + jnp.exp(-gate))
    silu = gate * sigmoid
    return silu * up, grad * up * (sigmoid * (1.0 + gate * (1.0 - sigmoid))), grad * silu


def step_chips(w, step):
    group = lax.rem(w.g + 1 + step // 2, w.n_groups)
    return [group * 4 + lax.rem(w.p + d, 4) for d in StreamSum.distances(step)]


def hot_rows(place, rows, core, slot_count):
    mine = place[:, core * rows : (core + 1) * rows]
    return lax.broadcasted_iota(jnp.int32, (slot_count, rows), 0) == mine


def moe_kernel(
    n_groups, experts, first_logit, slot_count,
    h2_hbm, cot_hbm, place_ref, wg_ref, wu_ref, wd_ref, sc_ref, sd_ref,
    sum_ref, rows_ref, gin_ref, act_ref, gg_ref, gu_ref, rw_ref, sact_ref, sgrad_ref, tok_ref,
    h2_buf, cot_buf, load_sems, *comm,
):
    rows = sum_ref.shape[0]
    step, steps = pl.program_id(0), 2 * n_groups
    w = Wires(n_groups, 8, None, None)
    stream = StreamSum(w, steps, *comm[:6], comm[6:10], comm[10])
    expert_id = w.g * 4 + w.p
    half = sc_ref.shape[1] // 2

    def loads(at):
        slot = lax.rem(at, 2)
        for i, chip in enumerate(step_chips(w, at)):
            source = pl.ds(pl.multiple_of(chip * 2 * rows, 2 * rows), 2 * rows)
            target = pl.ds(i * 2 * rows, 2 * rows)
            for k, (hbm, buf) in enumerate(((h2_hbm, h2_buf), (cot_hbm, cot_buf))):
                yield pltpu.make_async_copy(
                    hbm.at[source], buf.at[slot, target], load_sems.at[slot, i, k]
                )

    @pl.when(step == 0)
    def _():
        for copy in loads(step):
            copy.start()
        w.meet()

    @pl.when(step + 1 < steps)
    def _():
        for copy in loads(step + 1):
            copy.start()

    for copy in loads(step):
        copy.wait()
    slot = lax.rem(step, 2)
    h2, cot = h2_buf[slot], cot_buf[slot]
    chips = step_chips(w, step)

    pre = jnp.dot(h2, sc_ref[...], preferred_element_type=F32)
    back = dot_nt(cot, sd_ref[...])
    gate, up = pre[:, :half], pre[:, half:]
    lane = lax.broadcasted_iota(jnp.int32, gate.shape, 1)
    logits = jnp.where((lane >= first_logit) & (lane < first_logit + experts), gate, -1e30)
    exps = jnp.exp(logits - jnp.max(logits, axis=1, keepdims=True))
    chosen = jnp.where(lane == first_logit + expert_id, exps, 0.0)
    weight = jnp.sum(chosen, axis=1, keepdims=True) / jnp.sum(exps, axis=1, keepdims=True)
    act, grad_gate, grad_up = swiglu_both(gate, up, back)
    shared_act = act.astype(BF)
    shared_grad = jnp.concatenate([grad_gate.astype(BF), grad_up.astype(BF)], axis=1)
    for i, chip in enumerate(chips):
        at = pl.ds(pl.multiple_of(chip * 2 * rows, 2 * rows), 2 * rows)
        sact_ref[at, :] = shared_act[i * 2 * rows : (i + 1) * 2 * rows]
        sgrad_ref[at, :] = shared_grad[i * 2 * rows : (i + 1) * 2 * rows]

    hots, weights = [], []
    for q in range(4):
        place = place_ref[pl.ds(chips[q // 2], 1), :]
        hot = hot_rows(place, rows, q % 2, slot_count).astype(F32)
        hots.append(hot)
        tokens = slice(q * rows, (q + 1) * rows)
        slots = slice(q * slot_count, (q + 1) * slot_count)
        low = hot.astype(BF)
        rows_ref[slots, :] = jnp.dot(low, h2[tokens], preferred_element_type=F32).astype(BF)
        gin_ref[slots, :] = jnp.dot(low, cot[tokens], preferred_element_type=F32).astype(BF)
        spread = jnp.broadcast_to(weight[tokens], (rows, 128))
        weights.append(
            jnp.dot(hot, spread, preferred_element_type=F32, precision=lax.Precision.HIGHEST)[:, :1]
        )
    row_weight = jnp.concatenate(weights, axis=0)
    rw_ref[...] = row_weight
    expert_rows = rows_ref[...]
    picked_cot = gin_ref[...]
    back = dot_nt(picked_cot, wd_ref[...])
    gin_ref[...] = (picked_cot.astype(F32) * row_weight).astype(BF)
    gate = jnp.dot(expert_rows, wg_ref[...], preferred_element_type=F32)
    up = jnp.dot(expert_rows, wu_ref[...], preferred_element_type=F32)
    act, grad_gate, grad_up = swiglu_both(gate, up, back * row_weight)
    act_low, grad_gate, grad_up = act.astype(BF), grad_gate.astype(BF), grad_up.astype(BF)
    act_ref[...] = act_low
    gg_ref[...] = grad_gate
    gu_ref[...] = grad_up
    picked = jnp.sum(act_low.astype(F32) * back, axis=1, keepdims=True)
    grad_rows = (dot_nt(grad_gate, wg_ref[...]) + dot_nt(grad_up, wu_ref[...])).astype(BF)
    stream.open_stage(step)
    for q in range(4):
        tokens = slice(q * rows, (q + 1) * rows)
        slots = slice(q * slot_count, (q + 1) * slot_count)
        tok_ref[pl.ds(chips[q // 2] * 2 + q % 2, 1), :] = jnp.sum(
            hots[q] * picked[slots], axis=0, keepdims=True
        )
        total = dot_tn(hots[q].astype(BF), grad_rows[slots]) + dot_nt(
            shared_grad[tokens], sc_ref[...]
        )
        stream.stage[slot, q] = total.astype(BF)
    stream.push(step)
    stream.advance(step)

    @pl.when(step == steps - 1)
    def _():
        stream.finish(sum_ref)


def out_kernel(
    n_groups, slot_count, act_ref, rw_ref, place_ref, sact_ref, wd_ref, sd_ref, sum_ref, *comm
):
    rows = sum_ref.shape[0]
    step, steps = pl.program_id(0), 2 * n_groups
    w = Wires(n_groups, 8, None, None)
    stream = StreamSum(w, steps, *comm[:6], comm[6:10], comm[10])

    @pl.when(step == 0)
    def _():
        w.meet()

    slot = lax.rem(step, 2)
    chips = step_chips(w, step)
    out_rows = jnp.dot(act_ref[...], wd_ref[...], preferred_element_type=F32) * rw_ref[...]
    out_rows = out_rows.astype(BF)
    stream.open_stage(step)
    for q in range(4):
        chip = chips[q // 2]
        place = place_ref[pl.ds(chip, 1), :]
        low = hot_rows(place, rows, q % 2, slot_count).astype(F32).astype(BF)
        slots = slice(q * slot_count, (q + 1) * slot_count)
        shared = sact_ref[pl.ds(pl.multiple_of((chip * 2 + q % 2) * rows, rows), rows), :]
        total = dot_tn(low, out_rows[slots]) + jnp.dot(
            shared, sd_ref[...], preferred_element_type=F32
        )
        stream.stage[slot, q] = total.astype(BF)
    stream.push(step)
    stream.advance(step)

    @pl.when(step == steps - 1)
    def _():
        stream.finish(sum_ref)


def experts_sums(
    n_groups, rows, h2, cot, place, slot_count, expert_w, shared_w, router_weight, first_id
):
    w_gate, w_up, w_down = expert_w
    s_both, s_down = shared_w
    tokens, width = h2.shape
    hidden, hidden_s = w_down.shape[0], s_down.shape[0]
    experts = router_weight.shape[1]
    steps = 2 * n_groups
    devices = tokens // rows
    step_slots = slot_count * 4
    all_slots = step_slots * steps
    half = 128
    s_cat = jnp.concatenate(
        [
            s_both[:, :hidden_s],
            router_weight,
            jnp.zeros((width, half - hidden_s - experts), BF),
            s_both[:, hidden_s:],
            jnp.zeros((width, half - hidden_s), BF),
        ],
        axis=1,
    )
    s_tall = jnp.pad(s_down, ((0, half - hidden_s), (0, 0)))

    def whole(array):
        return pl.BlockSpec(array.shape, lambda i: (0, 0), pipeline_mode=pl.Buffered(1))

    def blocked(rows, cols):
        return pl.BlockSpec((rows, cols), lambda i: (i, 0))

    shape = jax.ShapeDtypeStruct
    flops = 2 * all_slots * width * hidden * 5 + 2 * tokens * width * (4 * half + 3 * slot_count)
    shapes = [
        shape((rows, width), F32),
        shape((all_slots, width), BF),
        shape((all_slots, width), BF),
        shape((all_slots, hidden), BF),
        shape((all_slots, hidden), BF),
        shape((all_slots, hidden), BF),
        shape((all_slots, 1), F32),
        shape((tokens, half), BF),
        shape((tokens, 2 * half), BF),
        shape((devices, rows), F32),
    ]
    specs = [
        blocked(step_slots, s.shape[1]) if s.shape[0] == all_slots else whole(s) for s in shapes
    ]
    hbm = pl.BlockSpec(memory_space=pl.ANY)
    grad_h2, rows_in, grad_in, act, grad_gate, grad_up, row_weight, s_act, s_grad, token_grad = (
        pl.pallas_call(
            functools.partial(moe_kernel, n_groups, experts, hidden_s, slot_count),
            grid=(steps,),
            in_specs=[
                hbm,
                hbm,
                whole(place),
                whole(w_gate),
                whole(w_up),
                whole(w_down),
                whole(s_cat),
                whole(s_tall),
            ],
            out_specs=specs,
            out_shape=shapes,
            scratch_shapes=[
                pltpu.VMEM((2, 4 * rows, width), BF),
                pltpu.VMEM((2, 4 * rows, width), BF),
                pltpu.SemaphoreType.DMA((2, 2, 2)),
            ]
            + StreamSum.scratch(n_groups, rows, width),
            cost_estimate=pl.CostEstimate(
                flops=flops, bytes_accessed=12 * tokens * width, transcendentals=tokens * 1024
            ),
            compiler_params=pltpu.CompilerParams(
                collective_id=first_id,
                has_side_effects=True,
                vmem_limit_bytes=67043328,
            ),
            name="experts",
        )(h2, cot, place, w_gate, w_up, w_down, s_cat, s_tall)
    )
    out = pl.pallas_call(
        functools.partial(out_kernel, n_groups, slot_count),
        grid=(steps,),
        in_specs=[
            blocked(step_slots, hidden),
            blocked(step_slots, 1),
            whole(place),
            whole(s_act),
            whole(w_down),
            whole(s_tall),
        ],
        out_specs=whole(grad_h2),
        out_shape=shape((rows, width), F32),
        scratch_shapes=StreamSum.scratch(n_groups, rows, width),
        cost_estimate=pl.CostEstimate(
            flops=2 * width * (all_slots * hidden + tokens * (half + slot_count)),
            bytes_accessed=4 * tokens * width,
            transcendentals=0,
        ),
        compiler_params=pltpu.CompilerParams(
            collective_id=first_id + 1,
            has_side_effects=True,
            vmem_limit_bytes=56 * 1024 * 1024,
        ),
        name="expert_out",
    )(act, row_weight, place, s_act, w_down, s_tall)
    g_both = dot_tn(h2, s_grad)
    g_both = jnp.concatenate([g_both[:, :hidden_s], g_both[:, half : half + hidden_s]], axis=1)
    grads = (
        dot_tn(rows_in, grad_gate),
        dot_tn(rows_in, grad_up),
        dot_tn(act, grad_in),
        g_both,
        dot_tn(s_act, cot)[:hidden_s],
    )
    return out, grad_h2, token_grad, grads


def body(
    n_groups, n_plane, layer_input, attn_gain, w_query, w_latent, kv_gain, w_expand, w_output,
    ffn_gain, w_router, shared_gate, shared_up, shared_down, expert_gate, expert_up,
    expert_down, routes, segments, cotangent,
):
    tok, width = layer_input.shape
    devices = n_groups * n_plane
    experts = w_router.shape[1]
    local_heads = HEADS // n_plane
    scale = (NOPE + ROPE) ** (-0.5)
    group = lax.axis_index("g")
    place_in = lax.axis_index(PLANE)
    me = lax.axis_index(ALL)
    expert_id = lax.axis_index(("g", "p"))
    plane_tok = n_plane * tok
    plane_start = group * plane_tok

    rows_w = w_router.shape[0]
    kv_n = kv_gain.shape[0]
    small = jnp.concatenate(
        [
            attn_gain,
            ffn_gain,
            kv_gain,
            w_router.reshape(-1),
            routes.reshape(-1).astype(BF),
            segments.astype(BF),
        ]
    )
    small = jnp.pad(small, (0, -small.shape[0] % 4096)).reshape(-1, 128)
    head_cols = local_heads * (NOPE + ROPE)
    kv_cols = local_heads * (NOPE + VDIM)
    fold = kv_n * kv_cols // rows_w
    pair = jnp.concatenate(
        [
            w_query.reshape(rows_w, n_plane, head_cols).transpose(1, 0, 2),
            w_expand.reshape(kv_n, n_plane, kv_cols // fold, fold)
            .transpose(1, 0, 2, 3)
            .reshape(n_plane, rows_w, fold),
        ],
        axis=2,
    )
    swap = functools.partial(exchange, n_groups, n_plane)
    x_plane, small, latent_weight, pair = swap(
        0,
        ("plane_gather", layer_input),
        ("whole_gather", small),
        ("whole_gather", w_latent),
        ("plane_swap_gather", pair),
    )
    x_plane = x_plane.reshape(plane_tok, width).astype(F32)
    latent_weight = latent_weight.reshape(width, RANK + ROPE)
    pair = pair.reshape(width, head_cols + fold)
    small = small.reshape(devices, -1)
    cuts = [rows_w, 2 * rows_w, 2 * rows_w + kv_n, 2 * rows_w + kv_n + rows_w * experts]
    cuts = cuts + [cuts[-1] + tok * TOP, cuts[-1] + tok * TOP + tok]
    gain_one = small[:, : cuts[0]].reshape(-1).astype(F32)
    gain_two = small[:, cuts[0] : cuts[1]].reshape(-1).astype(F32)
    gain_kv = small[:, cuts[1] : cuts[2]].reshape(-1).astype(F32)
    router_weight = small[:, cuts[2] : cuts[3]].reshape(width, experts)
    routes_all = small[:, cuts[3] : cuts[4]].astype(jnp.int32).reshape(devices, tok, TOP)
    segments_all = small[:, cuts[4] : cuts[5]].astype(jnp.int32).reshape(-1)

    query_weight = pair[:, :head_cols].reshape(width, local_heads, NOPE + ROPE)
    wq_nope = query_weight[:, :, :NOPE].reshape(width, local_heads * NOPE)
    wq_rope = query_weight[:, :, NOPE:].reshape(width, local_heads * ROPE)
    expand_weight = pair[:, head_cols:].reshape(RANK, kv_cols)
    output_weight = gather_all(w_output)

    shared_n = shared_down.shape[0]
    s_both = jnp.concatenate(
        [
            shared_gate.reshape(rows_w, devices, shared_n),
            shared_up.reshape(rows_w, devices, shared_n),
        ],
        axis=2,
    )
    s_both = lax.all_to_all(s_both, ALL, split_axis=1, concat_axis=0).reshape(width, 2 * shared_n)

    hidden = rms_norm(x_plane, gain_one).astype(BF)
    rope_half = ROPE // 2
    positions = plane_start + jnp.arange(plane_tok, dtype=jnp.int32)
    frequency = 10000.0 ** (-jnp.arange(rope_half, dtype=F32) / rope_half)
    angles = positions.astype(F32)[:, None] * frequency[None, :]
    cosine = jnp.cos(angles)
    sine_part = jnp.sin(angles)
    cos_h, sin_h = cosine[:, None, :], sine_part[:, None, :]
    latent = matmul(hidden, latent_weight)
    compressed_own = rms_norm(latent[:, :RANK], gain_kv).astype(BF)
    key_rope_own = rotate(latent[:, RANK:], cosine, sine_part).astype(BF)

    def own_rows(table):
        return lax.dynamic_slice_in_dim(table, place_in * tok, tok, 0)

    down_pairs = [(i + 1, i) for i in range(n_groups - 1)]
    piece = own_rows(jnp.concatenate([compressed_own, key_rope_own], axis=1))
    before = swap(1, ("shift_gather", piece))[0].reshape(plane_tok, RANK + ROPE)
    compressed = jnp.concatenate([before[:, :RANK], compressed_own], axis=0)
    key_rope = jnp.concatenate([before[:, RANK:], key_rope_own], axis=0)
    q_nope = matmul(hidden, wq_nope).astype(BF)
    q_rope = rotate(
        matmul(hidden, wq_rope).reshape(plane_tok, local_heads, ROPE), cos_h, sin_h
    ).reshape(plane_tok, local_heads * ROPE).astype(BF)
    expanded = matmul(compressed, expand_weight).astype(BF)
    plane_segments = lax.dynamic_slice_in_dim(segments_all, plane_start, plane_tok, 0)
    doc_start = jnp.sum(
        (segments_all[None, :] < plane_segments[:, None]).astype(jnp.int32), axis=1, keepdims=True
    )
    low_bound = doc_start - plane_start + DOC_MAX
    mixed_heads, lse = attend(low_bound, q_nope, q_rope, expanded, key_rope, scale)
    mixed = swap(2, ("plane_swap", mixed_heads.reshape(n_plane, tok, local_heads * VDIM)))[0]
    mixed = mixed.transpose(1, 0, 2).reshape(tok, width)

    input_float = layer_input.astype(F32)
    residual_one = input_float + matmul(mixed, output_weight)
    h_two_f, norm_two_back = jax.vjp(rms_norm, residual_one, gain_two)
    h_two = h_two_f.astype(BF)
    router_probs = softmax_rows(matmul(h_two, router_weight))

    expert_w = (expert_gate[0], expert_up[0], expert_down[0])
    shared_w = (s_both, shared_down)
    slot_limit = 2 * tok * TOP // experts

    def on_rows(h2, cot_gathered, routes_here):
        rows = h2.shape[0]
        h2_all = gather_all(h2)
        slot_count = min(slot_limit, rows)
        member = jnp.any(routes_here == expert_id, axis=2)
        member_int = member.astype(jnp.int32)
        rank = jnp.cumsum(member_int, axis=1) - member_int
        place = jnp.where(member, rank, -1).reshape(devices // 2, 2 * rows)
        out, grad_h2, token_grad, grads = experts_sums(
            n_groups,
            rows,
            h2_all,
            cot_gathered,
            place,
            slot_count,
            expert_w,
            shared_w,
            router_weight,
            8,
        )
        picked = lax.all_to_all(token_grad, ALL, split_axis=0, concat_axis=0, tiled=True)
        picked = jnp.sum(picked.reshape(experts, devices // experts, rows), axis=1).T
        return out, grad_h2, picked, grads

    parts = max(1, devices * tok // 4096)
    if parts == 1:
        cot_all = gather_all(cotangent)
        out_own, grad_h2_own, grad_router_probs, grads = on_rows(
            h_two, cot_all, routes_all
        )
    else:
        rows = tok // parts

        def step(total, inputs):
            h2, cot, routes_here = inputs
            cot_part = gather_all(cot)
            out, grad_h2, picked, grads = on_rows(h2, cot_part, routes_here)
            total = tuple(a + b for a, b in zip(total, grads))
            return total, (out, grad_h2, picked)

        shapes = expert_w + shared_w
        grads, (out_own, grad_h2_own, grad_router_probs) = lax.scan(
            step,
            tuple(jnp.zeros(s.shape, F32) for s in shapes),
            (
                h_two.reshape(parts, rows, width),
                cotangent.reshape(parts, rows, width),
                routes_all.reshape(devices, parts, rows, TOP).transpose(1, 0, 2, 3),
            ),
        )
        out_own = out_own.reshape(tok, width)
        grad_h2_own = grad_h2_own.reshape(tok, width)
        grad_router_probs = grad_router_probs.reshape(tok, experts)
    g_gate, g_up, g_down, g_both, g_sdown = grads
    grad_logits = router_probs * (
        grad_router_probs - jnp.sum(router_probs * grad_router_probs, axis=1, keepdims=True)
    )
    grad_logits = grad_logits.astype(BF)
    grad_router = dot_tn(h_two, grad_logits)
    grad_h_two = grad_h2_own + dot_nt(grad_logits, router_weight)
    output = residual_one + out_own

    grad_x_one, grad_gain_two = norm_two_back(grad_h_two)
    grad_x_one = grad_x_one + cotangent.astype(F32)
    grad_attn_out = grad_x_one.astype(BF)
    plane_grad = swap(3, ("plane_gather", grad_attn_out))[0].reshape(plane_tok, width)
    head_rows = local_heads * VDIM
    own_output = lax.dynamic_slice_in_dim(output_weight, place_in * head_rows, head_rows, 0)
    grad_mixed = dot_nt(plane_grad, own_output).astype(BF)
    dqn, dqr, dex, dkr = attend_back(
        low_bound, q_nope, q_rope, expanded, key_rope, lse, grad_mixed, scale
    )

    g_output = dot_tn(mixed_heads, plane_grad).astype(BF).reshape(n_groups, rows_w, width)

    grad_expanded = dex.astype(BF)
    grad_expand = dot_tn(compressed, grad_expanded)
    grad_comp = dot_nt(grad_expanded, expand_weight)
    key_grads = jnp.concatenate([grad_comp, dkr], axis=1).astype(BF)
    key_grads = (
        key_grads.reshape(2, n_plane, tok, RANK + ROPE)
        .transpose(1, 0, 2, 3)
        .reshape(n_plane, 2 * tok, RANK + ROPE)
    )

    gq_nope = dqn.astype(BF)
    gq_rope = (
        unrotate(dqr.reshape(plane_tok, local_heads, ROPE), cos_h, sin_h)
        .reshape(plane_tok, local_heads * ROPE)
        .astype(BF)
    )
    grad_hidden = (dot_nt(gq_nope, wq_nope) + dot_nt(gq_rope, wq_rope)).astype(BF)
    key_grads, grad_hidden, grad_output_weight, g_shared = swap(
        4,
        ("plane_sum", key_grads),
        ("plane_sum", grad_hidden.reshape(n_plane, tok, width)),
        ("group_sum", g_output),
        ("whole_swap", g_both.astype(BF).reshape(n_groups, n_plane, rows_w, 2 * shared_n)),
    )
    row_pairs = [
        (g * n_plane + j, n_groups * j + g) for g in range(n_groups) for j in range(n_plane)
    ]
    grad_output_weight = lax.ppermute(grad_output_weight, ALL, row_pairs)
    later = lax.ppermute(key_grads[:tok].astype(BF), "g", down_pairs).astype(F32)
    key_grad = key_grads[tok:] + later
    latent_own = own_rows(latent)
    kv_norm_back = jax.vjp(rms_norm, latent_own[:, :RANK], gain_kv)[1]
    grad_comp_in, grad_gain_kv = kv_norm_back(key_grad[:, :RANK])
    grad_rope_in = unrotate(key_grad[:, RANK:], own_rows(cosine), own_rows(sine_part))
    grad_latent = jnp.concatenate([grad_comp_in, grad_rope_in], axis=1).astype(BF)

    g_query = jnp.concatenate(
        [
            dot_tn(hidden, gq_nope).reshape(width, local_heads, NOPE),
            dot_tn(hidden, gq_rope).reshape(width, local_heads, ROPE),
        ],
        axis=2,
    ).reshape(width, local_heads * (NOPE + ROPE))

    g_query = g_query.astype(BF).reshape(n_groups, n_plane, rows_w, head_cols)
    g_expand = grad_expand.astype(BF).reshape(n_groups, n_plane, kv_n, kv_cols)
    g_query, g_expand, latent_grads = swap(
        5,
        ("group_sum_swap", g_query),
        ("group_sum_swap", g_expand),
        ("plane_gather", grad_latent),
    )
    grad_query_weight = g_query.transpose(1, 0, 2).reshape(rows_w, -1).astype(F32)
    grad_expand_weight = g_expand.transpose(1, 0, 2).reshape(kv_n, -1).astype(F32)

    latent_grads = latent_grads.reshape(plane_tok, RANK + ROPE)
    g_latent = dot_tn(hidden, latent_grads).astype(BF)
    g_latent = g_latent.reshape(n_groups, n_plane, rows_w, RANK + ROPE)
    g_latent = lax.dynamic_index_in_dim(g_latent, place_in, 1, keepdims=False)
    grad_hidden = grad_hidden + dot_nt(grad_latent, latent_weight)
    norm_one_back = jax.vjp(rms_norm, input_float, gain_one)[1]
    grad_x_norm, grad_gain_one = norm_one_back(grad_hidden)
    grad_input = grad_x_one + grad_x_norm

    small_grads = jnp.concatenate(
        [
            p.reshape(devices, -1)
            for p in (grad_gain_one, grad_gain_two, grad_gain_kv, grad_router)
        ],
        axis=1,
    )
    small_grads = jnp.pad(small_grads, ((0, 0), (0, -small_grads.shape[1] % 1024)))
    grad_latent_weight, small_grads = swap(
        6,
        ("group_sum", g_latent),
        ("whole_sum", small_grads.reshape(n_groups, n_plane, -1, 128)),
    )
    small_grads = small_grads.reshape(-1)
    g_shared = g_shared.transpose(2, 0, 1, 3).reshape(rows_w, devices, 2 * shared_n).astype(F32)
    grad_shared_gate = g_shared[:, :, :shared_n].reshape(rows_w, devices * shared_n)
    grad_shared_up = g_shared[:, :, shared_n:].reshape(rows_w, devices * shared_n)
    return (
        output,
        grad_input,
        small_grads[: cuts[0]],
        grad_query_weight,
        grad_latent_weight,
        small_grads[cuts[1] : cuts[2]],
        grad_expand_weight,
        grad_output_weight,
        small_grads[cuts[0] : cuts[1]],
        small_grads[cuts[2] : cuts[3]].reshape(rows_w, experts),
        grad_shared_gate,
        grad_shared_up,
        g_sdown,
        g_gate[None],
        g_up[None],
        g_down[None],
    )


def solution(mesh):
    n_expert, n_shard = mesh.shape["expert"], mesh.shape["wshard"]
    devices = n_expert * n_shard

    def program(*args):
        tok = args[0].shape[0] // devices
        n_plane = DOC_MAX // tok
        n_groups = devices // n_plane
        inner = Mesh(mesh.devices.reshape(n_groups, n_plane // n_shard, n_shard), ALL)
        rows, vector = P(ALL, None), P(ALL)
        wide, tall = P(("g", "p"), None, "c"), P(("g", "p"), "c", None)
        step = jax.shard_map(
            functools.partial(body, n_groups, n_plane),
            mesh=inner,
            in_specs=(
                rows, vector, rows, rows, vector, rows, rows, vector, rows, rows, rows, rows,
                wide, wide, tall, rows, vector, rows,
            ),
            out_specs=(
                rows, rows, vector, rows, rows, vector, rows, rows, vector, rows, rows, rows,
                rows, wide, wide, tall,
            ),
            check_vma=False,
        )
        return step(*args)

    return program
```

```python
import functools

import jax
import jax.numpy as jnp
from jax import lax
from jax.experimental import pallas as pl
from jax.experimental.pallas import tpu as pltpu
from jax.sharding import Mesh, PartitionSpec as P

HEADS = 16
NOPE = 128
ROPE = 64
VDIM = 128
RANK = 512
TOP = 6
DOC_MAX = 1024
QUERY_BLOCK = 256

BF = jnp.bfloat16
F32 = jnp.float32
ALL = ("g", "p", "c")
PLANE = ("p", "c")

epsilon = 1e-06


def rms_norm(vector, scaling):
    return vector * lax.rsqrt(jnp.mean(vector * vector, axis=-1, keepdims=True) + epsilon) * scaling


def rotate(vector, cosine, sine_part):
    half_width = vector.shape[-1] // 2
    front_half = vector[..., :half_width]
    back_half = vector[..., half_width:]
    return jnp.concatenate(
        [front_half * cosine - back_half * sine_part, back_half * cosine + front_half * sine_part],
        axis=-1,
    )


def unrotate(vector, cosine, sine_part):
    return rotate(vector, cosine, -sine_part)


def matmul(left, right):
    return jnp.dot(left, right, preferred_element_type=F32)


def dot_nt(left, right):
    return lax.dot_general(left, right, (((1,), (1,)), ((), ())), preferred_element_type=F32)


def dot_tn(left, right):
    return lax.dot_general(left, right, (((0,), (0,)), ((), ())), preferred_element_type=F32)


def swiglu(gate_pre, up_pre):
    return jax.nn.silu(gate_pre) * up_pre


def softmax_rows(scores):
    row_top = jnp.max(scores, axis=-1, keepdims=True)
    exp_scores = jnp.exp(scores - row_top)
    return exp_scores / jnp.sum(exp_scores, axis=-1, keepdims=True)


def masked_scores(base, low_bound, q_nope, q_rope, k_nope, k_rope, scale):
    rows, span = q_nope.shape[0], k_nope.shape[0]
    key_at = lax.broadcasted_iota(jnp.int32, (rows, span), 1) + base
    query_at = lax.broadcasted_iota(jnp.int32, (rows, span), 0) + (base + DOC_MAX)
    allowed = (key_at >= low_bound) & (key_at <= query_at)
    scores = (dot_nt(q_nope, k_nope) + dot_nt(q_rope, k_rope)) * scale
    return jnp.where(allowed, scores, -1e30)


def attend_kernel(heads, scale, low_ref, qn_ref, qr_ref, ex_ref, kr_ref, out_ref, lse_ref):
    rows = qn_ref.shape[0]
    base = pl.multiple_of(pl.program_id(0) * rows, rows)
    window = pl.ds(base, rows + DOC_MAX)
    k_rope = kr_ref[window, :]
    low_bound = low_ref[...]
    for h in range(heads):
        at = h * (NOPE + VDIM)
        k_nope = ex_ref[window, at : at + NOPE]
        value = ex_ref[window, at + NOPE : at + NOPE + VDIM]
        scores = masked_scores(
            base,
            low_bound,
            qn_ref[:, h * NOPE : (h + 1) * NOPE],
            qr_ref[:, h * ROPE : (h + 1) * ROPE],
            k_nope,
            k_rope,
            scale,
        )
        top = jnp.max(scores, axis=-1, keepdims=True)
        exps = jnp.exp(scores - top)
        total = jnp.sum(exps, axis=-1, keepdims=True)
        probs = (exps / total).astype(BF)
        out_ref[:, h * VDIM : (h + 1) * VDIM] = jnp.dot(
            probs, value, preferred_element_type=F32
        ).astype(BF)
        lse_ref[:, h : h + 1] = top + jnp.log(total)


def attend(low_bound, q_nope, q_rope, expanded, key_rope, scale):
    queries = q_nope.shape[0]
    heads = q_nope.shape[1] // NOPE
    rows = QUERY_BLOCK

    def whole(array):
        return pl.BlockSpec(array.shape, lambda i: (0, 0))

    def blocked(width):
        return pl.BlockSpec((rows, width), lambda i: (i, 0))

    flops = 2 * heads * queries * (rows + DOC_MAX) * (NOPE + ROPE + VDIM)
    return pl.pallas_call(
        functools.partial(attend_kernel, heads, scale),
        grid=(queries // rows,),
        in_specs=[
            blocked(1),
            blocked(heads * NOPE),
            blocked(heads * ROPE),
            whole(expanded),
            whole(key_rope),
        ],
        out_specs=[blocked(heads * VDIM), blocked(heads)],
        out_shape=[
            jax.ShapeDtypeStruct((queries, heads * VDIM), BF),
            jax.ShapeDtypeStruct((queries, heads), F32),
        ],
        cost_estimate=pl.CostEstimate(
            flops=flops, bytes_accessed=4 * expanded.size, transcendentals=flops // 640
        ),
        compiler_params=pltpu.CompilerParams(vmem_limit_bytes=50 * 1024 * 1024),
        name="attend",
    )(low_bound, q_nope, q_rope, expanded, key_rope)


def attend_back_kernel(
    heads, scale, low_ref, qn_ref, qr_ref, ex_ref, kr_ref, lse_ref, gm_ref,
    dqn_ref, dqr_ref, dex_ref, dkr_ref,
):
    rows = qn_ref.shape[0]
    step = pl.program_id(0)
    base = pl.multiple_of(step * rows, rows)
    window = pl.ds(base, rows + DOC_MAX)

    @pl.when(step == 0)
    def _():
        dex_ref[...] = jnp.zeros_like(dex_ref)
        dkr_ref[...] = jnp.zeros_like(dkr_ref)

    k_rope = kr_ref[window, :]
    low_bound = low_ref[...]
    for h in range(heads):
        at = h * (NOPE + VDIM)
        k_nope = ex_ref[window, at : at + NOPE]
        value = ex_ref[window, at + NOPE : at + NOPE + VDIM]
        q_nope = qn_ref[:, h * NOPE : (h + 1) * NOPE]
        q_rope = qr_ref[:, h * ROPE : (h + 1) * ROPE]
        grad_out = gm_ref[:, h * VDIM : (h + 1) * VDIM]
        scores = masked_scores(base, low_bound, q_nope, q_rope, k_nope, k_rope, scale)
        probs = jnp.exp(scores - lse_ref[:, h : h + 1])
        grad_probs = dot_nt(grad_out, value)
        mean_grad = jnp.sum(probs * grad_probs, axis=-1, keepdims=True)
        grad_scores = (probs * (grad_probs - mean_grad) * scale).astype(BF)
        probs_low = probs.astype(BF)
        dqn_ref[:, h * NOPE : (h + 1) * NOPE] = jnp.dot(
            grad_scores, k_nope, preferred_element_type=F32
        )
        dqr_ref[:, h * ROPE : (h + 1) * ROPE] = jnp.dot(
            grad_scores, k_rope, preferred_element_type=F32
        )
        dex_ref[window, at : at + NOPE] += dot_tn(grad_scores, q_nope)
        dex_ref[window, at + NOPE : at + NOPE + VDIM] += dot_tn(probs_low, grad_out)
        dkr_ref[window, :] += dot_tn(grad_scores, q_rope)


def attend_back(low_bound, q_nope, q_rope, expanded, key_rope, lse, grad_mixed, scale):
    queries = q_nope.shape[0]
    heads = q_nope.shape[1] // NOPE
    rows = QUERY_BLOCK

    def whole(shape):
        return pl.BlockSpec(shape, lambda i: (0, 0))

    def blocked(width):
        return pl.BlockSpec((rows, width), lambda i: (i, 0))

    flops = 2 * heads * queries * (rows + DOC_MAX) * (3 * NOPE + 3 * ROPE + 2 * VDIM)
    return pl.pallas_call(
        functools.partial(attend_back_kernel, heads, scale),
        grid=(queries // rows,),
        in_specs=[
            blocked(1),
            blocked(heads * NOPE),
            blocked(heads * ROPE),
            whole(expanded.shape),
            whole(key_rope.shape),
            blocked(heads),
            blocked(heads * VDIM),
        ],
        out_specs=[
            blocked(heads * NOPE),
            blocked(heads * ROPE),
            whole(expanded.shape),
            whole(key_rope.shape),
        ],
        out_shape=[
            jax.ShapeDtypeStruct(q_nope.shape, F32),
            jax.ShapeDtypeStruct(q_rope.shape, F32),
            jax.ShapeDtypeStruct(expanded.shape, F32),
            jax.ShapeDtypeStruct(key_rope.shape, F32),
        ],
        cost_estimate=pl.CostEstimate(
            flops=flops, bytes_accessed=8 * expanded.size, transcendentals=flops // 1664
        ),
        compiler_params=pltpu.CompilerParams(vmem_limit_bytes=56 * 1024 * 1024),
        name="attend_back",
    )(low_bound, q_nope, q_rope, expanded, key_rope, lse, grad_mixed)


MESH = pl.DeviceIdType.MESH


class Wires:
    def __init__(self, n_groups, n_plane, send, recv):
        self.n_groups, self.n_plane, self.send, self.recv = n_groups, n_plane, send, recv
        self.cores = 2
        self.g, self.p, self.c = lax.axis_index("g"), lax.axis_index("p"), lax.axis_index("c")
        self.j = self.p * self.cores + self.c
        self.used = 0

    def at_plane(self, j):
        return {"g": self.g, "p": j // self.cores, "c": j % self.cores}

    def at_chip(self, p):
        return {"g": self.g, "p": p, "c": self.c}

    def at_group(self, g):
        return {"g": g, "p": self.p, "c": self.c}

    def partner(self):
        return {"g": self.g, "p": self.p, "c": 1 - self.c}

    def plane_peer(self, d):
        return lax.rem(self.j + d, self.n_plane)

    def group_peer(self, d):
        return lax.rem(self.g + d, self.n_groups)

    def start(self, src, dst, device):
        copy = pltpu.make_async_remote_copy(
            src_ref=src,
            dst_ref=dst,
            send_sem=self.send.at[self.used],
            recv_sem=self.recv.at[self.used],
            device_id=device,
            device_id_type=MESH,
        )
        self.used += 1
        copy.start()
        return copy

    def at_device(self, index):
        return {"g": index // self.n_plane, **self.on_plane(lax.rem(index, self.n_plane))}

    def on_plane(self, j):
        return {"p": j // self.cores, "c": j % self.cores}

    def meet(self, heads=False):
        barrier = pltpu.get_barrier_semaphore()
        waits = self.n_plane - 1 + self.n_groups - 1
        if heads:
            mine = self.head_owner() == self.j
            part = lax.rem(self.g * self.n_plane + self.j, self.n_groups)
            for r in range(self.n_groups):

                @pl.when(jnp.logical_not(mine) | (part != r))
                def _():
                    source = self.at_device(self.n_groups * self.j + r)
                    pl.semaphore_signal(barrier, inc=1, device_id=source, device_id_type=MESH)

            waits = waits + jnp.where(mine, self.n_groups - 1, self.n_groups)
        for d in range(1, self.n_plane):
            pl.semaphore_signal(
                barrier, inc=1, device_id=self.at_plane(self.plane_peer(d)), device_id_type=MESH
            )
        for d in range(1, self.n_groups):
            pl.semaphore_signal(
                barrier, inc=1, device_id=self.at_group(self.group_peer(d)), device_id_type=MESH
            )
        pl.semaphore_wait(barrier, waits)

    def head_owner(self):
        return (self.g * self.n_plane + self.j) // self.n_groups


def sum_rows(dst, sources):
    rows = dst.shape[0]
    tile = 32 if rows % 32 == 0 else rows

    def step(i, carry):
        at = pl.ds(pl.multiple_of(i * tile, tile), tile)
        total = sources[0][at, :].astype(F32)
        for source in sources[1:]:
            total = total + source[at, :].astype(F32)
        dst[at, :] = total.astype(dst.dtype)
        return carry

    lax.fori_loop(0, rows // tile, step, 0)


def wait_all(copies):
    for copy in copies:
        copy.wait()


def wait_received(copies):
    for copy in copies:
        copy.wait_recv()


def wait_sent(copies):
    for copy in copies:
        copy.wait_send()


def plane_gather(w, src, out):
    chips = w.n_plane // w.cores
    first = [
        w.start(src, out.at[w.j], w.at_chip(lax.rem(w.p + d, chips))) for d in range(1, chips)
    ]
    second = [w.start(src, out.at[w.j], w.partner())]
    out[w.j] = src[...]
    yield
    for d in range(1, chips):
        first[d - 1].wait_recv()
        at = lax.rem(w.p + chips - d, chips) * w.cores + w.c
        second.append(w.start(out.at[at], out.at[at], w.partner()))
    yield
    wait_sent(first)
    wait_all(second)


def shift_gather(w, src, mid, out):
    copy = w.start(src, mid, w.at_group(lax.rem(w.g + 1, w.n_groups)))
    yield
    copy.wait()
    yield from plane_gather(w, mid, out)


def whole_gather(w, src, out):
    first = [
        w.start(src, out.at[w.g, w.j], w.at_group(w.group_peer(d))) for d in range(1, w.n_groups)
    ]
    out[w.g, w.j] = src[...]
    yield
    wait_received(first)
    second = [
        w.start(out.at[:, w.j], out.at[:, w.j], w.at_plane(w.plane_peer(d)))
        for d in range(1, w.n_plane)
    ]
    yield
    wait_sent(first)
    wait_all(second)


def plane_swap_gather(w, src, out):
    first = []
    for d in range(1, w.n_plane):
        to = w.plane_peer(d)
        first.append(w.start(src.at[to], out.at[w.g, w.j], w.at_plane(to)))
    out[w.g, w.j] = src[w.j]
    yield
    wait_received(first)
    second = [
        w.start(out.at[w.g], out.at[w.g], w.at_group(w.group_peer(d)))
        for d in range(1, w.n_groups)
    ]
    yield
    wait_sent(first)
    wait_all(second)


def head_rows(w, src, out):
    index = w.g * w.n_plane + w.j
    owner, part = w.head_owner(), lax.rem(index, w.n_groups)
    mine = owner == w.j

    def to(d):
        return pltpu.make_async_remote_copy(
            src_ref=src,
            dst_ref=out.at[part],
            send_sem=w.send.at[base + d],
            recv_sem=w.recv.at[base + part],
            device_id={"g": w.group_peer(d), **w.on_plane(owner)},
            device_id_type=MESH,
        )

    def arrival(r):
        return pltpu.make_async_remote_copy(
            src_ref=src,
            dst_ref=out.at[r],
            send_sem=w.send.at[base],
            recv_sem=w.recv.at[base + r],
            device_id=w.at_device(w.n_groups * w.j + r),
            device_id_type=MESH,
        )

    base = w.used
    w.used += w.n_groups
    for d in range(w.n_groups):

        @pl.when((d > 0) | jnp.logical_not(mine))
        def _():
            to(d).start()

    @pl.when(mine)
    def _():
        out[part] = src[...]

    yield
    for r in range(w.n_groups):

        @pl.when(jnp.logical_not(mine) | (part != r))
        def _():
            arrival(r).wait_recv()

    for d in range(w.n_groups):

        @pl.when((d > 0) | jnp.logical_not(mine))
        def _():
            to(d).wait_send()


def plane_swap(w, src, out):
    copies = []
    for d in range(1, w.n_plane):
        to = w.plane_peer(d)
        copies.append(w.start(src.at[to], out.at[w.j], w.at_plane(to)))
    out[w.j] = src[w.j]
    yield
    wait_all(copies)


def plane_sum(w, src, out, from_core, pairs, from_chips):
    chips = w.n_plane // w.cores
    first = []
    for d in range(chips):
        p = lax.rem(w.p + d, chips)
        first.append(w.start(src.at[p * w.cores + 1 - w.c], from_core.at[d], w.partner()))
    yield
    second = []
    for d in list(range(1, chips)) + [0]:
        p = lax.rem(w.p + d, chips)
        first[d].wait_recv()
        sum_rows(pairs.at[d], [src.at[p * w.cores + w.c], from_core.at[d]])
        if d:
            second.append(w.start(pairs.at[d], from_chips.at[d - 1], w.at_chip(p)))
    yield
    wait_received(second)
    sum_rows(out, [pairs.at[0]] + [from_chips.at[d] for d in range(chips - 1)])
    wait_sent(first)
    wait_sent(second)


def whole_sum(w, src, out, from_plane, total, parts):
    first = []
    for d in range(1, w.n_plane):
        to = w.plane_peer(d)
        first.append(w.start(src.at[:, to], from_plane.at[d - 1], w.at_plane(to)))
    yield
    wait_received(first)

    def step(i, carry):
        sum_rows(
            total.at[i], [src.at[i, w.j]] + [from_plane.at[d, i] for d in range(w.n_plane - 1)]
        )
        return carry

    lax.fori_loop(0, w.n_groups, step, 0)
    wait_sent(first)
    yield from group_sum(w, total, out, parts)


def whole_swap(w, src, out, mid):
    first = []
    for d in range(1, w.n_plane):
        to = w.plane_peer(d)
        first.append(w.start(src.at[:, to], mid.at[w.j], w.at_plane(to)))
    mid[w.j] = src[:, w.j]
    yield
    wait_received(first)
    second = []
    for d in range(1, w.n_groups):
        to = w.group_peer(d)
        second.append(w.start(mid.at[:, to], out.at[w.g], w.at_group(to)))
    out[w.g] = mid[:, w.g]
    yield
    wait_sent(first)
    wait_all(second)


def plane_sum_shift(w, src, out, from_core, pairs, from_chips, low, later):
    rows = out.shape[0]
    yield from plane_sum(w, src, low, from_core, pairs, from_chips)
    copy = w.start(
        low.at[pl.ds(0, rows)], later, w.at_group(lax.rem(w.g + w.n_groups - 1, w.n_groups))
    )
    yield
    copy.wait()
    keep = jnp.where(w.g == w.n_groups - 1, 0.0, 1.0)
    out[...] = low[rows:, :].astype(F32) + later[...].astype(F32) * keep


def group_sum(w, src, out, parts):
    copies = []
    for d in range(1, w.n_groups):
        to = w.group_peer(d)
        copies.append(w.start(src.at[to], parts.at[d - 1], w.at_group(to)))
    yield
    wait_received(copies)
    sum_rows(out, [src.at[w.g]] + [parts.at[d] for d in range(w.n_groups - 1)])
    wait_sent(copies)


def group_sum_swap(w, src, out, total, parts):
    copies = []
    for d in range(1, w.n_groups):
        to = w.group_peer(d)
        copies.append(w.start(src.at[to], parts.at[d - 1], w.at_group(to)))
    yield
    wait_received(copies)

    def step(i, carry):
        sum_rows(total.at[i], [src.at[w.g, i]] + [parts.at[d, i] for d in range(w.n_groups - 1)])
        return carry

    lax.fori_loop(0, w.n_plane, step, 0)
    second = []
    for d in range(1, w.n_plane):
        to = w.plane_peer(d)
        second.append(w.start(total.at[to], out.at[w.j], w.at_plane(to)))
    out[w.j] = total[w.j]
    yield
    wait_sent(copies)
    wait_all(second)


ROUTINES = {
    "plane_gather": plane_gather,
    "shift_gather": shift_gather,
    "whole_gather": whole_gather,
    "plane_swap_gather": plane_swap_gather,
    "plane_swap": plane_swap,
    "plane_sum": plane_sum,
    "plane_sum_shift": plane_sum_shift,
    "head_rows": head_rows,
    "group_sum": group_sum,
    "whole_sum": whole_sum,
    "whole_swap": whole_swap,
    "group_sum_swap": group_sum_swap,
}


def exchange_kernel(n_groups, n_plane, kinds, extra, *refs):
    count = len(kinds)
    sources, outs = refs[:count], refs[count : 2 * count]
    scratch = list(refs[2 * count : -2])
    w = Wires(n_groups, n_plane, refs[-2], refs[-1])
    w.meet("head_rows" in kinds)
    running = []
    for kind, source, out, number in zip(kinds, sources, outs, extra):
        mine, scratch = scratch[:number], scratch[number:]
        if kind == "shift_gather":
            running.append(shift_gather(w, source, mine[0], out))
        else:
            running.append(ROUTINES[kind](w, source, out, *mine))
    while running:
        still = []
        for routine in running:
            try:
                next(routine)
                still.append(routine)
            except StopIteration:
                pass
        running = still


def exchange(n_groups, n_plane, number, *items):
    kinds = [kind for kind, _ in items]
    arrays = [array for _, array in items]
    shapes, scratch, extra = [], [], []
    chips = n_plane // 2
    for kind, array in items:
        shape, dtype = array.shape, array.dtype
        own = []
        if kind in ("plane_gather", "shift_gather"):
            out = (n_plane,) + shape
            if kind == "shift_gather":
                own = [shape]
        elif kind == "whole_gather":
            out = (n_groups, n_plane) + shape
        elif kind == "plane_swap_gather":
            out = (n_groups,) + shape
        elif kind == "plane_swap":
            out = shape
        elif kind == "head_rows":
            out = (n_groups,) + shape
        elif kind == "plane_sum_shift":
            pair = shape[1:]
            out = (shape[1] // 2, shape[2])
            own = [(chips,) + pair, (chips,) + pair, (chips - 1,) + pair, pair, out]
        elif kind == "plane_sum":
            out = shape[1:]
            own = [(chips,) + out, (chips,) + out, (chips - 1,) + out]
        elif kind == "group_sum":
            out = shape[1:]
            own = [(n_groups - 1,) + out]
        elif kind == "whole_swap":
            out = shape
            own = [(n_plane, n_groups) + shape[2:]]
        elif kind == "whole_sum":
            out = shape[2:]
            own = [(n_plane - 1, n_groups) + out, (n_groups,) + out, (n_groups - 1,) + out]
        elif kind == "group_sum_swap":
            out = shape[1:]
            own = [out, (n_groups - 1,) + out]
        if kind in ("plane_sum", "plane_sum_shift", "group_sum", "whole_sum"):
            shapes.append(jax.ShapeDtypeStruct(out, F32))
        else:
            shapes.append(jax.ShapeDtypeStruct(out, dtype))
        scratch += [pltpu.VMEM(s, dtype) for s in own]
        extra.append(len(own))
    copies = 64 + 32 * len(items)
    vmem = pl.BlockSpec(memory_space=pltpu.VMEM)
    return pl.pallas_call(
        functools.partial(exchange_kernel, n_groups, n_plane, kinds, extra),
        out_shape=shapes,
        in_specs=[vmem] * len(items),
        out_specs=[vmem] * len(items),
        scratch_shapes=scratch
        + [pltpu.SemaphoreType.DMA((copies,)), pltpu.SemaphoreType.DMA((copies,))],
        compiler_params=pltpu.CompilerParams(
            collective_id=number,
            has_side_effects=True,
            vmem_limit_bytes=60 * 1024 * 1024,
        ),
        name="exchange_%d" % number,
    )(*arrays)


def gather_all(x):
    return lax.all_gather(x, ALL, axis=0, tiled=True)


class StreamSum:
    def __init__(self, w, steps, stage, from_core, pairs, from_chips, totals, parts, sems, credit):
        self.w, self.steps = w, steps
        self.stage, self.from_core, self.pairs = stage, from_core, pairs
        self.from_chips, self.totals, self.parts = from_chips, totals, parts
        self.core_sems, self.chip_sems, self.chip_recv, self.group_sems = sems
        self.credit = credit

    @staticmethod
    def distances(step):
        half = lax.rem(step, 2)
        return 1 + 2 * half, 2 - 2 * half

    def core_copy(self, step, i):
        slot = lax.rem(step, 2)
        return pltpu.make_async_remote_copy(
            src_ref=self.stage.at[slot, 2 * i + 1 - self.w.c],
            dst_ref=self.from_core.at[slot, i],
            send_sem=self.core_sems.at[0, slot, i],
            recv_sem=self.core_sems.at[1, slot, i],
            device_id=self.w.partner(),
            device_id_type=MESH,
        )

    def chip_copy(self, step, i):
        slot, distance = lax.rem(step, 2), self.distances(step)[i]
        group_at = step // 2
        return pltpu.make_async_remote_copy(
            src_ref=self.pairs.at[slot, i],
            dst_ref=self.from_chips.at[group_at, distance - 1],
            send_sem=self.chip_sems.at[slot, i],
            recv_sem=self.chip_recv.at[group_at, distance - 1],
            device_id=self.w.at_chip(lax.rem(self.w.p + distance, 4)),
            device_id_type=MESH,
        )

    def chip_arrival(self, group_at, distance):
        return pltpu.make_async_remote_copy(
            src_ref=self.pairs.at[0, 0],
            dst_ref=self.from_chips.at[group_at, distance - 1],
            send_sem=self.chip_sems.at[0, 0],
            recv_sem=self.chip_recv.at[group_at, distance - 1],
            device_id=self.w.at_chip(lax.rem(self.w.p + distance, 4)),
            device_id_type=MESH,
        )

    def group_copy(self, group_at):
        return pltpu.make_async_remote_copy(
            src_ref=self.totals.at[group_at],
            dst_ref=self.parts.at[group_at],
            send_sem=self.group_sems.at[0, group_at],
            recv_sem=self.group_sems.at[1, group_at],
            device_id=self.w.at_group(self.w.group_peer(group_at + 1)),
            device_id_type=MESH,
        )

    def open_stage(self, step):
        @pl.when(step >= 2)
        def _():
            for i in range(2):
                self.core_copy(step, i).wait_send()

    def push(self, step):
        @pl.when(step >= 2)
        def _():
            pl.semaphore_wait(self.credit, 1)

        for i in range(2):
            self.core_copy(step, i).start()

    def merge(self, step):
        slot = lax.rem(step, 2)
        for i in range(2):
            self.core_copy(step, i).wait_recv()
            sends = slot == 0 if i else slot >= 0

            @pl.when(sends & (step >= 2))
            def _():
                self.chip_copy(step, i).wait_send()

            sum_rows(
                self.pairs.at[slot, i],
                [self.stage.at[slot, 2 * i + self.w.c], self.from_core.at[slot, i]],
            )

            @pl.when(sends)
            def _():
                self.chip_copy(step, i).start()

        @pl.when(step + 2 < self.steps)
        def _():
            pl.semaphore_signal(
                self.credit, inc=1, device_id=self.w.partner(), device_id_type=MESH
            )

    def plane_total(self, group_at):
        for distance in (1, 2, 3):
            self.chip_arrival(group_at, distance).wait_recv()
        return [self.pairs.at[1, 1]] + [self.from_chips.at[group_at, d] for d in range(3)]

    def advance(self, step):
        @pl.when(step >= 1)
        def _():
            last = step - 1

            @pl.when((lax.rem(last, 2) == 0) & (last >= 2))
            def _():
                group_at = last // 2 - 1
                sum_rows(self.totals.at[group_at], self.plane_total(group_at))
                self.group_copy(group_at).start()

            self.merge(last)

    def finish(self, out):
        steps = self.steps
        self.merge(steps - 1)
        sources = self.plane_total(steps // 2 - 1)
        groups = steps // 2 - 1
        for d in range(groups):
            self.group_copy(d).wait_recv()
            sources.append(self.parts.at[d])
        sum_rows(out, sources)
        for d in range(groups):
            self.group_copy(d).wait_send()
        for i in range(2):
            self.core_copy(steps - 2, i).wait_send()
            self.core_copy(steps - 1, i).wait_send()
            self.chip_copy(steps - 2, i).wait_send()
        self.chip_copy(steps - 1, 0).wait_send()

    @staticmethod
    def scratch(n_groups, rows, width):
        dma = pltpu.SemaphoreType.DMA
        return [
            pltpu.VMEM((2, 4, rows, width), BF),
            pltpu.VMEM((2, 2, rows, width), BF),
            pltpu.VMEM((2, 2, rows, width), BF),
            pltpu.VMEM((n_groups, 3, rows, width), BF),
            pltpu.VMEM((n_groups - 1, rows, width), BF),
            pltpu.VMEM((n_groups - 1, rows, width), BF),
            dma((2, 2, 2)),
            dma((2, 2)),
            dma((n_groups, 3)),
            dma((2, n_groups - 1)),
            pltpu.SemaphoreType.REGULAR,
        ]


def swiglu_both(gate, up, grad):
    sigmoid = 1.0 / (1.0 + jnp.exp(-gate))
    silu = gate * sigmoid
    return silu * up, grad * up * (sigmoid * (1.0 + gate * (1.0 - sigmoid))), grad * silu


def step_chips(w, step):
    group = lax.rem(w.g + 1 + step // 2, w.n_groups)
    return [group * 4 + lax.rem(w.p + d, 4) for d in StreamSum.distances(step)]


def hot_rows(place, rows, core, slot_count):
    mine = place[:, core * rows : (core + 1) * rows]
    return lax.broadcasted_iota(jnp.int32, (slot_count, rows), 0) == mine


def moe_kernel(
    n_groups, experts, first_logit, slot_count,
    h2_hbm, cot_hbm, place_ref, wg_ref, wu_ref, wd_ref, sc_ref, sd_ref,
    sum_ref, rows_ref, gin_ref, act_ref, gg_ref, gu_ref, rw_ref, sact_ref, sgrad_ref, tok_ref,
    h2_buf, cot_buf, load_sems, *comm,
):
    rows = sum_ref.shape[0]
    step, steps = pl.program_id(0), 2 * n_groups
    w = Wires(n_groups, 8, None, None)
    stream = StreamSum(w, steps, *comm[:6], comm[6:10], comm[10])
    expert_id = w.g * 4 + w.p
    half = sc_ref.shape[1] // 2

    def loads(at):
        slot = lax.rem(at, 2)
        for i, chip in enumerate(step_chips(w, at)):
            source = pl.ds(pl.multiple_of(chip * 2 * rows, 2 * rows), 2 * rows)
            target = pl.ds(i * 2 * rows, 2 * rows)
            for k, (hbm, buf) in enumerate(((h2_hbm, h2_buf), (cot_hbm, cot_buf))):
                yield pltpu.make_async_copy(
                    hbm.at[source], buf.at[slot, target], load_sems.at[slot, i, k]
                )

    @pl.when(step == 0)
    def _():
        for copy in loads(step):
            copy.start()
        w.meet()

    @pl.when(step + 1 < steps)
    def _():
        for copy in loads(step + 1):
            copy.start()

    for copy in loads(step):
        copy.wait()
    slot = lax.rem(step, 2)
    h2, cot = h2_buf[slot], cot_buf[slot]
    chips = step_chips(w, step)

    pre = jnp.dot(h2, sc_ref[...], preferred_element_type=F32)
    back = dot_nt(cot, sd_ref[...])
    gate, up = pre[:, :half], pre[:, half:]
    lane = lax.broadcasted_iota(jnp.int32, gate.shape, 1)
    logits = jnp.where((lane >= first_logit) & (lane < first_logit + experts), gate, -1e30)
    exps = jnp.exp(logits - jnp.max(logits, axis=1, keepdims=True))
    chosen = jnp.where(lane == first_logit + expert_id, exps, 0.0)
    weight = jnp.sum(chosen, axis=1, keepdims=True) / jnp.sum(exps, axis=1, keepdims=True)
    act, grad_gate, grad_up = swiglu_both(gate, up, back)
    shared_act = act.astype(BF)
    shared_grad = jnp.concatenate([grad_gate.astype(BF), grad_up.astype(BF)], axis=1)
    for i, chip in enumerate(chips):
        at = pl.ds(pl.multiple_of(chip * 2 * rows, 2 * rows), 2 * rows)
        sact_ref[at, :] = shared_act[i * 2 * rows : (i + 1) * 2 * rows]
        sgrad_ref[at, :] = shared_grad[i * 2 * rows : (i + 1) * 2 * rows]

    hots, weights = [], []
    for q in range(4):
        place = place_ref[pl.ds(chips[q // 2], 1), :]
        hot = hot_rows(place, rows, q % 2, slot_count).astype(F32)
        hots.append(hot)
        tokens = slice(q * rows, (q + 1) * rows)
        slots = slice(q * slot_count, (q + 1) * slot_count)
        low = hot.astype(BF)
        rows_ref[slots, :] = jnp.dot(low, h2[tokens], preferred_element_type=F32).astype(BF)
        gin_ref[slots, :] = jnp.dot(low, cot[tokens], preferred_element_type=F32).astype(BF)
        spread = jnp.broadcast_to(weight[tokens], (rows, 128))
        weights.append(
            jnp.dot(hot, spread, preferred_element_type=F32, precision=lax.Precision.HIGHEST)[:, :1]
        )
    row_weight = jnp.concatenate(weights, axis=0)
    rw_ref[...] = row_weight
    expert_rows = rows_ref[...]
    picked_cot = gin_ref[...]
    back = dot_nt(picked_cot, wd_ref[...])
    gin_ref[...] = (picked_cot.astype(F32) * row_weight).astype(BF)
    gate = jnp.dot(expert_rows, wg_ref[...], preferred_element_type=F32)
    up = jnp.dot(expert_rows, wu_ref[...], preferred_element_type=F32)
    act, grad_gate, grad_up = swiglu_both(gate, up, back * row_weight)
    act_low, grad_gate, grad_up = act.astype(BF), grad_gate.astype(BF), grad_up.astype(BF)
    act_ref[...] = act_low
    gg_ref[...] = grad_gate
    gu_ref[...] = grad_up
    picked = jnp.sum(act_low.astype(F32) * back, axis=1, keepdims=True)
    grad_rows = (dot_nt(grad_gate, wg_ref[...]) + dot_nt(grad_up, wu_ref[...])).astype(BF)
    stream.open_stage(step)
    for q in range(4):
        tokens = slice(q * rows, (q + 1) * rows)
        slots = slice(q * slot_count, (q + 1) * slot_count)
        tok_ref[pl.ds(chips[q // 2] * 2 + q % 2, 1), :] = jnp.sum(
            hots[q] * picked[slots], axis=0, keepdims=True
        )
        total = dot_tn(hots[q].astype(BF), grad_rows[slots]) + dot_nt(
            shared_grad[tokens], sc_ref[...]
        )
        stream.stage[slot, q] = total.astype(BF)
    stream.push(step)
    stream.advance(step)

    @pl.when(step == steps - 1)
    def _():
        stream.finish(sum_ref)


def out_kernel(
    n_groups, slot_count,
    act_ref, rw_ref, rows_ref, gin_ref, gg_ref, gu_ref, place_ref, sact_ref, wd_ref, sd_ref,
    sum_ref, dg_ref, du_ref, dd_ref, *comm,
):
    rows = sum_ref.shape[0]
    step, steps = pl.program_id(0), 2 * n_groups
    w = Wires(n_groups, 8, None, None)
    stream = StreamSum(w, steps, *comm[:6], comm[6:10], comm[10])

    @pl.when(step == 0)
    def _():
        w.meet()
        for ref in (dg_ref, du_ref, dd_ref):
            ref[...] = jnp.zeros_like(ref)

    slot = lax.rem(step, 2)
    chips = step_chips(w, step)
    out_rows = jnp.dot(act_ref[...], wd_ref[...], preferred_element_type=F32) * rw_ref[...]
    out_rows = out_rows.astype(BF)
    stream.open_stage(step)
    for q in range(4):
        chip = chips[q // 2]
        place = place_ref[pl.ds(chip, 1), :]
        low = hot_rows(place, rows, q % 2, slot_count).astype(F32).astype(BF)
        slots = slice(q * slot_count, (q + 1) * slot_count)
        shared = sact_ref[pl.ds(pl.multiple_of((chip * 2 + q % 2) * rows, rows), rows), :]
        total = dot_tn(low, out_rows[slots]) + jnp.dot(
            shared, sd_ref[...], preferred_element_type=F32
        )
        stream.stage[slot, q] = total.astype(BF)
    stream.push(step)
    stream.advance(step)

    width = rows_ref.shape[1]
    piece = width // 4
    for k in range(4):
        cols = slice(k * piece, (k + 1) * piece)
        turned = rows_ref[:, cols].T
        dg_ref[cols, :] += jnp.dot(turned, gg_ref[...], preferred_element_type=F32)
        du_ref[cols, :] += jnp.dot(turned, gu_ref[...], preferred_element_type=F32)
    turned = act_ref[...].T
    for k in range(4):
        cols = slice(k * piece, (k + 1) * piece)
        dd_ref[:, cols] += jnp.dot(turned, gin_ref[:, cols], preferred_element_type=F32)

    @pl.when(step == steps - 1)
    def _():
        stream.finish(sum_ref)


def experts_sums(
    n_groups, rows, h2, cot, place, slot_count, expert_w, shared_w, router_weight, first_id
):
    w_gate, w_up, w_down = expert_w
    s_both, s_down = shared_w
    tokens, width = h2.shape
    hidden, hidden_s = w_down.shape[0], s_down.shape[0]
    experts = router_weight.shape[1]
    steps = 2 * n_groups
    devices = tokens // rows
    step_slots = slot_count * 4
    all_slots = step_slots * steps
    half = 128
    s_cat = jnp.concatenate(
        [
            s_both[:, :hidden_s],
            router_weight,
            jnp.zeros((width, half - hidden_s - experts), BF),
            s_both[:, hidden_s:],
            jnp.zeros((width, half - hidden_s), BF),
        ],
        axis=1,
    )
    s_tall = jnp.pad(s_down, ((0, half - hidden_s), (0, 0)))

    def whole(array):
        return pl.BlockSpec(array.shape, lambda i: (0, 0), pipeline_mode=pl.Buffered(1))

    def blocked(rows, cols):
        return pl.BlockSpec((rows, cols), lambda i: (i, 0))

    shape = jax.ShapeDtypeStruct
    flops = 2 * all_slots * width * hidden * 5 + 2 * tokens * width * (4 * half + 3 * slot_count)
    shapes = [
        shape((rows, width), F32),
        shape((all_slots, width), BF),
        shape((all_slots, width), BF),
        shape((all_slots, hidden), BF),
        shape((all_slots, hidden), BF),
        shape((all_slots, hidden), BF),
        shape((all_slots, 1), F32),
        shape((tokens, half), BF),
        shape((tokens, 2 * half), BF),
        shape((devices, rows), F32),
    ]
    specs = [
        blocked(step_slots, s.shape[1]) if s.shape[0] == all_slots else whole(s) for s in shapes
    ]
    hbm = pl.BlockSpec(memory_space=pl.ANY)
    grad_h2, rows_in, grad_in, act, grad_gate, grad_up, row_weight, s_act, s_grad, token_grad = (
        pl.pallas_call(
            functools.partial(moe_kernel, n_groups, experts, hidden_s, slot_count),
            grid=(steps,),
            in_specs=[
                hbm,
                hbm,
                whole(place),
                whole(w_gate),
                whole(w_up),
                whole(w_down),
                whole(s_cat),
                whole(s_tall),
            ],
            out_specs=specs,
            out_shape=shapes,
            scratch_shapes=[
                pltpu.VMEM((2, 4 * rows, width), BF),
                pltpu.VMEM((2, 4 * rows, width), BF),
                pltpu.SemaphoreType.DMA((2, 2, 2)),
            ]
            + StreamSum.scratch(n_groups, rows, width),
            cost_estimate=pl.CostEstimate(
                flops=flops, bytes_accessed=12 * tokens * width, transcendentals=tokens * 1024
            ),
            compiler_params=pltpu.CompilerParams(
                collective_id=first_id,
                has_side_effects=True,
                vmem_limit_bytes=67043328,
            ),
            name="experts",
        )(h2, cot, place, w_gate, w_up, w_down, s_cat, s_tall)
    )
    shapes = [grad_h2] + [shape(x.shape, F32) for x in expert_w]
    out, d_gate, d_up, d_down = pl.pallas_call(
        functools.partial(out_kernel, n_groups, slot_count),
        grid=(steps,),
        in_specs=[
            blocked(step_slots, hidden),
            blocked(step_slots, 1),
            blocked(step_slots, width),
            blocked(step_slots, width),
            blocked(step_slots, hidden),
            blocked(step_slots, hidden),
            whole(place),
            whole(s_act),
            whole(w_down),
            whole(s_tall),
        ],
        out_specs=[whole(x) for x in shapes],
        out_shape=[shape(x.shape, F32) for x in shapes],
        scratch_shapes=StreamSum.scratch(n_groups, rows, width),
        cost_estimate=pl.CostEstimate(
            flops=2 * width * (4 * all_slots * hidden + tokens * (half + slot_count)),
            bytes_accessed=4 * tokens * width,
            transcendentals=0,
        ),
        compiler_params=pltpu.CompilerParams(
            collective_id=first_id + 1,
            has_side_effects=True,
            vmem_limit_bytes=67043328,
        ),
        name="expert_out",
    )(act, row_weight, rows_in, grad_in, grad_gate, grad_up, place, s_act, w_down, s_tall)
    g_both = dot_tn(h2, s_grad)
    g_both = jnp.concatenate([g_both[:, :hidden_s], g_both[:, half : half + hidden_s]], axis=1)
    grads = (
        d_gate,
        d_up,
        d_down,
        g_both,
        dot_tn(s_act, cot)[:hidden_s],
    )
    return out, grad_h2, token_grad, grads


def body(
    n_groups, n_plane, layer_input, attn_gain, w_query, w_latent, kv_gain, w_expand, w_output,
    ffn_gain, w_router, shared_gate, shared_up, shared_down, expert_gate, expert_up,
    expert_down, routes, segments, cotangent,
):
    tok, width = layer_input.shape
    devices = n_groups * n_plane
    experts = w_router.shape[1]
    local_heads = HEADS // n_plane
    scale = (NOPE + ROPE) ** (-0.5)
    group = lax.axis_index("g")
    place_in = lax.axis_index(PLANE)
    me = lax.axis_index(ALL)
    expert_id = lax.axis_index(("g", "p"))
    plane_tok = n_plane * tok
    plane_start = group * plane_tok

    rows_w = w_router.shape[0]
    kv_n = kv_gain.shape[0]
    small = jnp.concatenate(
        [
            attn_gain,
            ffn_gain,
            kv_gain,
            w_router.reshape(-1),
            routes.reshape(-1).astype(BF),
            segments.astype(BF),
        ]
    )
    small = jnp.pad(small, (0, -small.shape[0] % 4096)).reshape(-1, 128)
    head_cols = local_heads * (NOPE + ROPE)
    kv_cols = local_heads * (NOPE + VDIM)
    fold = kv_n * kv_cols // rows_w
    pair = jnp.concatenate(
        [
            w_query.reshape(rows_w, n_plane, head_cols).transpose(1, 0, 2),
            w_expand.reshape(kv_n, n_plane, kv_cols // fold, fold)
            .transpose(1, 0, 2, 3)
            .reshape(n_plane, rows_w, fold),
        ],
        axis=2,
    )
    swap = functools.partial(exchange, n_groups, n_plane)
    x_plane, small, latent_weight, pair = swap(
        0,
        ("plane_gather", layer_input),
        ("whole_gather", small),
        ("whole_gather", w_latent),
        ("plane_swap_gather", pair),
    )
    x_plane = x_plane.reshape(plane_tok, width).astype(F32)
    latent_weight = latent_weight.reshape(width, RANK + ROPE)
    pair = pair.reshape(width, head_cols + fold)
    small = small.reshape(devices, -1)
    cuts = [rows_w, 2 * rows_w, 2 * rows_w + kv_n, 2 * rows_w + kv_n + rows_w * experts]
    cuts = cuts + [cuts[-1] + tok * TOP, cuts[-1] + tok * TOP + tok]
    gain_one = small[:, : cuts[0]].reshape(-1).astype(F32)
    gain_two = small[:, cuts[0] : cuts[1]].reshape(-1).astype(F32)
    gain_kv = small[:, cuts[1] : cuts[2]].reshape(-1).astype(F32)
    router_weight = small[:, cuts[2] : cuts[3]].reshape(width, experts)
    routes_all = small[:, cuts[3] : cuts[4]].astype(jnp.int32).reshape(devices, tok, TOP)
    segments_all = small[:, cuts[4] : cuts[5]].astype(jnp.int32).reshape(-1)

    query_weight = pair[:, :head_cols].reshape(width, local_heads, NOPE + ROPE)
    wq_nope = query_weight[:, :, :NOPE].reshape(width, local_heads * NOPE)
    wq_rope = query_weight[:, :, NOPE:].reshape(width, local_heads * ROPE)
    expand_weight = pair[:, head_cols:].reshape(RANK, kv_cols)
    cotangent_later = lax.optimization_barrier((cotangent, x_plane))[0]

    shared_n = shared_down.shape[0]
    s_both = jnp.concatenate(
        [
            shared_gate.reshape(rows_w, devices, shared_n),
            shared_up.reshape(rows_w, devices, shared_n),
        ],
        axis=2,
    )
    s_both = lax.all_to_all(s_both, ALL, split_axis=1, concat_axis=0).reshape(width, 2 * shared_n)

    hidden = rms_norm(x_plane, gain_one).astype(BF)
    rope_half = ROPE // 2
    positions = plane_start + jnp.arange(plane_tok, dtype=jnp.int32)
    frequency = 10000.0 ** (-jnp.arange(rope_half, dtype=F32) / rope_half)
    angles = positions.astype(F32)[:, None] * frequency[None, :]
    cosine = jnp.cos(angles)
    sine_part = jnp.sin(angles)
    cos_h, sin_h = cosine[:, None, :], sine_part[:, None, :]
    latent = matmul(hidden, latent_weight)
    compressed_own = rms_norm(latent[:, :RANK], gain_kv).astype(BF)
    key_rope_own = rotate(latent[:, RANK:], cosine, sine_part).astype(BF)

    def own_rows(table):
        return lax.dynamic_slice_in_dim(table, place_in * tok, tok, 0)

    piece = own_rows(jnp.concatenate([compressed_own, key_rope_own], axis=1))
    before, own_output = swap(1, ("shift_gather", piece), ("head_rows", w_output))
    before = before.reshape(plane_tok, RANK + ROPE)
    own_output = own_output.reshape(local_heads * VDIM, width)
    compressed = jnp.concatenate([before[:, :RANK], compressed_own], axis=0)
    key_rope = jnp.concatenate([before[:, RANK:], key_rope_own], axis=0)
    q_nope = matmul(hidden, wq_nope).astype(BF)
    q_rope = rotate(
        matmul(hidden, wq_rope).reshape(plane_tok, local_heads, ROPE), cos_h, sin_h
    ).reshape(plane_tok, local_heads * ROPE).astype(BF)
    expanded = matmul(compressed, expand_weight).astype(BF)
    plane_segments = lax.dynamic_slice_in_dim(segments_all, plane_start, plane_tok, 0)
    doc_start = jnp.sum(
        (segments_all[None, :] < plane_segments[:, None]).astype(jnp.int32), axis=1, keepdims=True
    )
    low_bound = doc_start - plane_start + DOC_MAX
    mixed_heads, lse = attend(low_bound, q_nope, q_rope, expanded, key_rope, scale)
    attn_out = matmul(mixed_heads, own_output).astype(BF)
    attn_out = swap(2, ("plane_sum", attn_out.reshape(n_plane, tok, width)))[0]
    input_float = layer_input.astype(F32)
    residual_one = input_float + attn_out
    h_two_f, norm_two_back = jax.vjp(rms_norm, residual_one, gain_two)
    h_two = h_two_f.astype(BF)
    router_probs = softmax_rows(matmul(h_two, router_weight))

    expert_w = (expert_gate[0], expert_up[0], expert_down[0])
    shared_w = (s_both, shared_down)
    slot_limit = 2 * tok * TOP // experts

    def on_rows(h2, cot_gathered, routes_here):
        rows = h2.shape[0]
        h2_all = gather_all(h2)
        slot_count = min(slot_limit, rows)
        member = jnp.any(routes_here == expert_id, axis=2)
        member_int = member.astype(jnp.int32)
        rank = jnp.cumsum(member_int, axis=1) - member_int
        place = jnp.where(member, rank, -1).reshape(devices // 2, 2 * rows)
        out, grad_h2, token_grad, grads = experts_sums(
            n_groups,
            rows,
            h2_all,
            cot_gathered,
            place,
            slot_count,
            expert_w,
            shared_w,
            router_weight,
            8,
        )
        picked = lax.all_to_all(token_grad, ALL, split_axis=0, concat_axis=0, tiled=True)
        picked = jnp.sum(picked.reshape(experts, devices // experts, rows), axis=1).T
        return out, grad_h2, picked, grads

    parts = max(1, devices * tok // 4096)
    if parts == 1:
        cot_all = gather_all(cotangent_later)
        out_own, grad_h2_own, grad_router_probs, grads = on_rows(
            h_two, cot_all, routes_all
        )
    else:
        rows = tok // parts

        def step(total, inputs):
            h2, cot, routes_here = inputs
            cot_part = gather_all(cot)
            out, grad_h2, picked, grads = on_rows(h2, cot_part, routes_here)
            grads = lax.optimization_barrier(grads)
            total = tuple(a + b for a, b in zip(total, grads))
            return total, (out, grad_h2, picked)

        shapes = expert_w + shared_w
        grads, (out_own, grad_h2_own, grad_router_probs) = lax.scan(
            step,
            tuple(jnp.zeros(s.shape, F32) for s in shapes),
            (
                h_two.reshape(parts, rows, width),
                cotangent.reshape(parts, rows, width),
                routes_all.reshape(devices, parts, rows, TOP).transpose(1, 0, 2, 3),
            ),
        )
        out_own = out_own.reshape(tok, width)
        grad_h2_own = grad_h2_own.reshape(tok, width)
        grad_router_probs = grad_router_probs.reshape(tok, experts)
    g_gate, g_up, g_down, g_both, g_sdown = grads
    grad_logits = router_probs * (
        grad_router_probs - jnp.sum(router_probs * grad_router_probs, axis=1, keepdims=True)
    )
    grad_logits = grad_logits.astype(BF)
    grad_router = dot_tn(h_two, grad_logits)
    grad_h_two = grad_h2_own + dot_nt(grad_logits, router_weight)
    output = residual_one + out_own

    grad_x_one, grad_gain_two = norm_two_back(grad_h_two)
    grad_x_one = grad_x_one + cotangent.astype(F32)
    grad_attn_out = grad_x_one.astype(BF)
    plane_grad, g_shared = swap(
        3,
        ("plane_gather", grad_attn_out),
        ("whole_swap", g_both.astype(BF).reshape(n_groups, n_plane, rows_w, 2 * shared_n)),
    )
    plane_grad = plane_grad.reshape(plane_tok, width)
    grad_mixed = dot_nt(plane_grad, own_output).astype(BF)
    dqn, dqr, dex, dkr = attend_back(
        low_bound, q_nope, q_rope, expanded, key_rope, lse, grad_mixed, scale
    )

    g_output = dot_tn(mixed_heads, plane_grad).astype(BF).reshape(n_groups, rows_w, width)

    grad_expanded = dex.astype(BF)
    grad_expand = dot_tn(compressed, grad_expanded)
    grad_comp = dot_nt(grad_expanded, expand_weight)
    key_grads = jnp.concatenate([grad_comp, dkr], axis=1).astype(BF)
    key_grads = (
        key_grads.reshape(2, n_plane, tok, RANK + ROPE)
        .transpose(1, 0, 2, 3)
        .reshape(n_plane, 2 * tok, RANK + ROPE)
    )

    gq_nope = dqn.astype(BF)
    gq_rope = (
        unrotate(dqr.reshape(plane_tok, local_heads, ROPE), cos_h, sin_h)
        .reshape(plane_tok, local_heads * ROPE)
        .astype(BF)
    )
    grad_hidden = (dot_nt(gq_nope, wq_nope) + dot_nt(gq_rope, wq_rope)).astype(BF)
    gw_nope = dot_tn(hidden, gq_nope).astype(BF).reshape(n_groups, n_plane, rows_w, -1)
    gw_rope = dot_tn(hidden, gq_rope).astype(BF).reshape(n_groups, n_plane, rows_w, -1)
    g_expand = grad_expand.astype(BF).reshape(n_groups, n_plane, kv_n, kv_cols)
    key_grad, grad_hidden, gw_nope, gw_rope, g_expand = swap(
        4,
        ("plane_sum_shift", key_grads),
        ("plane_sum", grad_hidden.reshape(n_plane, tok, width)),
        ("group_sum_swap", gw_nope),
        ("group_sum_swap", gw_rope),
        ("group_sum_swap", g_expand),
    )
    latent_own = own_rows(latent)
    kv_norm_back = jax.vjp(rms_norm, latent_own[:, :RANK], gain_kv)[1]
    grad_comp_in, grad_gain_kv = kv_norm_back(key_grad[:, :RANK])
    grad_rope_in = unrotate(key_grad[:, RANK:], own_rows(cosine), own_rows(sine_part))
    grad_latent = jnp.concatenate([grad_comp_in, grad_rope_in], axis=1).astype(BF)

    latent_grads = swap(5, ("plane_gather", grad_latent))[0]

    def per_head(table, cols):
        return table.transpose(1, 0, 2).reshape(rows_w, HEADS, cols)

    grad_query_weight = jnp.concatenate(
        [per_head(gw_nope, NOPE), per_head(gw_rope, ROPE)], axis=2
    ).reshape(rows_w, -1).astype(F32)
    grad_expand_weight = g_expand.transpose(1, 0, 2).reshape(kv_n, -1).astype(F32)

    latent_grads = latent_grads.reshape(plane_tok, RANK + ROPE)
    g_latent = dot_tn(hidden, latent_grads).astype(BF)
    g_latent = g_latent.reshape(n_groups, n_plane, rows_w, RANK + ROPE)
    g_latent = lax.dynamic_index_in_dim(g_latent, place_in, 1, keepdims=False)
    grad_hidden = grad_hidden + dot_nt(grad_latent, latent_weight)
    norm_one_back = jax.vjp(rms_norm, input_float, gain_one)[1]
    grad_x_norm, grad_gain_one = norm_one_back(grad_hidden)
    grad_input = grad_x_one + grad_x_norm

    small_grads = jnp.concatenate(
        [
            p.reshape(devices, -1)
            for p in (grad_gain_one, grad_gain_two, grad_gain_kv, grad_router)
        ],
        axis=1,
    )
    small_grads = jnp.pad(small_grads, ((0, 0), (0, -small_grads.shape[1] % 1024)))
    grad_latent_weight, grad_output_weight, small_grads = swap(
        6,
        ("group_sum", g_latent),
        ("group_sum", g_output),
        ("whole_sum", small_grads.reshape(n_groups, n_plane, -1, 128)),
    )
    small_grads = small_grads.reshape(-1)
    row_pairs = [
        (g * n_plane + j, n_groups * j + g) for g in range(n_groups) for j in range(n_plane)
    ]
    grad_output_weight = lax.ppermute(grad_output_weight, ALL, row_pairs)
    g_shared = g_shared.transpose(2, 0, 1, 3).reshape(rows_w, devices, 2 * shared_n).astype(F32)
    grad_shared_gate = g_shared[:, :, :shared_n].reshape(rows_w, devices * shared_n)
    grad_shared_up = g_shared[:, :, shared_n:].reshape(rows_w, devices * shared_n)
    return (
        output,
        grad_input,
        small_grads[: cuts[0]],
        grad_query_weight,
        grad_latent_weight,
        small_grads[cuts[1] : cuts[2]],
        grad_expand_weight,
        grad_output_weight,
        small_grads[cuts[0] : cuts[1]],
        small_grads[cuts[2] : cuts[3]].reshape(rows_w, experts),
        grad_shared_gate,
        grad_shared_up,
        g_sdown,
        g_gate[None],
        g_up[None],
        g_down[None],
    )


def solution(mesh):
    n_expert, n_shard = mesh.shape["expert"], mesh.shape["wshard"]
    devices = n_expert * n_shard

    def program(*args):
        tok = args[0].shape[0] // devices
        n_plane = DOC_MAX // tok
        n_groups = devices // n_plane
        inner = Mesh(mesh.devices.reshape(n_groups, n_plane // n_shard, n_shard), ALL)
        rows, vector = P(ALL, None), P(ALL)
        wide, tall = P(("g", "p"), None, "c"), P(("g", "p"), "c", None)
        step = jax.shard_map(
            functools.partial(body, n_groups, n_plane),
            mesh=inner,
            in_specs=(
                rows, vector, rows, rows, vector, rows, rows, vector, rows, rows, rows, rows,
                wide, wide, tall, rows, vector, rows,
            ),
            out_specs=(
                rows, rows, vector, rows, rows, vector, rows, rows, vector, rows, rows, rows,
                rows, wide, wide, tall,
            ),
            check_vma=False,
        )
        return step(*args)

    return program
```

```python
import functools

import jax
import jax.numpy as jnp
from jax import lax
from jax.experimental import pallas as pl
from jax.experimental.pallas import tpu as pltpu
from jax.sharding import Mesh, PartitionSpec as P

HEADS = 16
NOPE = 128
ROPE = 64
VDIM = 128
RANK = 512
TOP = 6
DOC_MAX = 1024
QUERY_BLOCK = 256

BF = jnp.bfloat16
F32 = jnp.float32
ALL = ("g", "p", "c")
PLANE = ("p", "c")

epsilon = 1e-06


def rms_norm(vector, scaling):
    return vector * lax.rsqrt(jnp.mean(vector * vector, axis=-1, keepdims=True) + epsilon) * scaling


def rotate(vector, cosine, sine_part):
    half_width = vector.shape[-1] // 2
    front_half = vector[..., :half_width]
    back_half = vector[..., half_width:]
    return jnp.concatenate(
        [front_half * cosine - back_half * sine_part, back_half * cosine + front_half * sine_part],
        axis=-1,
    )


def unrotate(vector, cosine, sine_part):
    return rotate(vector, cosine, -sine_part)


def matmul(left, right):
    return jnp.dot(left, right, preferred_element_type=F32)


def dot_nt(left, right):
    return lax.dot_general(left, right, (((1,), (1,)), ((), ())), preferred_element_type=F32)


def dot_tn(left, right):
    return lax.dot_general(left, right, (((0,), (0,)), ((), ())), preferred_element_type=F32)


def swiglu(gate_pre, up_pre):
    return jax.nn.silu(gate_pre) * up_pre


def softmax_rows(scores):
    row_top = jnp.max(scores, axis=-1, keepdims=True)
    exp_scores = jnp.exp(scores - row_top)
    return exp_scores / jnp.sum(exp_scores, axis=-1, keepdims=True)


def masked_scores(base, low_bound, q_nope, q_rope, k_nope, k_rope, scale):
    rows, span = q_nope.shape[0], k_nope.shape[0]
    key_at = lax.broadcasted_iota(jnp.int32, (rows, span), 1) + base
    query_at = lax.broadcasted_iota(jnp.int32, (rows, span), 0) + (base + DOC_MAX)
    allowed = (key_at >= low_bound) & (key_at <= query_at)
    scores = (dot_nt(q_nope, k_nope) + dot_nt(q_rope, k_rope)) * scale
    return jnp.where(allowed, scores, -1e30)


def attend_kernel(heads, scale, low_ref, qn_ref, qr_ref, ex_ref, kr_ref, out_ref, lse_ref):
    rows = qn_ref.shape[0]
    base = pl.multiple_of(pl.program_id(0) * rows, rows)
    window = pl.ds(base, rows + DOC_MAX)
    k_rope = kr_ref[window, :]
    low_bound = low_ref[...]
    for h in range(heads):
        at = h * (NOPE + VDIM)
        k_nope = ex_ref[window, at : at + NOPE]
        value = ex_ref[window, at + NOPE : at + NOPE + VDIM]
        scores = masked_scores(
            base,
            low_bound,
            qn_ref[:, h * NOPE : (h + 1) * NOPE],
            qr_ref[:, h * ROPE : (h + 1) * ROPE],
            k_nope,
            k_rope,
            scale,
        )
        top = jnp.max(scores, axis=-1, keepdims=True)
        exps = jnp.exp(scores - top)
        total = jnp.sum(exps, axis=-1, keepdims=True)
        probs = (exps / total).astype(BF)
        out_ref[:, h * VDIM : (h + 1) * VDIM] = jnp.dot(
            probs, value, preferred_element_type=F32
        ).astype(BF)
        lse_ref[:, h : h + 1] = top + jnp.log(total)


def attend(low_bound, q_nope, q_rope, expanded, key_rope, scale):
    queries = q_nope.shape[0]
    heads = q_nope.shape[1] // NOPE
    rows = QUERY_BLOCK

    def whole(array):
        return pl.BlockSpec(array.shape, lambda i: (0, 0))

    def blocked(width):
        return pl.BlockSpec((rows, width), lambda i: (i, 0))

    flops = 2 * heads * queries * (rows + DOC_MAX) * (NOPE + ROPE + VDIM)
    return pl.pallas_call(
        functools.partial(attend_kernel, heads, scale),
        grid=(queries // rows,),
        in_specs=[
            blocked(1),
            blocked(heads * NOPE),
            blocked(heads * ROPE),
            whole(expanded),
            whole(key_rope),
        ],
        out_specs=[blocked(heads * VDIM), blocked(heads)],
        out_shape=[
            jax.ShapeDtypeStruct((queries, heads * VDIM), BF),
            jax.ShapeDtypeStruct((queries, heads), F32),
        ],
        cost_estimate=pl.CostEstimate(
            flops=flops, bytes_accessed=4 * expanded.size, transcendentals=flops // 640
        ),
        compiler_params=pltpu.CompilerParams(vmem_limit_bytes=50 * 1024 * 1024),
        name="attend",
    )(low_bound, q_nope, q_rope, expanded, key_rope)


def attend_back_kernel(
    heads, scale, low_ref, qn_ref, qr_ref, ex_ref, kr_ref, lse_ref, gm_ref,
    dqn_ref, dqr_ref, dex_ref, dkr_ref,
):
    rows = qn_ref.shape[0]
    step = pl.program_id(0)
    base = pl.multiple_of(step * rows, rows)
    window = pl.ds(base, rows + DOC_MAX)

    @pl.when(step == 0)
    def _():
        dex_ref[...] = jnp.zeros_like(dex_ref)
        dkr_ref[...] = jnp.zeros_like(dkr_ref)

    k_rope = kr_ref[window, :]
    low_bound = low_ref[...]
    for h in range(heads):
        at = h * (NOPE + VDIM)
        k_nope = ex_ref[window, at : at + NOPE]
        value = ex_ref[window, at + NOPE : at + NOPE + VDIM]
        q_nope = qn_ref[:, h * NOPE : (h + 1) * NOPE]
        q_rope = qr_ref[:, h * ROPE : (h + 1) * ROPE]
        grad_out = gm_ref[:, h * VDIM : (h + 1) * VDIM]
        scores = masked_scores(base, low_bound, q_nope, q_rope, k_nope, k_rope, scale)
        probs = jnp.exp(scores - lse_ref[:, h : h + 1])
        grad_probs = dot_nt(grad_out, value)
        mean_grad = jnp.sum(probs * grad_probs, axis=-1, keepdims=True)
        grad_scores = (probs * (grad_probs - mean_grad) * scale).astype(BF)
        probs_low = probs.astype(BF)
        dqn_ref[:, h * NOPE : (h + 1) * NOPE] = jnp.dot(
            grad_scores, k_nope, preferred_element_type=F32
        )
        dqr_ref[:, h * ROPE : (h + 1) * ROPE] = jnp.dot(
            grad_scores, k_rope, preferred_element_type=F32
        )
        dex_ref[window, at : at + NOPE] += dot_tn(grad_scores, q_nope)
        dex_ref[window, at + NOPE : at + NOPE + VDIM] += dot_tn(probs_low, grad_out)
        dkr_ref[window, :] += dot_tn(grad_scores, q_rope)


def attend_back(low_bound, q_nope, q_rope, expanded, key_rope, lse, grad_mixed, scale):
    queries = q_nope.shape[0]
    heads = q_nope.shape[1] // NOPE
    rows = QUERY_BLOCK

    def whole(shape):
        return pl.BlockSpec(shape, lambda i: (0, 0))

    def blocked(width):
        return pl.BlockSpec((rows, width), lambda i: (i, 0))

    flops = 2 * heads * queries * (rows + DOC_MAX) * (3 * NOPE + 3 * ROPE + 2 * VDIM)
    return pl.pallas_call(
        functools.partial(attend_back_kernel, heads, scale),
        grid=(queries // rows,),
        in_specs=[
            blocked(1),
            blocked(heads * NOPE),
            blocked(heads * ROPE),
            whole(expanded.shape),
            whole(key_rope.shape),
            blocked(heads),
            blocked(heads * VDIM),
        ],
        out_specs=[
            blocked(heads * NOPE),
            blocked(heads * ROPE),
            whole(expanded.shape),
            whole(key_rope.shape),
        ],
        out_shape=[
            jax.ShapeDtypeStruct(q_nope.shape, F32),
            jax.ShapeDtypeStruct(q_rope.shape, F32),
            jax.ShapeDtypeStruct(expanded.shape, F32),
            jax.ShapeDtypeStruct(key_rope.shape, F32),
        ],
        cost_estimate=pl.CostEstimate(
            flops=flops, bytes_accessed=8 * expanded.size, transcendentals=flops // 1664
        ),
        compiler_params=pltpu.CompilerParams(vmem_limit_bytes=56 * 1024 * 1024),
        name="attend_back",
    )(low_bound, q_nope, q_rope, expanded, key_rope, lse, grad_mixed)


MESH = pl.DeviceIdType.MESH


class Wires:
    def __init__(self, n_groups, n_plane, send, recv):
        self.n_groups, self.n_plane, self.send, self.recv = n_groups, n_plane, send, recv
        self.cores = 2
        self.g, self.p, self.c = lax.axis_index("g"), lax.axis_index("p"), lax.axis_index("c")
        self.j = self.p * self.cores + self.c
        self.used = 0

    def at_plane(self, j):
        return {"g": self.g, "p": j // self.cores, "c": j % self.cores}

    def at_chip(self, p):
        return {"g": self.g, "p": p, "c": self.c}

    def at_group(self, g):
        return {"g": g, "p": self.p, "c": self.c}

    def partner(self):
        return {"g": self.g, "p": self.p, "c": 1 - self.c}

    def plane_peer(self, d):
        return lax.rem(self.j + d, self.n_plane)

    def group_peer(self, d):
        return lax.rem(self.g + d, self.n_groups)

    def start(self, src, dst, device):
        copy = pltpu.make_async_remote_copy(
            src_ref=src,
            dst_ref=dst,
            send_sem=self.send.at[self.used],
            recv_sem=self.recv.at[self.used],
            device_id=device,
            device_id_type=MESH,
        )
        self.used += 1
        copy.start()
        return copy

    def at_device(self, index):
        return {"g": index // self.n_plane, **self.on_plane(lax.rem(index, self.n_plane))}

    def on_plane(self, j):
        return {"p": j // self.cores, "c": j % self.cores}

    def meet(self, heads=False, home=False):
        barrier = pltpu.get_barrier_semaphore()
        waits = self.n_plane - 1 + self.n_groups - 1
        if heads:
            mine = self.head_owner() == self.j
            part = lax.rem(self.g * self.n_plane + self.j, self.n_groups)
            for r in range(self.n_groups):

                @pl.when(jnp.logical_not(mine) | (part != r))
                def _():
                    source = self.at_device(self.n_groups * self.j + r)
                    pl.semaphore_signal(barrier, inc=1, device_id=source, device_id_type=MESH)

            waits = waits + jnp.where(mine, self.n_groups - 1, self.n_groups)
        if home:
            source = self.home_source()
            stays = source == self.g * self.n_plane + self.j

            @pl.when(jnp.logical_not(stays))
            def _():
                pl.semaphore_signal(
                    barrier, inc=1, device_id=self.at_device(source), device_id_type=MESH
                )

            waits = waits + jnp.where(stays, 0, 1)
        for d in range(1, self.n_plane):
            pl.semaphore_signal(
                barrier, inc=1, device_id=self.at_plane(self.plane_peer(d)), device_id_type=MESH
            )
        for d in range(1, self.n_groups):
            pl.semaphore_signal(
                barrier, inc=1, device_id=self.at_group(self.group_peer(d)), device_id_type=MESH
            )
        pl.semaphore_wait(barrier, waits)

    def home_source(self):
        index = self.g * self.n_plane + self.j
        return lax.rem(index, self.n_groups) * self.n_plane + index // self.n_groups

    def head_owner(self):
        return (self.g * self.n_plane + self.j) // self.n_groups


def sum_rows(dst, sources):
    rows = dst.shape[0]
    tile = 32 if rows % 32 == 0 else rows

    def step(i, carry):
        at = pl.ds(pl.multiple_of(i * tile, tile), tile)
        total = sources[0][at, :].astype(F32)
        for source in sources[1:]:
            total = total + source[at, :].astype(F32)
        dst[at, :] = total.astype(dst.dtype)
        return carry

    lax.fori_loop(0, rows // tile, step, 0)


def wait_all(copies):
    for copy in copies:
        copy.wait()


def wait_received(copies):
    for copy in copies:
        copy.wait_recv()


def wait_sent(copies):
    for copy in copies:
        copy.wait_send()


def plane_gather(w, src, out):
    chips = w.n_plane // w.cores
    first = [
        w.start(src, out.at[w.j], w.at_chip(lax.rem(w.p + d, chips))) for d in range(1, chips)
    ]
    second = [w.start(src, out.at[w.j], w.partner())]
    out[w.j] = src[...]
    yield
    for d in range(1, chips):
        first[d - 1].wait_recv()
        at = lax.rem(w.p + chips - d, chips) * w.cores + w.c
        second.append(w.start(out.at[at], out.at[at], w.partner()))
    yield
    wait_sent(first)
    wait_all(second)


def shift_gather(w, src, mid, out):
    copy = w.start(src, mid, w.at_group(lax.rem(w.g + 1, w.n_groups)))
    yield
    copy.wait()
    yield from plane_gather(w, mid, out)


def whole_gather(w, src, out):
    first = [
        w.start(src, out.at[w.g, w.j], w.at_group(w.group_peer(d))) for d in range(1, w.n_groups)
    ]
    out[w.g, w.j] = src[...]
    yield
    wait_received(first)
    second = [
        w.start(out.at[:, w.j], out.at[:, w.j], w.at_plane(w.plane_peer(d)))
        for d in range(1, w.n_plane)
    ]
    yield
    wait_sent(first)
    wait_all(second)


def plane_swap_gather(w, src, out):
    first = []
    for d in range(1, w.n_plane):
        to = w.plane_peer(d)
        first.append(w.start(src.at[to], out.at[w.g, w.j], w.at_plane(to)))
    out[w.g, w.j] = src[w.j]
    yield
    wait_received(first)
    second = [
        w.start(out.at[w.g], out.at[w.g], w.at_group(w.group_peer(d)))
        for d in range(1, w.n_groups)
    ]
    yield
    wait_sent(first)
    wait_all(second)


def head_rows(w, src, out):
    index = w.g * w.n_plane + w.j
    owner, part = w.head_owner(), lax.rem(index, w.n_groups)
    mine = owner == w.j

    def to(d):
        return pltpu.make_async_remote_copy(
            src_ref=src,
            dst_ref=out.at[part],
            send_sem=w.send.at[base + d],
            recv_sem=w.recv.at[base + part],
            device_id={"g": w.group_peer(d), **w.on_plane(owner)},
            device_id_type=MESH,
        )

    def arrival(r):
        return pltpu.make_async_remote_copy(
            src_ref=src,
            dst_ref=out.at[r],
            send_sem=w.send.at[base],
            recv_sem=w.recv.at[base + r],
            device_id=w.at_device(w.n_groups * w.j + r),
            device_id_type=MESH,
        )

    base = w.used
    w.used += w.n_groups
    for d in range(w.n_groups):

        @pl.when((d > 0) | jnp.logical_not(mine))
        def _():
            to(d).start()

    @pl.when(mine)
    def _():
        out[part] = src[...]

    yield
    for r in range(w.n_groups):

        @pl.when(jnp.logical_not(mine) | (part != r))
        def _():
            arrival(r).wait_recv()

    for d in range(w.n_groups):

        @pl.when((d > 0) | jnp.logical_not(mine))
        def _():
            to(d).wait_send()


def plane_swap(w, src, out):
    copies = []
    for d in range(1, w.n_plane):
        to = w.plane_peer(d)
        copies.append(w.start(src.at[to], out.at[w.j], w.at_plane(to)))
    out[w.j] = src[w.j]
    yield
    wait_all(copies)


def plane_sum(w, src, out, from_core, pairs, from_chips):
    chips = w.n_plane // w.cores
    first = []
    for d in range(chips):
        p = lax.rem(w.p + d, chips)
        first.append(w.start(src.at[p * w.cores + 1 - w.c], from_core.at[d], w.partner()))
    yield
    second = []
    for d in list(range(1, chips)) + [0]:
        p = lax.rem(w.p + d, chips)
        first[d].wait_recv()
        sum_rows(pairs.at[d], [src.at[p * w.cores + w.c], from_core.at[d]])
        if d:
            second.append(w.start(pairs.at[d], from_chips.at[d - 1], w.at_chip(p)))
    yield
    wait_received(second)
    sum_rows(out, [pairs.at[0]] + [from_chips.at[d] for d in range(chips - 1)])
    wait_sent(first)
    wait_sent(second)


def whole_sum(w, src, out, from_plane, total, parts):
    first = []
    for d in range(1, w.n_plane):
        to = w.plane_peer(d)
        first.append(w.start(src.at[:, to], from_plane.at[d - 1], w.at_plane(to)))
    yield
    wait_received(first)

    def step(i, carry):
        sum_rows(
            total.at[i], [src.at[i, w.j]] + [from_plane.at[d, i] for d in range(w.n_plane - 1)]
        )
        return carry

    lax.fori_loop(0, w.n_groups, step, 0)
    wait_sent(first)
    yield from group_sum(w, total, out, parts)


def whole_swap(w, src, out, mid):
    first = []
    for d in range(1, w.n_groups):
        to = w.group_peer(d)
        first.append(w.start(src.at[to], mid.at[w.g], w.at_group(to)))
    mid[w.g] = src[w.g]
    yield
    wait_received(first)
    second = []
    for d in range(1, w.n_plane):
        to = w.plane_peer(d)
        second.append(w.start(mid.at[:, to], out.at[:, w.j], w.at_plane(to)))
    out[:, w.j] = mid[:, w.j]
    yield
    wait_sent(first)
    wait_all(second)


def group_sum_home(w, src, out, parts, low, home):
    copies = []
    for d in range(1, w.n_groups):
        to = w.group_peer(d)
        copies.append(w.start(src.at[to], parts.at[d - 1], w.at_group(to)))
    yield
    wait_received(copies)
    sum_rows(low, [src.at[w.g]] + [parts.at[d] for d in range(w.n_groups - 1)])
    stays = w.home_source() == w.g * w.n_plane + w.j
    copy = pltpu.make_async_remote_copy(
        src_ref=low,
        dst_ref=home,
        send_sem=w.send.at[w.used],
        recv_sem=w.recv.at[w.used],
        device_id=w.at_device(w.n_groups * w.j + w.g),
        device_id_type=MESH,
    )
    w.used += 1

    @pl.when(jnp.logical_not(stays))
    def _():
        copy.start()

    @pl.when(stays)
    def _():
        home[...] = low[...]

    yield

    @pl.when(jnp.logical_not(stays))
    def _():
        copy.wait()

    out[...] = home[...].astype(F32)
    wait_sent(copies)


def plane_sum_shift(w, src, out, from_core, pairs, from_chips, low, later):
    rows = out.shape[0]
    yield from plane_sum(w, src, low, from_core, pairs, from_chips)
    copy = w.start(
        low.at[pl.ds(0, rows)], later, w.at_group(lax.rem(w.g + w.n_groups - 1, w.n_groups))
    )
    yield
    copy.wait()
    keep = jnp.where(w.g == w.n_groups - 1, 0.0, 1.0)
    out[...] = low[rows:, :].astype(F32) + later[...].astype(F32) * keep


def group_sum(w, src, out, parts):
    copies = []
    for d in range(1, w.n_groups):
        to = w.group_peer(d)
        copies.append(w.start(src.at[to], parts.at[d - 1], w.at_group(to)))
    yield
    wait_received(copies)
    sum_rows(out, [src.at[w.g]] + [parts.at[d] for d in range(w.n_groups - 1)])
    wait_sent(copies)


def group_sum_swap(w, src, out, total, parts):
    copies = []
    for d in range(1, w.n_groups):
        to = w.group_peer(d)
        copies.append(w.start(src.at[to], parts.at[d - 1], w.at_group(to)))
    yield
    wait_received(copies)

    def step(i, carry):
        sum_rows(total.at[i], [src.at[w.g, i]] + [parts.at[d, i] for d in range(w.n_groups - 1)])
        return carry

    lax.fori_loop(0, w.n_plane, step, 0)
    second = []
    for d in range(1, w.n_plane):
        to = w.plane_peer(d)
        second.append(w.start(total.at[to], out.at[w.j], w.at_plane(to)))
    out[w.j] = total[w.j]
    yield
    wait_sent(copies)
    wait_all(second)


ROUTINES = {
    "plane_gather": plane_gather,
    "shift_gather": shift_gather,
    "whole_gather": whole_gather,
    "plane_swap_gather": plane_swap_gather,
    "plane_swap": plane_swap,
    "plane_sum": plane_sum,
    "plane_sum_shift": plane_sum_shift,
    "head_rows": head_rows,
    "group_sum": group_sum,
    "whole_sum": whole_sum,
    "whole_swap": whole_swap,
    "group_sum_home": group_sum_home,
    "group_sum_swap": group_sum_swap,
}


def exchange_kernel(n_groups, n_plane, kinds, extra, *refs):
    count = len(kinds)
    sources, outs = refs[:count], refs[count : 2 * count]
    scratch = list(refs[2 * count : -2])
    w = Wires(n_groups, n_plane, refs[-2], refs[-1])
    w.meet("head_rows" in kinds, "group_sum_home" in kinds)
    running = []
    for kind, source, out, number in zip(kinds, sources, outs, extra):
        mine, scratch = scratch[:number], scratch[number:]
        if kind == "shift_gather":
            running.append(shift_gather(w, source, mine[0], out))
        else:
            running.append(ROUTINES[kind](w, source, out, *mine))
    while running:
        still = []
        for routine in running:
            try:
                next(routine)
                still.append(routine)
            except StopIteration:
                pass
        running = still


def exchange(n_groups, n_plane, number, *items):
    kinds = [kind for kind, _ in items]
    arrays = [array for _, array in items]
    shapes, scratch, extra = [], [], []
    chips = n_plane // 2
    for kind, array in items:
        shape, dtype = array.shape, array.dtype
        own = []
        if kind in ("plane_gather", "shift_gather"):
            out = (n_plane,) + shape
            if kind == "shift_gather":
                own = [shape]
        elif kind == "whole_gather":
            out = (n_groups, n_plane) + shape
        elif kind == "plane_swap_gather":
            out = (n_groups,) + shape
        elif kind == "plane_swap":
            out = shape
        elif kind == "head_rows":
            out = (n_groups,) + shape
        elif kind == "plane_sum_shift":
            pair = shape[1:]
            out = (shape[1] // 2, shape[2])
            own = [(chips,) + pair, (chips,) + pair, (chips - 1,) + pair, pair, out]
        elif kind == "plane_sum":
            out = shape[1:]
            own = [(chips,) + out, (chips,) + out, (chips - 1,) + out]
        elif kind == "group_sum_home":
            out = shape[1:]
            own = [(n_groups - 1,) + out, out, out]
        elif kind == "group_sum":
            out = shape[1:]
            own = [(n_groups - 1,) + out]
        elif kind == "whole_swap":
            out = shape
            own = [shape]
        elif kind == "whole_sum":
            out = shape[2:]
            own = [(n_plane - 1, n_groups) + out, (n_groups,) + out, (n_groups - 1,) + out]
        elif kind == "group_sum_swap":
            out = shape[1:]
            own = [out, (n_groups - 1,) + out]
        if kind in ("plane_sum", "plane_sum_shift", "group_sum", "group_sum_home", "whole_sum"):
            shapes.append(jax.ShapeDtypeStruct(out, F32))
        else:
            shapes.append(jax.ShapeDtypeStruct(out, dtype))
        scratch += [pltpu.VMEM(s, dtype) for s in own]
        extra.append(len(own))
    copies = 64 + 32 * len(items)
    vmem = pl.BlockSpec(memory_space=pltpu.VMEM)
    return pl.pallas_call(
        functools.partial(exchange_kernel, n_groups, n_plane, kinds, extra),
        out_shape=shapes,
        in_specs=[vmem] * len(items),
        out_specs=[vmem] * len(items),
        scratch_shapes=scratch
        + [pltpu.SemaphoreType.DMA((copies,)), pltpu.SemaphoreType.DMA((copies,))],
        compiler_params=pltpu.CompilerParams(
            collective_id=number,
            has_side_effects=True,
            vmem_limit_bytes=60 * 1024 * 1024,
        ),
        name="exchange_%d" % number,
    )(*arrays)


def gather_all(x):
    return lax.all_gather(x, ALL, axis=0, tiled=True)


class StreamSum:
    def __init__(self, w, steps, stage, from_core, pairs, from_chips, totals, parts, sems, credit):
        self.w, self.steps = w, steps
        self.stage, self.from_core, self.pairs = stage, from_core, pairs
        self.from_chips, self.totals, self.parts = from_chips, totals, parts
        self.core_sems, self.chip_sems, self.chip_recv, self.group_sems = sems
        self.credit = credit

    @staticmethod
    def chips(w, step):
        half = lax.rem(step, 2)
        beside = w.p + 1 - 2 * lax.rem(w.p, 2)
        above = w.p + 2 - 4 * (w.p // 2)
        return beside + half * (above - beside), 3 - w.p + half * (2 * w.p - 3)

    def core_copy(self, step, i):
        slot = lax.rem(step, 2)
        return pltpu.make_async_remote_copy(
            src_ref=self.stage.at[slot, 2 * i + 1 - self.w.c],
            dst_ref=self.from_core.at[slot, i],
            send_sem=self.core_sems.at[0, slot, i],
            recv_sem=self.core_sems.at[1, slot, i],
            device_id=self.w.partner(),
            device_id_type=MESH,
        )

    def part(self, ref, upper):
        rows = ref.shape[0] // 2
        return ref.at[pl.ds(rows, rows)] if upper else ref.at[pl.ds(0, rows)]

    def chip_copy(self, group_at, which):
        slot, i, upper, up = (
            (0, 0, False, False),
            (0, 1, False, False),
            (0, 1, True, True),
            (1, 0, True, True),
            (1, 0, False, True),
            (0, 0, True, False),
        )[which]
        p = self.w.p
        to = p + 2 - 4 * (p // 2) if up else p + 1 - 2 * lax.rem(p, 2)
        return pltpu.make_async_remote_copy(
            src_ref=self.part(self.pairs.at[slot, i], upper),
            dst_ref=self.from_chips.at[group_at, which],
            send_sem=self.chip_sems.at[which],
            recv_sem=self.chip_recv.at[group_at, which],
            device_id=self.w.at_chip(to),
            device_id_type=MESH,
        )

    def group_copy(self, group_at):
        return pltpu.make_async_remote_copy(
            src_ref=self.totals.at[group_at],
            dst_ref=self.parts.at[group_at],
            send_sem=self.group_sems.at[0, group_at],
            recv_sem=self.group_sems.at[1, group_at],
            device_id=self.w.at_group(self.w.group_peer(group_at + 1)),
            device_id_type=MESH,
        )

    def open_stage(self, step):
        @pl.when(step >= 2)
        def _():
            for i in range(2):
                self.core_copy(step, i).wait_send()

    def push(self, step):
        @pl.when(step >= 2)
        def _():
            pl.semaphore_wait(self.credit, 1)

        for i in range(2):
            self.core_copy(step, i).start()

    def merge(self, step):
        slot, group_at = lax.rem(step, 2), step // 2
        for half, sends in ((0, (0, 1, 2, 5)), (1, (3, 4))):

            @pl.when((slot == half) & (step >= 2))
            def _():
                for which in sends:
                    self.chip_copy(group_at, which).wait_send()

        for i in range(2):
            self.core_copy(step, i).wait_recv()
            sum_rows(
                self.pairs.at[slot, i],
                [self.stage.at[slot, 2 * i + self.w.c], self.from_core.at[slot, i]],
            )

        @pl.when(step + 2 < self.steps)
        def _():
            pl.semaphore_signal(
                self.credit, inc=1, device_id=self.w.partner(), device_id_type=MESH
            )

        @pl.when(slot == 0)
        def _():
            for which in (0, 1, 2):
                self.chip_copy(group_at, which).start()

        @pl.when(slot == 1)
        def _():
            self.chip_copy(group_at, 3).start()
            for source, i, upper, which in ((1, (1, 0), False, 4), (2, (0, 0), True, 5)):
                self.chip_copy(group_at, source).wait_recv()
                target = self.part(self.pairs.at[i], upper)
                sum_rows(target, [target, self.from_chips.at[group_at, source]])
                self.chip_copy(group_at, which).start()

    def plane_total(self, group_at):
        for which in (0, 3, 4, 5):
            self.chip_copy(group_at, which).wait_recv()
        return [
            [self.part(self.pairs.at[1, 1], upper)]
            + [self.from_chips.at[group_at, which] for which in arrived]
            for upper, arrived in ((False, (0, 4)), (True, (3, 5)))
        ]

    def advance(self, step):
        @pl.when(step >= 1)
        def _():
            last = step - 1

            @pl.when((lax.rem(last, 2) == 0) & (last >= 2))
            def _():
                group_at = last // 2 - 1
                for upper, sources in enumerate(self.plane_total(group_at)):
                    sum_rows(self.part(self.totals.at[group_at], upper), sources)
                self.group_copy(group_at).start()

            self.merge(last)

    def finish(self, out):
        steps = self.steps
        self.merge(steps - 1)
        groups = steps // 2 - 1
        halves = self.plane_total(groups)
        for d in range(groups):
            self.group_copy(d).wait_recv()
        for upper, sources in enumerate(halves):
            parts = [self.part(self.parts.at[d], upper) for d in range(groups)]
            sum_rows(self.part(out, upper), sources + parts)
        for d in range(groups):
            self.group_copy(d).wait_send()
        for i in range(2):
            self.core_copy(steps - 2, i).wait_send()
            self.core_copy(steps - 1, i).wait_send()
        for which in range(6):
            self.chip_copy(groups, which).wait_send()

    @staticmethod
    def scratch(n_groups, rows, width):
        dma = pltpu.SemaphoreType.DMA
        return [
            pltpu.VMEM((2, 4, rows, width), BF),
            pltpu.VMEM((2, 2, rows, width), BF),
            pltpu.VMEM((2, 2, rows, width), BF),
            pltpu.VMEM((n_groups, 6, rows // 2, width), BF),
            pltpu.VMEM((n_groups - 1, rows, width), BF),
            pltpu.VMEM((n_groups - 1, rows, width), BF),
            dma((2, 2, 2)),
            dma((6,)),
            dma((n_groups, 6)),
            dma((2, n_groups - 1)),
            pltpu.SemaphoreType.REGULAR,
        ]


def swiglu_both(gate, up, grad):
    sigmoid = 1.0 / (1.0 + jnp.exp(-gate))
    silu = gate * sigmoid
    return silu * up, grad * up * (sigmoid * (1.0 + gate * (1.0 - sigmoid))), grad * silu


def step_chips(w, step):
    group = lax.rem(w.g + 1 + step // 2, w.n_groups)
    return [group * 4 + chip for chip in StreamSum.chips(w, step)]


def hot_rows(place, rows, core, slot_count):
    mine = place[:, core * rows : (core + 1) * rows]
    return lax.broadcasted_iota(jnp.int32, (slot_count, rows), 0) == mine


def moe_kernel(
    n_groups, experts, first_logit, slot_count,
    h2_hbm, cot_hbm, place_ref, wg_ref, wu_ref, wd_ref, sc_ref, sd_ref,
    sum_ref, rows_ref, gin_ref, act_ref, gg_ref, gu_ref, rw_ref, sact_ref, sgrad_ref, tok_ref,
    h2_buf, cot_buf, load_sems, *comm,
):
    rows = sum_ref.shape[0]
    step, steps = pl.program_id(0), 2 * n_groups
    w = Wires(n_groups, 8, None, None)
    stream = StreamSum(w, steps, *comm[:6], comm[6:10], comm[10])
    expert_id = w.g * 4 + w.p
    half = sc_ref.shape[1] // 2

    def loads(at):
        slot = lax.rem(at, 2)
        for i, chip in enumerate(step_chips(w, at)):
            source = pl.ds(pl.multiple_of(chip * 2 * rows, 2 * rows), 2 * rows)
            target = pl.ds(i * 2 * rows, 2 * rows)
            for k, (hbm, buf) in enumerate(((h2_hbm, h2_buf), (cot_hbm, cot_buf))):
                yield pltpu.make_async_copy(
                    hbm.at[source], buf.at[slot, target], load_sems.at[slot, i, k]
                )

    @pl.when(step == 0)
    def _():
        for copy in loads(step):
            copy.start()
        w.meet()

    @pl.when(step + 1 < steps)
    def _():
        for copy in loads(step + 1):
            copy.start()

    for copy in loads(step):
        copy.wait()
    slot = lax.rem(step, 2)
    h2, cot = h2_buf[slot], cot_buf[slot]
    chips = step_chips(w, step)

    pre = jnp.dot(h2, sc_ref[...], preferred_element_type=F32)
    back = dot_nt(cot, sd_ref[...])
    gate, up = pre[:, :half], pre[:, half:]
    lane = lax.broadcasted_iota(jnp.int32, gate.shape, 1)
    logits = jnp.where((lane >= first_logit) & (lane < first_logit + experts), gate, -1e30)
    exps = jnp.exp(logits - jnp.max(logits, axis=1, keepdims=True))
    chosen = jnp.where(lane == first_logit + expert_id, exps, 0.0)
    weight = jnp.sum(chosen, axis=1, keepdims=True) / jnp.sum(exps, axis=1, keepdims=True)
    act, grad_gate, grad_up = swiglu_both(gate, up, back)
    shared_act = act.astype(BF)
    shared_grad = jnp.concatenate([grad_gate.astype(BF), grad_up.astype(BF)], axis=1)
    for i, chip in enumerate(chips):
        at = pl.ds(pl.multiple_of(chip * 2 * rows, 2 * rows), 2 * rows)
        sact_ref[at, :] = shared_act[i * 2 * rows : (i + 1) * 2 * rows]
        sgrad_ref[at, :] = shared_grad[i * 2 * rows : (i + 1) * 2 * rows]

    hots, weights = [], []
    for q in range(4):
        place = place_ref[pl.ds(chips[q // 2], 1), :]
        hot = hot_rows(place, rows, q % 2, slot_count).astype(F32)
        hots.append(hot)
        tokens = slice(q * rows, (q + 1) * rows)
        slots = slice(q * slot_count, (q + 1) * slot_count)
        low = hot.astype(BF)
        rows_ref[slots, :] = jnp.dot(low, h2[tokens], preferred_element_type=F32).astype(BF)
        gin_ref[slots, :] = jnp.dot(low, cot[tokens], preferred_element_type=F32).astype(BF)
        spread = jnp.broadcast_to(weight[tokens], (rows, 128))
        weights.append(
            jnp.dot(hot, spread, preferred_element_type=F32, precision=lax.Precision.HIGHEST)[:, :1]
        )
    row_weight = jnp.concatenate(weights, axis=0)
    rw_ref[...] = row_weight
    expert_rows = rows_ref[...]
    picked_cot = gin_ref[...]
    back = dot_nt(picked_cot, wd_ref[...])
    gin_ref[...] = (picked_cot.astype(F32) * row_weight).astype(BF)
    gate = jnp.dot(expert_rows, wg_ref[...], preferred_element_type=F32)
    up = jnp.dot(expert_rows, wu_ref[...], preferred_element_type=F32)
    act, grad_gate, grad_up = swiglu_both(gate, up, back * row_weight)
    act_low, grad_gate, grad_up = act.astype(BF), grad_gate.astype(BF), grad_up.astype(BF)
    act_ref[...] = act_low
    gg_ref[...] = grad_gate
    gu_ref[...] = grad_up
    picked = jnp.sum(act_low.astype(F32) * back, axis=1, keepdims=True)
    grad_rows = (dot_nt(grad_gate, wg_ref[...]) + dot_nt(grad_up, wu_ref[...])).astype(BF)
    stream.open_stage(step)
    for q in range(4):
        tokens = slice(q * rows, (q + 1) * rows)
        slots = slice(q * slot_count, (q + 1) * slot_count)
        tok_ref[pl.ds(chips[q // 2] * 2 + q % 2, 1), :] = jnp.sum(
            hots[q] * picked[slots], axis=0, keepdims=True
        )
        total = dot_tn(hots[q].astype(BF), grad_rows[slots]) + dot_nt(
            shared_grad[tokens], sc_ref[...]
        )
        stream.stage[slot, q] = total.astype(BF)
    stream.push(step)
    stream.advance(step)

    @pl.when(step == steps - 1)
    def _():
        stream.finish(sum_ref)


def out_kernel(
    n_groups, slot_count,
    act_ref, rw_ref, rows_ref, gin_ref, gg_ref, gu_ref, place_ref, sact_ref, wd_ref, sd_ref,
    sum_ref, dg_ref, du_ref, dd_ref, *comm,
):
    rows = sum_ref.shape[0]
    step, steps = pl.program_id(0), 2 * n_groups
    w = Wires(n_groups, 8, None, None)
    stream = StreamSum(w, steps, *comm[:6], comm[6:10], comm[10])

    @pl.when(step == 0)
    def _():
        w.meet()
        for ref in (dg_ref, du_ref, dd_ref):
            ref[...] = jnp.zeros_like(ref)

    slot = lax.rem(step, 2)
    chips = step_chips(w, step)
    out_rows = jnp.dot(act_ref[...], wd_ref[...], preferred_element_type=F32) * rw_ref[...]
    out_rows = out_rows.astype(BF)
    stream.open_stage(step)
    for q in range(4):
        chip = chips[q // 2]
        place = place_ref[pl.ds(chip, 1), :]
        low = hot_rows(place, rows, q % 2, slot_count).astype(F32).astype(BF)
        slots = slice(q * slot_count, (q + 1) * slot_count)
        shared = sact_ref[pl.ds(pl.multiple_of((chip * 2 + q % 2) * rows, rows), rows), :]
        total = dot_tn(low, out_rows[slots]) + jnp.dot(
            shared, sd_ref[...], preferred_element_type=F32
        )
        stream.stage[slot, q] = total.astype(BF)
    stream.push(step)
    stream.advance(step)

    width = rows_ref.shape[1]
    piece = width // 4
    for k in range(4):
        cols = slice(k * piece, (k + 1) * piece)
        turned = rows_ref[:, cols].T
        dg_ref[cols, :] += jnp.dot(turned, gg_ref[...], preferred_element_type=F32)
        du_ref[cols, :] += jnp.dot(turned, gu_ref[...], preferred_element_type=F32)
    turned = act_ref[...].T
    for k in range(4):
        cols = slice(k * piece, (k + 1) * piece)
        dd_ref[:, cols] += jnp.dot(turned, gin_ref[:, cols], preferred_element_type=F32)

    @pl.when(step == steps - 1)
    def _():
        stream.finish(sum_ref)


def experts_sums(
    n_groups, rows, h2, cot, place, slot_count, expert_w, shared_w, router_weight, first_id
):
    w_gate, w_up, w_down = expert_w
    s_both, s_down = shared_w
    tokens, width = h2.shape
    hidden, hidden_s = w_down.shape[0], s_down.shape[0]
    experts = router_weight.shape[1]
    steps = 2 * n_groups
    devices = tokens // rows
    step_slots = slot_count * 4
    all_slots = step_slots * steps
    half = 128
    s_cat = jnp.concatenate(
        [
            s_both[:, :hidden_s],
            router_weight,
            jnp.zeros((width, half - hidden_s - experts), BF),
            s_both[:, hidden_s:],
            jnp.zeros((width, half - hidden_s), BF),
        ],
        axis=1,
    )
    s_tall = jnp.pad(s_down, ((0, half - hidden_s), (0, 0)))

    def whole(array):
        return pl.BlockSpec(array.shape, lambda i: (0, 0), pipeline_mode=pl.Buffered(1))

    def blocked(rows, cols):
        return pl.BlockSpec((rows, cols), lambda i: (i, 0))

    shape = jax.ShapeDtypeStruct
    flops = 2 * all_slots * width * hidden * 5 + 2 * tokens * width * (4 * half + 3 * slot_count)
    shapes = [
        shape((rows, width), F32),
        shape((all_slots, width), BF),
        shape((all_slots, width), BF),
        shape((all_slots, hidden), BF),
        shape((all_slots, hidden), BF),
        shape((all_slots, hidden), BF),
        shape((all_slots, 1), F32),
        shape((tokens, half), BF),
        shape((tokens, 2 * half), BF),
        shape((devices, rows), F32),
    ]
    specs = [
        blocked(step_slots, s.shape[1]) if s.shape[0] == all_slots else whole(s) for s in shapes
    ]
    hbm = pl.BlockSpec(memory_space=pl.ANY)
    grad_h2, rows_in, grad_in, act, grad_gate, grad_up, row_weight, s_act, s_grad, token_grad = (
        pl.pallas_call(
            functools.partial(moe_kernel, n_groups, experts, hidden_s, slot_count),
            grid=(steps,),
            in_specs=[
                hbm,
                hbm,
                whole(place),
                whole(w_gate),
                whole(w_up),
                whole(w_down),
                whole(s_cat),
                whole(s_tall),
            ],
            out_specs=specs,
            out_shape=shapes,
            scratch_shapes=[
                pltpu.VMEM((2, 4 * rows, width), BF),
                pltpu.VMEM((2, 4 * rows, width), BF),
                pltpu.SemaphoreType.DMA((2, 2, 2)),
            ]
            + StreamSum.scratch(n_groups, rows, width),
            cost_estimate=pl.CostEstimate(
                flops=flops, bytes_accessed=12 * tokens * width, transcendentals=tokens * 1024
            ),
            compiler_params=pltpu.CompilerParams(
                collective_id=first_id,
                has_side_effects=True,
                vmem_limit_bytes=67043328,
            ),
            name="experts",
        )(h2, cot, place, w_gate, w_up, w_down, s_cat, s_tall)
    )
    shapes = [grad_h2] + [shape(x.shape, F32) for x in expert_w]
    out, d_gate, d_up, d_down = pl.pallas_call(
        functools.partial(out_kernel, n_groups, slot_count),
        grid=(steps,),
        in_specs=[
            blocked(step_slots, hidden),
            blocked(step_slots, 1),
            blocked(step_slots, width),
            blocked(step_slots, width),
            blocked(step_slots, hidden),
            blocked(step_slots, hidden),
            whole(place),
            whole(s_act),
            whole(w_down),
            whole(s_tall),
        ],
        out_specs=[whole(x) for x in shapes],
        out_shape=[shape(x.shape, F32) for x in shapes],
        scratch_shapes=StreamSum.scratch(n_groups, rows, width),
        cost_estimate=pl.CostEstimate(
            flops=2 * width * (4 * all_slots * hidden + tokens * (half + slot_count)),
            bytes_accessed=4 * tokens * width,
            transcendentals=0,
        ),
        compiler_params=pltpu.CompilerParams(
            collective_id=first_id + 1,
            has_side_effects=True,
            vmem_limit_bytes=67043328,
        ),
        name="expert_out",
    )(act, row_weight, rows_in, grad_in, grad_gate, grad_up, place, s_act, w_down, s_tall)
    g_both = dot_tn(h2, s_grad)
    g_both = jnp.concatenate([g_both[:, :hidden_s], g_both[:, half : half + hidden_s]], axis=1)
    grads = (
        d_gate,
        d_up,
        d_down,
        g_both,
        dot_tn(s_act, cot)[:hidden_s],
    )
    return out, grad_h2, token_grad, grads


def body(
    n_groups, n_plane, layer_input, attn_gain, w_query, w_latent, kv_gain, w_expand, w_output,
    ffn_gain, w_router, shared_gate, shared_up, shared_down, expert_gate, expert_up,
    expert_down, routes, segments, cotangent,
):
    tok, width = layer_input.shape
    devices = n_groups * n_plane
    experts = w_router.shape[1]
    local_heads = HEADS // n_plane
    scale = (NOPE + ROPE) ** (-0.5)
    group = lax.axis_index("g")
    place_in = lax.axis_index(PLANE)
    me = lax.axis_index(ALL)
    expert_id = lax.axis_index(("g", "p"))
    plane_tok = n_plane * tok
    plane_start = group * plane_tok

    rows_w = w_router.shape[0]
    kv_n = kv_gain.shape[0]
    small = jnp.concatenate(
        [
            attn_gain,
            ffn_gain,
            kv_gain,
            w_router.reshape(-1),
            routes.reshape(-1).astype(BF),
            segments.astype(BF),
        ]
    )
    small = jnp.pad(small, (0, -small.shape[0] % 4096)).reshape(-1, 128)
    head_cols = local_heads * (NOPE + ROPE)
    kv_cols = local_heads * (NOPE + VDIM)
    fold = kv_n * kv_cols // rows_w
    pair = jnp.concatenate(
        [
            w_query.reshape(rows_w, n_plane, head_cols).transpose(1, 0, 2),
            w_expand.reshape(kv_n, n_plane, kv_cols // fold, fold)
            .transpose(1, 0, 2, 3)
            .reshape(n_plane, rows_w, fold),
        ],
        axis=2,
    )
    swap = functools.partial(exchange, n_groups, n_plane)
    x_plane, small, latent_weight, pair = swap(
        0,
        ("plane_gather", layer_input),
        ("whole_gather", small),
        ("whole_gather", w_latent),
        ("plane_swap_gather", pair),
    )
    x_plane = x_plane.reshape(plane_tok, width).astype(F32)
    latent_weight = latent_weight.reshape(width, RANK + ROPE)
    pair = pair.reshape(width, head_cols + fold)
    small = small.reshape(devices, -1)
    cuts = [rows_w, 2 * rows_w, 2 * rows_w + kv_n, 2 * rows_w + kv_n + rows_w * experts]
    cuts = cuts + [cuts[-1] + tok * TOP, cuts[-1] + tok * TOP + tok]
    gain_one = small[:, : cuts[0]].reshape(-1).astype(F32)
    gain_two = small[:, cuts[0] : cuts[1]].reshape(-1).astype(F32)
    gain_kv = small[:, cuts[1] : cuts[2]].reshape(-1).astype(F32)
    router_weight = small[:, cuts[2] : cuts[3]].reshape(width, experts)
    routes_all = small[:, cuts[3] : cuts[4]].astype(jnp.int32).reshape(devices, tok, TOP)
    segments_all = small[:, cuts[4] : cuts[5]].astype(jnp.int32).reshape(-1)

    query_weight = pair[:, :head_cols].reshape(width, local_heads, NOPE + ROPE)
    wq_nope = query_weight[:, :, :NOPE].reshape(width, local_heads * NOPE)
    wq_rope = query_weight[:, :, NOPE:].reshape(width, local_heads * ROPE)
    expand_weight = pair[:, head_cols:].reshape(RANK, kv_cols)
    cotangent_later = lax.optimization_barrier((cotangent, x_plane))[0]

    shared_n = shared_down.shape[0]
    s_both = jnp.concatenate(
        [
            shared_gate.reshape(rows_w, devices, shared_n),
            shared_up.reshape(rows_w, devices, shared_n),
        ],
        axis=2,
    )
    s_both = lax.all_to_all(s_both, ALL, split_axis=1, concat_axis=0).reshape(width, 2 * shared_n)

    hidden = rms_norm(x_plane, gain_one).astype(BF)
    rope_half = ROPE // 2
    positions = plane_start + jnp.arange(plane_tok, dtype=jnp.int32)
    frequency = 10000.0 ** (-jnp.arange(rope_half, dtype=F32) / rope_half)
    angles = positions.astype(F32)[:, None] * frequency[None, :]
    cosine = jnp.cos(angles)
    sine_part = jnp.sin(angles)
    cos_h, sin_h = cosine[:, None, :], sine_part[:, None, :]
    latent = matmul(hidden, latent_weight)
    compressed_own = rms_norm(latent[:, :RANK], gain_kv).astype(BF)
    key_rope_own = rotate(latent[:, RANK:], cosine, sine_part).astype(BF)

    def own_rows(table):
        return lax.dynamic_slice_in_dim(table, place_in * tok, tok, 0)

    piece = own_rows(jnp.concatenate([compressed_own, key_rope_own], axis=1))
    before, own_output = swap(1, ("shift_gather", piece), ("head_rows", w_output))
    before = before.reshape(plane_tok, RANK + ROPE)
    own_output = own_output.reshape(local_heads * VDIM, width)
    compressed = jnp.concatenate([before[:, :RANK], compressed_own], axis=0)
    key_rope = jnp.concatenate([before[:, RANK:], key_rope_own], axis=0)
    q_nope = matmul(hidden, wq_nope).astype(BF)
    q_rope = rotate(
        matmul(hidden, wq_rope).reshape(plane_tok, local_heads, ROPE), cos_h, sin_h
    ).reshape(plane_tok, local_heads * ROPE).astype(BF)
    expanded = matmul(compressed, expand_weight).astype(BF)
    plane_segments = lax.dynamic_slice_in_dim(segments_all, plane_start, plane_tok, 0)
    doc_start = jnp.sum(
        (segments_all[None, :] < plane_segments[:, None]).astype(jnp.int32), axis=1, keepdims=True
    )
    low_bound = doc_start - plane_start + DOC_MAX
    mixed_heads, lse = attend(low_bound, q_nope, q_rope, expanded, key_rope, scale)
    attn_out = matmul(mixed_heads, own_output).astype(BF)
    attn_out = swap(2, ("plane_sum", attn_out.reshape(n_plane, tok, width)))[0]
    input_float = layer_input.astype(F32)
    residual_one = input_float + attn_out
    h_two_f, norm_two_back = jax.vjp(rms_norm, residual_one, gain_two)
    h_two = h_two_f.astype(BF)
    router_probs = softmax_rows(matmul(h_two, router_weight))

    expert_w = (expert_gate[0], expert_up[0], expert_down[0])
    shared_w = (s_both, shared_down)
    slot_limit = 2 * tok * TOP // experts

    def on_rows(h2, cot_gathered, routes_here):
        rows = h2.shape[0]
        h2_all = gather_all(h2)
        slot_count = min(slot_limit, rows)
        member = jnp.any(routes_here == expert_id, axis=2)
        member_int = member.astype(jnp.int32)
        rank = jnp.cumsum(member_int, axis=1) - member_int
        place = jnp.where(member, rank, -1).reshape(devices // 2, 2 * rows)
        out, grad_h2, token_grad, grads = experts_sums(
            n_groups,
            rows,
            h2_all,
            cot_gathered,
            place,
            slot_count,
            expert_w,
            shared_w,
            router_weight,
            8,
        )
        picked = lax.all_to_all(token_grad, ALL, split_axis=0, concat_axis=0, tiled=True)
        picked = jnp.sum(picked.reshape(experts, devices // experts, rows), axis=1).T
        return out, grad_h2, picked, grads

    parts = max(1, devices * tok // 4096)
    if parts == 1:
        cot_all = gather_all(cotangent_later)
        out_own, grad_h2_own, grad_router_probs, grads = on_rows(
            h_two, cot_all, routes_all
        )
    else:
        rows = tok // parts

        def step(total, inputs):
            h2, cot, routes_here = inputs
            cot_part = gather_all(cot)
            out, grad_h2, picked, grads = on_rows(h2, cot_part, routes_here)
            grads = lax.optimization_barrier(grads)
            total = tuple(a + b for a, b in zip(total, grads))
            return total, (out, grad_h2, picked)

        shapes = expert_w + shared_w
        grads, (out_own, grad_h2_own, grad_router_probs) = lax.scan(
            step,
            tuple(jnp.zeros(s.shape, F32) for s in shapes),
            (
                h_two.reshape(parts, rows, width),
                cotangent.reshape(parts, rows, width),
                routes_all.reshape(devices, parts, rows, TOP).transpose(1, 0, 2, 3),
            ),
        )
        out_own = out_own.reshape(tok, width)
        grad_h2_own = grad_h2_own.reshape(tok, width)
        grad_router_probs = grad_router_probs.reshape(tok, experts)
    g_gate, g_up, g_down, g_both, g_sdown = grads
    grad_logits = router_probs * (
        grad_router_probs - jnp.sum(router_probs * grad_router_probs, axis=1, keepdims=True)
    )
    grad_logits = grad_logits.astype(BF)
    grad_router = dot_tn(h_two, grad_logits)
    grad_h_two = grad_h2_own + dot_nt(grad_logits, router_weight)
    output = residual_one + out_own

    grad_x_one, grad_gain_two = norm_two_back(grad_h_two)
    grad_x_one = grad_x_one + cotangent.astype(F32)
    grad_attn_out = grad_x_one.astype(BF)
    plane_grad, g_shared = swap(
        3,
        ("plane_gather", grad_attn_out),
        ("whole_swap", g_both.astype(BF).reshape(n_groups, n_plane, rows_w, 2 * shared_n)),
    )
    plane_grad = plane_grad.reshape(plane_tok, width)
    grad_mixed = dot_nt(plane_grad, own_output).astype(BF)
    dqn, dqr, dex, dkr = attend_back(
        low_bound, q_nope, q_rope, expanded, key_rope, lse, grad_mixed, scale
    )

    g_output = dot_tn(mixed_heads, plane_grad).astype(BF).reshape(n_groups, rows_w, width)

    grad_expanded = dex.astype(BF)
    grad_expand = dot_tn(compressed, grad_expanded)
    grad_comp = dot_nt(grad_expanded, expand_weight)
    key_grads = jnp.concatenate([grad_comp, dkr], axis=1).astype(BF)
    key_grads = (
        key_grads.reshape(2, n_plane, tok, RANK + ROPE)
        .transpose(1, 0, 2, 3)
        .reshape(n_plane, 2 * tok, RANK + ROPE)
    )

    gq_nope = dqn.astype(BF)
    gq_rope = (
        unrotate(dqr.reshape(plane_tok, local_heads, ROPE), cos_h, sin_h)
        .reshape(plane_tok, local_heads * ROPE)
        .astype(BF)
    )
    grad_hidden = (dot_nt(gq_nope, wq_nope) + dot_nt(gq_rope, wq_rope)).astype(BF)
    gw_nope = dot_tn(hidden, gq_nope).astype(BF).reshape(n_groups, n_plane, rows_w, -1)
    gw_rope = dot_tn(hidden, gq_rope).astype(BF).reshape(n_groups, n_plane, rows_w, -1)
    g_expand = grad_expand.astype(BF).reshape(n_groups, n_plane, kv_n, kv_cols)
    key_grad, grad_hidden, gw_nope, gw_rope, g_expand = swap(
        4,
        ("plane_sum_shift", key_grads),
        ("plane_sum", grad_hidden.reshape(n_plane, tok, width)),
        ("group_sum_swap", gw_nope),
        ("group_sum_swap", gw_rope),
        ("group_sum_swap", g_expand),
    )
    latent_own = own_rows(latent)
    kv_norm_back = jax.vjp(rms_norm, latent_own[:, :RANK], gain_kv)[1]
    grad_comp_in, grad_gain_kv = kv_norm_back(key_grad[:, :RANK])
    grad_rope_in = unrotate(key_grad[:, RANK:], own_rows(cosine), own_rows(sine_part))
    grad_latent = jnp.concatenate([grad_comp_in, grad_rope_in], axis=1).astype(BF)

    def per_head(table, cols):
        return table.transpose(1, 0, 2).reshape(rows_w, HEADS, cols)

    grad_query_weight = jnp.concatenate(
        [per_head(gw_nope, NOPE), per_head(gw_rope, ROPE)], axis=2
    ).reshape(rows_w, -1).astype(F32)
    grad_expand_weight = g_expand.transpose(1, 0, 2).reshape(kv_n, -1).astype(F32)

    g_latent = dot_tn(own_rows(hidden), grad_latent).astype(BF)
    g_latent = g_latent.reshape(n_groups, n_plane, rows_w, RANK + ROPE)
    grad_hidden = grad_hidden + dot_nt(grad_latent, latent_weight)
    norm_one_back = jax.vjp(rms_norm, input_float, gain_one)[1]
    grad_x_norm, grad_gain_one = norm_one_back(grad_hidden)
    grad_input = grad_x_one + grad_x_norm

    small_grads = jnp.concatenate(
        [
            p.reshape(devices, -1)
            for p in (grad_gain_one, grad_gain_two, grad_gain_kv, grad_router)
        ],
        axis=1,
    )
    small_grads = jnp.pad(small_grads, ((0, 0), (0, -small_grads.shape[1] % 1024)))
    grad_latent_weight, grad_output_weight, small_grads = swap(
        6,
        ("whole_sum", g_latent),
        ("group_sum_home", g_output),
        ("whole_sum", small_grads.reshape(n_groups, n_plane, -1, 128)),
    )
    small_grads = small_grads.reshape(-1)
    g_shared = g_shared.transpose(2, 0, 1, 3).reshape(rows_w, devices, 2 * shared_n).astype(F32)
    grad_shared_gate = g_shared[:, :, :shared_n].reshape(rows_w, devices * shared_n)
    grad_shared_up = g_shared[:, :, shared_n:].reshape(rows_w, devices * shared_n)
    return (
        output,
        grad_input,
        small_grads[: cuts[0]],
        grad_query_weight,
        grad_latent_weight,
        small_grads[cuts[1] : cuts[2]],
        grad_expand_weight,
        grad_output_weight,
        small_grads[cuts[0] : cuts[1]],
        small_grads[cuts[2] : cuts[3]].reshape(rows_w, experts),
        grad_shared_gate,
        grad_shared_up,
        g_sdown,
        g_gate[None],
        g_up[None],
        g_down[None],
    )


def solution(mesh):
    n_expert, n_shard = mesh.shape["expert"], mesh.shape["wshard"]
    devices = n_expert * n_shard

    def program(*args):
        tok = args[0].shape[0] // devices
        n_plane = DOC_MAX // tok
        n_groups = devices // n_plane
        inner = Mesh(mesh.devices.reshape(n_groups, n_plane // n_shard, n_shard), ALL)
        rows, vector = P(ALL, None), P(ALL)
        wide, tall = P(("g", "p"), None, "c"), P(("g", "p"), "c", None)
        step = jax.shard_map(
            functools.partial(body, n_groups, n_plane),
            mesh=inner,
            in_specs=(
                rows, vector, rows, rows, vector, rows, rows, vector, rows, rows, rows, rows,
                wide, wide, tall, rows, vector, rows,
            ),
            out_specs=(
                rows, rows, vector, rows, rows, vector, rows, rows, vector, rows, rows, rows,
                rows, wide, wide, tall,
            ),
            check_vma=False,
        )
        return step(*args)

    return program
```

```python
import functools

import jax
import jax.numpy as jnp
from jax import lax
from jax.experimental import pallas as pl
from jax.experimental.pallas import tpu as pltpu
from jax.sharding import Mesh, PartitionSpec as P

HEADS = 16
NOPE = 128
ROPE = 64
VDIM = 128
RANK = 512
TOP = 6
DOC_MAX = 1024
QUERY_BLOCK = 256

BF = jnp.bfloat16
F32 = jnp.float32
ALL = ("g", "p", "c")
PLANE = ("p", "c")

epsilon = 1e-06


def rms_norm(vector, scaling):
    return vector * lax.rsqrt(jnp.mean(vector * vector, axis=-1, keepdims=True) + epsilon) * scaling


def rotate(vector, cosine, sine_part):
    half_width = vector.shape[-1] // 2
    front_half = vector[..., :half_width]
    back_half = vector[..., half_width:]
    return jnp.concatenate(
        [front_half * cosine - back_half * sine_part, back_half * cosine + front_half * sine_part],
        axis=-1,
    )


def unrotate(vector, cosine, sine_part):
    return rotate(vector, cosine, -sine_part)


def matmul(left, right):
    return jnp.dot(left, right, preferred_element_type=F32)


def dot_nt(left, right):
    return lax.dot_general(left, right, (((1,), (1,)), ((), ())), preferred_element_type=F32)


def dot_tn(left, right):
    return lax.dot_general(left, right, (((0,), (0,)), ((), ())), preferred_element_type=F32)


def swiglu(gate_pre, up_pre):
    return jax.nn.silu(gate_pre) * up_pre


def softmax_rows(scores):
    row_top = jnp.max(scores, axis=-1, keepdims=True)
    exp_scores = jnp.exp(scores - row_top)
    return exp_scores / jnp.sum(exp_scores, axis=-1, keepdims=True)


def masked_scores(base, low_bound, q_nope, q_rope, k_nope, k_rope, scale):
    rows, span = q_nope.shape[0], k_nope.shape[0]
    key_at = lax.broadcasted_iota(jnp.int32, (rows, span), 1) + base
    query_at = lax.broadcasted_iota(jnp.int32, (rows, span), 0) + (base + DOC_MAX)
    allowed = (key_at >= low_bound) & (key_at <= query_at)
    scores = (dot_nt(q_nope, k_nope) + dot_nt(q_rope, k_rope)) * scale
    return jnp.where(allowed, scores, -1e30)


def attend_kernel(heads, scale, low_ref, qn_ref, qr_ref, ex_ref, kr_ref, out_ref, lse_ref):
    rows = qn_ref.shape[0]
    base = pl.multiple_of(pl.program_id(0) * rows, rows)
    window = pl.ds(base, rows + DOC_MAX)
    k_rope = kr_ref[window, :]
    low_bound = low_ref[...]
    for h in range(heads):
        at = h * (NOPE + VDIM)
        k_nope = ex_ref[window, at : at + NOPE]
        value = ex_ref[window, at + NOPE : at + NOPE + VDIM]
        scores = masked_scores(
            base,
            low_bound,
            qn_ref[:, h * NOPE : (h + 1) * NOPE],
            qr_ref[:, h * ROPE : (h + 1) * ROPE],
            k_nope,
            k_rope,
            scale,
        )
        top = jnp.max(scores, axis=-1, keepdims=True)
        exps = jnp.exp(scores - top)
        total = jnp.sum(exps, axis=-1, keepdims=True)
        probs = (exps / total).astype(BF)
        out_ref[:, h * VDIM : (h + 1) * VDIM] = jnp.dot(
            probs, value, preferred_element_type=F32
        ).astype(BF)
        lse_ref[:, h : h + 1] = top + jnp.log(total)


def attend(low_bound, q_nope, q_rope, expanded, key_rope, scale):
    queries = q_nope.shape[0]
    heads = q_nope.shape[1] // NOPE
    rows = QUERY_BLOCK

    def whole(array):
        return pl.BlockSpec(array.shape, lambda i: (0, 0))

    def blocked(width):
        return pl.BlockSpec((rows, width), lambda i: (i, 0))

    flops = 2 * heads * queries * (rows + DOC_MAX) * (NOPE + ROPE + VDIM)
    return pl.pallas_call(
        functools.partial(attend_kernel, heads, scale),
        grid=(queries // rows,),
        in_specs=[
            blocked(1),
            blocked(heads * NOPE),
            blocked(heads * ROPE),
            whole(expanded),
            whole(key_rope),
        ],
        out_specs=[blocked(heads * VDIM), blocked(heads)],
        out_shape=[
            jax.ShapeDtypeStruct((queries, heads * VDIM), BF),
            jax.ShapeDtypeStruct((queries, heads), F32),
        ],
        cost_estimate=pl.CostEstimate(
            flops=flops, bytes_accessed=4 * expanded.size, transcendentals=flops // 640
        ),
        compiler_params=pltpu.CompilerParams(vmem_limit_bytes=50 * 1024 * 1024),
        name="attend",
    )(low_bound, q_nope, q_rope, expanded, key_rope)


def attend_back_kernel(
    heads, scale, low_ref, qn_ref, qr_ref, ex_ref, kr_ref, lse_ref, gm_ref,
    dqn_ref, dqr_ref, dex_ref, dkr_ref,
):
    rows = qn_ref.shape[0]
    step = pl.program_id(0)
    base = pl.multiple_of(step * rows, rows)
    window = pl.ds(base, rows + DOC_MAX)

    @pl.when(step == 0)
    def _():
        dex_ref[...] = jnp.zeros_like(dex_ref)
        dkr_ref[...] = jnp.zeros_like(dkr_ref)

    k_rope = kr_ref[window, :]
    low_bound = low_ref[...]
    for h in range(heads):
        at = h * (NOPE + VDIM)
        k_nope = ex_ref[window, at : at + NOPE]
        value = ex_ref[window, at + NOPE : at + NOPE + VDIM]
        q_nope = qn_ref[:, h * NOPE : (h + 1) * NOPE]
        q_rope = qr_ref[:, h * ROPE : (h + 1) * ROPE]
        grad_out = gm_ref[:, h * VDIM : (h + 1) * VDIM]
        scores = masked_scores(base, low_bound, q_nope, q_rope, k_nope, k_rope, scale)
        probs = jnp.exp(scores - lse_ref[:, h : h + 1])
        grad_probs = dot_nt(grad_out, value)
        mean_grad = jnp.sum(probs * grad_probs, axis=-1, keepdims=True)
        grad_scores = (probs * (grad_probs - mean_grad) * scale).astype(BF)
        probs_low = probs.astype(BF)
        dqn_ref[:, h * NOPE : (h + 1) * NOPE] = jnp.dot(
            grad_scores, k_nope, preferred_element_type=F32
        )
        dqr_ref[:, h * ROPE : (h + 1) * ROPE] = jnp.dot(
            grad_scores, k_rope, preferred_element_type=F32
        )
        dex_ref[window, at : at + NOPE] += dot_tn(grad_scores, q_nope)
        dex_ref[window, at + NOPE : at + NOPE + VDIM] += dot_tn(probs_low, grad_out)
        dkr_ref[window, :] += dot_tn(grad_scores, q_rope)


def attend_back(low_bound, q_nope, q_rope, expanded, key_rope, lse, grad_mixed, scale):
    queries = q_nope.shape[0]
    heads = q_nope.shape[1] // NOPE
    rows = QUERY_BLOCK

    def whole(shape):
        return pl.BlockSpec(shape, lambda i: (0, 0))

    def blocked(width):
        return pl.BlockSpec((rows, width), lambda i: (i, 0))

    flops = 2 * heads * queries * (rows + DOC_MAX) * (3 * NOPE + 3 * ROPE + 2 * VDIM)
    return pl.pallas_call(
        functools.partial(attend_back_kernel, heads, scale),
        grid=(queries // rows,),
        in_specs=[
            blocked(1),
            blocked(heads * NOPE),
            blocked(heads * ROPE),
            whole(expanded.shape),
            whole(key_rope.shape),
            blocked(heads),
            blocked(heads * VDIM),
        ],
        out_specs=[
            blocked(heads * NOPE),
            blocked(heads * ROPE),
            whole(expanded.shape),
            whole(key_rope.shape),
        ],
        out_shape=[
            jax.ShapeDtypeStruct(q_nope.shape, F32),
            jax.ShapeDtypeStruct(q_rope.shape, F32),
            jax.ShapeDtypeStruct(expanded.shape, F32),
            jax.ShapeDtypeStruct(key_rope.shape, F32),
        ],
        cost_estimate=pl.CostEstimate(
            flops=flops, bytes_accessed=8 * expanded.size, transcendentals=flops // 1664
        ),
        compiler_params=pltpu.CompilerParams(vmem_limit_bytes=56 * 1024 * 1024),
        name="attend_back",
    )(low_bound, q_nope, q_rope, expanded, key_rope, lse, grad_mixed)


MESH = pl.DeviceIdType.MESH


class Wires:
    def __init__(self, n_groups, n_plane, send, recv):
        self.n_groups, self.n_plane, self.send, self.recv = n_groups, n_plane, send, recv
        self.cores = 2
        self.g, self.p, self.c = lax.axis_index("g"), lax.axis_index("p"), lax.axis_index("c")
        self.j = self.p * self.cores + self.c
        self.used = 0

    def at_plane(self, j):
        return {"g": self.g, "p": j // self.cores, "c": j % self.cores}

    def at_chip(self, p):
        return {"g": self.g, "p": p, "c": self.c}

    def at_group(self, g):
        return {"g": g, "p": self.p, "c": self.c}

    def partner(self):
        return {"g": self.g, "p": self.p, "c": 1 - self.c}

    def beside(self):
        return self.p + 1 - 2 * lax.rem(self.p, 2)

    def above(self):
        return self.p + 2 - 4 * (self.p // 2)

    def core_of(self, p):
        return p * self.cores + self.c

    def plane_peer(self, d):
        return lax.rem(self.j + d, self.n_plane)

    def group_peer(self, d):
        return lax.rem(self.g + d, self.n_groups)

    def start(self, src, dst, device):
        copy = pltpu.make_async_remote_copy(
            src_ref=src,
            dst_ref=dst,
            send_sem=self.send.at[self.used],
            recv_sem=self.recv.at[self.used],
            device_id=device,
            device_id_type=MESH,
        )
        self.used += 1
        copy.start()
        return copy

    def at_device(self, index):
        return {"g": index // self.n_plane, **self.on_plane(lax.rem(index, self.n_plane))}

    def on_plane(self, j):
        return {"p": j // self.cores, "c": j % self.cores}

    def meet(self, heads=False, home=False):
        barrier = pltpu.get_barrier_semaphore()
        waits = self.n_plane - 1 + self.n_groups - 1
        if heads:
            mine = self.head_owner() == self.j
            part = lax.rem(self.g * self.n_plane + self.j, self.n_groups)
            for r in range(self.n_groups):

                @pl.when(jnp.logical_not(mine) | (part != r))
                def _():
                    source = self.at_device(self.n_groups * self.j + r)
                    pl.semaphore_signal(barrier, inc=1, device_id=source, device_id_type=MESH)

            waits = waits + jnp.where(mine, self.n_groups - 1, self.n_groups)
        if home:
            source = self.home_source()
            stays = source == self.g * self.n_plane + self.j

            @pl.when(jnp.logical_not(stays))
            def _():
                pl.semaphore_signal(
                    barrier, inc=1, device_id=self.at_device(source), device_id_type=MESH
                )

            waits = waits + jnp.where(stays, 0, 1)
        for d in range(1, self.n_plane):
            pl.semaphore_signal(
                barrier, inc=1, device_id=self.at_plane(self.plane_peer(d)), device_id_type=MESH
            )
        for d in range(1, self.n_groups):
            pl.semaphore_signal(
                barrier, inc=1, device_id=self.at_group(self.group_peer(d)), device_id_type=MESH
            )
        pl.semaphore_wait(barrier, waits)

    def home_source(self):
        index = self.g * self.n_plane + self.j
        return lax.rem(index, self.n_groups) * self.n_plane + index // self.n_groups

    def head_owner(self):
        return (self.g * self.n_plane + self.j) // self.n_groups


def sum_rows(dst, sources):
    rows = dst.shape[0]
    tile = 32 if rows % 32 == 0 else rows

    def step(i, carry):
        at = pl.ds(pl.multiple_of(i * tile, tile), tile)
        total = sources[0][at, :].astype(F32)
        for source in sources[1:]:
            total = total + source[at, :].astype(F32)
        dst[at, :] = total.astype(dst.dtype)
        return carry

    lax.fori_loop(0, rows // tile, step, 0)


def wait_all(copies):
    for copy in copies:
        copy.wait()


def wait_received(copies):
    for copy in copies:
        copy.wait_recv()


def wait_sent(copies):
    for copy in copies:
        copy.wait_send()


def part_of(ref, upper):
    rows = ref.shape[0] // 2
    return ref.at[pl.ds(rows, rows)] if upper else ref.at[pl.ds(0, rows)]


def spread(w, own, at):
    beside, above = w.at_chip(w.beside()), w.at_chip(w.above())
    mine = at(w.j)
    halves = [(part_of(own, u), part_of(mine, u)) for u in (0, 1)]
    lower = w.start(*halves[0], beside)
    upper = w.start(*halves[1], above)
    rest = [w.start(*halves[1], beside), w.start(*halves[0], above)]
    on_chip = [w.start(own, mine, w.partner())]
    yield
    lower.wait_recv()
    block = part_of(at(w.core_of(w.beside())), 0)
    rest.append(w.start(block, block, above))
    upper.wait_recv()
    block = part_of(at(w.core_of(w.above())), 1)
    rest.append(w.start(block, block, beside))
    yield
    wait_received(rest)
    for p in (w.beside(), w.above(), 3 - w.p):
        block = at(w.core_of(p))
        on_chip.append(w.start(block, block, w.partner()))
    yield
    wait_sent([lower, upper] + rest)
    wait_all(on_chip)


def plane_gather(w, src, out):
    out[w.j] = src[...]
    yield from spread(w, src, lambda j: out.at[j])


def far_gather(w, src, out, sem):
    mine = out.at[w.g, w.j]
    away = [w.start(src, mine, w.at_group(w.group_peer(d))) for d in range(1, w.n_groups)]
    local = pltpu.make_async_copy(src, mine, sem)
    local.start()
    running = [spread(w, src, lambda j: out.at[w.g, j])]
    next(running[0])
    for d in range(1, w.n_groups):
        away[d - 1].wait_recv()
        g = w.group_peer(w.n_groups - d)
        running.append(spread(w, out.at[g, w.j], lambda j, g=g: out.at[g, j]))
        next(running[d])
    for _ in range(3):
        for routine in running:
            next(routine, None)
        yield
    local.wait()
    wait_sent(away)


def shift_gather(w, src, mid, out):
    copy = w.start(src, mid, w.at_group(lax.rem(w.g + 1, w.n_groups)))
    yield
    copy.wait()
    yield from plane_gather(w, mid, out)


def whole_gather(w, src, out):
    chips = w.n_plane // w.cores
    first = [
        w.start(src, out.at[w.g, w.j], w.at_group(w.group_peer(d))) for d in range(1, w.n_groups)
    ]
    out[w.g, w.j] = src[...]
    yield
    wait_received(first)
    mine = out.at[:, w.j]
    second = [w.start(mine, mine, w.at_chip(lax.rem(w.p + d, chips))) for d in range(1, chips)]
    third = [w.start(mine, mine, w.partner())]
    yield
    for d in range(1, chips):
        second[d - 1].wait_recv()
        block = out.at[:, w.core_of(lax.rem(w.p + chips - d, chips))]
        third.append(w.start(block, block, w.partner()))
    yield
    wait_sent(first)
    wait_sent(second)
    wait_all(third)


def plane_swap_gather(w, src, out):
    first = []
    for d in range(1, w.n_plane):
        to = w.plane_peer(d)
        first.append(w.start(src.at[to], out.at[w.g, w.j], w.at_plane(to)))
    out[w.g, w.j] = src[w.j]
    yield
    wait_received(first)
    second = [
        w.start(out.at[w.g], out.at[w.g], w.at_group(w.group_peer(d)))
        for d in range(1, w.n_groups)
    ]
    yield
    wait_sent(first)
    wait_all(second)


def head_rows(w, src, out):
    index = w.g * w.n_plane + w.j
    owner, part = w.head_owner(), lax.rem(index, w.n_groups)
    mine = owner == w.j

    def to(d):
        return pltpu.make_async_remote_copy(
            src_ref=src,
            dst_ref=out.at[part],
            send_sem=w.send.at[base + d],
            recv_sem=w.recv.at[base + part],
            device_id={"g": w.group_peer(d), **w.on_plane(owner)},
            device_id_type=MESH,
        )

    def arrival(r):
        return pltpu.make_async_remote_copy(
            src_ref=src,
            dst_ref=out.at[r],
            send_sem=w.send.at[base],
            recv_sem=w.recv.at[base + r],
            device_id=w.at_device(w.n_groups * w.j + r),
            device_id_type=MESH,
        )

    base = w.used
    w.used += w.n_groups
    for d in range(w.n_groups):

        @pl.when((d > 0) | jnp.logical_not(mine))
        def _():
            to(d).start()

    @pl.when(mine)
    def _():
        out[part] = src[...]

    yield
    for r in range(w.n_groups):

        @pl.when(jnp.logical_not(mine) | (part != r))
        def _():
            arrival(r).wait_recv()

    for d in range(w.n_groups):

        @pl.when((d > 0) | jnp.logical_not(mine))
        def _():
            to(d).wait_send()


def plane_swap(w, src, out):
    copies = []
    for d in range(1, w.n_plane):
        to = w.plane_peer(d)
        copies.append(w.start(src.at[to], out.at[w.j], w.at_plane(to)))
    out[w.j] = src[w.j]
    yield
    wait_all(copies)


def plane_sum(w, src, out, from_core, pairs, from_chips):
    to = (w.beside(), 3 - w.p, w.above(), w.p)
    beside, above = w.at_chip(w.beside()), w.at_chip(w.above())
    first = [
        w.start(src.at[p * w.cores + 1 - w.c], from_core.at[i], w.partner())
        for i, p in enumerate(to)
    ]
    yield
    sent = []

    def send(i, upper, slot, device):
        sent.append(w.start(part_of(pairs.at[i], upper), from_chips.at[slot], device))

    for i, p in enumerate(to):
        first[i].wait_recv()
        sum_rows(pairs.at[i], [src.at[w.core_of(p)], from_core.at[i]])
        if i < 2:
            send(i, 0, i, beside)
        if i == 1:
            send(1, 1, 2, above)
        if i == 2:
            send(2, 1, 3, above)
    yield
    for wire, i, upper, slot, device in ((1, 2, 0, 4, above), (2, 0, 1, 5, beside)):
        sent[wire].wait_recv()
        target = part_of(pairs.at[i], upper)
        sum_rows(target, [target, from_chips.at[wire]])
        send(i, upper, slot, device)
    yield
    for wire in (0, 3, 4, 5):
        sent[wire].wait_recv()
    for upper, arrived in ((0, (0, 4)), (1, (3, 5))):
        sum_rows(
            part_of(out, upper),
            [part_of(pairs.at[3], upper)] + [from_chips.at[slot] for slot in arrived],
        )
    wait_sent(first)
    wait_sent(sent)


def whole_sum(w, src, out, from_core, pairs, from_chips, total, parts):
    chips = w.n_plane // w.cores
    to = [lax.rem(w.p + d, chips) for d in range(chips)]
    first = [
        w.start(src.at[:, p * w.cores + 1 - w.c], from_core.at[d], w.partner())
        for d, p in enumerate(to)
    ]
    yield
    second = []
    for d in list(range(1, chips)) + [0]:
        first[d].wait_recv()

        def step(i, carry):
            sum_rows(pairs.at[d, i], [src.at[i, w.core_of(to[d])], from_core.at[d, i]])
            return carry

        lax.fori_loop(0, w.n_groups, step, 0)
        if d:
            second.append(w.start(pairs.at[d], from_chips.at[d - 1], w.at_chip(to[d])))
    yield
    wait_received(second)

    def step(i, carry):
        sum_rows(total.at[i], [pairs.at[0, i]] + [from_chips.at[d, i] for d in range(chips - 1)])
        return carry

    lax.fori_loop(0, w.n_groups, step, 0)
    wait_sent(first)
    wait_sent(second)
    yield from group_sum(w, total, out, parts)


def whole_swap(w, src, out, mid):
    first = []
    for d in range(1, w.n_groups):
        to = w.group_peer(d)
        first.append(w.start(src.at[to], mid.at[w.g], w.at_group(to)))
    mid[w.g] = src[w.g]
    yield
    wait_received(first)
    second = []
    for d in range(1, w.n_plane):
        to = w.plane_peer(d)
        second.append(w.start(mid.at[:, to], out.at[:, w.j], w.at_plane(to)))
    out[:, w.j] = mid[:, w.j]
    yield
    wait_sent(first)
    wait_all(second)


def group_sum_home(w, src, out, parts, low, home):
    copies = []
    for d in range(1, w.n_groups):
        to = w.group_peer(d)
        copies.append(w.start(src.at[to], parts.at[d - 1], w.at_group(to)))
    yield
    wait_received(copies)
    sum_rows(low, [src.at[w.g]] + [parts.at[d] for d in range(w.n_groups - 1)])
    stays = w.home_source() == w.g * w.n_plane + w.j
    copy = pltpu.make_async_remote_copy(
        src_ref=low,
        dst_ref=home,
        send_sem=w.send.at[w.used],
        recv_sem=w.recv.at[w.used],
        device_id=w.at_device(w.n_groups * w.j + w.g),
        device_id_type=MESH,
    )
    w.used += 1

    @pl.when(jnp.logical_not(stays))
    def _():
        copy.start()

    @pl.when(stays)
    def _():
        home[...] = low[...]

    yield

    @pl.when(jnp.logical_not(stays))
    def _():
        copy.wait()

    out[...] = home[...].astype(F32)
    wait_sent(copies)


def plane_sum_shift(w, src, out, from_core, pairs, from_chips, low, later):
    rows = out.shape[0]
    yield from plane_sum(w, src, low, from_core, pairs, from_chips)
    copy = w.start(
        low.at[pl.ds(0, rows)], later, w.at_group(lax.rem(w.g + w.n_groups - 1, w.n_groups))
    )
    yield
    copy.wait()
    keep = jnp.where(w.g == w.n_groups - 1, 0.0, 1.0)
    out[...] = low[rows:, :].astype(F32) + later[...].astype(F32) * keep


def group_sum(w, src, out, parts):
    copies = []
    for d in range(1, w.n_groups):
        to = w.group_peer(d)
        copies.append(w.start(src.at[to], parts.at[d - 1], w.at_group(to)))
    yield
    wait_received(copies)
    sum_rows(out, [src.at[w.g]] + [parts.at[d] for d in range(w.n_groups - 1)])
    wait_sent(copies)


def group_sum_swap(w, src, out, total, parts):
    copies = []
    for d in range(1, w.n_groups):
        to = w.group_peer(d)
        copies.append(w.start(src.at[to], parts.at[d - 1], w.at_group(to)))
    yield
    wait_received(copies)

    def step(i, carry):
        sum_rows(total.at[i], [src.at[w.g, i]] + [parts.at[d, i] for d in range(w.n_groups - 1)])
        return carry

    lax.fori_loop(0, w.n_plane, step, 0)
    second = []
    for d in range(1, w.n_plane):
        to = w.plane_peer(d)
        second.append(w.start(total.at[to], out.at[w.j], w.at_plane(to)))
    out[w.j] = total[w.j]
    yield
    wait_sent(copies)
    wait_all(second)


ROUTINES = {
    "plane_gather": plane_gather,
    "shift_gather": shift_gather,
    "whole_gather": whole_gather,
    "far_gather": far_gather,
    "plane_swap_gather": plane_swap_gather,
    "plane_swap": plane_swap,
    "plane_sum": plane_sum,
    "plane_sum_shift": plane_sum_shift,
    "head_rows": head_rows,
    "group_sum": group_sum,
    "whole_sum": whole_sum,
    "whole_swap": whole_swap,
    "group_sum_home": group_sum_home,
    "group_sum_swap": group_sum_swap,
}


def exchange_kernel(n_groups, n_plane, kinds, extra, *refs):
    count = len(kinds)
    sources, outs = refs[:count], refs[count : 2 * count]
    scratch = list(refs[2 * count : -2])
    w = Wires(n_groups, n_plane, refs[-2], refs[-1])
    w.meet("head_rows" in kinds, "group_sum_home" in kinds)
    running = []
    for kind, source, out, number in zip(kinds, sources, outs, extra):
        mine, scratch = scratch[:number], scratch[number:]
        if kind == "shift_gather":
            running.append(shift_gather(w, source, mine[0], out))
        else:
            running.append(ROUTINES[kind](w, source, out, *mine))
    while running:
        still = []
        for routine in running:
            try:
                next(routine)
                still.append(routine)
            except StopIteration:
                pass
        running = still


def exchange(n_groups, n_plane, number, *items):
    kinds = [kind for kind, _ in items]
    arrays = [array for _, array in items]
    shapes, scratch, extra = [], [], []
    chips = n_plane // 2
    for kind, array in items:
        shape, dtype = array.shape, array.dtype
        own = []
        if kind in ("plane_gather", "shift_gather"):
            out = (n_plane,) + shape
            if kind == "shift_gather":
                own = [shape]
        elif kind in ("whole_gather", "far_gather"):
            out = (n_groups, n_plane) + shape
        elif kind == "plane_swap_gather":
            out = (n_groups,) + shape
        elif kind == "plane_swap":
            out = shape
        elif kind == "head_rows":
            out = (n_groups,) + shape
        elif kind == "plane_sum_shift":
            pair = shape[1:]
            out = (shape[1] // 2, shape[2])
            half = (pair[0] // 2, pair[1])
            own = [(chips,) + pair, (chips,) + pair, (6,) + half, pair, out]
        elif kind == "plane_sum":
            out = shape[1:]
            own = [(chips,) + out, (chips,) + out, (6, out[0] // 2, out[1])]
        elif kind == "group_sum_home":
            out = shape[1:]
            own = [(n_groups - 1,) + out, out, out]
        elif kind == "group_sum":
            out = shape[1:]
            own = [(n_groups - 1,) + out]
        elif kind == "whole_swap":
            out = shape
            own = [shape]
        elif kind == "whole_sum":
            out = shape[2:]
            full = (n_groups,) + out
            own = [(chips,) + full, (chips,) + full, (chips - 1,) + full, full]
            own = own + [(n_groups - 1,) + out]
        elif kind == "group_sum_swap":
            out = shape[1:]
            own = [out, (n_groups - 1,) + out]
        if kind in ("plane_sum", "plane_sum_shift", "group_sum", "group_sum_home", "whole_sum"):
            shapes.append(jax.ShapeDtypeStruct(out, F32))
        else:
            shapes.append(jax.ShapeDtypeStruct(out, dtype))
        scratch += [pltpu.VMEM(s, dtype) for s in own]
        if kind == "far_gather":
            own = [None]
            scratch.append(pltpu.SemaphoreType.DMA)
        extra.append(len(own))
    copies = 64 + 32 * len(items)
    vmem = pl.BlockSpec(memory_space=pltpu.VMEM)
    return pl.pallas_call(
        functools.partial(exchange_kernel, n_groups, n_plane, kinds, extra),
        out_shape=shapes,
        in_specs=[vmem] * len(items),
        out_specs=[
            pl.BlockSpec(memory_space=pl.ANY) if kind == "far_gather" else vmem for kind in kinds
        ],
        scratch_shapes=scratch
        + [pltpu.SemaphoreType.DMA((copies,)), pltpu.SemaphoreType.DMA((copies,))],
        compiler_params=pltpu.CompilerParams(
            collective_id=number,
            has_side_effects=True,
            vmem_limit_bytes=60 * 1024 * 1024,
        ),
        name="exchange_%d" % number,
    )(*arrays)


def gather_all(x):
    return lax.all_gather(x, ALL, axis=0, tiled=True)


class StreamSum:
    def __init__(self, w, steps, stage, from_core, pairs, from_chips, totals, parts, sems, credit):
        self.w, self.steps = w, steps
        self.stage, self.from_core, self.pairs = stage, from_core, pairs
        self.from_chips, self.totals, self.parts = from_chips, totals, parts
        self.core_sems, self.chip_sems, self.chip_recv, self.group_sems = sems
        self.credit = credit

    @staticmethod
    def chips(w, step):
        half = lax.rem(step, 2)
        beside = w.p + 1 - 2 * lax.rem(w.p, 2)
        above = w.p + 2 - 4 * (w.p // 2)
        return beside + half * (above - beside), 3 - w.p + half * (2 * w.p - 3)

    def core_copy(self, step, i):
        slot = lax.rem(step, 2)
        return pltpu.make_async_remote_copy(
            src_ref=self.stage.at[slot, 2 * i + 1 - self.w.c],
            dst_ref=self.from_core.at[slot, i],
            send_sem=self.core_sems.at[0, slot, i],
            recv_sem=self.core_sems.at[1, slot, i],
            device_id=self.w.partner(),
            device_id_type=MESH,
        )

    def part(self, ref, upper):
        rows = ref.shape[0] // 2
        return ref.at[pl.ds(rows, rows)] if upper else ref.at[pl.ds(0, rows)]

    def chip_copy(self, group_at, which):
        slot, i, upper, up = (
            (0, 0, False, False),
            (0, 1, False, False),
            (0, 1, True, True),
            (1, 0, True, True),
            (1, 0, False, True),
            (0, 0, True, False),
        )[which]
        p = self.w.p
        to = p + 2 - 4 * (p // 2) if up else p + 1 - 2 * lax.rem(p, 2)
        return pltpu.make_async_remote_copy(
            src_ref=self.part(self.pairs.at[slot, i], upper),
            dst_ref=self.from_chips.at[group_at, which],
            send_sem=self.chip_sems.at[which],
            recv_sem=self.chip_recv.at[group_at, which],
            device_id=self.w.at_chip(to),
            device_id_type=MESH,
        )

    def group_copy(self, group_at):
        return pltpu.make_async_remote_copy(
            src_ref=self.totals.at[group_at],
            dst_ref=self.parts.at[group_at],
            send_sem=self.group_sems.at[0, group_at],
            recv_sem=self.group_sems.at[1, group_at],
            device_id=self.w.at_group(self.w.group_peer(group_at + 1)),
            device_id_type=MESH,
        )

    def open_stage(self, step):
        @pl.when(step >= 2)
        def _():
            for i in range(2):
                self.core_copy(step, i).wait_send()

    def push(self, step):
        @pl.when(step >= 2)
        def _():
            pl.semaphore_wait(self.credit, 1)

        for i in range(2):
            self.core_copy(step, i).start()

    def merge(self, step):
        slot, group_at = lax.rem(step, 2), step // 2
        for half, sends in ((0, (0, 1, 2, 5)), (1, (3, 4))):

            @pl.when((slot == half) & (step >= 2))
            def _():
                for which in sends:
                    self.chip_copy(group_at, which).wait_send()

        for i in range(2):
            self.core_copy(step, i).wait_recv()
            sum_rows(
                self.pairs.at[slot, i],
                [self.stage.at[slot, 2 * i + self.w.c], self.from_core.at[slot, i]],
            )

        @pl.when(step + 2 < self.steps)
        def _():
            pl.semaphore_signal(
                self.credit, inc=1, device_id=self.w.partner(), device_id_type=MESH
            )

        @pl.when(slot == 0)
        def _():
            for which in (0, 1, 2):
                self.chip_copy(group_at, which).start()

        @pl.when(slot == 1)
        def _():
            self.chip_copy(group_at, 3).start()
            for source, i, upper, which in ((1, (1, 0), False, 4), (2, (0, 0), True, 5)):
                self.chip_copy(group_at, source).wait_recv()
                target = self.part(self.pairs.at[i], upper)
                sum_rows(target, [target, self.from_chips.at[group_at, source]])
                self.chip_copy(group_at, which).start()

    def plane_total(self, group_at):
        for which in (0, 3, 4, 5):
            self.chip_copy(group_at, which).wait_recv()
        return [
            [self.part(self.pairs.at[1, 1], upper)]
            + [self.from_chips.at[group_at, which] for which in arrived]
            for upper, arrived in ((False, (0, 4)), (True, (3, 5)))
        ]

    def advance(self, step):
        @pl.when(step >= 1)
        def _():
            last = step - 1

            @pl.when((lax.rem(last, 2) == 0) & (last >= 2))
            def _():
                group_at = last // 2 - 1
                for upper, sources in enumerate(self.plane_total(group_at)):
                    sum_rows(self.part(self.totals.at[group_at], upper), sources)
                self.group_copy(group_at).start()

            self.merge(last)

    def finish(self, out):
        steps = self.steps
        self.merge(steps - 1)
        groups = steps // 2 - 1
        halves = self.plane_total(groups)
        for d in range(groups):
            self.group_copy(d).wait_recv()
        for upper, sources in enumerate(halves):
            parts = [self.part(self.parts.at[d], upper) for d in range(groups)]
            sum_rows(self.part(out, upper), sources + parts)
        for d in range(groups):
            self.group_copy(d).wait_send()
        for i in range(2):
            self.core_copy(steps - 2, i).wait_send()
            self.core_copy(steps - 1, i).wait_send()
        for which in range(6):
            self.chip_copy(groups, which).wait_send()

    @staticmethod
    def scratch(n_groups, rows, width):
        dma = pltpu.SemaphoreType.DMA
        return [
            pltpu.VMEM((2, 4, rows, width), BF),
            pltpu.VMEM((2, 2, rows, width), BF),
            pltpu.VMEM((2, 2, rows, width), BF),
            pltpu.VMEM((n_groups, 6, rows // 2, width), BF),
            pltpu.VMEM((n_groups - 1, rows, width), BF),
            pltpu.VMEM((n_groups - 1, rows, width), BF),
            dma((2, 2, 2)),
            dma((6,)),
            dma((n_groups, 6)),
            dma((2, n_groups - 1)),
            pltpu.SemaphoreType.REGULAR,
        ]


def swiglu_both(gate, up, grad):
    sigmoid = 1.0 / (1.0 + jnp.exp(-gate))
    silu = gate * sigmoid
    return silu * up, grad * up * (sigmoid * (1.0 + gate * (1.0 - sigmoid))), grad * silu


def step_chips(w, step):
    group = lax.rem(w.g + 1 + step // 2, w.n_groups)
    return [group * 4 + chip for chip in StreamSum.chips(w, step)]


def hot_rows(place, rows, core, slot_count):
    mine = place[:, core * rows : (core + 1) * rows]
    return lax.broadcasted_iota(jnp.int32, (slot_count, rows), 0) == mine


def moe_kernel(
    n_groups, experts, first_logit, slot_count,
    h2_hbm, cot_hbm, place_ref, wg_ref, wu_ref, wd_ref, sc_ref, sd_ref,
    sum_ref, rows_ref, gin_ref, act_ref, gg_ref, gu_ref, rw_ref, sact_ref, sgrad_ref, tok_ref,
    h2_buf, cot_buf, load_sems, *comm,
):
    rows = sum_ref.shape[0]
    step, steps = pl.program_id(0), 2 * n_groups
    w = Wires(n_groups, 8, None, None)
    stream = StreamSum(w, steps, *comm[:6], comm[6:10], comm[10])
    expert_id = w.g * 4 + w.p
    half = sc_ref.shape[1] // 2

    def loads(at):
        slot = lax.rem(at, 2)
        for i, chip in enumerate(step_chips(w, at)):
            source = pl.ds(pl.multiple_of(chip * 2 * rows, 2 * rows), 2 * rows)
            target = pl.ds(i * 2 * rows, 2 * rows)
            for k, (hbm, buf) in enumerate(((h2_hbm, h2_buf), (cot_hbm, cot_buf))):
                yield pltpu.make_async_copy(
                    hbm.at[source], buf.at[slot, target], load_sems.at[slot, i, k]
                )

    @pl.when(step == 0)
    def _():
        for copy in loads(step):
            copy.start()
        w.meet()

    @pl.when(step + 1 < steps)
    def _():
        for copy in loads(step + 1):
            copy.start()

    for copy in loads(step):
        copy.wait()
    slot = lax.rem(step, 2)
    h2, cot = h2_buf[slot], cot_buf[slot]
    chips = step_chips(w, step)

    pre = jnp.dot(h2, sc_ref[...], preferred_element_type=F32)
    back = dot_nt(cot, sd_ref[...])
    gate, up = pre[:, :half], pre[:, half:]
    lane = lax.broadcasted_iota(jnp.int32, gate.shape, 1)
    logits = jnp.where((lane >= first_logit) & (lane < first_logit + experts), gate, -1e30)
    exps = jnp.exp(logits - jnp.max(logits, axis=1, keepdims=True))
    chosen = jnp.where(lane == first_logit + expert_id, exps, 0.0)
    weight = jnp.sum(chosen, axis=1, keepdims=True) / jnp.sum(exps, axis=1, keepdims=True)
    act, grad_gate, grad_up = swiglu_both(gate, up, back)
    shared_act = act.astype(BF)
    shared_grad = jnp.concatenate([grad_gate.astype(BF), grad_up.astype(BF)], axis=1)
    for i, chip in enumerate(chips):
        at = pl.ds(pl.multiple_of(chip * 2 * rows, 2 * rows), 2 * rows)
        sact_ref[at, :] = shared_act[i * 2 * rows : (i + 1) * 2 * rows]
        sgrad_ref[at, :] = shared_grad[i * 2 * rows : (i + 1) * 2 * rows]

    hots, weights = [], []
    for q in range(4):
        place = place_ref[pl.ds(chips[q // 2], 1), :]
        hot = hot_rows(place, rows, q % 2, slot_count).astype(F32)
        hots.append(hot)
        tokens = slice(q * rows, (q + 1) * rows)
        slots = slice(q * slot_count, (q + 1) * slot_count)
        low = hot.astype(BF)
        rows_ref[slots, :] = jnp.dot(low, h2[tokens], preferred_element_type=F32).astype(BF)
        gin_ref[slots, :] = jnp.dot(low, cot[tokens], preferred_element_type=F32).astype(BF)
        spread = jnp.broadcast_to(weight[tokens], (rows, 128))
        weights.append(
            jnp.dot(hot, spread, preferred_element_type=F32, precision=lax.Precision.HIGHEST)[:, :1]
        )
    row_weight = jnp.concatenate(weights, axis=0)
    rw_ref[...] = row_weight
    expert_rows = rows_ref[...]
    picked_cot = gin_ref[...]
    back = dot_nt(picked_cot, wd_ref[...])
    gin_ref[...] = (picked_cot.astype(F32) * row_weight).astype(BF)
    gate = jnp.dot(expert_rows, wg_ref[...], preferred_element_type=F32)
    up = jnp.dot(expert_rows, wu_ref[...], preferred_element_type=F32)
    act, grad_gate, grad_up = swiglu_both(gate, up, back * row_weight)
    act_low, grad_gate, grad_up = act.astype(BF), grad_gate.astype(BF), grad_up.astype(BF)
    act_ref[...] = act_low
    gg_ref[...] = grad_gate
    gu_ref[...] = grad_up
    picked = jnp.sum(act_low.astype(F32) * back, axis=1, keepdims=True)
    grad_rows = (dot_nt(grad_gate, wg_ref[...]) + dot_nt(grad_up, wu_ref[...])).astype(BF)
    stream.open_stage(step)
    for q in range(4):
        tokens = slice(q * rows, (q + 1) * rows)
        slots = slice(q * slot_count, (q + 1) * slot_count)
        tok_ref[pl.ds(chips[q // 2] * 2 + q % 2, 1), :] = jnp.sum(
            hots[q] * picked[slots], axis=0, keepdims=True
        )
        total = dot_tn(hots[q].astype(BF), grad_rows[slots]) + dot_nt(
            shared_grad[tokens], sc_ref[...]
        )
        stream.stage[slot, q] = total.astype(BF)
    stream.push(step)
    stream.advance(step)

    @pl.when(step == steps - 1)
    def _():
        stream.finish(sum_ref)


def out_kernel(
    n_groups, slot_count,
    act_ref, rw_ref, rows_ref, gin_ref, gg_ref, gu_ref, place_ref, sact_ref, wd_ref, sd_ref,
    sum_ref, dg_ref, du_ref, dd_ref, *comm,
):
    rows = sum_ref.shape[0]
    step, steps = pl.program_id(0), 2 * n_groups
    w = Wires(n_groups, 8, None, None)
    stream = StreamSum(w, steps, *comm[:6], comm[6:10], comm[10])

    @pl.when(step == 0)
    def _():
        w.meet()
        for ref in (dg_ref, du_ref, dd_ref):
            ref[...] = jnp.zeros_like(ref)

    slot = lax.rem(step, 2)
    chips = step_chips(w, step)
    out_rows = jnp.dot(act_ref[...], wd_ref[...], preferred_element_type=F32) * rw_ref[...]
    out_rows = out_rows.astype(BF)
    stream.open_stage(step)
    for q in range(4):
        chip = chips[q // 2]
        place = place_ref[pl.ds(chip, 1), :]
        low = hot_rows(place, rows, q % 2, slot_count).astype(F32).astype(BF)
        slots = slice(q * slot_count, (q + 1) * slot_count)
        shared = sact_ref[pl.ds(pl.multiple_of((chip * 2 + q % 2) * rows, rows), rows), :]
        total = dot_tn(low, out_rows[slots]) + jnp.dot(
            shared, sd_ref[...], preferred_element_type=F32
        )
        stream.stage[slot, q] = total.astype(BF)
    stream.push(step)
    stream.advance(step)

    width = rows_ref.shape[1]
    piece = width // 4
    for k in range(4):
        cols = slice(k * piece, (k + 1) * piece)
        turned = rows_ref[:, cols].T
        dg_ref[cols, :] += jnp.dot(turned, gg_ref[...], preferred_element_type=F32)
        du_ref[cols, :] += jnp.dot(turned, gu_ref[...], preferred_element_type=F32)
    turned = act_ref[...].T
    for k in range(4):
        cols = slice(k * piece, (k + 1) * piece)
        dd_ref[:, cols] += jnp.dot(turned, gin_ref[:, cols], preferred_element_type=F32)

    @pl.when(step == steps - 1)
    def _():
        stream.finish(sum_ref)


def experts_sums(
    n_groups, rows, h2, cot, place, slot_count, expert_w, shared_w, router_weight, first_id
):
    w_gate, w_up, w_down = expert_w
    s_both, s_down = shared_w
    tokens, width = h2.shape
    hidden, hidden_s = w_down.shape[0], s_down.shape[0]
    experts = router_weight.shape[1]
    steps = 2 * n_groups
    devices = tokens // rows
    step_slots = slot_count * 4
    all_slots = step_slots * steps
    half = 128
    s_cat = jnp.concatenate(
        [
            s_both[:, :hidden_s],
            router_weight,
            jnp.zeros((width, half - hidden_s - experts), BF),
            s_both[:, hidden_s:],
            jnp.zeros((width, half - hidden_s), BF),
        ],
        axis=1,
    )
    s_tall = jnp.pad(s_down, ((0, half - hidden_s), (0, 0)))

    def whole(array):
        return pl.BlockSpec(array.shape, lambda i: (0, 0), pipeline_mode=pl.Buffered(1))

    def blocked(rows, cols):
        return pl.BlockSpec((rows, cols), lambda i: (i, 0))

    shape = jax.ShapeDtypeStruct
    flops = 2 * all_slots * width * hidden * 5 + 2 * tokens * width * (4 * half + 3 * slot_count)
    shapes = [
        shape((rows, width), F32),
        shape((all_slots, width), BF),
        shape((all_slots, width), BF),
        shape((all_slots, hidden), BF),
        shape((all_slots, hidden), BF),
        shape((all_slots, hidden), BF),
        shape((all_slots, 1), F32),
        shape((tokens, half), BF),
        shape((tokens, 2 * half), BF),
        shape((devices, rows), F32),
    ]
    specs = [
        blocked(step_slots, s.shape[1]) if s.shape[0] == all_slots else whole(s) for s in shapes
    ]
    hbm = pl.BlockSpec(memory_space=pl.ANY)
    grad_h2, rows_in, grad_in, act, grad_gate, grad_up, row_weight, s_act, s_grad, token_grad = (
        pl.pallas_call(
            functools.partial(moe_kernel, n_groups, experts, hidden_s, slot_count),
            grid=(steps,),
            in_specs=[
                hbm,
                hbm,
                whole(place),
                whole(w_gate),
                whole(w_up),
                whole(w_down),
                whole(s_cat),
                whole(s_tall),
            ],
            out_specs=specs,
            out_shape=shapes,
            scratch_shapes=[
                pltpu.VMEM((2, 4 * rows, width), BF),
                pltpu.VMEM((2, 4 * rows, width), BF),
                pltpu.SemaphoreType.DMA((2, 2, 2)),
            ]
            + StreamSum.scratch(n_groups, rows, width),
            cost_estimate=pl.CostEstimate(
                flops=flops, bytes_accessed=12 * tokens * width, transcendentals=tokens * 1024
            ),
            compiler_params=pltpu.CompilerParams(
                collective_id=first_id,
                has_side_effects=True,
                vmem_limit_bytes=67043328,
            ),
            name="experts",
        )(h2, cot, place, w_gate, w_up, w_down, s_cat, s_tall)
    )
    shapes = [grad_h2] + [shape(x.shape, F32) for x in expert_w]
    out, d_gate, d_up, d_down = pl.pallas_call(
        functools.partial(out_kernel, n_groups, slot_count),
        grid=(steps,),
        in_specs=[
            blocked(step_slots, hidden),
            blocked(step_slots, 1),
            blocked(step_slots, width),
            blocked(step_slots, width),
            blocked(step_slots, hidden),
            blocked(step_slots, hidden),
            whole(place),
            whole(s_act),
            whole(w_down),
            whole(s_tall),
        ],
        out_specs=[whole(x) for x in shapes],
        out_shape=[shape(x.shape, F32) for x in shapes],
        scratch_shapes=StreamSum.scratch(n_groups, rows, width),
        cost_estimate=pl.CostEstimate(
            flops=2 * width * (4 * all_slots * hidden + tokens * (half + slot_count)),
            bytes_accessed=4 * tokens * width,
            transcendentals=0,
        ),
        compiler_params=pltpu.CompilerParams(
            collective_id=first_id + 1,
            has_side_effects=True,
            vmem_limit_bytes=67043328,
        ),
        name="expert_out",
    )(act, row_weight, rows_in, grad_in, grad_gate, grad_up, place, s_act, w_down, s_tall)
    g_both = dot_tn(h2, s_grad)
    g_both = jnp.concatenate([g_both[:, :hidden_s], g_both[:, half : half + hidden_s]], axis=1)
    grads = (
        d_gate,
        d_up,
        d_down,
        g_both,
        dot_tn(s_act, cot)[:hidden_s],
    )
    return out, grad_h2, token_grad, grads


def body(
    n_groups, n_plane, layer_input, attn_gain, w_query, w_latent, kv_gain, w_expand, w_output,
    ffn_gain, w_router, shared_gate, shared_up, shared_down, expert_gate, expert_up,
    expert_down, routes, segments, cotangent,
):
    tok, width = layer_input.shape
    devices = n_groups * n_plane
    experts = w_router.shape[1]
    local_heads = HEADS // n_plane
    scale = (NOPE + ROPE) ** (-0.5)
    group = lax.axis_index("g")
    place_in = lax.axis_index(PLANE)
    me = lax.axis_index(ALL)
    expert_id = lax.axis_index(("g", "p"))
    plane_tok = n_plane * tok
    plane_start = group * plane_tok

    rows_w = w_router.shape[0]
    kv_n = kv_gain.shape[0]
    small = jnp.concatenate(
        [
            attn_gain,
            ffn_gain,
            kv_gain,
            w_router.reshape(-1),
            routes.reshape(-1).astype(BF),
            segments.astype(BF),
        ]
    )
    small = jnp.pad(small, (0, -small.shape[0] % 4096)).reshape(-1, 128)
    head_cols = local_heads * (NOPE + ROPE)
    kv_cols = local_heads * (NOPE + VDIM)
    fold = kv_n * kv_cols // rows_w
    pair = jnp.concatenate(
        [
            w_query.reshape(rows_w, n_plane, head_cols).transpose(1, 0, 2),
            w_expand.reshape(kv_n, n_plane, kv_cols // fold, fold)
            .transpose(1, 0, 2, 3)
            .reshape(n_plane, rows_w, fold),
        ],
        axis=2,
    )
    swap = functools.partial(exchange, n_groups, n_plane)
    pair, latent_weight, small, x_plane = swap(
        0,
        ("plane_swap_gather", pair),
        ("whole_gather", w_latent),
        ("whole_gather", small),
        ("plane_gather", layer_input),
    )
    x_plane = x_plane.reshape(plane_tok, width).astype(F32)
    latent_weight = latent_weight.reshape(width, RANK + ROPE)
    pair = pair.reshape(width, head_cols + fold)
    small = small.reshape(devices, -1)
    cuts = [rows_w, 2 * rows_w, 2 * rows_w + kv_n, 2 * rows_w + kv_n + rows_w * experts]
    cuts = cuts + [cuts[-1] + tok * TOP, cuts[-1] + tok * TOP + tok]
    gain_one = small[:, : cuts[0]].reshape(-1).astype(F32)
    gain_two = small[:, cuts[0] : cuts[1]].reshape(-1).astype(F32)
    gain_kv = small[:, cuts[1] : cuts[2]].reshape(-1).astype(F32)
    router_weight = small[:, cuts[2] : cuts[3]].reshape(width, experts)
    routes_all = small[:, cuts[3] : cuts[4]].astype(jnp.int32).reshape(devices, tok, TOP)
    segments_all = small[:, cuts[4] : cuts[5]].astype(jnp.int32).reshape(-1)

    query_weight = pair[:, :head_cols].reshape(width, local_heads, NOPE + ROPE)
    wq_nope = query_weight[:, :, :NOPE].reshape(width, local_heads * NOPE)
    wq_rope = query_weight[:, :, NOPE:].reshape(width, local_heads * ROPE)
    expand_weight = pair[:, head_cols:].reshape(RANK, kv_cols)
    cotangent_later = lax.optimization_barrier((cotangent, x_plane))[0]

    shared_n = shared_down.shape[0]
    s_both = jnp.concatenate(
        [
            shared_gate.reshape(rows_w, devices, shared_n),
            shared_up.reshape(rows_w, devices, shared_n),
        ],
        axis=2,
    )
    s_both = lax.all_to_all(s_both, ALL, split_axis=1, concat_axis=0).reshape(width, 2 * shared_n)

    hidden = rms_norm(x_plane, gain_one).astype(BF)
    rope_half = ROPE // 2
    positions = plane_start + jnp.arange(plane_tok, dtype=jnp.int32)
    frequency = 10000.0 ** (-jnp.arange(rope_half, dtype=F32) / rope_half)
    angles = positions.astype(F32)[:, None] * frequency[None, :]
    cosine = jnp.cos(angles)
    sine_part = jnp.sin(angles)
    cos_h, sin_h = cosine[:, None, :], sine_part[:, None, :]
    latent = matmul(hidden, latent_weight)
    compressed_own = rms_norm(latent[:, :RANK], gain_kv).astype(BF)
    key_rope_own = rotate(latent[:, RANK:], cosine, sine_part).astype(BF)

    def own_rows(table):
        return lax.dynamic_slice_in_dim(table, place_in * tok, tok, 0)

    piece = own_rows(jnp.concatenate([compressed_own, key_rope_own], axis=1))
    before, own_output = swap(1, ("shift_gather", piece), ("head_rows", w_output))
    before = before.reshape(plane_tok, RANK + ROPE)
    own_output = own_output.reshape(local_heads * VDIM, width)
    compressed = jnp.concatenate([before[:, :RANK], compressed_own], axis=0)
    key_rope = jnp.concatenate([before[:, RANK:], key_rope_own], axis=0)
    q_nope = matmul(hidden, wq_nope).astype(BF)
    q_rope = rotate(
        matmul(hidden, wq_rope).reshape(plane_tok, local_heads, ROPE), cos_h, sin_h
    ).reshape(plane_tok, local_heads * ROPE).astype(BF)
    expanded = matmul(compressed, expand_weight).astype(BF)
    plane_segments = lax.dynamic_slice_in_dim(segments_all, plane_start, plane_tok, 0)
    doc_start = jnp.sum(
        (segments_all[None, :] < plane_segments[:, None]).astype(jnp.int32), axis=1, keepdims=True
    )
    low_bound = doc_start - plane_start + DOC_MAX
    mixed_heads, lse = attend(low_bound, q_nope, q_rope, expanded, key_rope, scale)
    attn_out = matmul(mixed_heads, own_output).astype(BF)
    attn_out = swap(2, ("plane_sum", attn_out.reshape(n_plane, tok, width)))[0]
    input_float = layer_input.astype(F32)
    residual_one = input_float + attn_out
    h_two_f, norm_two_back = jax.vjp(rms_norm, residual_one, gain_two)
    h_two = h_two_f.astype(BF)
    router_probs = softmax_rows(matmul(h_two, router_weight))

    expert_w = (expert_gate[0], expert_up[0], expert_down[0])
    shared_w = (s_both, shared_down)
    slot_limit = 2 * tok * TOP // experts

    def on_rows(h2, h2_all, cot_gathered, routes_here):
        rows = h2.shape[0]
        slot_count = min(slot_limit, rows)
        member = jnp.any(routes_here == expert_id, axis=2)
        member_int = member.astype(jnp.int32)
        rank = jnp.cumsum(member_int, axis=1) - member_int
        place = jnp.where(member, rank, -1).reshape(devices // 2, 2 * rows)
        out, grad_h2, token_grad, grads = experts_sums(
            n_groups,
            rows,
            h2_all,
            cot_gathered,
            place,
            slot_count,
            expert_w,
            shared_w,
            router_weight,
            8,
        )
        picked = lax.all_to_all(token_grad, ALL, split_axis=0, concat_axis=0, tiled=True)
        picked = jnp.sum(picked.reshape(experts, devices // experts, rows), axis=1).T
        return out, grad_h2, picked, grads

    parts = max(1, devices * tok // 4096)
    if parts == 1:
        cot_all = gather_all(cotangent_later)
        out_own, grad_h2_own, grad_router_probs, grads = on_rows(
            h_two, swap(5, ("far_gather", h_two))[0].reshape(-1, width), cot_all, routes_all
        )
    else:
        rows = tok // parts

        def step(total, inputs):
            h2, cot, routes_here = inputs
            cot_part = gather_all(cot)
            out, grad_h2, picked, grads = on_rows(h2, gather_all(h2), cot_part, routes_here)
            grads = lax.optimization_barrier(grads)
            total = tuple(a + b for a, b in zip(total, grads))
            return total, (out, grad_h2, picked)

        shapes = expert_w + shared_w
        grads, (out_own, grad_h2_own, grad_router_probs) = lax.scan(
            step,
            tuple(jnp.zeros(s.shape, F32) for s in shapes),
            (
                h_two.reshape(parts, rows, width),
                cotangent.reshape(parts, rows, width),
                routes_all.reshape(devices, parts, rows, TOP).transpose(1, 0, 2, 3),
            ),
        )
        out_own = out_own.reshape(tok, width)
        grad_h2_own = grad_h2_own.reshape(tok, width)
        grad_router_probs = grad_router_probs.reshape(tok, experts)
    g_gate, g_up, g_down, g_both, g_sdown = grads
    grad_logits = router_probs * (
        grad_router_probs - jnp.sum(router_probs * grad_router_probs, axis=1, keepdims=True)
    )
    grad_logits = grad_logits.astype(BF)
    grad_router = dot_tn(h_two, grad_logits)
    grad_h_two = grad_h2_own + dot_nt(grad_logits, router_weight)
    output = residual_one + out_own

    grad_x_one, grad_gain_two = norm_two_back(grad_h_two)
    grad_x_one = grad_x_one + cotangent.astype(F32)
    grad_attn_out = grad_x_one.astype(BF)
    g_shared, plane_grad = swap(
        3,
        ("whole_swap", g_both.astype(BF).reshape(n_groups, n_plane, rows_w, 2 * shared_n)),
        ("plane_gather", grad_attn_out),
    )
    plane_grad = plane_grad.reshape(plane_tok, width)
    grad_mixed = dot_nt(plane_grad, own_output).astype(BF)
    dqn, dqr, dex, dkr = attend_back(
        low_bound, q_nope, q_rope, expanded, key_rope, lse, grad_mixed, scale
    )

    g_output = dot_tn(mixed_heads, plane_grad).astype(BF).reshape(n_groups, rows_w, width)

    grad_expanded = dex.astype(BF)
    grad_expand = dot_tn(compressed, grad_expanded)
    grad_comp = dot_nt(grad_expanded, expand_weight)
    key_grads = jnp.concatenate([grad_comp, dkr], axis=1).astype(BF)
    key_grads = (
        key_grads.reshape(2, n_plane, tok, RANK + ROPE)
        .transpose(1, 0, 2, 3)
        .reshape(n_plane, 2 * tok, RANK + ROPE)
    )

    gq_nope = dqn.astype(BF)
    gq_rope = (
        unrotate(dqr.reshape(plane_tok, local_heads, ROPE), cos_h, sin_h)
        .reshape(plane_tok, local_heads * ROPE)
        .astype(BF)
    )
    grad_hidden = (dot_nt(gq_nope, wq_nope) + dot_nt(gq_rope, wq_rope)).astype(BF)
    gw_nope = dot_tn(hidden, gq_nope).astype(BF).reshape(n_groups, n_plane, rows_w, -1)
    gw_rope = dot_tn(hidden, gq_rope).astype(BF).reshape(n_groups, n_plane, rows_w, -1)
    g_expand = grad_expand.astype(BF).reshape(n_groups, n_plane, kv_n, kv_cols)
    key_grad, grad_hidden, gw_nope, gw_rope, g_expand = swap(
        4,
        ("plane_sum_shift", key_grads),
        ("plane_sum", grad_hidden.reshape(n_plane, tok, width)),
        ("group_sum_swap", gw_nope),
        ("group_sum_swap", gw_rope),
        ("group_sum_swap", g_expand),
    )
    latent_own = own_rows(latent)
    kv_norm_back = jax.vjp(rms_norm, latent_own[:, :RANK], gain_kv)[1]
    grad_comp_in, grad_gain_kv = kv_norm_back(key_grad[:, :RANK])
    grad_rope_in = unrotate(key_grad[:, RANK:], own_rows(cosine), own_rows(sine_part))
    grad_latent = jnp.concatenate([grad_comp_in, grad_rope_in], axis=1).astype(BF)

    def per_head(table, cols):
        return table.transpose(1, 0, 2).reshape(rows_w, HEADS, cols)

    grad_query_weight = jnp.concatenate(
        [per_head(gw_nope, NOPE), per_head(gw_rope, ROPE)], axis=2
    ).reshape(rows_w, -1).astype(F32)
    grad_expand_weight = g_expand.transpose(1, 0, 2).reshape(kv_n, -1).astype(F32)

    g_latent = dot_tn(own_rows(hidden), grad_latent).astype(BF)
    g_latent = g_latent.reshape(n_groups, n_plane, rows_w, RANK + ROPE)
    grad_hidden = grad_hidden + dot_nt(grad_latent, latent_weight)
    norm_one_back = jax.vjp(rms_norm, input_float, gain_one)[1]
    grad_x_norm, grad_gain_one = norm_one_back(grad_hidden)
    grad_input = grad_x_one + grad_x_norm

    small_grads = jnp.concatenate(
        [
            p.reshape(devices, -1)
            for p in (grad_gain_one, grad_gain_two, grad_gain_kv, grad_router)
        ],
        axis=1,
    )
    small_grads = jnp.pad(small_grads, ((0, 0), (0, -small_grads.shape[1] % 1024)))
    grad_latent_weight, grad_output_weight, small_grads = swap(
        6,
        ("whole_sum", g_latent),
        ("group_sum_home", g_output),
        ("whole_sum", small_grads.reshape(n_groups, n_plane, -1, 128)),
    )
    small_grads = small_grads.reshape(-1)
    g_shared = g_shared.transpose(2, 0, 1, 3).reshape(rows_w, devices, 2 * shared_n).astype(F32)
    grad_shared_gate = g_shared[:, :, :shared_n].reshape(rows_w, devices * shared_n)
    grad_shared_up = g_shared[:, :, shared_n:].reshape(rows_w, devices * shared_n)
    return (
        output,
        grad_input,
        small_grads[: cuts[0]],
        grad_query_weight,
        grad_latent_weight,
        small_grads[cuts[1] : cuts[2]],
        grad_expand_weight,
        grad_output_weight,
        small_grads[cuts[0] : cuts[1]],
        small_grads[cuts[2] : cuts[3]].reshape(rows_w, experts),
        grad_shared_gate,
        grad_shared_up,
        g_sdown,
        g_gate[None],
        g_up[None],
        g_down[None],
    )


def solution(mesh):
    n_expert, n_shard = mesh.shape["expert"], mesh.shape["wshard"]
    devices = n_expert * n_shard

    def program(*args):
        tok = args[0].shape[0] // devices
        n_plane = DOC_MAX // tok
        n_groups = devices // n_plane
        inner = Mesh(mesh.devices.reshape(n_groups, n_plane // n_shard, n_shard), ALL)
        rows, vector = P(ALL, None), P(ALL)
        wide, tall = P(("g", "p"), None, "c"), P(("g", "p"), "c", None)
        step = jax.shard_map(
            functools.partial(body, n_groups, n_plane),
            mesh=inner,
            in_specs=(
                rows, vector, rows, rows, vector, rows, rows, vector, rows, rows, rows, rows,
                wide, wide, tall, rows, vector, rows,
            ),
            out_specs=(
                rows, rows, vector, rows, rows, vector, rows, rows, vector, rows, rows, rows,
                rows, wide, wide, tall,
            ),
            check_vma=False,
        )
        return step(*args)

    return program
```

```python
import functools

import jax
import jax.numpy as jnp
from jax import lax
from jax.experimental import pallas as pl
from jax.experimental.pallas import tpu as pltpu
from jax.sharding import Mesh, PartitionSpec as P

HEADS = 16
NOPE = 128
ROPE = 64
VDIM = 128
RANK = 512
TOP = 6
DOC_MAX = 1024
QUERY_BLOCK = 256

BF = jnp.bfloat16
F32 = jnp.float32
ALL = ("g", "p", "c")
PLANE = ("p", "c")

epsilon = 1e-06


def rms_norm(vector, scaling):
    return vector * lax.rsqrt(jnp.mean(vector * vector, axis=-1, keepdims=True) + epsilon) * scaling


def rotate(vector, cosine, sine_part):
    half_width = vector.shape[-1] // 2
    front_half = vector[..., :half_width]
    back_half = vector[..., half_width:]
    return jnp.concatenate(
        [front_half * cosine - back_half * sine_part, back_half * cosine + front_half * sine_part],
        axis=-1,
    )


def unrotate(vector, cosine, sine_part):
    return rotate(vector, cosine, -sine_part)


def matmul(left, right):
    return jnp.dot(left, right, preferred_element_type=F32)


def dot_nt(left, right):
    return lax.dot_general(left, right, (((1,), (1,)), ((), ())), preferred_element_type=F32)


def dot_tn(left, right):
    return lax.dot_general(left, right, (((0,), (0,)), ((), ())), preferred_element_type=F32)


def swiglu(gate_pre, up_pre):
    return jax.nn.silu(gate_pre) * up_pre


def softmax_rows(scores):
    row_top = jnp.max(scores, axis=-1, keepdims=True)
    exp_scores = jnp.exp(scores - row_top)
    return exp_scores / jnp.sum(exp_scores, axis=-1, keepdims=True)


def masked_scores(base, low_bound, q_nope, q_rope, k_nope, k_rope, scale):
    rows, span = q_nope.shape[0], k_nope.shape[0]
    key_at = lax.broadcasted_iota(jnp.int32, (rows, span), 1) + base
    query_at = lax.broadcasted_iota(jnp.int32, (rows, span), 0) + (base + DOC_MAX)
    allowed = (key_at >= low_bound) & (key_at <= query_at)
    scores = (dot_nt(q_nope, k_nope) + dot_nt(q_rope, k_rope)) * scale
    return jnp.where(allowed, scores, -1e30)


def attend_kernel(heads, scale, low_ref, qn_ref, qr_ref, ex_ref, kr_ref, out_ref, lse_ref):
    rows = qn_ref.shape[0]
    base = pl.multiple_of(pl.program_id(0) * rows, rows)
    window = pl.ds(base, rows + DOC_MAX)
    k_rope = kr_ref[window, :]
    low_bound = low_ref[...]
    for h in range(heads):
        at = h * (NOPE + VDIM)
        k_nope = ex_ref[window, at : at + NOPE]
        value = ex_ref[window, at + NOPE : at + NOPE + VDIM]
        scores = masked_scores(
            base,
            low_bound,
            qn_ref[:, h * NOPE : (h + 1) * NOPE],
            qr_ref[:, h * ROPE : (h + 1) * ROPE],
            k_nope,
            k_rope,
            scale,
        )
        top = jnp.max(scores, axis=-1, keepdims=True)
        exps = jnp.exp(scores - top)
        total = jnp.sum(exps, axis=-1, keepdims=True)
        probs = (exps / total).astype(BF)
        out_ref[:, h * VDIM : (h + 1) * VDIM] = jnp.dot(
            probs, value, preferred_element_type=F32
        ).astype(BF)
        lse_ref[:, h : h + 1] = top + jnp.log(total)


def attend(low_bound, q_nope, q_rope, expanded, key_rope, scale):
    queries = q_nope.shape[0]
    heads = q_nope.shape[1] // NOPE
    rows = QUERY_BLOCK

    def whole(array):
        return pl.BlockSpec(array.shape, lambda i: (0, 0))

    def blocked(width):
        return pl.BlockSpec((rows, width), lambda i: (i, 0))

    flops = 2 * heads * queries * (rows + DOC_MAX) * (NOPE + ROPE + VDIM)
    return pl.pallas_call(
        functools.partial(attend_kernel, heads, scale),
        grid=(queries // rows,),
        in_specs=[
            blocked(1),
            blocked(heads * NOPE),
            blocked(heads * ROPE),
            whole(expanded),
            whole(key_rope),
        ],
        out_specs=[blocked(heads * VDIM), blocked(heads)],
        out_shape=[
            jax.ShapeDtypeStruct((queries, heads * VDIM), BF),
            jax.ShapeDtypeStruct((queries, heads), F32),
        ],
        cost_estimate=pl.CostEstimate(
            flops=flops, bytes_accessed=4 * expanded.size, transcendentals=flops // 640
        ),
        compiler_params=pltpu.CompilerParams(vmem_limit_bytes=50 * 1024 * 1024),
        name="attend",
    )(low_bound, q_nope, q_rope, expanded, key_rope)


def attend_back_kernel(
    heads, scale, low_ref, qn_ref, qr_ref, ex_ref, kr_ref, lse_ref, gm_ref,
    dqn_ref, dqr_ref, dex_ref, dkr_ref,
):
    rows = qn_ref.shape[0]
    step = pl.program_id(0)
    base = pl.multiple_of(step * rows, rows)
    window = pl.ds(base, rows + DOC_MAX)

    @pl.when(step == 0)
    def _():
        dex_ref[...] = jnp.zeros_like(dex_ref)
        dkr_ref[...] = jnp.zeros_like(dkr_ref)

    k_rope = kr_ref[window, :]
    low_bound = low_ref[...]
    for h in range(heads):
        at = h * (NOPE + VDIM)
        k_nope = ex_ref[window, at : at + NOPE]
        value = ex_ref[window, at + NOPE : at + NOPE + VDIM]
        q_nope = qn_ref[:, h * NOPE : (h + 1) * NOPE]
        q_rope = qr_ref[:, h * ROPE : (h + 1) * ROPE]
        grad_out = gm_ref[:, h * VDIM : (h + 1) * VDIM]
        scores = masked_scores(base, low_bound, q_nope, q_rope, k_nope, k_rope, scale)
        probs = jnp.exp(scores - lse_ref[:, h : h + 1])
        grad_probs = dot_nt(grad_out, value)
        mean_grad = jnp.sum(probs * grad_probs, axis=-1, keepdims=True)
        grad_scores = (probs * (grad_probs - mean_grad) * scale).astype(BF)
        probs_low = probs.astype(BF)
        dqn_ref[:, h * NOPE : (h + 1) * NOPE] = jnp.dot(
            grad_scores, k_nope, preferred_element_type=F32
        )
        dqr_ref[:, h * ROPE : (h + 1) * ROPE] = jnp.dot(
            grad_scores, k_rope, preferred_element_type=F32
        )
        dex_ref[window, at : at + NOPE] += dot_tn(grad_scores, q_nope)
        dex_ref[window, at + NOPE : at + NOPE + VDIM] += dot_tn(probs_low, grad_out)
        dkr_ref[window, :] += dot_tn(grad_scores, q_rope)


def attend_back(low_bound, q_nope, q_rope, expanded, key_rope, lse, grad_mixed, scale):
    queries = q_nope.shape[0]
    heads = q_nope.shape[1] // NOPE
    rows = QUERY_BLOCK

    def whole(shape):
        return pl.BlockSpec(shape, lambda i: (0, 0))

    def blocked(width):
        return pl.BlockSpec((rows, width), lambda i: (i, 0))

    flops = 2 * heads * queries * (rows + DOC_MAX) * (3 * NOPE + 3 * ROPE + 2 * VDIM)
    return pl.pallas_call(
        functools.partial(attend_back_kernel, heads, scale),
        grid=(queries // rows,),
        in_specs=[
            blocked(1),
            blocked(heads * NOPE),
            blocked(heads * ROPE),
            whole(expanded.shape),
            whole(key_rope.shape),
            blocked(heads),
            blocked(heads * VDIM),
        ],
        out_specs=[
            blocked(heads * NOPE),
            blocked(heads * ROPE),
            whole(expanded.shape),
            whole(key_rope.shape),
        ],
        out_shape=[
            jax.ShapeDtypeStruct(q_nope.shape, F32),
            jax.ShapeDtypeStruct(q_rope.shape, F32),
            jax.ShapeDtypeStruct(expanded.shape, F32),
            jax.ShapeDtypeStruct(key_rope.shape, F32),
        ],
        cost_estimate=pl.CostEstimate(
            flops=flops, bytes_accessed=8 * expanded.size, transcendentals=flops // 1664
        ),
        compiler_params=pltpu.CompilerParams(vmem_limit_bytes=56 * 1024 * 1024),
        name="attend_back",
    )(low_bound, q_nope, q_rope, expanded, key_rope, lse, grad_mixed)


MESH = pl.DeviceIdType.MESH


def pause(rounds):
    for _ in range(rounds):
        yield


class Wires:
    def __init__(self, n_groups, n_plane, send, recv):
        self.n_groups, self.n_plane, self.send, self.recv = n_groups, n_plane, send, recv
        self.cores = 2
        self.g, self.p, self.c = lax.axis_index("g"), lax.axis_index("p"), lax.axis_index("c")
        self.j = self.p * self.cores + self.c
        self.used = 0

    def at_plane(self, j):
        return {"g": self.g, "p": j // self.cores, "c": j % self.cores}

    def at_chip(self, p):
        return {"g": self.g, "p": p, "c": self.c}

    def at_group(self, g):
        return {"g": g, "p": self.p, "c": self.c}

    def partner(self):
        return {"g": self.g, "p": self.p, "c": 1 - self.c}

    def beside(self):
        return self.p + 1 - 2 * lax.rem(self.p, 2)

    def above(self):
        return self.p + 2 - 4 * (self.p // 2)

    def core_of(self, p):
        return p * self.cores + self.c

    def plane_peer(self, d):
        return lax.rem(self.j + d, self.n_plane)

    def group_peer(self, d):
        return lax.rem(self.g + d, self.n_groups)

    def start(self, src, dst, device):
        copy = pltpu.make_async_remote_copy(
            src_ref=src,
            dst_ref=dst,
            send_sem=self.send.at[self.used],
            recv_sem=self.recv.at[self.used],
            device_id=device,
            device_id_type=MESH,
        )
        self.used += 1
        copy.start()
        return copy

    def at_device(self, index):
        return {"g": index // self.n_plane, **self.on_plane(lax.rem(index, self.n_plane))}

    def on_plane(self, j):
        return {"p": j // self.cores, "c": j % self.cores}

    def meet(self, heads=False, home=False):
        barrier = pltpu.get_barrier_semaphore()
        waits = self.n_plane - 1 + self.n_groups - 1
        if heads:
            mine = self.head_owner() == self.j
            part = lax.rem(self.g * self.n_plane + self.j, self.n_groups)
            for r in range(self.n_groups):

                @pl.when(jnp.logical_not(mine) | (part != r))
                def _():
                    source = self.at_device(self.n_groups * self.j + r)
                    pl.semaphore_signal(barrier, inc=1, device_id=source, device_id_type=MESH)

            waits = waits + jnp.where(mine, self.n_groups - 1, self.n_groups)
        if home:
            source = self.home_source()
            stays = source == self.g * self.n_plane + self.j

            @pl.when(jnp.logical_not(stays))
            def _():
                pl.semaphore_signal(
                    barrier, inc=1, device_id=self.at_device(source), device_id_type=MESH
                )

            waits = waits + jnp.where(stays, 0, 1)
        for d in range(1, self.n_plane):
            pl.semaphore_signal(
                barrier, inc=1, device_id=self.at_plane(self.plane_peer(d)), device_id_type=MESH
            )
        for d in range(1, self.n_groups):
            pl.semaphore_signal(
                barrier, inc=1, device_id=self.at_group(self.group_peer(d)), device_id_type=MESH
            )
        pl.semaphore_wait(barrier, waits)

    def home_source(self):
        index = self.g * self.n_plane + self.j
        return lax.rem(index, self.n_groups) * self.n_plane + index // self.n_groups

    def head_owner(self):
        return (self.g * self.n_plane + self.j) // self.n_groups


def sum_rows(dst, sources):
    rows = dst.shape[0]
    tile = 32 if rows % 32 == 0 else rows

    def step(i, carry):
        at = pl.ds(pl.multiple_of(i * tile, tile), tile)
        total = sources[0][at, :].astype(F32)
        for source in sources[1:]:
            total = total + source[at, :].astype(F32)
        dst[at, :] = total.astype(dst.dtype)
        return carry

    lax.fori_loop(0, rows // tile, step, 0)


def wait_all(copies):
    for copy in copies:
        copy.wait()


def wait_received(copies):
    for copy in copies:
        copy.wait_recv()


def wait_sent(copies):
    for copy in copies:
        copy.wait_send()


def part_of(ref, upper):
    rows = ref.shape[0] // 2
    return ref.at[pl.ds(rows, rows)] if upper else ref.at[pl.ds(0, rows)]


def spread(w, own, at):
    beside, above = w.at_chip(w.beside()), w.at_chip(w.above())
    mine = at(w.j)
    halves = [(part_of(own, u), part_of(mine, u)) for u in (0, 1)]
    lower = w.start(*halves[0], beside)
    upper = w.start(*halves[1], above)
    rest = [w.start(*halves[1], beside), w.start(*halves[0], above)]
    on_chip = [w.start(own, mine, w.partner())]
    yield
    lower.wait_recv()
    block = part_of(at(w.core_of(w.beside())), 0)
    rest.append(w.start(block, block, above))
    upper.wait_recv()
    block = part_of(at(w.core_of(w.above())), 1)
    rest.append(w.start(block, block, beside))
    yield
    wait_received(rest)
    for p in (w.beside(), w.above(), 3 - w.p):
        block = at(w.core_of(p))
        on_chip.append(w.start(block, block, w.partner()))
    yield
    wait_sent([lower, upper] + rest)
    wait_all(on_chip)


def plane_gather(w, src, out):
    out[w.j] = src[...]
    yield from spread(w, src, lambda j: out.at[j])


def far_gather(w, src, out, sem):
    mine = out.at[w.g, w.j]
    away = [w.start(src, mine, w.at_group(w.group_peer(d))) for d in range(1, w.n_groups)]
    local = pltpu.make_async_copy(src, mine, sem)
    local.start()
    running = [spread(w, src, lambda j: out.at[w.g, j])]
    next(running[0])
    for d in range(1, w.n_groups):
        away[d - 1].wait_recv()
        g = w.group_peer(w.n_groups - d)
        running.append(spread(w, out.at[g, w.j], lambda j, g=g: out.at[g, j]))
        next(running[d])
    for _ in range(3):
        for routine in running:
            next(routine, None)
        yield
    local.wait()
    wait_sent(away)


def shift_gather(w, src, mid, out):
    copy = w.start(src, mid, w.at_group(lax.rem(w.g + 1, w.n_groups)))
    yield
    copy.wait()
    yield from plane_gather(w, mid, out)


def whole_gather(w, src, out):
    chips = w.n_plane // w.cores
    first = [
        w.start(src, out.at[w.g, w.j], w.at_group(w.group_peer(d))) for d in range(1, w.n_groups)
    ]
    out[w.g, w.j] = src[...]
    yield
    wait_received(first)
    mine = out.at[:, w.j]
    second = [w.start(mine, mine, w.at_chip(lax.rem(w.p + d, chips))) for d in range(1, chips)]
    third = [w.start(mine, mine, w.partner())]
    yield
    for d in range(1, chips):
        second[d - 1].wait_recv()
        block = out.at[:, w.core_of(lax.rem(w.p + chips - d, chips))]
        third.append(w.start(block, block, w.partner()))
    yield
    wait_sent(first)
    wait_sent(second)
    wait_all(third)


def plane_swap_gather(w, src, out):
    first = []
    for d in range(1, w.n_plane):
        to = w.plane_peer(d)
        first.append(w.start(src.at[to], out.at[w.g, w.j], w.at_plane(to)))
    out[w.g, w.j] = src[w.j]
    yield
    wait_received(first)
    second = [
        w.start(out.at[w.g], out.at[w.g], w.at_group(w.group_peer(d)))
        for d in range(1, w.n_groups)
    ]
    yield from pause(4)
    wait_sent(first)
    wait_all(second)


def head_rows(w, src, out):
    index = w.g * w.n_plane + w.j
    owner, part = w.head_owner(), lax.rem(index, w.n_groups)
    mine = owner == w.j

    def to(d):
        return pltpu.make_async_remote_copy(
            src_ref=src,
            dst_ref=out.at[part],
            send_sem=w.send.at[base + d],
            recv_sem=w.recv.at[base + part],
            device_id={"g": w.group_peer(d), **w.on_plane(owner)},
            device_id_type=MESH,
        )

    def arrival(r):
        return pltpu.make_async_remote_copy(
            src_ref=src,
            dst_ref=out.at[r],
            send_sem=w.send.at[base],
            recv_sem=w.recv.at[base + r],
            device_id=w.at_device(w.n_groups * w.j + r),
            device_id_type=MESH,
        )

    yield from pause(3)
    base = w.used
    w.used += w.n_groups
    for d in range(w.n_groups):

        @pl.when((d > 0) | jnp.logical_not(mine))
        def _():
            to(d).start()

    @pl.when(mine)
    def _():
        out[part] = src[...]

    yield from pause(2)
    for r in range(w.n_groups):

        @pl.when(jnp.logical_not(mine) | (part != r))
        def _():
            arrival(r).wait_recv()

    for d in range(w.n_groups):

        @pl.when((d > 0) | jnp.logical_not(mine))
        def _():
            to(d).wait_send()


def plane_swap(w, src, out):
    copies = []
    for d in range(1, w.n_plane):
        to = w.plane_peer(d)
        copies.append(w.start(src.at[to], out.at[w.j], w.at_plane(to)))
    out[w.j] = src[w.j]
    yield
    wait_all(copies)


def plane_sum(w, src, out, from_core, pairs, from_chips):
    to = (w.beside(), 3 - w.p, w.above(), w.p)
    beside, above = w.at_chip(w.beside()), w.at_chip(w.above())
    first = [
        w.start(src.at[p * w.cores + 1 - w.c], from_core.at[i], w.partner())
        for i, p in enumerate(to)
    ]
    yield
    sent = []

    def send(i, upper, slot, device):
        sent.append(w.start(part_of(pairs.at[i], upper), from_chips.at[slot], device))

    for i, p in enumerate(to):
        first[i].wait_recv()
        sum_rows(pairs.at[i], [src.at[w.core_of(p)], from_core.at[i]])
        if i < 2:
            send(i, 0, i, beside)
        if i == 1:
            send(1, 1, 2, above)
        if i == 2:
            send(2, 1, 3, above)
    yield
    for wire, i, upper, slot, device in ((1, 2, 0, 4, above), (2, 0, 1, 5, beside)):
        sent[wire].wait_recv()
        target = part_of(pairs.at[i], upper)
        sum_rows(target, [target, from_chips.at[wire]])
        send(i, upper, slot, device)
    yield
    for wire in (0, 3, 4, 5):
        sent[wire].wait_recv()
    for upper, arrived in ((0, (0, 4)), (1, (3, 5))):
        sum_rows(
            part_of(out, upper),
            [part_of(pairs.at[3], upper)] + [from_chips.at[slot] for slot in arrived],
        )
    wait_sent(first)
    wait_sent(sent)


def whole_sum(w, src, out, from_core, pairs, from_chips, total, parts):
    chips = w.n_plane // w.cores
    to = [lax.rem(w.p + d, chips) for d in range(chips)]
    first = [
        w.start(src.at[:, p * w.cores + 1 - w.c], from_core.at[d], w.partner())
        for d, p in enumerate(to)
    ]
    yield
    second = []
    for d in list(range(1, chips)) + [0]:
        first[d].wait_recv()

        def step(i, carry):
            sum_rows(pairs.at[d, i], [src.at[i, w.core_of(to[d])], from_core.at[d, i]])
            return carry

        lax.fori_loop(0, w.n_groups, step, 0)
        if d:
            second.append(w.start(pairs.at[d], from_chips.at[d - 1], w.at_chip(to[d])))
    yield
    wait_received(second)

    def step(i, carry):
        sum_rows(total.at[i], [pairs.at[0, i]] + [from_chips.at[d, i] for d in range(chips - 1)])
        return carry

    lax.fori_loop(0, w.n_groups, step, 0)
    wait_sent(first)
    wait_sent(second)
    yield from group_sum(w, total, out, parts)


def whole_swap(w, src, out, mid):
    first = []
    for d in range(1, w.n_groups):
        to = w.group_peer(d)
        first.append(w.start(src.at[to], mid.at[w.g], w.at_group(to)))
    mid[w.g] = src[w.g]
    yield from pause(3)
    wait_received(first)
    second = []
    for d in range(1, w.n_plane):
        to = w.plane_peer(d)
        second.append(w.start(mid.at[:, to], out.at[:, w.j], w.at_plane(to)))
    out[:, w.j] = mid[:, w.j]
    yield
    wait_sent(first)
    wait_all(second)


def group_sum_home(w, src, out, parts, low, home):
    copies = []
    for d in range(1, w.n_groups):
        to = w.group_peer(d)
        copies.append(w.start(src.at[to], parts.at[d - 1], w.at_group(to)))
    yield from pause(3)
    wait_received(copies)
    sum_rows(low, [src.at[w.g]] + [parts.at[d] for d in range(w.n_groups - 1)])
    stays = w.home_source() == w.g * w.n_plane + w.j
    copy = pltpu.make_async_remote_copy(
        src_ref=low,
        dst_ref=home,
        send_sem=w.send.at[w.used],
        recv_sem=w.recv.at[w.used],
        device_id=w.at_device(w.n_groups * w.j + w.g),
        device_id_type=MESH,
    )
    w.used += 1

    @pl.when(jnp.logical_not(stays))
    def _():
        copy.start()

    @pl.when(stays)
    def _():
        home[...] = low[...]

    yield

    @pl.when(jnp.logical_not(stays))
    def _():
        copy.wait()

    out[...] = home[...].astype(F32)
    wait_sent(copies)


def plane_sum_shift(w, src, out, from_core, pairs, from_chips, low, later):
    rows = out.shape[0]
    yield from plane_sum(w, src, low, from_core, pairs, from_chips)
    copy = w.start(
        low.at[pl.ds(0, rows)], later, w.at_group(lax.rem(w.g + w.n_groups - 1, w.n_groups))
    )
    yield
    copy.wait()
    keep = jnp.where(w.g == w.n_groups - 1, 0.0, 1.0)
    out[...] = low[rows:, :].astype(F32) + later[...].astype(F32) * keep


def group_sum(w, src, out, parts):
    copies = []
    for d in range(1, w.n_groups):
        to = w.group_peer(d)
        copies.append(w.start(src.at[to], parts.at[d - 1], w.at_group(to)))
    yield
    wait_received(copies)
    sum_rows(out, [src.at[w.g]] + [parts.at[d] for d in range(w.n_groups - 1)])
    wait_sent(copies)


def group_sum_swap(w, src, out, total, parts):
    copies = []
    for d in range(1, w.n_groups):
        to = w.group_peer(d)
        copies.append(w.start(src.at[to], parts.at[d - 1], w.at_group(to)))
    yield from pause(4)
    wait_received(copies)

    def step(i, carry):
        sum_rows(total.at[i], [src.at[w.g, i]] + [parts.at[d, i] for d in range(w.n_groups - 1)])
        return carry

    lax.fori_loop(0, w.n_plane, step, 0)
    second = []
    for d in range(1, w.n_plane):
        to = w.plane_peer(d)
        second.append(w.start(total.at[to], out.at[w.j], w.at_plane(to)))
    out[w.j] = total[w.j]
    yield
    wait_sent(copies)
    wait_all(second)


ROUTINES = {
    "plane_gather": plane_gather,
    "shift_gather": shift_gather,
    "whole_gather": whole_gather,
    "far_gather": far_gather,
    "plane_swap_gather": plane_swap_gather,
    "plane_swap": plane_swap,
    "plane_sum": plane_sum,
    "plane_sum_shift": plane_sum_shift,
    "head_rows": head_rows,
    "group_sum": group_sum,
    "whole_sum": whole_sum,
    "whole_swap": whole_swap,
    "group_sum_home": group_sum_home,
    "group_sum_swap": group_sum_swap,
}


def exchange_kernel(n_groups, n_plane, kinds, extra, *refs):
    count = len(kinds)
    sources, outs = refs[:count], refs[count : 2 * count]
    scratch = list(refs[2 * count : -2])
    w = Wires(n_groups, n_plane, refs[-2], refs[-1])
    w.meet("head_rows" in kinds, "group_sum_home" in kinds)
    running = []
    for kind, source, out, number in zip(kinds, sources, outs, extra):
        mine, scratch = scratch[:number], scratch[number:]
        if kind == "shift_gather":
            running.append(shift_gather(w, source, mine[0], out))
        else:
            running.append(ROUTINES[kind](w, source, out, *mine))
    while running:
        still = []
        for routine in running:
            try:
                next(routine)
                still.append(routine)
            except StopIteration:
                pass
        running = still


def exchange(n_groups, n_plane, number, *items):
    kinds = [kind for kind, _ in items]
    arrays = [array for _, array in items]
    shapes, scratch, extra = [], [], []
    chips = n_plane // 2
    for kind, array in items:
        shape, dtype = array.shape, array.dtype
        own = []
        if kind in ("plane_gather", "shift_gather"):
            out = (n_plane,) + shape
            if kind == "shift_gather":
                own = [shape]
        elif kind in ("whole_gather", "far_gather"):
            out = (n_groups, n_plane) + shape
        elif kind == "plane_swap_gather":
            out = (n_groups,) + shape
        elif kind == "plane_swap":
            out = shape
        elif kind == "head_rows":
            out = (n_groups,) + shape
        elif kind == "plane_sum_shift":
            pair = shape[1:]
            out = (shape[1] // 2, shape[2])
            half = (pair[0] // 2, pair[1])
            own = [(chips,) + pair, (chips,) + pair, (6,) + half, pair, out]
        elif kind == "plane_sum":
            out = shape[1:]
            own = [(chips,) + out, (chips,) + out, (6, out[0] // 2, out[1])]
        elif kind == "group_sum_home":
            out = shape[1:]
            own = [(n_groups - 1,) + out, out, out]
        elif kind == "group_sum":
            out = shape[1:]
            own = [(n_groups - 1,) + out]
        elif kind == "whole_swap":
            out = shape
            own = [shape]
        elif kind == "whole_sum":
            out = shape[2:]
            full = (n_groups,) + out
            own = [(chips,) + full, (chips,) + full, (chips - 1,) + full, full]
            own = own + [(n_groups - 1,) + out]
        elif kind == "group_sum_swap":
            out = shape[1:]
            own = [out, (n_groups - 1,) + out]
        if kind in ("plane_sum", "plane_sum_shift", "group_sum", "group_sum_home", "whole_sum"):
            shapes.append(jax.ShapeDtypeStruct(out, F32))
        else:
            shapes.append(jax.ShapeDtypeStruct(out, dtype))
        scratch += [pltpu.VMEM(s, dtype) for s in own]
        if kind == "far_gather":
            own = [None]
            scratch.append(pltpu.SemaphoreType.DMA)
        extra.append(len(own))
    copies = 64 + 32 * len(items)
    vmem = pl.BlockSpec(memory_space=pltpu.VMEM)
    return pl.pallas_call(
        functools.partial(exchange_kernel, n_groups, n_plane, kinds, extra),
        out_shape=shapes,
        in_specs=[vmem] * len(items),
        out_specs=[
            pl.BlockSpec(memory_space=pl.ANY) if kind == "far_gather" else vmem for kind in kinds
        ],
        scratch_shapes=scratch
        + [pltpu.SemaphoreType.DMA((copies,)), pltpu.SemaphoreType.DMA((copies,))],
        compiler_params=pltpu.CompilerParams(
            collective_id=number,
            has_side_effects=True,
            vmem_limit_bytes=60 * 1024 * 1024,
        ),
        name="exchange_%d" % number,
    )(*arrays)


def gather_all(x):
    return lax.all_gather(x, ALL, axis=0, tiled=True)


class StreamSum:
    def __init__(self, w, steps, stage, from_core, pairs, from_chips, totals, parts, sems, credit):
        self.w, self.steps = w, steps
        self.stage, self.from_core, self.pairs = stage, from_core, pairs
        self.from_chips, self.totals, self.parts = from_chips, totals, parts
        self.core_sems, self.chip_sems, self.chip_recv, self.group_sems = sems
        self.credit = credit

    @staticmethod
    def chips(w, step):
        half = lax.rem(step, 2)
        beside = w.p + 1 - 2 * lax.rem(w.p, 2)
        above = w.p + 2 - 4 * (w.p // 2)
        return beside + half * (above - beside), 3 - w.p + half * (2 * w.p - 3)

    def core_copy(self, step, i):
        slot = lax.rem(step, 2)
        return pltpu.make_async_remote_copy(
            src_ref=self.stage.at[slot, 2 * i + 1 - self.w.c],
            dst_ref=self.from_core.at[slot, i],
            send_sem=self.core_sems.at[0, slot, i],
            recv_sem=self.core_sems.at[1, slot, i],
            device_id=self.w.partner(),
            device_id_type=MESH,
        )

    def part(self, ref, upper):
        rows = ref.shape[0] // 2
        return ref.at[pl.ds(rows, rows)] if upper else ref.at[pl.ds(0, rows)]

    def chip_copy(self, group_at, which):
        slot, i, upper, up = (
            (0, 0, False, False),
            (0, 1, False, False),
            (0, 1, True, True),
            (1, 0, True, True),
            (1, 0, False, True),
            (0, 0, True, False),
        )[which]
        p = self.w.p
        to = p + 2 - 4 * (p // 2) if up else p + 1 - 2 * lax.rem(p, 2)
        return pltpu.make_async_remote_copy(
            src_ref=self.part(self.pairs.at[slot, i], upper),
            dst_ref=self.from_chips.at[group_at, which],
            send_sem=self.chip_sems.at[which],
            recv_sem=self.chip_recv.at[group_at, which],
            device_id=self.w.at_chip(to),
            device_id_type=MESH,
        )

    def group_copy(self, group_at):
        return pltpu.make_async_remote_copy(
            src_ref=self.totals.at[group_at],
            dst_ref=self.parts.at[group_at],
            send_sem=self.group_sems.at[0, group_at],
            recv_sem=self.group_sems.at[1, group_at],
            device_id=self.w.at_group(self.w.group_peer(group_at + 1)),
            device_id_type=MESH,
        )

    def open_stage(self, step):
        @pl.when(step >= 2)
        def _():
            for i in range(2):
                self.core_copy(step, i).wait_send()

    def push(self, step):
        @pl.when(step >= 2)
        def _():
            pl.semaphore_wait(self.credit, 1)

        for i in range(2):
            self.core_copy(step, i).start()

    def merge(self, step):
        slot, group_at = lax.rem(step, 2), step // 2
        for half, sends in ((0, (0, 1, 2, 5)), (1, (3, 4))):

            @pl.when((slot == half) & (step >= 2))
            def _():
                for which in sends:
                    self.chip_copy(group_at, which).wait_send()

        for i in range(2):
            self.core_copy(step, i).wait_recv()
            sum_rows(
                self.pairs.at[slot, i],
                [self.stage.at[slot, 2 * i + self.w.c], self.from_core.at[slot, i]],
            )

        @pl.when(step + 2 < self.steps)
        def _():
            pl.semaphore_signal(
                self.credit, inc=1, device_id=self.w.partner(), device_id_type=MESH
            )

        @pl.when(slot == 0)
        def _():
            for which in (0, 1, 2):
                self.chip_copy(group_at, which).start()

        @pl.when(slot == 1)
        def _():
            self.chip_copy(group_at, 3).start()
            for source, i, upper, which in ((1, (1, 0), False, 4), (2, (0, 0), True, 5)):
                self.chip_copy(group_at, source).wait_recv()
                target = self.part(self.pairs.at[i], upper)
                sum_rows(target, [target, self.from_chips.at[group_at, source]])
                self.chip_copy(group_at, which).start()

    def plane_total(self, group_at):
        for which in (0, 3, 4, 5):
            self.chip_copy(group_at, which).wait_recv()
        return [
            [self.part(self.pairs.at[1, 1], upper)]
            + [self.from_chips.at[group_at, which] for which in arrived]
            for upper, arrived in ((False, (0, 4)), (True, (3, 5)))
        ]

    def advance(self, step):
        @pl.when(step >= 1)
        def _():
            last = step - 1

            @pl.when((lax.rem(last, 2) == 0) & (last >= 2))
            def _():
                group_at = last // 2 - 1
                for upper, sources in enumerate(self.plane_total(group_at)):
                    sum_rows(self.part(self.totals.at[group_at], upper), sources)
                self.group_copy(group_at).start()

            self.merge(last)

    def finish(self, out):
        steps = self.steps
        self.merge(steps - 1)
        groups = steps // 2 - 1
        halves = self.plane_total(groups)
        for d in range(groups):
            self.group_copy(d).wait_recv()
        for upper, sources in enumerate(halves):
            parts = [self.part(self.parts.at[d], upper) for d in range(groups)]
            sum_rows(self.part(out, upper), sources + parts)
        for d in range(groups):
            self.group_copy(d).wait_send()
        for i in range(2):
            self.core_copy(steps - 2, i).wait_send()
            self.core_copy(steps - 1, i).wait_send()
        for which in range(6):
            self.chip_copy(groups, which).wait_send()

    @staticmethod
    def scratch(n_groups, rows, width):
        dma = pltpu.SemaphoreType.DMA
        return [
            pltpu.VMEM((2, 4, rows, width), BF),
            pltpu.VMEM((2, 2, rows, width), BF),
            pltpu.VMEM((2, 2, rows, width), BF),
            pltpu.VMEM((n_groups, 6, rows // 2, width), BF),
            pltpu.VMEM((n_groups - 1, rows, width), BF),
            pltpu.VMEM((n_groups - 1, rows, width), BF),
            dma((2, 2, 2)),
            dma((6,)),
            dma((n_groups, 6)),
            dma((2, n_groups - 1)),
            pltpu.SemaphoreType.REGULAR,
        ]


def swiglu_both(gate, up, grad):
    sigmoid = 1.0 / (1.0 + jnp.exp(-gate))
    silu = gate * sigmoid
    return silu * up, grad * up * (sigmoid * (1.0 + gate * (1.0 - sigmoid))), grad * silu


def step_chips(w, step):
    group = lax.rem(w.g + 1 + step // 2, w.n_groups)
    return [group * 4 + chip for chip in StreamSum.chips(w, step)]


def hot_rows(place, rows, core, slot_count):
    mine = place[:, core * rows : (core + 1) * rows]
    return lax.broadcasted_iota(jnp.int32, (slot_count, rows), 0) == mine


def moe_kernel(
    n_groups, experts, first_logit, slot_count,
    h2_hbm, cot_hbm, place_ref, wg_ref, wu_ref, wd_ref, sc_ref, sd_ref,
    sum_ref, rows_ref, gin_ref, act_ref, gg_ref, gu_ref, rw_ref, sact_ref, sgrad_ref, tok_ref,
    h2_buf, cot_buf, load_sems, *comm,
):
    rows = sum_ref.shape[0]
    step, steps = pl.program_id(0), 2 * n_groups
    w = Wires(n_groups, 8, None, None)
    stream = StreamSum(w, steps, *comm[:6], comm[6:10], comm[10])
    expert_id = w.g * 4 + w.p
    half = sc_ref.shape[1] // 2

    def loads(at):
        slot = lax.rem(at, 2)
        for i, chip in enumerate(step_chips(w, at)):
            source = pl.ds(pl.multiple_of(chip * 2 * rows, 2 * rows), 2 * rows)
            target = pl.ds(i * 2 * rows, 2 * rows)
            for k, (hbm, buf) in enumerate(((h2_hbm, h2_buf), (cot_hbm, cot_buf))):
                yield pltpu.make_async_copy(
                    hbm.at[source], buf.at[slot, target], load_sems.at[slot, i, k]
                )

    @pl.when(step == 0)
    def _():
        for copy in loads(step):
            copy.start()
        w.meet()

    @pl.when(step + 1 < steps)
    def _():
        for copy in loads(step + 1):
            copy.start()

    for copy in loads(step):
        copy.wait()
    slot = lax.rem(step, 2)
    h2, cot = h2_buf[slot], cot_buf[slot]
    chips = step_chips(w, step)

    pre = jnp.dot(h2, sc_ref[...], preferred_element_type=F32)
    back = dot_nt(cot, sd_ref[...])
    gate, up = pre[:, :half], pre[:, half:]
    lane = lax.broadcasted_iota(jnp.int32, gate.shape, 1)
    logits = jnp.where((lane >= first_logit) & (lane < first_logit + experts), gate, -1e30)
    exps = jnp.exp(logits - jnp.max(logits, axis=1, keepdims=True))
    chosen = jnp.where(lane == first_logit + expert_id, exps, 0.0)
    weight = jnp.sum(chosen, axis=1, keepdims=True) / jnp.sum(exps, axis=1, keepdims=True)
    act, grad_gate, grad_up = swiglu_both(gate, up, back)
    shared_act = act.astype(BF)
    shared_grad = jnp.concatenate([grad_gate.astype(BF), grad_up.astype(BF)], axis=1)
    for i, chip in enumerate(chips):
        at = pl.ds(pl.multiple_of(chip * 2 * rows, 2 * rows), 2 * rows)
        sact_ref[at, :] = shared_act[i * 2 * rows : (i + 1) * 2 * rows]
        sgrad_ref[at, :] = shared_grad[i * 2 * rows : (i + 1) * 2 * rows]

    hots, weights = [], []
    for q in range(4):
        place = place_ref[pl.ds(chips[q // 2], 1), :]
        hot = hot_rows(place, rows, q % 2, slot_count).astype(F32)
        hots.append(hot)
        tokens = slice(q * rows, (q + 1) * rows)
        slots = slice(q * slot_count, (q + 1) * slot_count)
        low = hot.astype(BF)
        rows_ref[slots, :] = jnp.dot(low, h2[tokens], preferred_element_type=F32).astype(BF)
        gin_ref[slots, :] = jnp.dot(low, cot[tokens], preferred_element_type=F32).astype(BF)
        spread = jnp.broadcast_to(weight[tokens], (rows, 128))
        weights.append(
            jnp.dot(hot, spread, preferred_element_type=F32, precision=lax.Precision.HIGHEST)[:, :1]
        )
    row_weight = jnp.concatenate(weights, axis=0)
    rw_ref[...] = row_weight
    expert_rows = rows_ref[...]
    picked_cot = gin_ref[...]
    back = dot_nt(picked_cot, wd_ref[...])
    gin_ref[...] = (picked_cot.astype(F32) * row_weight).astype(BF)
    gate = jnp.dot(expert_rows, wg_ref[...], preferred_element_type=F32)
    up = jnp.dot(expert_rows, wu_ref[...], preferred_element_type=F32)
    act, grad_gate, grad_up = swiglu_both(gate, up, back * row_weight)
    act_low, grad_gate, grad_up = act.astype(BF), grad_gate.astype(BF), grad_up.astype(BF)
    act_ref[...] = act_low
    gg_ref[...] = grad_gate
    gu_ref[...] = grad_up
    picked = jnp.sum(act_low.astype(F32) * back, axis=1, keepdims=True)
    grad_rows = (dot_nt(grad_gate, wg_ref[...]) + dot_nt(grad_up, wu_ref[...])).astype(BF)
    stream.open_stage(step)
    for q in range(4):
        tokens = slice(q * rows, (q + 1) * rows)
        slots = slice(q * slot_count, (q + 1) * slot_count)
        tok_ref[pl.ds(chips[q // 2] * 2 + q % 2, 1), :] = jnp.sum(
            hots[q] * picked[slots], axis=0, keepdims=True
        )
        total = dot_tn(hots[q].astype(BF), grad_rows[slots]) + dot_nt(
            shared_grad[tokens], sc_ref[...]
        )
        stream.stage[slot, q] = total.astype(BF)
    stream.push(step)
    stream.advance(step)

    @pl.when(step == steps - 1)
    def _():
        stream.finish(sum_ref)


def out_kernel(
    n_groups, slot_count,
    act_ref, rw_ref, rows_ref, gin_ref, gg_ref, gu_ref, place_ref, sact_ref, wd_ref, sd_ref,
    sum_ref, dg_ref, du_ref, dd_ref, *comm,
):
    rows = sum_ref.shape[0]
    step, steps = pl.program_id(0), 2 * n_groups
    w = Wires(n_groups, 8, None, None)
    stream = StreamSum(w, steps, *comm[:6], comm[6:10], comm[10])

    @pl.when(step == 0)
    def _():
        w.meet()
        for ref in (dg_ref, du_ref, dd_ref):
            ref[...] = jnp.zeros_like(ref)

    slot = lax.rem(step, 2)
    chips = step_chips(w, step)
    out_rows = jnp.dot(act_ref[...], wd_ref[...], preferred_element_type=F32) * rw_ref[...]
    out_rows = out_rows.astype(BF)
    stream.open_stage(step)
    for q in range(4):
        chip = chips[q // 2]
        place = place_ref[pl.ds(chip, 1), :]
        low = hot_rows(place, rows, q % 2, slot_count).astype(F32).astype(BF)
        slots = slice(q * slot_count, (q + 1) * slot_count)
        shared = sact_ref[pl.ds(pl.multiple_of((chip * 2 + q % 2) * rows, rows), rows), :]
        total = dot_tn(low, out_rows[slots]) + jnp.dot(
            shared, sd_ref[...], preferred_element_type=F32
        )
        stream.stage[slot, q] = total.astype(BF)
    stream.push(step)
    stream.advance(step)

    width = rows_ref.shape[1]
    piece = width // 4
    for k in range(4):
        cols = slice(k * piece, (k + 1) * piece)
        turned = rows_ref[:, cols].T
        dg_ref[cols, :] += jnp.dot(turned, gg_ref[...], preferred_element_type=F32)
        du_ref[cols, :] += jnp.dot(turned, gu_ref[...], preferred_element_type=F32)
    turned = act_ref[...].T
    for k in range(4):
        cols = slice(k * piece, (k + 1) * piece)
        dd_ref[:, cols] += jnp.dot(turned, gin_ref[:, cols], preferred_element_type=F32)

    @pl.when(step == steps - 1)
    def _():
        stream.finish(sum_ref)


def experts_sums(
    n_groups, rows, h2, cot, place, slot_count, expert_w, shared_w, router_weight, first_id
):
    w_gate, w_up, w_down = expert_w
    s_both, s_down = shared_w
    tokens, width = h2.shape
    hidden, hidden_s = w_down.shape[0], s_down.shape[0]
    experts = router_weight.shape[1]
    steps = 2 * n_groups
    devices = tokens // rows
    step_slots = slot_count * 4
    all_slots = step_slots * steps
    half = 128
    s_cat = jnp.concatenate(
        [
            s_both[:, :hidden_s],
            router_weight,
            jnp.zeros((width, half - hidden_s - experts), BF),
            s_both[:, hidden_s:],
            jnp.zeros((width, half - hidden_s), BF),
        ],
        axis=1,
    )
    s_tall = jnp.pad(s_down, ((0, half - hidden_s), (0, 0)))

    def whole(array):
        return pl.BlockSpec(array.shape, lambda i: (0, 0), pipeline_mode=pl.Buffered(1))

    def blocked(rows, cols):
        return pl.BlockSpec((rows, cols), lambda i: (i, 0))

    shape = jax.ShapeDtypeStruct
    flops = 2 * all_slots * width * hidden * 5 + 2 * tokens * width * (4 * half + 3 * slot_count)
    shapes = [
        shape((rows, width), F32),
        shape((all_slots, width), BF),
        shape((all_slots, width), BF),
        shape((all_slots, hidden), BF),
        shape((all_slots, hidden), BF),
        shape((all_slots, hidden), BF),
        shape((all_slots, 1), F32),
        shape((tokens, half), BF),
        shape((tokens, 2 * half), BF),
        shape((devices, rows), F32),
    ]
    specs = [
        blocked(step_slots, s.shape[1]) if s.shape[0] == all_slots else whole(s) for s in shapes
    ]
    hbm = pl.BlockSpec(memory_space=pl.ANY)
    grad_h2, rows_in, grad_in, act, grad_gate, grad_up, row_weight, s_act, s_grad, token_grad = (
        pl.pallas_call(
            functools.partial(moe_kernel, n_groups, experts, hidden_s, slot_count),
            grid=(steps,),
            in_specs=[
                hbm,
                hbm,
                whole(place),
                whole(w_gate),
                whole(w_up),
                whole(w_down),
                whole(s_cat),
                whole(s_tall),
            ],
            out_specs=specs,
            out_shape=shapes,
            scratch_shapes=[
                pltpu.VMEM((2, 4 * rows, width), BF),
                pltpu.VMEM((2, 4 * rows, width), BF),
                pltpu.SemaphoreType.DMA((2, 2, 2)),
            ]
            + StreamSum.scratch(n_groups, rows, width),
            cost_estimate=pl.CostEstimate(
                flops=flops, bytes_accessed=12 * tokens * width, transcendentals=tokens * 1024
            ),
            compiler_params=pltpu.CompilerParams(
                collective_id=first_id,
                has_side_effects=True,
                vmem_limit_bytes=67043328,
            ),
            name="experts",
        )(h2, cot, place, w_gate, w_up, w_down, s_cat, s_tall)
    )
    shapes = [grad_h2] + [shape(x.shape, F32) for x in expert_w]
    out, d_gate, d_up, d_down = pl.pallas_call(
        functools.partial(out_kernel, n_groups, slot_count),
        grid=(steps,),
        in_specs=[
            blocked(step_slots, hidden),
            blocked(step_slots, 1),
            blocked(step_slots, width),
            blocked(step_slots, width),
            blocked(step_slots, hidden),
            blocked(step_slots, hidden),
            whole(place),
            whole(s_act),
            whole(w_down),
            whole(s_tall),
        ],
        out_specs=[whole(x) for x in shapes],
        out_shape=[shape(x.shape, F32) for x in shapes],
        scratch_shapes=StreamSum.scratch(n_groups, rows, width),
        cost_estimate=pl.CostEstimate(
            flops=2 * width * (4 * all_slots * hidden + tokens * (half + slot_count)),
            bytes_accessed=4 * tokens * width,
            transcendentals=0,
        ),
        compiler_params=pltpu.CompilerParams(
            collective_id=first_id + 1,
            has_side_effects=True,
            vmem_limit_bytes=67043328,
        ),
        name="expert_out",
    )(act, row_weight, rows_in, grad_in, grad_gate, grad_up, place, s_act, w_down, s_tall)
    g_both = dot_tn(h2, s_grad)
    g_both = jnp.concatenate([g_both[:, :hidden_s], g_both[:, half : half + hidden_s]], axis=1)
    grads = (
        d_gate,
        d_up,
        d_down,
        g_both,
        dot_tn(s_act, cot)[:hidden_s],
    )
    return out, grad_h2, token_grad, grads


def body(
    n_groups, n_plane, layer_input, attn_gain, w_query, w_latent, kv_gain, w_expand, w_output,
    ffn_gain, w_router, shared_gate, shared_up, shared_down, expert_gate, expert_up,
    expert_down, routes, segments, cotangent,
):
    tok, width = layer_input.shape
    devices = n_groups * n_plane
    experts = w_router.shape[1]
    local_heads = HEADS // n_plane
    scale = (NOPE + ROPE) ** (-0.5)
    group = lax.axis_index("g")
    place_in = lax.axis_index(PLANE)
    me = lax.axis_index(ALL)
    expert_id = lax.axis_index(("g", "p"))
    plane_tok = n_plane * tok
    plane_start = group * plane_tok

    rows_w = w_router.shape[0]
    kv_n = kv_gain.shape[0]
    small = jnp.concatenate(
        [
            attn_gain,
            ffn_gain,
            kv_gain,
            w_router.reshape(-1),
            routes.reshape(-1).astype(BF),
            segments.astype(BF),
        ]
    )
    small = jnp.pad(small, (0, -small.shape[0] % 4096)).reshape(-1, 128)
    head_cols = local_heads * (NOPE + ROPE)
    kv_cols = local_heads * (NOPE + VDIM)
    fold = kv_n * kv_cols // rows_w
    pair = jnp.concatenate(
        [
            w_query.reshape(rows_w, n_plane, head_cols).transpose(1, 0, 2),
            w_expand.reshape(kv_n, n_plane, kv_cols // fold, fold)
            .transpose(1, 0, 2, 3)
            .reshape(n_plane, rows_w, fold),
        ],
        axis=2,
    )
    swap = functools.partial(exchange, n_groups, n_plane)
    pair, latent_weight, small, x_plane = swap(
        0,
        ("plane_swap_gather", pair),
        ("whole_gather", w_latent),
        ("whole_gather", small),
        ("plane_gather", layer_input),
    )
    x_plane = x_plane.reshape(plane_tok, width).astype(F32)
    latent_weight = latent_weight.reshape(width, RANK + ROPE)
    pair = pair.reshape(width, head_cols + fold)
    small = small.reshape(devices, -1)
    cuts = [rows_w, 2 * rows_w, 2 * rows_w + kv_n, 2 * rows_w + kv_n + rows_w * experts]
    cuts = cuts + [cuts[-1] + tok * TOP, cuts[-1] + tok * TOP + tok]
    gain_one = small[:, : cuts[0]].reshape(-1).astype(F32)
    gain_two = small[:, cuts[0] : cuts[1]].reshape(-1).astype(F32)
    gain_kv = small[:, cuts[1] : cuts[2]].reshape(-1).astype(F32)
    router_weight = small[:, cuts[2] : cuts[3]].reshape(width, experts)
    routes_all = small[:, cuts[3] : cuts[4]].astype(jnp.int32).reshape(devices, tok, TOP)
    segments_all = small[:, cuts[4] : cuts[5]].astype(jnp.int32).reshape(-1)

    query_weight = pair[:, :head_cols].reshape(width, local_heads, NOPE + ROPE)
    wq_nope = query_weight[:, :, :NOPE].reshape(width, local_heads * NOPE)
    wq_rope = query_weight[:, :, NOPE:].reshape(width, local_heads * ROPE)
    expand_weight = pair[:, head_cols:].reshape(RANK, kv_cols)
    cotangent_later = jnp.where(x_plane[0, 0] < 1e6, cotangent, jnp.zeros_like(cotangent))

    shared_n = shared_down.shape[0]
    s_both = jnp.concatenate(
        [
            shared_gate.reshape(rows_w, devices, shared_n),
            shared_up.reshape(rows_w, devices, shared_n),
        ],
        axis=2,
    )
    s_both = lax.all_to_all(s_both, ALL, split_axis=1, concat_axis=0).reshape(width, 2 * shared_n)

    hidden = rms_norm(x_plane, gain_one).astype(BF)
    rope_half = ROPE // 2
    positions = plane_start + jnp.arange(plane_tok, dtype=jnp.int32)
    frequency = 10000.0 ** (-jnp.arange(rope_half, dtype=F32) / rope_half)
    angles = positions.astype(F32)[:, None] * frequency[None, :]
    cosine = jnp.cos(angles)
    sine_part = jnp.sin(angles)
    cos_h, sin_h = cosine[:, None, :], sine_part[:, None, :]
    latent = matmul(hidden, latent_weight)
    compressed_own = rms_norm(latent[:, :RANK], gain_kv).astype(BF)
    key_rope_own = rotate(latent[:, RANK:], cosine, sine_part).astype(BF)

    def own_rows(table):
        return lax.dynamic_slice_in_dim(table, place_in * tok, tok, 0)

    piece = own_rows(jnp.concatenate([compressed_own, key_rope_own], axis=1))
    before, own_output = swap(1, ("shift_gather", piece), ("head_rows", w_output))
    before = before.reshape(plane_tok, RANK + ROPE)
    own_output = own_output.reshape(local_heads * VDIM, width)
    compressed = jnp.concatenate([before[:, :RANK], compressed_own], axis=0)
    key_rope = jnp.concatenate([before[:, RANK:], key_rope_own], axis=0)
    q_nope = matmul(hidden, wq_nope).astype(BF)
    q_rope = rotate(
        matmul(hidden, wq_rope).reshape(plane_tok, local_heads, ROPE), cos_h, sin_h
    ).reshape(plane_tok, local_heads * ROPE).astype(BF)
    expanded = matmul(compressed, expand_weight).astype(BF)
    plane_segments = lax.dynamic_slice_in_dim(segments_all, plane_start, plane_tok, 0)
    doc_start = jnp.sum(
        (segments_all[None, :] < plane_segments[:, None]).astype(jnp.int32), axis=1, keepdims=True
    )
    low_bound = doc_start - plane_start + DOC_MAX
    mixed_heads, lse = attend(low_bound, q_nope, q_rope, expanded, key_rope, scale)
    attn_out = matmul(mixed_heads, own_output).astype(BF)
    attn_out = swap(2, ("plane_sum", attn_out.reshape(n_plane, tok, width)))[0]
    input_float = layer_input.astype(F32)
    residual_one = input_float + attn_out
    h_two_f, norm_two_back = jax.vjp(rms_norm, residual_one, gain_two)
    h_two = h_two_f.astype(BF)
    router_probs = softmax_rows(matmul(h_two, router_weight))

    expert_w = (expert_gate[0], expert_up[0], expert_down[0])
    shared_w = (s_both, shared_down)
    slot_limit = 2 * tok * TOP // experts

    def on_rows(h2, h2_all, cot_gathered, routes_here):
        rows = h2.shape[0]
        slot_count = min(slot_limit, rows)
        member = jnp.any(routes_here == expert_id, axis=2)
        member_int = member.astype(jnp.int32)
        rank = jnp.cumsum(member_int, axis=1) - member_int
        place = jnp.where(member, rank, -1).reshape(devices // 2, 2 * rows)
        out, grad_h2, token_grad, grads = experts_sums(
            n_groups,
            rows,
            h2_all,
            cot_gathered,
            place,
            slot_count,
            expert_w,
            shared_w,
            router_weight,
            8,
        )
        picked = lax.all_to_all(token_grad, ALL, split_axis=0, concat_axis=0, tiled=True)
        picked = jnp.sum(picked.reshape(experts, devices // experts, rows), axis=1).T
        return out, grad_h2, picked, grads

    parts = max(1, devices * tok // 4096)
    if parts == 1:
        cot_all = gather_all(cotangent_later)
        out_own, grad_h2_own, grad_router_probs, grads = on_rows(
            h_two, swap(5, ("far_gather", h_two))[0].reshape(-1, width), cot_all, routes_all
        )
    else:
        rows = tok // parts

        def step(total, inputs):
            h2, cot, routes_here = inputs
            cot_part = gather_all(cot)
            out, grad_h2, picked, grads = on_rows(h2, gather_all(h2), cot_part, routes_here)
            grads = lax.optimization_barrier(grads)
            total = tuple(a + b for a, b in zip(total, grads))
            return total, (out, grad_h2, picked)

        shapes = expert_w + shared_w
        grads, (out_own, grad_h2_own, grad_router_probs) = lax.scan(
            step,
            tuple(jnp.zeros(s.shape, F32) for s in shapes),
            (
                h_two.reshape(parts, rows, width),
                cotangent.reshape(parts, rows, width),
                routes_all.reshape(devices, parts, rows, TOP).transpose(1, 0, 2, 3),
            ),
        )
        out_own = out_own.reshape(tok, width)
        grad_h2_own = grad_h2_own.reshape(tok, width)
        grad_router_probs = grad_router_probs.reshape(tok, experts)
    g_gate, g_up, g_down, g_both, g_sdown = grads
    grad_logits = router_probs * (
        grad_router_probs - jnp.sum(router_probs * grad_router_probs, axis=1, keepdims=True)
    )
    grad_logits = grad_logits.astype(BF)
    grad_router = dot_tn(h_two, grad_logits)
    grad_h_two = grad_h2_own + dot_nt(grad_logits, router_weight)
    output = residual_one + out_own

    grad_x_one, grad_gain_two = norm_two_back(grad_h_two)
    grad_x_one = grad_x_one + cotangent.astype(F32)
    grad_attn_out = grad_x_one.astype(BF)
    g_shared, plane_grad = swap(
        3,
        ("whole_swap", g_both.astype(BF).reshape(n_groups, n_plane, rows_w, 2 * shared_n)),
        ("plane_gather", grad_attn_out),
    )
    plane_grad = plane_grad.reshape(plane_tok, width)
    grad_mixed = dot_nt(plane_grad, own_output).astype(BF)
    dqn, dqr, dex, dkr = attend_back(
        low_bound, q_nope, q_rope, expanded, key_rope, lse, grad_mixed, scale
    )

    g_output = dot_tn(mixed_heads, plane_grad).astype(BF).reshape(n_groups, rows_w, width)

    grad_expanded = dex.astype(BF)
    grad_expand = dot_tn(compressed, grad_expanded)
    grad_comp = dot_nt(grad_expanded, expand_weight)
    key_grads = jnp.concatenate([grad_comp, dkr], axis=1).astype(BF)
    key_grads = (
        key_grads.reshape(2, n_plane, tok, RANK + ROPE)
        .transpose(1, 0, 2, 3)
        .reshape(n_plane, 2 * tok, RANK + ROPE)
    )

    gq_nope = dqn.astype(BF)
    gq_rope = (
        unrotate(dqr.reshape(plane_tok, local_heads, ROPE), cos_h, sin_h)
        .reshape(plane_tok, local_heads * ROPE)
        .astype(BF)
    )
    grad_hidden = (dot_nt(gq_nope, wq_nope) + dot_nt(gq_rope, wq_rope)).astype(BF)
    gw_nope = dot_tn(hidden, gq_nope).astype(BF).reshape(n_groups, n_plane, rows_w, -1)
    gw_rope = dot_tn(hidden, gq_rope).astype(BF).reshape(n_groups, n_plane, rows_w, -1)
    g_expand = grad_expand.astype(BF).reshape(n_groups, n_plane, kv_n, kv_cols)
    key_grad, grad_hidden, gw_nope, gw_rope, g_expand = swap(
        4,
        ("plane_sum_shift", key_grads),
        ("plane_sum", grad_hidden.reshape(n_plane, tok, width)),
        ("group_sum_swap", gw_nope),
        ("group_sum_swap", gw_rope),
        ("group_sum_swap", g_expand),
    )
    latent_own = own_rows(latent)
    kv_norm_back = jax.vjp(rms_norm, latent_own[:, :RANK], gain_kv)[1]
    grad_comp_in, grad_gain_kv = kv_norm_back(key_grad[:, :RANK])
    grad_rope_in = unrotate(key_grad[:, RANK:], own_rows(cosine), own_rows(sine_part))
    grad_latent = jnp.concatenate([grad_comp_in, grad_rope_in], axis=1).astype(BF)

    def per_head(table, cols):
        return table.transpose(1, 0, 2).reshape(rows_w, HEADS, cols)

    grad_query_weight = jnp.concatenate(
        [per_head(gw_nope, NOPE), per_head(gw_rope, ROPE)], axis=2
    ).reshape(rows_w, -1).astype(F32)
    grad_expand_weight = g_expand.transpose(1, 0, 2).reshape(kv_n, -1).astype(F32)

    g_latent = dot_tn(own_rows(hidden), grad_latent).astype(BF)
    g_latent = g_latent.reshape(n_groups, n_plane, rows_w, RANK + ROPE)
    grad_hidden = grad_hidden + dot_nt(grad_latent, latent_weight)
    norm_one_back = jax.vjp(rms_norm, input_float, gain_one)[1]
    grad_x_norm, grad_gain_one = norm_one_back(grad_hidden)
    grad_input = grad_x_one + grad_x_norm

    small_grads = jnp.concatenate(
        [
            p.reshape(devices, -1)
            for p in (grad_gain_one, grad_gain_two, grad_gain_kv, grad_router)
        ],
        axis=1,
    )
    small_grads = jnp.pad(small_grads, ((0, 0), (0, -small_grads.shape[1] % 1024)))
    grad_latent_weight, grad_output_weight, small_grads = swap(
        6,
        ("whole_sum", g_latent),
        ("group_sum_home", g_output),
        ("whole_sum", small_grads.reshape(n_groups, n_plane, -1, 128)),
    )
    small_grads = small_grads.reshape(-1)
    g_shared = g_shared.transpose(2, 0, 1, 3).reshape(rows_w, devices, 2 * shared_n).astype(F32)
    grad_shared_gate = g_shared[:, :, :shared_n].reshape(rows_w, devices * shared_n)
    grad_shared_up = g_shared[:, :, shared_n:].reshape(rows_w, devices * shared_n)
    return (
        output,
        grad_input,
        small_grads[: cuts[0]],
        grad_query_weight,
        grad_latent_weight,
        small_grads[cuts[1] : cuts[2]],
        grad_expand_weight,
        grad_output_weight,
        small_grads[cuts[0] : cuts[1]],
        small_grads[cuts[2] : cuts[3]].reshape(rows_w, experts),
        grad_shared_gate,
        grad_shared_up,
        g_sdown,
        g_gate[None],
        g_up[None],
        g_down[None],
    )


def solution(mesh):
    n_expert, n_shard = mesh.shape["expert"], mesh.shape["wshard"]
    devices = n_expert * n_shard

    def program(*args):
        tok = args[0].shape[0] // devices
        n_plane = DOC_MAX // tok
        n_groups = devices // n_plane
        inner = Mesh(mesh.devices.reshape(n_groups, n_plane // n_shard, n_shard), ALL)
        rows, vector = P(ALL, None), P(ALL)
        wide, tall = P(("g", "p"), None, "c"), P(("g", "p"), "c", None)
        step = jax.shard_map(
            functools.partial(body, n_groups, n_plane),
            mesh=inner,
            in_specs=(
                rows, vector, rows, rows, vector, rows, rows, vector, rows, rows, rows, rows,
                wide, wide, tall, rows, vector, rows,
            ),
            out_specs=(
                rows, rows, vector, rows, rows, vector, rows, rows, vector, rows, rows, rows,
                rows, wide, wide, tall,
            ),
            check_vma=False,
        )
        return step(*args)

    return program
```

```python
import functools

import jax
import jax.numpy as jnp
from jax import lax
from jax.experimental import pallas as pl
from jax.experimental.pallas import tpu as pltpu
from jax.sharding import Mesh, PartitionSpec as P

HEADS = 16
NOPE = 128
ROPE = 64
VDIM = 128
RANK = 512
TOP = 6
DOC_MAX = 1024
QUERY_BLOCK = 256

BF = jnp.bfloat16
F32 = jnp.float32
ALL = ("g", "p", "c")
PLANE = ("p", "c")

epsilon = 1e-06


def rms_norm(vector, scaling):
    return vector * lax.rsqrt(jnp.mean(vector * vector, axis=-1, keepdims=True) + epsilon) * scaling


def rotate(vector, cosine, sine_part):
    half_width = vector.shape[-1] // 2
    front_half = vector[..., :half_width]
    back_half = vector[..., half_width:]
    return jnp.concatenate(
        [front_half * cosine - back_half * sine_part, back_half * cosine + front_half * sine_part],
        axis=-1,
    )


def unrotate(vector, cosine, sine_part):
    return rotate(vector, cosine, -sine_part)


def matmul(left, right):
    return jnp.dot(left, right, preferred_element_type=F32)


def dot_nt(left, right):
    return lax.dot_general(left, right, (((1,), (1,)), ((), ())), preferred_element_type=F32)


def dot_tn(left, right):
    return lax.dot_general(left, right, (((0,), (0,)), ((), ())), preferred_element_type=F32)


def swiglu(gate_pre, up_pre):
    return jax.nn.silu(gate_pre) * up_pre


def softmax_rows(scores):
    row_top = jnp.max(scores, axis=-1, keepdims=True)
    exp_scores = jnp.exp(scores - row_top)
    return exp_scores / jnp.sum(exp_scores, axis=-1, keepdims=True)


def masked_scores(base, low_bound, q_nope, q_rope, k_nope, k_rope, scale):
    rows, span = q_nope.shape[0], k_nope.shape[0]
    key_at = lax.broadcasted_iota(jnp.int32, (rows, span), 1) + base
    query_at = lax.broadcasted_iota(jnp.int32, (rows, span), 0) + (base + DOC_MAX)
    allowed = (key_at >= low_bound) & (key_at <= query_at)
    scores = (dot_nt(q_nope, k_nope) + dot_nt(q_rope, k_rope)) * scale
    return jnp.where(allowed, scores, -1e30)


def attend_kernel(heads, scale, low_ref, qn_ref, qr_ref, ex_ref, kr_ref, out_ref, lse_ref):
    rows = qn_ref.shape[0]
    base = pl.multiple_of(pl.program_id(0) * rows, rows)
    window = pl.ds(base, rows + DOC_MAX)
    k_rope = kr_ref[window, :]
    low_bound = low_ref[...]
    for h in range(heads):
        at = h * (NOPE + VDIM)
        k_nope = ex_ref[window, at : at + NOPE]
        value = ex_ref[window, at + NOPE : at + NOPE + VDIM]
        scores = masked_scores(
            base,
            low_bound,
            qn_ref[:, h * NOPE : (h + 1) * NOPE],
            qr_ref[:, h * ROPE : (h + 1) * ROPE],
            k_nope,
            k_rope,
            scale,
        )
        top = jnp.max(scores, axis=-1, keepdims=True)
        exps = jnp.exp(scores - top)
        total = jnp.sum(exps, axis=-1, keepdims=True)
        probs = (exps / total).astype(BF)
        out_ref[:, h * VDIM : (h + 1) * VDIM] = jnp.dot(
            probs, value, preferred_element_type=F32
        ).astype(BF)
        lse_ref[:, h : h + 1] = top + jnp.log(total)


def attend(low_bound, q_nope, q_rope, expanded, key_rope, scale):
    queries = q_nope.shape[0]
    heads = q_nope.shape[1] // NOPE
    rows = QUERY_BLOCK

    def whole(array):
        return pl.BlockSpec(array.shape, lambda i: (0, 0))

    def blocked(width):
        return pl.BlockSpec((rows, width), lambda i: (i, 0))

    flops = 2 * heads * queries * (rows + DOC_MAX) * (NOPE + ROPE + VDIM)
    return pl.pallas_call(
        functools.partial(attend_kernel, heads, scale),
        grid=(queries // rows,),
        in_specs=[
            blocked(1),
            blocked(heads * NOPE),
            blocked(heads * ROPE),
            whole(expanded),
            whole(key_rope),
        ],
        out_specs=[blocked(heads * VDIM), blocked(heads)],
        out_shape=[
            jax.ShapeDtypeStruct((queries, heads * VDIM), BF),
            jax.ShapeDtypeStruct((queries, heads), F32),
        ],
        cost_estimate=pl.CostEstimate(
            flops=flops, bytes_accessed=4 * expanded.size, transcendentals=flops // 640
        ),
        compiler_params=pltpu.CompilerParams(vmem_limit_bytes=50 * 1024 * 1024),
        name="attend",
    )(low_bound, q_nope, q_rope, expanded, key_rope)


def attend_back_kernel(
    heads, scale, low_ref, qn_ref, qr_ref, ex_ref, kr_ref, lse_ref, gm_ref,
    dqn_ref, dqr_ref, dex_ref, dkr_ref,
):
    rows = qn_ref.shape[0]
    step = pl.program_id(0)
    base = pl.multiple_of(step * rows, rows)
    window = pl.ds(base, rows + DOC_MAX)

    @pl.when(step == 0)
    def _():
        dex_ref[...] = jnp.zeros_like(dex_ref)
        dkr_ref[...] = jnp.zeros_like(dkr_ref)

    k_rope = kr_ref[window, :]
    low_bound = low_ref[...]
    for h in range(heads):
        at = h * (NOPE + VDIM)
        k_nope = ex_ref[window, at : at + NOPE]
        value = ex_ref[window, at + NOPE : at + NOPE + VDIM]
        q_nope = qn_ref[:, h * NOPE : (h + 1) * NOPE]
        q_rope = qr_ref[:, h * ROPE : (h + 1) * ROPE]
        grad_out = gm_ref[:, h * VDIM : (h + 1) * VDIM]
        scores = masked_scores(base, low_bound, q_nope, q_rope, k_nope, k_rope, scale)
        probs = jnp.exp(scores - lse_ref[:, h : h + 1])
        grad_probs = dot_nt(grad_out, value)
        mean_grad = jnp.sum(probs * grad_probs, axis=-1, keepdims=True)
        grad_scores = (probs * (grad_probs - mean_grad) * scale).astype(BF)
        probs_low = probs.astype(BF)
        dqn_ref[:, h * NOPE : (h + 1) * NOPE] = jnp.dot(
            grad_scores, k_nope, preferred_element_type=F32
        )
        dqr_ref[:, h * ROPE : (h + 1) * ROPE] = jnp.dot(
            grad_scores, k_rope, preferred_element_type=F32
        )
        dex_ref[window, at : at + NOPE] += dot_tn(grad_scores, q_nope)
        dex_ref[window, at + NOPE : at + NOPE + VDIM] += dot_tn(probs_low, grad_out)
        dkr_ref[window, :] += dot_tn(grad_scores, q_rope)


def attend_back(low_bound, q_nope, q_rope, expanded, key_rope, lse, grad_mixed, scale):
    queries = q_nope.shape[0]
    heads = q_nope.shape[1] // NOPE
    rows = QUERY_BLOCK

    def whole(shape):
        return pl.BlockSpec(shape, lambda i: (0, 0))

    def blocked(width):
        return pl.BlockSpec((rows, width), lambda i: (i, 0))

    flops = 2 * heads * queries * (rows + DOC_MAX) * (3 * NOPE + 3 * ROPE + 2 * VDIM)
    return pl.pallas_call(
        functools.partial(attend_back_kernel, heads, scale),
        grid=(queries // rows,),
        in_specs=[
            blocked(1),
            blocked(heads * NOPE),
            blocked(heads * ROPE),
            whole(expanded.shape),
            whole(key_rope.shape),
            blocked(heads),
            blocked(heads * VDIM),
        ],
        out_specs=[
            blocked(heads * NOPE),
            blocked(heads * ROPE),
            whole(expanded.shape),
            whole(key_rope.shape),
        ],
        out_shape=[
            jax.ShapeDtypeStruct(q_nope.shape, F32),
            jax.ShapeDtypeStruct(q_rope.shape, F32),
            jax.ShapeDtypeStruct(expanded.shape, F32),
            jax.ShapeDtypeStruct(key_rope.shape, F32),
        ],
        cost_estimate=pl.CostEstimate(
            flops=flops, bytes_accessed=8 * expanded.size, transcendentals=flops // 1664
        ),
        compiler_params=pltpu.CompilerParams(vmem_limit_bytes=56 * 1024 * 1024),
        name="attend_back",
    )(low_bound, q_nope, q_rope, expanded, key_rope, lse, grad_mixed)


MESH = pl.DeviceIdType.MESH


def pause(rounds):
    for _ in range(rounds):
        yield


class Wires:
    def __init__(self, n_groups, n_plane, send, recv):
        self.n_groups, self.n_plane, self.send, self.recv = n_groups, n_plane, send, recv
        self.cores = 2
        self.g, self.p, self.c = lax.axis_index("g"), lax.axis_index("p"), lax.axis_index("c")
        self.j = self.p * self.cores + self.c
        self.used = 0

    def at_plane(self, j):
        return {"g": self.g, "p": j // self.cores, "c": j % self.cores}

    def at_chip(self, p):
        return {"g": self.g, "p": p, "c": self.c}

    def at_group(self, g):
        return {"g": g, "p": self.p, "c": self.c}

    def partner(self):
        return {"g": self.g, "p": self.p, "c": 1 - self.c}

    def beside(self):
        return self.p + 1 - 2 * lax.rem(self.p, 2)

    def above(self):
        return self.p + 2 - 4 * (self.p // 2)

    def core_of(self, p):
        return p * self.cores + self.c

    def plane_peer(self, d):
        return lax.rem(self.j + d, self.n_plane)

    def group_peer(self, d):
        return lax.rem(self.g + d, self.n_groups)

    def start(self, src, dst, device):
        copy = pltpu.make_async_remote_copy(
            src_ref=src,
            dst_ref=dst,
            send_sem=self.send.at[self.used],
            recv_sem=self.recv.at[self.used],
            device_id=device,
            device_id_type=MESH,
        )
        self.used += 1
        copy.start()
        return copy

    def at_device(self, index):
        return {"g": index // self.n_plane, **self.on_plane(lax.rem(index, self.n_plane))}

    def on_plane(self, j):
        return {"p": j // self.cores, "c": j % self.cores}

    def meet(self, heads=False, home=False):
        barrier = pltpu.get_barrier_semaphore()
        waits = self.n_plane - 1 + self.n_groups - 1
        if heads:
            mine = self.head_owner() == self.j
            part = lax.rem(self.g * self.n_plane + self.j, self.n_groups)
            for r in range(self.n_groups):

                @pl.when(jnp.logical_not(mine) | (part != r))
                def _():
                    source = self.at_device(self.n_groups * self.j + r)
                    pl.semaphore_signal(barrier, inc=1, device_id=source, device_id_type=MESH)

            waits = waits + jnp.where(mine, self.n_groups - 1, self.n_groups)
        if home:
            source = self.home_source()
            stays = source == self.g * self.n_plane + self.j

            @pl.when(jnp.logical_not(stays))
            def _():
                pl.semaphore_signal(
                    barrier, inc=1, device_id=self.at_device(source), device_id_type=MESH
                )

            waits = waits + jnp.where(stays, 0, 1)
        for d in range(1, self.n_plane):
            pl.semaphore_signal(
                barrier, inc=1, device_id=self.at_plane(self.plane_peer(d)), device_id_type=MESH
            )
        for d in range(1, self.n_groups):
            pl.semaphore_signal(
                barrier, inc=1, device_id=self.at_group(self.group_peer(d)), device_id_type=MESH
            )
        pl.semaphore_wait(barrier, waits)

    def home_source(self):
        index = self.g * self.n_plane + self.j
        return lax.rem(index, self.n_groups) * self.n_plane + index // self.n_groups

    def head_owner(self):
        return (self.g * self.n_plane + self.j) // self.n_groups


def sum_rows(dst, sources):
    rows = dst.shape[0]
    tile = 32 if rows % 32 == 0 else rows

    def step(i, carry):
        at = pl.ds(pl.multiple_of(i * tile, tile), tile)
        if len(sources) == 2 and all(r.dtype == BF for r in [dst] + sources):
            dst[at, :] = sources[0][at, :] + sources[1][at, :]
        else:
            total = sources[0][at, :].astype(F32)
            for source in sources[1:]:
                total = total + source[at, :].astype(F32)
            dst[at, :] = total.astype(dst.dtype)
        return carry

    lax.fori_loop(0, rows // tile, step, 0)


def wait_all(copies):
    for copy in copies:
        copy.wait()


def wait_received(copies):
    for copy in copies:
        copy.wait_recv()


def wait_sent(copies):
    for copy in copies:
        copy.wait_send()


def part_of(ref, upper):
    rows = ref.shape[0] // 2
    return ref.at[pl.ds(rows, rows)] if upper else ref.at[pl.ds(0, rows)]


def spread(w, own, at):
    beside, above = w.at_chip(w.beside()), w.at_chip(w.above())
    mine = at(w.j)
    halves = [(part_of(own, u), part_of(mine, u)) for u in (0, 1)]
    lower = w.start(*halves[0], beside)
    upper = w.start(*halves[1], above)
    rest = [w.start(*halves[1], beside), w.start(*halves[0], above)]
    on_chip = [w.start(own, mine, w.partner())]
    yield
    lower.wait_recv()
    block = part_of(at(w.core_of(w.beside())), 0)
    rest.append(w.start(block, block, above))
    upper.wait_recv()
    block = part_of(at(w.core_of(w.above())), 1)
    rest.append(w.start(block, block, beside))
    yield
    wait_received(rest)
    for p in (w.beside(), w.above(), 3 - w.p):
        block = at(w.core_of(p))
        on_chip.append(w.start(block, block, w.partner()))
    yield
    wait_sent([lower, upper] + rest)
    wait_all(on_chip)


def plane_gather(w, src, out):
    out[w.j] = src[...]
    yield from spread(w, src, lambda j: out.at[j])


def far_gather(w, src, out, sem):
    mine = out.at[w.g, w.j]
    away = [w.start(src, mine, w.at_group(w.group_peer(d))) for d in range(1, w.n_groups)]
    local = pltpu.make_async_copy(src, mine, sem)
    local.start()
    running = [spread(w, src, lambda j: out.at[w.g, j])]
    next(running[0])
    for d in range(1, w.n_groups):
        away[d - 1].wait_recv()
        g = w.group_peer(w.n_groups - d)
        running.append(spread(w, out.at[g, w.j], lambda j, g=g: out.at[g, j]))
        next(running[d])
    for _ in range(3):
        for routine in running:
            next(routine, None)
        yield
    local.wait()
    wait_sent(away)


def shift_gather(w, src, mid, out):
    copy = w.start(src, mid, w.at_group(lax.rem(w.g + 1, w.n_groups)))
    yield
    copy.wait()
    yield from plane_gather(w, mid, out)


def whole_gather(w, src, out):
    chips = w.n_plane // w.cores
    first = [
        w.start(src, out.at[w.g, w.j], w.at_group(w.group_peer(d))) for d in range(1, w.n_groups)
    ]
    out[w.g, w.j] = src[...]
    yield
    wait_received(first)
    mine = out.at[:, w.j]
    second = [w.start(mine, mine, w.at_chip(lax.rem(w.p + d, chips))) for d in range(1, chips)]
    third = [w.start(mine, mine, w.partner())]
    yield
    for d in range(1, chips):
        second[d - 1].wait_recv()
        block = out.at[:, w.core_of(lax.rem(w.p + chips - d, chips))]
        third.append(w.start(block, block, w.partner()))
    yield
    wait_sent(first)
    wait_sent(second)
    wait_all(third)


def plane_swap_gather(w, src, out):
    first = []
    for d in range(1, w.n_plane):
        to = w.plane_peer(d)
        first.append(w.start(src.at[to], out.at[w.g, w.j], w.at_plane(to)))
    out[w.g, w.j] = src[w.j]
    yield
    wait_received(first)
    second = [
        w.start(out.at[w.g], out.at[w.g], w.at_group(w.group_peer(d)))
        for d in range(1, w.n_groups)
    ]
    yield from pause(4)
    wait_sent(first)
    wait_all(second)


def head_rows(w, src, out):
    index = w.g * w.n_plane + w.j
    owner, part = w.head_owner(), lax.rem(index, w.n_groups)
    mine = owner == w.j

    def to(d):
        return pltpu.make_async_remote_copy(
            src_ref=src,
            dst_ref=out.at[part],
            send_sem=w.send.at[base + d],
            recv_sem=w.recv.at[base + part],
            device_id={"g": w.group_peer(d), **w.on_plane(owner)},
            device_id_type=MESH,
        )

    def arrival(r):
        return pltpu.make_async_remote_copy(
            src_ref=src,
            dst_ref=out.at[r],
            send_sem=w.send.at[base],
            recv_sem=w.recv.at[base + r],
            device_id=w.at_device(w.n_groups * w.j + r),
            device_id_type=MESH,
        )

    yield from pause(3)
    base = w.used
    w.used += w.n_groups
    for d in range(w.n_groups):

        @pl.when((d > 0) | jnp.logical_not(mine))
        def _():
            to(d).start()

    @pl.when(mine)
    def _():
        out[part] = src[...]

    yield from pause(2)
    for r in range(w.n_groups):

        @pl.when(jnp.logical_not(mine) | (part != r))
        def _():
            arrival(r).wait_recv()

    for d in range(w.n_groups):

        @pl.when((d > 0) | jnp.logical_not(mine))
        def _():
            to(d).wait_send()


def plane_swap(w, src, out):
    copies = []
    for d in range(1, w.n_plane):
        to = w.plane_peer(d)
        copies.append(w.start(src.at[to], out.at[w.j], w.at_plane(to)))
    out[w.j] = src[w.j]
    yield
    wait_all(copies)


def plane_sum(w, src, out, from_core, pairs, from_chips):
    to = (w.beside(), 3 - w.p, w.above(), w.p)
    beside, above = w.at_chip(w.beside()), w.at_chip(w.above())
    first = [
        w.start(src.at[p * w.cores + 1 - w.c], from_core.at[i], w.partner())
        for i, p in enumerate(to)
    ]
    yield
    sent = []

    def send(i, upper, slot, device):
        sent.append(w.start(part_of(pairs.at[i], upper), from_chips.at[slot], device))

    for i, p in enumerate(to):
        first[i].wait_recv()
        sum_rows(pairs.at[i], [src.at[w.core_of(p)], from_core.at[i]])
        if i < 2:
            send(i, 0, i, beside)
        if i == 1:
            send(1, 1, 2, above)
        if i == 2:
            send(2, 1, 3, above)
    yield
    for wire, i, upper, slot, device in ((1, 2, 0, 4, above), (2, 0, 1, 5, beside)):
        sent[wire].wait_recv()
        target = part_of(pairs.at[i], upper)
        sum_rows(target, [target, from_chips.at[wire]])
        send(i, upper, slot, device)
    yield
    for wire in (0, 3, 4, 5):
        sent[wire].wait_recv()
    for upper, arrived in ((0, (0, 4)), (1, (3, 5))):
        sum_rows(
            part_of(out, upper),
            [part_of(pairs.at[3], upper)] + [from_chips.at[slot] for slot in arrived],
        )
    wait_sent(first)
    wait_sent(sent)


def whole_sum(w, src, out, from_core, pairs, from_chips, total, parts):
    chips = w.n_plane // w.cores
    to = [lax.rem(w.p + d, chips) for d in range(chips)]
    first = [
        w.start(src.at[:, p * w.cores + 1 - w.c], from_core.at[d], w.partner())
        for d, p in enumerate(to)
    ]
    yield
    second = []
    for d in list(range(1, chips)) + [0]:
        first[d].wait_recv()

        def step(i, carry):
            sum_rows(pairs.at[d, i], [src.at[i, w.core_of(to[d])], from_core.at[d, i]])
            return carry

        lax.fori_loop(0, w.n_groups, step, 0)
        if d:
            second.append(w.start(pairs.at[d], from_chips.at[d - 1], w.at_chip(to[d])))
    yield
    wait_received(second)

    def step(i, carry):
        sum_rows(total.at[i], [pairs.at[0, i]] + [from_chips.at[d, i] for d in range(chips - 1)])
        return carry

    lax.fori_loop(0, w.n_groups, step, 0)
    wait_sent(first)
    wait_sent(second)
    yield from group_sum(w, total, out, parts)


def whole_swap(w, src, out, mid):
    first = []
    for d in range(1, w.n_groups):
        to = w.group_peer(d)
        first.append(w.start(src.at[to], mid.at[w.g], w.at_group(to)))
    mid[w.g] = src[w.g]
    yield from pause(3)
    wait_received(first)
    second = []
    for d in range(1, w.n_plane):
        to = w.plane_peer(d)
        second.append(w.start(mid.at[:, to], out.at[:, w.j], w.at_plane(to)))
    out[:, w.j] = mid[:, w.j]
    yield
    wait_sent(first)
    wait_all(second)


def group_sum_home(w, src, out, parts, low, home):
    copies = []
    for d in range(1, w.n_groups):
        to = w.group_peer(d)
        copies.append(w.start(src.at[to], parts.at[d - 1], w.at_group(to)))
    yield from pause(3)
    wait_received(copies)
    sum_rows(low, [src.at[w.g]] + [parts.at[d] for d in range(w.n_groups - 1)])
    stays = w.home_source() == w.g * w.n_plane + w.j
    copy = pltpu.make_async_remote_copy(
        src_ref=low,
        dst_ref=home,
        send_sem=w.send.at[w.used],
        recv_sem=w.recv.at[w.used],
        device_id=w.at_device(w.n_groups * w.j + w.g),
        device_id_type=MESH,
    )
    w.used += 1

    @pl.when(jnp.logical_not(stays))
    def _():
        copy.start()

    @pl.when(stays)
    def _():
        home[...] = low[...]

    yield

    @pl.when(jnp.logical_not(stays))
    def _():
        copy.wait()

    out[...] = home[...].astype(F32)
    wait_sent(copies)


def plane_sum_shift(w, src, out, from_core, pairs, from_chips, low, later):
    rows = out.shape[0]
    yield from plane_sum(w, src, low, from_core, pairs, from_chips)
    copy = w.start(
        low.at[pl.ds(0, rows)], later, w.at_group(lax.rem(w.g + w.n_groups - 1, w.n_groups))
    )
    yield
    copy.wait()
    keep = jnp.where(w.g == w.n_groups - 1, 0.0, 1.0)
    out[...] = low[rows:, :].astype(F32) + later[...].astype(F32) * keep


def group_sum(w, src, out, parts):
    copies = []
    for d in range(1, w.n_groups):
        to = w.group_peer(d)
        copies.append(w.start(src.at[to], parts.at[d - 1], w.at_group(to)))
    yield
    wait_received(copies)
    sum_rows(out, [src.at[w.g]] + [parts.at[d] for d in range(w.n_groups - 1)])
    wait_sent(copies)


def group_sum_swap(w, src, out, total, parts):
    copies = []
    for d in range(1, w.n_groups):
        to = w.group_peer(d)
        copies.append(w.start(src.at[to], parts.at[d - 1], w.at_group(to)))
    yield from pause(4)
    wait_received(copies)

    def step(i, carry):
        sum_rows(total.at[i], [src.at[w.g, i]] + [parts.at[d, i] for d in range(w.n_groups - 1)])
        return carry

    lax.fori_loop(0, w.n_plane, step, 0)
    second = []
    for d in range(1, w.n_plane):
        to = w.plane_peer(d)
        second.append(w.start(total.at[to], out.at[w.j], w.at_plane(to)))
    out[w.j] = total[w.j]
    yield
    wait_sent(copies)
    wait_all(second)


ROUTINES = {
    "plane_gather": plane_gather,
    "shift_gather": shift_gather,
    "whole_gather": whole_gather,
    "far_gather": far_gather,
    "plane_swap_gather": plane_swap_gather,
    "plane_swap": plane_swap,
    "plane_sum": plane_sum,
    "plane_sum_shift": plane_sum_shift,
    "head_rows": head_rows,
    "group_sum": group_sum,
    "whole_sum": whole_sum,
    "whole_swap": whole_swap,
    "group_sum_home": group_sum_home,
    "group_sum_swap": group_sum_swap,
}


def exchange_kernel(n_groups, n_plane, kinds, extra, *refs):
    count = len(kinds)
    sources, outs = refs[:count], refs[count : 2 * count]
    scratch = list(refs[2 * count : -2])
    w = Wires(n_groups, n_plane, refs[-2], refs[-1])
    w.meet("head_rows" in kinds, "group_sum_home" in kinds)
    running = []
    for kind, source, out, number in zip(kinds, sources, outs, extra):
        mine, scratch = scratch[:number], scratch[number:]
        if kind == "shift_gather":
            running.append(shift_gather(w, source, mine[0], out))
        else:
            running.append(ROUTINES[kind](w, source, out, *mine))
    while running:
        still = []
        for routine in running:
            try:
                next(routine)
                still.append(routine)
            except StopIteration:
                pass
        running = still


def exchange(n_groups, n_plane, number, *items):
    kinds = [kind for kind, _ in items]
    arrays = [array for _, array in items]
    shapes, scratch, extra = [], [], []
    chips = n_plane // 2
    for kind, array in items:
        shape, dtype = array.shape, array.dtype
        own = []
        if kind in ("plane_gather", "shift_gather"):
            out = (n_plane,) + shape
            if kind == "shift_gather":
                own = [shape]
        elif kind in ("whole_gather", "far_gather"):
            out = (n_groups, n_plane) + shape
        elif kind == "plane_swap_gather":
            out = (n_groups,) + shape
        elif kind == "plane_swap":
            out = shape
        elif kind == "head_rows":
            out = (n_groups,) + shape
        elif kind == "plane_sum_shift":
            pair = shape[1:]
            out = (shape[1] // 2, shape[2])
            half = (pair[0] // 2, pair[1])
            own = [(chips,) + pair, (chips,) + pair, (6,) + half, pair, out]
        elif kind == "plane_sum":
            out = shape[1:]
            own = [(chips,) + out, (chips,) + out, (6, out[0] // 2, out[1])]
        elif kind == "group_sum_home":
            out = shape[1:]
            own = [(n_groups - 1,) + out, out, out]
        elif kind == "group_sum":
            out = shape[1:]
            own = [(n_groups - 1,) + out]
        elif kind == "whole_swap":
            out = shape
            own = [shape]
        elif kind == "whole_sum":
            out = shape[2:]
            full = (n_groups,) + out
            own = [(chips,) + full, (chips,) + full, (chips - 1,) + full, full]
            own = own + [(n_groups - 1,) + out]
        elif kind == "group_sum_swap":
            out = shape[1:]
            own = [out, (n_groups - 1,) + out]
        if kind in ("plane_sum", "plane_sum_shift", "group_sum", "group_sum_home", "whole_sum"):
            shapes.append(jax.ShapeDtypeStruct(out, F32))
        else:
            shapes.append(jax.ShapeDtypeStruct(out, dtype))
        scratch += [pltpu.VMEM(s, dtype) for s in own]
        if kind == "far_gather":
            own = [None]
            scratch.append(pltpu.SemaphoreType.DMA)
        extra.append(len(own))
    copies = 64 + 32 * len(items)
    vmem = pl.BlockSpec(memory_space=pltpu.VMEM)
    return pl.pallas_call(
        functools.partial(exchange_kernel, n_groups, n_plane, kinds, extra),
        out_shape=shapes,
        in_specs=[vmem] * len(items),
        out_specs=[
            pl.BlockSpec(memory_space=pl.ANY) if kind == "far_gather" else vmem for kind in kinds
        ],
        scratch_shapes=scratch
        + [pltpu.SemaphoreType.DMA((copies,)), pltpu.SemaphoreType.DMA((copies,))],
        compiler_params=pltpu.CompilerParams(
            collective_id=number,
            has_side_effects=True,
            vmem_limit_bytes=60 * 1024 * 1024,
        ),
        name="exchange_%d" % number,
    )(*arrays)


def gather_all(x):
    return lax.all_gather(x, ALL, axis=0, tiled=True)


class StreamSum:
    def __init__(self, w, steps, stage, from_core, pairs, from_chips, totals, parts, sems, credit):
        self.w, self.steps = w, steps
        self.stage, self.from_core, self.pairs = stage, from_core, pairs
        self.from_chips, self.totals, self.parts = from_chips, totals, parts
        self.core_sems, self.chip_sems, self.chip_recv, self.group_sems = sems
        self.credit = credit

    @staticmethod
    def chips(w, step):
        half = lax.rem(step, 2)
        beside = w.p + 1 - 2 * lax.rem(w.p, 2)
        above = w.p + 2 - 4 * (w.p // 2)
        return beside + half * (above - beside), 3 - w.p + half * (2 * w.p - 3)

    def core_copy(self, step, i):
        slot = lax.rem(step, 2)
        return pltpu.make_async_remote_copy(
            src_ref=self.stage.at[slot, 2 * i + 1 - self.w.c],
            dst_ref=self.from_core.at[slot, i],
            send_sem=self.core_sems.at[0, slot, i],
            recv_sem=self.core_sems.at[1, slot, i],
            device_id=self.w.partner(),
            device_id_type=MESH,
        )

    def part(self, ref, upper):
        rows = ref.shape[0] // 2
        return ref.at[pl.ds(rows, rows)] if upper else ref.at[pl.ds(0, rows)]

    def chip_copy(self, group_at, which):
        slot, i, upper, up = (
            (0, 0, False, False),
            (0, 1, False, False),
            (0, 1, True, True),
            (1, 0, True, True),
            (1, 0, False, True),
            (0, 0, True, False),
        )[which]
        p = self.w.p
        to = p + 2 - 4 * (p // 2) if up else p + 1 - 2 * lax.rem(p, 2)
        return pltpu.make_async_remote_copy(
            src_ref=self.part(self.pairs.at[slot, i], upper),
            dst_ref=self.from_chips.at[group_at, which],
            send_sem=self.chip_sems.at[which],
            recv_sem=self.chip_recv.at[group_at, which],
            device_id=self.w.at_chip(to),
            device_id_type=MESH,
        )

    def group_copy(self, group_at):
        return pltpu.make_async_remote_copy(
            src_ref=self.totals.at[group_at],
            dst_ref=self.parts.at[group_at],
            send_sem=self.group_sems.at[0, group_at],
            recv_sem=self.group_sems.at[1, group_at],
            device_id=self.w.at_group(self.w.group_peer(group_at + 1)),
            device_id_type=MESH,
        )

    def open_stage(self, step):
        @pl.when(step >= 2)
        def _():
            for i in range(2):
                self.core_copy(step, i).wait_send()

    def push(self, step):
        @pl.when(step >= 2)
        def _():
            pl.semaphore_wait(self.credit, 1)

        for i in range(2):
            self.core_copy(step, i).start()

    def merge(self, step):
        slot, group_at = lax.rem(step, 2), step // 2
        for half, sends in ((0, (0, 1, 2, 5)), (1, (3, 4))):

            @pl.when((slot == half) & (step >= 2))
            def _():
                for which in sends:
                    self.chip_copy(group_at, which).wait_send()

        for i in range(2):
            self.core_copy(step, i).wait_recv()
            sum_rows(
                self.pairs.at[slot, i],
                [self.stage.at[slot, 2 * i + self.w.c], self.from_core.at[slot, i]],
            )

        @pl.when(step + 2 < self.steps)
        def _():
            pl.semaphore_signal(
                self.credit, inc=1, device_id=self.w.partner(), device_id_type=MESH
            )

        @pl.when(slot == 0)
        def _():
            for which in (0, 1, 2):
                self.chip_copy(group_at, which).start()

        @pl.when(slot == 1)
        def _():
            self.chip_copy(group_at, 3).start()
            for source, i, upper, which in ((1, (1, 0), False, 4), (2, (0, 0), True, 5)):
                self.chip_copy(group_at, source).wait_recv()
                target = self.part(self.pairs.at[i], upper)
                sum_rows(target, [target, self.from_chips.at[group_at, source]])
                self.chip_copy(group_at, which).start()

    def plane_total(self, group_at):
        for which in (0, 3, 4, 5):
            self.chip_copy(group_at, which).wait_recv()
        return [
            [self.part(self.pairs.at[1, 1], upper)]
            + [self.from_chips.at[group_at, which] for which in arrived]
            for upper, arrived in ((False, (0, 4)), (True, (3, 5)))
        ]

    def advance(self, step):
        @pl.when(step >= 1)
        def _():
            last = step - 1

            @pl.when((lax.rem(last, 2) == 0) & (last >= 2))
            def _():
                group_at = last // 2 - 1
                for upper, sources in enumerate(self.plane_total(group_at)):
                    sum_rows(self.part(self.totals.at[group_at], upper), sources)
                self.group_copy(group_at).start()

            self.merge(last)

    def finish(self, out):
        steps = self.steps
        self.merge(steps - 1)
        groups = steps // 2 - 1
        halves = self.plane_total(groups)
        for d in range(groups):
            self.group_copy(d).wait_recv()
        for upper, sources in enumerate(halves):
            parts = [self.part(self.parts.at[d], upper) for d in range(groups)]
            sum_rows(self.part(out, upper), sources + parts)
        for d in range(groups):
            self.group_copy(d).wait_send()
        for i in range(2):
            self.core_copy(steps - 2, i).wait_send()
            self.core_copy(steps - 1, i).wait_send()
        for which in range(6):
            self.chip_copy(groups, which).wait_send()

    @staticmethod
    def scratch(n_groups, rows, width):
        dma = pltpu.SemaphoreType.DMA
        return [
            pltpu.VMEM((2, 4, rows, width), BF),
            pltpu.VMEM((2, 2, rows, width), BF),
            pltpu.VMEM((2, 2, rows, width), BF),
            pltpu.VMEM((n_groups, 6, rows // 2, width), BF),
            pltpu.VMEM((n_groups - 1, rows, width), BF),
            pltpu.VMEM((n_groups - 1, rows, width), BF),
            dma((2, 2, 2)),
            dma((6,)),
            dma((n_groups, 6)),
            dma((2, n_groups - 1)),
            pltpu.SemaphoreType.REGULAR,
        ]


def swiglu_both(gate, up, grad):
    sigmoid = 1.0 / (1.0 + jnp.exp(-gate))
    silu = gate * sigmoid
    return silu * up, grad * up * (sigmoid * (1.0 + gate * (1.0 - sigmoid))), grad * silu


def step_chips(w, step):
    group = lax.rem(w.g + 1 + step // 2, w.n_groups)
    return [group * 4 + chip for chip in StreamSum.chips(w, step)]


def hot_rows(place, rows, core, slot_count):
    mine = place[:, core * rows : (core + 1) * rows]
    return lax.broadcasted_iota(jnp.int32, (slot_count, rows), 0) == mine


def moe_kernel(
    n_groups, experts, first_logit, slot_count,
    h2_hbm, cot_hbm, place_ref, wg_ref, wu_ref, wd_ref, sc_ref, sd_ref,
    sum_ref, rows_ref, gin_ref, act_ref, gg_ref, gu_ref, rw_ref, sact_ref, sgrad_ref, tok_ref,
    h2_buf, cot_buf, load_sems, *comm,
):
    rows = sum_ref.shape[0]
    step, steps = pl.program_id(0), 2 * n_groups
    w = Wires(n_groups, 8, None, None)
    stream = StreamSum(w, steps, *comm[:6], comm[6:10], comm[10])
    expert_id = w.g * 4 + w.p
    half = sc_ref.shape[1] // 2

    def loads(at):
        slot = lax.rem(at, 2)
        for i, chip in enumerate(step_chips(w, at)):
            source = pl.ds(pl.multiple_of(chip * 2 * rows, 2 * rows), 2 * rows)
            target = pl.ds(i * 2 * rows, 2 * rows)
            for k, (hbm, buf) in enumerate(((h2_hbm, h2_buf), (cot_hbm, cot_buf))):
                yield pltpu.make_async_copy(
                    hbm.at[source], buf.at[slot, target], load_sems.at[slot, i, k]
                )

    @pl.when(step == 0)
    def _():
        for copy in loads(step):
            copy.start()
        w.meet()

    @pl.when(step + 1 < steps)
    def _():
        for copy in loads(step + 1):
            copy.start()

    for copy in loads(step):
        copy.wait()
    slot = lax.rem(step, 2)
    h2, cot = h2_buf[slot], cot_buf[slot]
    chips = step_chips(w, step)

    pre = jnp.dot(h2, sc_ref[...], preferred_element_type=F32)
    back = dot_nt(cot, sd_ref[...])
    gate, up = pre[:, :half], pre[:, half:]
    lane = lax.broadcasted_iota(jnp.int32, gate.shape, 1)
    logits = jnp.where((lane >= first_logit) & (lane < first_logit + experts), gate, -1e30)
    exps = jnp.exp(logits - jnp.max(logits, axis=1, keepdims=True))
    chosen = jnp.where(lane == first_logit + expert_id, exps, 0.0)
    weight = jnp.sum(chosen, axis=1, keepdims=True) / jnp.sum(exps, axis=1, keepdims=True)
    act, grad_gate, grad_up = swiglu_both(gate, up, back)
    shared_act = act.astype(BF)
    shared_grad = jnp.concatenate([grad_gate.astype(BF), grad_up.astype(BF)], axis=1)
    for i, chip in enumerate(chips):
        at = pl.ds(pl.multiple_of(chip * 2 * rows, 2 * rows), 2 * rows)
        sact_ref[at, :] = shared_act[i * 2 * rows : (i + 1) * 2 * rows]
        sgrad_ref[at, :] = shared_grad[i * 2 * rows : (i + 1) * 2 * rows]

    hots, weights = [], []
    for q in range(4):
        place = place_ref[pl.ds(chips[q // 2], 1), :]
        hot = hot_rows(place, rows, q % 2, slot_count).astype(F32)
        hots.append(hot)
        tokens = slice(q * rows, (q + 1) * rows)
        slots = slice(q * slot_count, (q + 1) * slot_count)
        low = hot.astype(BF)
        rows_ref[slots, :] = jnp.dot(low, h2[tokens], preferred_element_type=F32).astype(BF)
        gin_ref[slots, :] = jnp.dot(low, cot[tokens], preferred_element_type=F32).astype(BF)
        spread = jnp.broadcast_to(weight[tokens], (rows, 128))
        weights.append(
            jnp.dot(hot, spread, preferred_element_type=F32, precision=lax.Precision.HIGHEST)[:, :1]
        )
    row_weight = jnp.concatenate(weights, axis=0)
    rw_ref[...] = row_weight
    expert_rows = rows_ref[...]
    picked_cot = gin_ref[...]
    back = dot_nt(picked_cot, wd_ref[...])
    gin_ref[...] = (picked_cot.astype(F32) * row_weight).astype(BF)
    gate = dot_nt(expert_rows, wg_ref[...])
    up = dot_nt(expert_rows, wu_ref[...])
    act, grad_gate, grad_up = swiglu_both(gate, up, back * row_weight)
    act_low, grad_gate, grad_up = act.astype(BF), grad_gate.astype(BF), grad_up.astype(BF)
    act_ref[...] = act_low
    gg_ref[...] = grad_gate
    gu_ref[...] = grad_up
    picked = jnp.sum(act_low.astype(F32) * back, axis=1, keepdims=True)
    grad_rows = jnp.dot(grad_gate, wg_ref[...], preferred_element_type=F32)
    grad_rows = grad_rows + jnp.dot(grad_up, wu_ref[...], preferred_element_type=F32)
    grad_rows = grad_rows.astype(BF)
    stream.open_stage(step)
    for q in range(4):
        tokens = slice(q * rows, (q + 1) * rows)
        slots = slice(q * slot_count, (q + 1) * slot_count)
        tok_ref[pl.ds(chips[q // 2] * 2 + q % 2, 1), :] = jnp.sum(
            hots[q] * picked[slots], axis=0, keepdims=True
        )
        total = dot_tn(hots[q].astype(BF), grad_rows[slots]) + dot_nt(
            shared_grad[tokens], sc_ref[...]
        )
        stream.stage[slot, q] = total.astype(BF)
    stream.push(step)
    stream.advance(step)

    @pl.when(step == steps - 1)
    def _():
        stream.finish(sum_ref)


def out_kernel(
    n_groups, slot_count,
    act_ref, rw_ref, rows_ref, gin_ref, gg_ref, gu_ref, place_ref, sact_ref, wd_ref, sd_ref,
    sum_ref, dg_ref, du_ref, dd_ref, *comm,
):
    rows = sum_ref.shape[0]
    step, steps = pl.program_id(0), 2 * n_groups
    w = Wires(n_groups, 8, None, None)
    stream = StreamSum(w, steps, *comm[:6], comm[6:10], comm[10])

    @pl.when(step == 0)
    def _():
        w.meet()
        for ref in (dg_ref, du_ref, dd_ref):
            ref[...] = jnp.zeros_like(ref)

    slot = lax.rem(step, 2)
    chips = step_chips(w, step)
    out_rows = jnp.dot(act_ref[...], wd_ref[...], preferred_element_type=F32) * rw_ref[...]
    out_rows = out_rows.astype(BF)
    stream.open_stage(step)
    for q in range(4):
        chip = chips[q // 2]
        place = place_ref[pl.ds(chip, 1), :]
        low = hot_rows(place, rows, q % 2, slot_count).astype(F32).astype(BF)
        slots = slice(q * slot_count, (q + 1) * slot_count)
        shared = sact_ref[pl.ds(pl.multiple_of((chip * 2 + q % 2) * rows, rows), rows), :]
        total = dot_tn(low, out_rows[slots]) + jnp.dot(
            shared, sd_ref[...], preferred_element_type=F32
        )
        stream.stage[slot, q] = total.astype(BF)
    stream.push(step)
    stream.advance(step)

    width = rows_ref.shape[1]
    piece = width // 4
    for left_ref, right_ref, total_ref in (
        (gg_ref, rows_ref, dg_ref),
        (gu_ref, rows_ref, du_ref),
        (act_ref, gin_ref, dd_ref),
    ):
        turned = left_ref[...].T
        for k in range(4):
            cols = slice(k * piece, (k + 1) * piece)
            total_ref[:, cols] += jnp.dot(
                turned, right_ref[:, cols], preferred_element_type=F32
            )

    @pl.when(step == steps - 1)
    def _():
        stream.finish(sum_ref)


def experts_sums(
    n_groups, rows, h2, cot, place, slot_count, expert_w, shared_w, router_weight, first_id
):
    w_gate, w_up, w_down = expert_w
    s_both, s_down = shared_w
    tokens, width = h2.shape
    hidden, hidden_s = w_down.shape[0], s_down.shape[0]
    experts = router_weight.shape[1]
    steps = 2 * n_groups
    devices = tokens // rows
    step_slots = slot_count * 4
    all_slots = step_slots * steps
    half = 128
    s_cat = jnp.concatenate(
        [
            s_both[:, :hidden_s],
            router_weight,
            jnp.zeros((width, half - hidden_s - experts), BF),
            s_both[:, hidden_s:],
            jnp.zeros((width, half - hidden_s), BF),
        ],
        axis=1,
    )
    s_tall = jnp.pad(s_down, ((0, half - hidden_s), (0, 0)))

    def whole(array):
        return pl.BlockSpec(array.shape, lambda i: (0, 0), pipeline_mode=pl.Buffered(1))

    def blocked(rows, cols):
        return pl.BlockSpec((rows, cols), lambda i: (i, 0))

    shape = jax.ShapeDtypeStruct
    flops = 2 * all_slots * width * hidden * 5 + 2 * tokens * width * (4 * half + 3 * slot_count)
    shapes = [
        shape((rows, width), F32),
        shape((all_slots, width), BF),
        shape((all_slots, width), BF),
        shape((all_slots, hidden), BF),
        shape((all_slots, hidden), BF),
        shape((all_slots, hidden), BF),
        shape((all_slots, 1), F32),
        shape((tokens, half), BF),
        shape((tokens, 2 * half), BF),
        shape((devices, rows), F32),
    ]
    specs = [
        blocked(step_slots, s.shape[1]) if s.shape[0] == all_slots else whole(s) for s in shapes
    ]
    hbm = pl.BlockSpec(memory_space=pl.ANY)
    grad_h2, rows_in, grad_in, act, grad_gate, grad_up, row_weight, s_act, s_grad, token_grad = (
        pl.pallas_call(
            functools.partial(moe_kernel, n_groups, experts, hidden_s, slot_count),
            grid=(steps,),
            in_specs=[
                hbm,
                hbm,
                whole(place),
                whole(w_gate),
                whole(w_up),
                whole(w_down),
                whole(s_cat),
                whole(s_tall),
            ],
            out_specs=specs,
            out_shape=shapes,
            scratch_shapes=[
                pltpu.VMEM((2, 4 * rows, width), BF),
                pltpu.VMEM((2, 4 * rows, width), BF),
                pltpu.SemaphoreType.DMA((2, 2, 2)),
            ]
            + StreamSum.scratch(n_groups, rows, width),
            cost_estimate=pl.CostEstimate(
                flops=flops, bytes_accessed=12 * tokens * width, transcendentals=tokens * 1024
            ),
            compiler_params=pltpu.CompilerParams(
                collective_id=first_id,
                has_side_effects=True,
                vmem_limit_bytes=67043328,
            ),
            name="experts",
        )(h2, cot, place, w_gate, w_up, w_down, s_cat, s_tall)
    )
    shapes = [grad_h2] + [shape(x.shape, F32) for x in expert_w]
    out, d_gate, d_up, d_down = pl.pallas_call(
        functools.partial(out_kernel, n_groups, slot_count),
        grid=(steps,),
        in_specs=[
            blocked(step_slots, hidden),
            blocked(step_slots, 1),
            blocked(step_slots, width),
            blocked(step_slots, width),
            blocked(step_slots, hidden),
            blocked(step_slots, hidden),
            whole(place),
            whole(s_act),
            whole(w_down),
            whole(s_tall),
        ],
        out_specs=[whole(x) for x in shapes],
        out_shape=[shape(x.shape, F32) for x in shapes],
        scratch_shapes=StreamSum.scratch(n_groups, rows, width),
        cost_estimate=pl.CostEstimate(
            flops=2 * width * (4 * all_slots * hidden + tokens * (half + slot_count)),
            bytes_accessed=4 * tokens * width,
            transcendentals=0,
        ),
        compiler_params=pltpu.CompilerParams(
            collective_id=first_id + 1,
            has_side_effects=True,
            vmem_limit_bytes=67043328,
        ),
        name="expert_out",
    )(act, row_weight, rows_in, grad_in, grad_gate, grad_up, place, s_act, w_down, s_tall)
    g_both = dot_tn(h2, s_grad)
    g_both = jnp.concatenate([g_both[:, :hidden_s], g_both[:, half : half + hidden_s]], axis=1)
    grads = (
        d_gate,
        d_up,
        d_down,
        g_both,
        dot_tn(s_act, cot)[:hidden_s],
    )
    return out, grad_h2, token_grad, grads


def body(
    n_groups, n_plane, layer_input, attn_gain, w_query, w_latent, kv_gain, w_expand, w_output,
    ffn_gain, w_router, shared_gate, shared_up, shared_down, expert_gate, expert_up,
    expert_down, routes, segments, cotangent,
):
    tok, width = layer_input.shape
    devices = n_groups * n_plane
    experts = w_router.shape[1]
    local_heads = HEADS // n_plane
    scale = (NOPE + ROPE) ** (-0.5)
    group = lax.axis_index("g")
    place_in = lax.axis_index(PLANE)
    me = lax.axis_index(ALL)
    expert_id = lax.axis_index(("g", "p"))
    plane_tok = n_plane * tok
    plane_start = group * plane_tok

    rows_w = w_router.shape[0]
    kv_n = kv_gain.shape[0]
    small = jnp.concatenate(
        [
            attn_gain,
            ffn_gain,
            kv_gain,
            w_router.reshape(-1),
            routes.reshape(-1).astype(BF),
            segments.astype(BF),
        ]
    )
    small = jnp.pad(small, (0, -small.shape[0] % 4096)).reshape(-1, 128)
    head_cols = local_heads * (NOPE + ROPE)
    kv_cols = local_heads * (NOPE + VDIM)
    fold = kv_n * kv_cols // rows_w
    pair = jnp.concatenate(
        [
            w_query.reshape(rows_w, n_plane, head_cols).transpose(1, 0, 2),
            w_expand.reshape(kv_n, n_plane, kv_cols // fold, fold)
            .transpose(1, 0, 2, 3)
            .reshape(n_plane, rows_w, fold),
        ],
        axis=2,
    )
    swap = functools.partial(exchange, n_groups, n_plane)
    pair, latent_weight, small, x_plane = swap(
        0,
        ("plane_swap_gather", pair),
        ("whole_gather", w_latent),
        ("whole_gather", small),
        ("plane_gather", layer_input),
    )
    x_plane = x_plane.reshape(plane_tok, width).astype(F32)
    latent_weight = latent_weight.reshape(width, RANK + ROPE)
    pair = pair.reshape(width, head_cols + fold)
    small = small.reshape(devices, -1)
    cuts = [rows_w, 2 * rows_w, 2 * rows_w + kv_n, 2 * rows_w + kv_n + rows_w * experts]
    cuts = cuts + [cuts[-1] + tok * TOP, cuts[-1] + tok * TOP + tok]
    gain_one = small[:, : cuts[0]].reshape(-1).astype(F32)
    gain_two = small[:, cuts[0] : cuts[1]].reshape(-1).astype(F32)
    gain_kv = small[:, cuts[1] : cuts[2]].reshape(-1).astype(F32)
    router_weight = small[:, cuts[2] : cuts[3]].reshape(width, experts)
    routes_all = small[:, cuts[3] : cuts[4]].astype(jnp.int32).reshape(devices, tok, TOP)
    segments_all = small[:, cuts[4] : cuts[5]].astype(jnp.int32).reshape(-1)

    query_weight = pair[:, :head_cols].reshape(width, local_heads, NOPE + ROPE)
    wq_nope = query_weight[:, :, :NOPE].reshape(width, local_heads * NOPE)
    wq_rope = query_weight[:, :, NOPE:].reshape(width, local_heads * ROPE)
    expand_weight = pair[:, head_cols:].reshape(RANK, kv_cols)
    cotangent_later = jnp.where(x_plane[0, 0] < 1e6, cotangent, jnp.zeros_like(cotangent))

    shared_n = shared_down.shape[0]
    s_both = jnp.concatenate(
        [
            shared_gate.reshape(rows_w, devices, shared_n),
            shared_up.reshape(rows_w, devices, shared_n),
        ],
        axis=2,
    )
    s_both = lax.all_to_all(s_both, ALL, split_axis=1, concat_axis=0).reshape(width, 2 * shared_n)

    hidden = rms_norm(x_plane, gain_one).astype(BF)
    rope_half = ROPE // 2
    positions = plane_start + jnp.arange(plane_tok, dtype=jnp.int32)
    frequency = 10000.0 ** (-jnp.arange(rope_half, dtype=F32) / rope_half)
    angles = positions.astype(F32)[:, None] * frequency[None, :]
    cosine = jnp.cos(angles)
    sine_part = jnp.sin(angles)
    cos_h, sin_h = cosine[:, None, :], sine_part[:, None, :]
    latent = matmul(hidden, latent_weight)
    compressed_own = rms_norm(latent[:, :RANK], gain_kv).astype(BF)
    key_rope_own = rotate(latent[:, RANK:], cosine, sine_part).astype(BF)

    def own_rows(table):
        return lax.dynamic_slice_in_dim(table, place_in * tok, tok, 0)

    piece = own_rows(jnp.concatenate([compressed_own, key_rope_own], axis=1))
    before, own_output = swap(1, ("shift_gather", piece), ("head_rows", w_output))
    before = before.reshape(plane_tok, RANK + ROPE)
    own_output = own_output.reshape(local_heads * VDIM, width)
    compressed = jnp.concatenate([before[:, :RANK], compressed_own], axis=0)
    key_rope = jnp.concatenate([before[:, RANK:], key_rope_own], axis=0)
    q_nope = matmul(hidden, wq_nope).astype(BF)
    q_rope = rotate(
        matmul(hidden, wq_rope).reshape(plane_tok, local_heads, ROPE), cos_h, sin_h
    ).reshape(plane_tok, local_heads * ROPE).astype(BF)
    expanded = matmul(compressed, expand_weight).astype(BF)
    plane_segments = lax.dynamic_slice_in_dim(segments_all, plane_start, plane_tok, 0)
    doc_start = jnp.sum(
        (segments_all[None, :] < plane_segments[:, None]).astype(jnp.int32), axis=1, keepdims=True
    )
    low_bound = doc_start - plane_start + DOC_MAX
    mixed_heads, lse = attend(low_bound, q_nope, q_rope, expanded, key_rope, scale)
    attn_out = matmul(mixed_heads, own_output).astype(BF)
    attn_out = swap(2, ("plane_sum", attn_out.reshape(n_plane, tok, width)))[0]
    input_float = layer_input.astype(F32)
    residual_one = input_float + attn_out
    h_two_f, norm_two_back = jax.vjp(rms_norm, residual_one, gain_two)
    h_two = h_two_f.astype(BF)
    router_probs = softmax_rows(matmul(h_two, router_weight))

    expert_w = (expert_gate[0].T, expert_up[0].T, expert_down[0])
    shared_w = (s_both, shared_down)
    slot_limit = 2 * tok * TOP // experts

    def on_rows(h2, h2_all, cot_gathered, routes_here):
        rows = h2.shape[0]
        slot_count = min(slot_limit, rows)
        member = jnp.any(routes_here == expert_id, axis=2)
        member_int = member.astype(jnp.int32)
        rank = jnp.cumsum(member_int, axis=1) - member_int
        place = jnp.where(member, rank, -1).reshape(devices // 2, 2 * rows)
        out, grad_h2, token_grad, grads = experts_sums(
            n_groups,
            rows,
            h2_all,
            cot_gathered,
            place,
            slot_count,
            expert_w,
            shared_w,
            router_weight,
            8,
        )
        picked = lax.all_to_all(token_grad, ALL, split_axis=0, concat_axis=0, tiled=True)
        picked = jnp.sum(picked.reshape(experts, devices // experts, rows), axis=1).T
        return out, grad_h2, picked, grads

    parts = max(1, devices * tok // 4096)
    if parts == 1:
        cot_all = gather_all(cotangent_later)
        out_own, grad_h2_own, grad_router_probs, grads = on_rows(
            h_two, swap(5, ("far_gather", h_two))[0].reshape(-1, width), cot_all, routes_all
        )
    else:
        rows = tok // parts

        def step(total, inputs):
            h2, cot, routes_here = inputs
            cot_part = gather_all(cot)
            out, grad_h2, picked, grads = on_rows(h2, gather_all(h2), cot_part, routes_here)
            grads = lax.optimization_barrier(grads)
            total = tuple(a + b for a, b in zip(total, grads))
            return total, (out, grad_h2, picked)

        shapes = expert_w + shared_w
        grads, (out_own, grad_h2_own, grad_router_probs) = lax.scan(
            step,
            tuple(jnp.zeros(s.shape, F32) for s in shapes),
            (
                h_two.reshape(parts, rows, width),
                cotangent.reshape(parts, rows, width),
                routes_all.reshape(devices, parts, rows, TOP).transpose(1, 0, 2, 3),
            ),
        )
        out_own = out_own.reshape(tok, width)
        grad_h2_own = grad_h2_own.reshape(tok, width)
        grad_router_probs = grad_router_probs.reshape(tok, experts)
    g_gate, g_up, g_down, g_both, g_sdown = grads
    grad_logits = router_probs * (
        grad_router_probs - jnp.sum(router_probs * grad_router_probs, axis=1, keepdims=True)
    )
    grad_logits = grad_logits.astype(BF)
    grad_router = dot_tn(h_two, grad_logits)
    grad_h_two = grad_h2_own + dot_nt(grad_logits, router_weight)
    output = residual_one + out_own

    grad_x_one, grad_gain_two = norm_two_back(grad_h_two)
    grad_x_one = grad_x_one + cotangent.astype(F32)
    grad_attn_out = grad_x_one.astype(BF)
    g_shared, plane_grad = swap(
        3,
        ("whole_swap", g_both.astype(BF).reshape(n_groups, n_plane, rows_w, 2 * shared_n)),
        ("plane_gather", grad_attn_out),
    )
    plane_grad = plane_grad.reshape(plane_tok, width)
    grad_mixed = dot_nt(plane_grad, own_output).astype(BF)
    dqn, dqr, dex, dkr = attend_back(
        low_bound, q_nope, q_rope, expanded, key_rope, lse, grad_mixed, scale
    )

    g_output = dot_tn(mixed_heads, plane_grad).astype(BF).reshape(n_groups, rows_w, width)

    grad_expanded = dex.astype(BF)
    grad_expand = dot_tn(compressed, grad_expanded)
    grad_comp = dot_nt(grad_expanded, expand_weight)
    key_grads = jnp.concatenate([grad_comp, dkr], axis=1).astype(BF)
    key_grads = (
        key_grads.reshape(2, n_plane, tok, RANK + ROPE)
        .transpose(1, 0, 2, 3)
        .reshape(n_plane, 2 * tok, RANK + ROPE)
    )

    gq_nope = dqn.astype(BF)
    gq_rope = (
        unrotate(dqr.reshape(plane_tok, local_heads, ROPE), cos_h, sin_h)
        .reshape(plane_tok, local_heads * ROPE)
        .astype(BF)
    )
    grad_hidden = (dot_nt(gq_nope, wq_nope) + dot_nt(gq_rope, wq_rope)).astype(BF)
    gw_nope = dot_tn(hidden, gq_nope).astype(BF).reshape(n_groups, n_plane, rows_w, -1)
    gw_rope = dot_tn(hidden, gq_rope).astype(BF).reshape(n_groups, n_plane, rows_w, -1)
    g_expand = grad_expand.astype(BF).reshape(n_groups, n_plane, kv_n, kv_cols)
    key_grad, grad_hidden, gw_nope, gw_rope, g_expand = swap(
        4,
        ("plane_sum_shift", key_grads),
        ("plane_sum", grad_hidden.reshape(n_plane, tok, width)),
        ("group_sum_swap", gw_nope),
        ("group_sum_swap", gw_rope),
        ("group_sum_swap", g_expand),
    )
    latent_own = own_rows(latent)
    kv_norm_back = jax.vjp(rms_norm, latent_own[:, :RANK], gain_kv)[1]
    grad_comp_in, grad_gain_kv = kv_norm_back(key_grad[:, :RANK])
    grad_rope_in = unrotate(key_grad[:, RANK:], own_rows(cosine), own_rows(sine_part))
    grad_latent = jnp.concatenate([grad_comp_in, grad_rope_in], axis=1).astype(BF)

    def per_head(table, cols):
        return table.transpose(1, 0, 2).reshape(rows_w, HEADS, cols)

    grad_query_weight = jnp.concatenate(
        [per_head(gw_nope, NOPE), per_head(gw_rope, ROPE)], axis=2
    ).reshape(rows_w, -1).astype(F32)
    grad_expand_weight = g_expand.transpose(1, 0, 2).reshape(kv_n, -1).astype(F32)

    g_latent = dot_tn(own_rows(hidden), grad_latent).astype(BF)
    g_latent = g_latent.reshape(n_groups, n_plane, rows_w, RANK + ROPE)
    grad_hidden = grad_hidden + dot_nt(grad_latent, latent_weight)
    norm_one_back = jax.vjp(rms_norm, input_float, gain_one)[1]
    grad_x_norm, grad_gain_one = norm_one_back(grad_hidden)
    grad_input = grad_x_one + grad_x_norm

    small_grads = jnp.concatenate(
        [
            p.reshape(devices, -1)
            for p in (grad_gain_one, grad_gain_two, grad_gain_kv, grad_router)
        ],
        axis=1,
    )
    small_grads = jnp.pad(small_grads, ((0, 0), (0, -small_grads.shape[1] % 1024)))
    grad_latent_weight, grad_output_weight, small_grads = swap(
        6,
        ("whole_sum", g_latent),
        ("group_sum_home", g_output),
        ("whole_sum", small_grads.reshape(n_groups, n_plane, -1, 128)),
    )
    small_grads = small_grads.reshape(-1)
    g_shared = g_shared.transpose(2, 0, 1, 3).reshape(rows_w, devices, 2 * shared_n).astype(F32)
    grad_shared_gate = g_shared[:, :, :shared_n].reshape(rows_w, devices * shared_n)
    grad_shared_up = g_shared[:, :, shared_n:].reshape(rows_w, devices * shared_n)
    return (
        output,
        grad_input,
        small_grads[: cuts[0]],
        grad_query_weight,
        grad_latent_weight,
        small_grads[cuts[1] : cuts[2]],
        grad_expand_weight,
        grad_output_weight,
        small_grads[cuts[0] : cuts[1]],
        small_grads[cuts[2] : cuts[3]].reshape(rows_w, experts),
        grad_shared_gate,
        grad_shared_up,
        g_sdown,
        g_gate.T[None],
        g_up.T[None],
        g_down[None],
    )


def solution(mesh):
    n_expert, n_shard = mesh.shape["expert"], mesh.shape["wshard"]
    devices = n_expert * n_shard

    def program(*args):
        tok = args[0].shape[0] // devices
        n_plane = DOC_MAX // tok
        n_groups = devices // n_plane
        inner = Mesh(mesh.devices.reshape(n_groups, n_plane // n_shard, n_shard), ALL)
        rows, vector = P(ALL, None), P(ALL)
        wide, tall = P(("g", "p"), None, "c"), P(("g", "p"), "c", None)
        step = jax.shard_map(
            functools.partial(body, n_groups, n_plane),
            mesh=inner,
            in_specs=(
                rows, vector, rows, rows, vector, rows, rows, vector, rows, rows, rows, rows,
                wide, wide, tall, rows, vector, rows,
            ),
            out_specs=(
                rows, rows, vector, rows, rows, vector, rows, rows, vector, rows, rows, rows,
                rows, wide, wide, tall,
            ),
            check_vma=False,
        )
        return step(*args)

    return program
```

```python
import functools

import jax
import jax.numpy as jnp
from jax import lax
from jax.experimental import pallas as pl
from jax.experimental.pallas import tpu as pltpu
from jax.sharding import Mesh, PartitionSpec as P

HEADS = 16
NOPE = 128
ROPE = 64
VDIM = 128
RANK = 512
TOP = 6
DOC_MAX = 1024
QUERY_BLOCK = 256

BF = jnp.bfloat16
F32 = jnp.float32
ALL = ("g", "p", "c")
PLANE = ("p", "c")

epsilon = 1e-06


def rms_norm(vector, scaling):
    return vector * lax.rsqrt(jnp.mean(vector * vector, axis=-1, keepdims=True) + epsilon) * scaling


def rotate(vector, cosine, sine_part):
    half_width = vector.shape[-1] // 2
    front_half = vector[..., :half_width]
    back_half = vector[..., half_width:]
    return jnp.concatenate(
        [front_half * cosine - back_half * sine_part, back_half * cosine + front_half * sine_part],
        axis=-1,
    )


def unrotate(vector, cosine, sine_part):
    return rotate(vector, cosine, -sine_part)


def matmul(left, right):
    return jnp.dot(left, right, preferred_element_type=F32)


def dot_nt(left, right):
    return lax.dot_general(left, right, (((1,), (1,)), ((), ())), preferred_element_type=F32)


def dot_tn(left, right):
    return lax.dot_general(left, right, (((0,), (0,)), ((), ())), preferred_element_type=F32)


def swiglu(gate_pre, up_pre):
    return jax.nn.silu(gate_pre) * up_pre


def softmax_rows(scores):
    row_top = jnp.max(scores, axis=-1, keepdims=True)
    exp_scores = jnp.exp(scores - row_top)
    return exp_scores / jnp.sum(exp_scores, axis=-1, keepdims=True)


def masked_scores(base, low_bound, q_nope, q_rope, k_nope, k_rope, scale):
    rows, span = q_nope.shape[0], k_nope.shape[0]
    key_at = lax.broadcasted_iota(jnp.int32, (rows, span), 1) + base
    query_at = lax.broadcasted_iota(jnp.int32, (rows, span), 0) + (base + DOC_MAX)
    allowed = (key_at >= low_bound) & (key_at <= query_at)
    scores = (dot_nt(q_nope, k_nope) + dot_nt(q_rope, k_rope)) * scale
    return jnp.where(allowed, scores, -1e30)


def attend_kernel(heads, scale, low_ref, qn_ref, qr_ref, ex_ref, kr_ref, out_ref, lse_ref):
    rows = qn_ref.shape[0]
    base = pl.multiple_of(pl.program_id(0) * rows, rows)
    window = pl.ds(base, rows + DOC_MAX)
    k_rope = kr_ref[window, :]
    low_bound = low_ref[...]
    for h in range(heads):
        at = h * (NOPE + VDIM)
        k_nope = ex_ref[window, at : at + NOPE]
        value = ex_ref[window, at + NOPE : at + NOPE + VDIM]
        scores = masked_scores(
            base,
            low_bound,
            qn_ref[:, h * NOPE : (h + 1) * NOPE],
            qr_ref[:, h * ROPE : (h + 1) * ROPE],
            k_nope,
            k_rope,
            scale,
        )
        top = jnp.max(scores, axis=-1, keepdims=True)
        exps = jnp.exp(scores - top)
        total = jnp.sum(exps, axis=-1, keepdims=True)
        probs = (exps / total).astype(BF)
        out_ref[:, h * VDIM : (h + 1) * VDIM] = jnp.dot(
            probs, value, preferred_element_type=F32
        ).astype(BF)
        lse_ref[:, h : h + 1] = top + jnp.log(total)


def attend(low_bound, q_nope, q_rope, expanded, key_rope, scale):
    queries = q_nope.shape[0]
    heads = q_nope.shape[1] // NOPE
    rows = QUERY_BLOCK

    def whole(array):
        return pl.BlockSpec(array.shape, lambda i: (0, 0))

    def blocked(width):
        return pl.BlockSpec((rows, width), lambda i: (i, 0))

    flops = 2 * heads * queries * (rows + DOC_MAX) * (NOPE + ROPE + VDIM)
    return pl.pallas_call(
        functools.partial(attend_kernel, heads, scale),
        grid=(queries // rows,),
        in_specs=[
            blocked(1),
            blocked(heads * NOPE),
            blocked(heads * ROPE),
            whole(expanded),
            whole(key_rope),
        ],
        out_specs=[blocked(heads * VDIM), blocked(heads)],
        out_shape=[
            jax.ShapeDtypeStruct((queries, heads * VDIM), BF),
            jax.ShapeDtypeStruct((queries, heads), F32),
        ],
        cost_estimate=pl.CostEstimate(
            flops=flops, bytes_accessed=4 * expanded.size, transcendentals=flops // 640
        ),
        compiler_params=pltpu.CompilerParams(vmem_limit_bytes=50 * 1024 * 1024),
        name="attend",
    )(low_bound, q_nope, q_rope, expanded, key_rope)


def attend_back_kernel(
    heads, scale, low_ref, qn_ref, qr_ref, ex_ref, kr_ref, lse_ref, gm_ref,
    dqn_ref, dqr_ref, dex_ref, dkr_ref,
):
    rows = qn_ref.shape[0]
    step = pl.program_id(0)
    base = pl.multiple_of(step * rows, rows)
    window = pl.ds(base, rows + DOC_MAX)

    @pl.when(step == 0)
    def _():
        dex_ref[...] = jnp.zeros_like(dex_ref)
        dkr_ref[...] = jnp.zeros_like(dkr_ref)

    k_rope = kr_ref[window, :]
    low_bound = low_ref[...]
    for h in range(heads):
        at = h * (NOPE + VDIM)
        k_nope = ex_ref[window, at : at + NOPE]
        value = ex_ref[window, at + NOPE : at + NOPE + VDIM]
        q_nope = qn_ref[:, h * NOPE : (h + 1) * NOPE]
        q_rope = qr_ref[:, h * ROPE : (h + 1) * ROPE]
        grad_out = gm_ref[:, h * VDIM : (h + 1) * VDIM]
        scores = masked_scores(base, low_bound, q_nope, q_rope, k_nope, k_rope, scale)
        probs = jnp.exp(scores - lse_ref[:, h : h + 1])
        grad_probs = dot_nt(grad_out, value)
        mean_grad = jnp.sum(probs * grad_probs, axis=-1, keepdims=True)
        grad_scores = (probs * (grad_probs - mean_grad) * scale).astype(BF)
        probs_low = probs.astype(BF)
        dqn_ref[:, h * NOPE : (h + 1) * NOPE] = jnp.dot(
            grad_scores, k_nope, preferred_element_type=F32
        )
        dqr_ref[:, h * ROPE : (h + 1) * ROPE] = jnp.dot(
            grad_scores, k_rope, preferred_element_type=F32
        )
        dex_ref[window, at : at + NOPE] += dot_tn(grad_scores, q_nope)
        dex_ref[window, at + NOPE : at + NOPE + VDIM] += dot_tn(probs_low, grad_out)
        dkr_ref[window, :] += dot_tn(grad_scores, q_rope)


def attend_back(low_bound, q_nope, q_rope, expanded, key_rope, lse, grad_mixed, scale):
    queries = q_nope.shape[0]
    heads = q_nope.shape[1] // NOPE
    rows = QUERY_BLOCK

    def whole(shape):
        return pl.BlockSpec(shape, lambda i: (0, 0))

    def blocked(width):
        return pl.BlockSpec((rows, width), lambda i: (i, 0))

    flops = 2 * heads * queries * (rows + DOC_MAX) * (3 * NOPE + 3 * ROPE + 2 * VDIM)
    return pl.pallas_call(
        functools.partial(attend_back_kernel, heads, scale),
        grid=(queries // rows,),
        in_specs=[
            blocked(1),
            blocked(heads * NOPE),
            blocked(heads * ROPE),
            whole(expanded.shape),
            whole(key_rope.shape),
            blocked(heads),
            blocked(heads * VDIM),
        ],
        out_specs=[
            blocked(heads * NOPE),
            blocked(heads * ROPE),
            whole(expanded.shape),
            whole(key_rope.shape),
        ],
        out_shape=[
            jax.ShapeDtypeStruct(q_nope.shape, F32),
            jax.ShapeDtypeStruct(q_rope.shape, F32),
            jax.ShapeDtypeStruct(expanded.shape, F32),
            jax.ShapeDtypeStruct(key_rope.shape, F32),
        ],
        cost_estimate=pl.CostEstimate(
            flops=flops, bytes_accessed=8 * expanded.size, transcendentals=flops // 1664
        ),
        compiler_params=pltpu.CompilerParams(vmem_limit_bytes=56 * 1024 * 1024),
        name="attend_back",
    )(low_bound, q_nope, q_rope, expanded, key_rope, lse, grad_mixed)


MESH = pl.DeviceIdType.MESH


def pause(rounds):
    for _ in range(rounds):
        yield


class Wires:
    def __init__(self, n_groups, n_plane, send, recv):
        self.n_groups, self.n_plane, self.send, self.recv = n_groups, n_plane, send, recv
        self.cores = 2
        self.g, self.p, self.c = lax.axis_index("g"), lax.axis_index("p"), lax.axis_index("c")
        self.j = self.p * self.cores + self.c
        self.used = 0

    def at_plane(self, j):
        return {"g": self.g, "p": j // self.cores, "c": j % self.cores}

    def at_chip(self, p):
        return {"g": self.g, "p": p, "c": self.c}

    def at_group(self, g):
        return {"g": g, "p": self.p, "c": self.c}

    def partner(self):
        return {"g": self.g, "p": self.p, "c": 1 - self.c}

    def beside(self):
        return self.p + 1 - 2 * lax.rem(self.p, 2)

    def above(self):
        return self.p + 2 - 4 * (self.p // 2)

    def core_of(self, p):
        return p * self.cores + self.c

    def plane_peer(self, d):
        return lax.rem(self.j + d, self.n_plane)

    def group_peer(self, d):
        return lax.rem(self.g + d, self.n_groups)

    def start(self, src, dst, device):
        copy = pltpu.make_async_remote_copy(
            src_ref=src,
            dst_ref=dst,
            send_sem=self.send.at[self.used],
            recv_sem=self.recv.at[self.used],
            device_id=device,
            device_id_type=MESH,
        )
        self.used += 1
        copy.start()
        return copy

    def at_device(self, index):
        return {"g": index // self.n_plane, **self.on_plane(lax.rem(index, self.n_plane))}

    def on_plane(self, j):
        return {"p": j // self.cores, "c": j % self.cores}

    def meet(self, heads=False, home=False):
        barrier = pltpu.get_barrier_semaphore()
        waits = self.n_plane - 1 + self.n_groups - 1
        if heads:
            mine = self.head_owner() == self.j
            part = lax.rem(self.g * self.n_plane + self.j, self.n_groups)
            for r in range(self.n_groups):

                @pl.when(jnp.logical_not(mine) | (part != r))
                def _():
                    source = self.at_device(self.n_groups * self.j + r)
                    pl.semaphore_signal(barrier, inc=1, device_id=source, device_id_type=MESH)

            waits = waits + jnp.where(mine, self.n_groups - 1, self.n_groups)
        if home:
            source = self.home_source()
            stays = source == self.g * self.n_plane + self.j

            @pl.when(jnp.logical_not(stays))
            def _():
                pl.semaphore_signal(
                    barrier, inc=1, device_id=self.at_device(source), device_id_type=MESH
                )

            waits = waits + jnp.where(stays, 0, 1)
        for d in range(1, self.n_plane):
            pl.semaphore_signal(
                barrier, inc=1, device_id=self.at_plane(self.plane_peer(d)), device_id_type=MESH
            )
        for d in range(1, self.n_groups):
            pl.semaphore_signal(
                barrier, inc=1, device_id=self.at_group(self.group_peer(d)), device_id_type=MESH
            )
        pl.semaphore_wait(barrier, waits)

    def home_source(self):
        index = self.g * self.n_plane + self.j
        return lax.rem(index, self.n_groups) * self.n_plane + index // self.n_groups

    def head_owner(self):
        return (self.g * self.n_plane + self.j) // self.n_groups


def sum_rows(dst, sources):
    rows = dst.shape[0]
    tile = 32 if rows % 32 == 0 else rows

    def step(i, carry):
        at = pl.ds(pl.multiple_of(i * tile, tile), tile)
        if len(sources) == 2 and all(r.dtype == BF for r in [dst] + sources):
            dst[at, :] = sources[0][at, :] + sources[1][at, :]
        else:
            total = sources[0][at, :].astype(F32)
            for source in sources[1:]:
                total = total + source[at, :].astype(F32)
            dst[at, :] = total.astype(dst.dtype)
        return carry

    lax.fori_loop(0, rows // tile, step, 0)


def wait_all(copies):
    for copy in copies:
        copy.wait()


def wait_received(copies):
    for copy in copies:
        copy.wait_recv()


def wait_sent(copies):
    for copy in copies:
        copy.wait_send()


def part_of(ref, upper):
    rows = ref.shape[0] // 2
    return ref.at[pl.ds(rows, rows)] if upper else ref.at[pl.ds(0, rows)]


def spread(w, own, at):
    beside, above = w.at_chip(w.beside()), w.at_chip(w.above())
    mine = at(w.j)
    halves = [(part_of(own, u), part_of(mine, u)) for u in (0, 1)]
    lower = w.start(*halves[0], beside)
    upper = w.start(*halves[1], above)
    rest = [w.start(*halves[1], beside), w.start(*halves[0], above)]
    on_chip = [w.start(own, mine, w.partner())]
    yield
    lower.wait_recv()
    block = part_of(at(w.core_of(w.beside())), 0)
    rest.append(w.start(block, block, above))
    upper.wait_recv()
    block = part_of(at(w.core_of(w.above())), 1)
    rest.append(w.start(block, block, beside))
    yield
    wait_received(rest)
    for p in (w.beside(), w.above(), 3 - w.p):
        block = at(w.core_of(p))
        on_chip.append(w.start(block, block, w.partner()))
    yield
    wait_sent([lower, upper] + rest)
    wait_all(on_chip)


def plane_gather(w, src, out):
    out[w.j] = src[...]
    yield from spread(w, src, lambda j: out.at[j])


def far_gather(w, src, out, sem):
    mine = out.at[w.g, w.j]
    away = [w.start(src, mine, w.at_group(w.group_peer(d))) for d in range(1, w.n_groups)]
    local = pltpu.make_async_copy(src, mine, sem)
    local.start()
    running = [spread(w, src, lambda j: out.at[w.g, j])]
    next(running[0])
    for d in range(1, w.n_groups):
        away[d - 1].wait_recv()
        g = w.group_peer(w.n_groups - d)
        running.append(spread(w, out.at[g, w.j], lambda j, g=g: out.at[g, j]))
        next(running[d])
    for _ in range(3):
        for routine in running:
            next(routine, None)
        yield
    local.wait()
    wait_sent(away)


def shift_gather(w, src, mid, out):
    copy = w.start(src, mid, w.at_group(lax.rem(w.g + 1, w.n_groups)))
    yield
    copy.wait()
    yield from plane_gather(w, mid, out)


def whole_gather(w, src, out):
    chips = w.n_plane // w.cores
    first = [
        w.start(src, out.at[w.g, w.j], w.at_group(w.group_peer(d))) for d in range(1, w.n_groups)
    ]
    out[w.g, w.j] = src[...]
    yield
    wait_received(first)
    mine = out.at[:, w.j]
    second = [w.start(mine, mine, w.at_chip(lax.rem(w.p + d, chips))) for d in range(1, chips)]
    third = [w.start(mine, mine, w.partner())]
    yield
    for d in range(1, chips):
        second[d - 1].wait_recv()
        block = out.at[:, w.core_of(lax.rem(w.p + chips - d, chips))]
        third.append(w.start(block, block, w.partner()))
    yield
    wait_sent(first)
    wait_sent(second)
    wait_all(third)


def plane_swap_gather(w, src, out):
    first = []
    for d in range(1, w.n_plane):
        to = w.plane_peer(d)
        first.append(w.start(src.at[to], out.at[w.g, w.j], w.at_plane(to)))
    out[w.g, w.j] = src[w.j]
    yield
    wait_received(first)
    second = [
        w.start(out.at[w.g], out.at[w.g], w.at_group(w.group_peer(d)))
        for d in range(1, w.n_groups)
    ]
    yield from pause(4)
    wait_sent(first)
    wait_all(second)


def head_rows(w, src, out):
    index = w.g * w.n_plane + w.j
    owner, part = w.head_owner(), lax.rem(index, w.n_groups)
    mine = owner == w.j

    def to(d):
        return pltpu.make_async_remote_copy(
            src_ref=src,
            dst_ref=out.at[part],
            send_sem=w.send.at[base + d],
            recv_sem=w.recv.at[base + part],
            device_id={"g": w.group_peer(d), **w.on_plane(owner)},
            device_id_type=MESH,
        )

    def arrival(r):
        return pltpu.make_async_remote_copy(
            src_ref=src,
            dst_ref=out.at[r],
            send_sem=w.send.at[base],
            recv_sem=w.recv.at[base + r],
            device_id=w.at_device(w.n_groups * w.j + r),
            device_id_type=MESH,
        )

    yield from pause(3)
    base = w.used
    w.used += w.n_groups
    for d in range(w.n_groups):

        @pl.when((d > 0) | jnp.logical_not(mine))
        def _():
            to(d).start()

    @pl.when(mine)
    def _():
        out[part] = src[...]

    yield from pause(2)
    for r in range(w.n_groups):

        @pl.when(jnp.logical_not(mine) | (part != r))
        def _():
            arrival(r).wait_recv()

    for d in range(w.n_groups):

        @pl.when((d > 0) | jnp.logical_not(mine))
        def _():
            to(d).wait_send()


def plane_swap(w, src, out):
    copies = []
    for d in range(1, w.n_plane):
        to = w.plane_peer(d)
        copies.append(w.start(src.at[to], out.at[w.j], w.at_plane(to)))
    out[w.j] = src[w.j]
    yield
    wait_all(copies)


def plane_sum(w, src, out, from_core, pairs, from_chips):
    to = (w.beside(), 3 - w.p, w.above(), w.p)
    beside, above = w.at_chip(w.beside()), w.at_chip(w.above())
    first = [
        w.start(src.at[p * w.cores + 1 - w.c], from_core.at[i], w.partner())
        for i, p in enumerate(to)
    ]
    yield
    sent = []

    def send(i, upper, slot, device):
        sent.append(w.start(part_of(pairs.at[i], upper), from_chips.at[slot], device))

    for i, p in enumerate(to):
        first[i].wait_recv()
        sum_rows(pairs.at[i], [src.at[w.core_of(p)], from_core.at[i]])
        if i < 2:
            send(i, 0, i, beside)
        if i == 1:
            send(1, 1, 2, above)
        if i == 2:
            send(2, 1, 3, above)
    yield
    for wire, i, upper, slot, device in ((1, 2, 0, 4, above), (2, 0, 1, 5, beside)):
        sent[wire].wait_recv()
        target = part_of(pairs.at[i], upper)
        sum_rows(target, [target, from_chips.at[wire]])
        send(i, upper, slot, device)
    yield
    for wire in (0, 3, 4, 5):
        sent[wire].wait_recv()
    for upper, arrived in ((0, (0, 4)), (1, (3, 5))):
        sum_rows(
            part_of(out, upper),
            [part_of(pairs.at[3], upper)] + [from_chips.at[slot] for slot in arrived],
        )
    wait_sent(first)
    wait_sent(sent)


def whole_sum(w, src, out, from_core, pairs, from_chips, total, parts):
    chips = w.n_plane // w.cores
    to = [lax.rem(w.p + d, chips) for d in range(chips)]
    first = [
        w.start(src.at[:, p * w.cores + 1 - w.c], from_core.at[d], w.partner())
        for d, p in enumerate(to)
    ]
    yield
    second = []
    for d in list(range(1, chips)) + [0]:
        first[d].wait_recv()

        def step(i, carry):
            sum_rows(pairs.at[d, i], [src.at[i, w.core_of(to[d])], from_core.at[d, i]])
            return carry

        lax.fori_loop(0, w.n_groups, step, 0)
        if d:
            second.append(w.start(pairs.at[d], from_chips.at[d - 1], w.at_chip(to[d])))
    yield
    wait_received(second)

    def step(i, carry):
        sum_rows(total.at[i], [pairs.at[0, i]] + [from_chips.at[d, i] for d in range(chips - 1)])
        return carry

    lax.fori_loop(0, w.n_groups, step, 0)
    wait_sent(first)
    wait_sent(second)
    yield from group_sum(w, total, out, parts)


def whole_swap(w, src, out, mid):
    first = []
    for d in range(1, w.n_groups):
        to = w.group_peer(d)
        first.append(w.start(src.at[to], mid.at[w.g], w.at_group(to)))
    mid[w.g] = src[w.g]
    yield from pause(3)
    wait_received(first)
    second = []
    for d in range(1, w.n_plane):
        to = w.plane_peer(d)
        second.append(w.start(mid.at[:, to], out.at[:, w.j], w.at_plane(to)))
    out[:, w.j] = mid[:, w.j]
    yield
    wait_sent(first)
    wait_all(second)


def group_sum_home(w, src, out, parts, low, home):
    copies = []
    for d in range(1, w.n_groups):
        to = w.group_peer(d)
        copies.append(w.start(src.at[to], parts.at[d - 1], w.at_group(to)))
    yield from pause(3)
    wait_received(copies)
    sum_rows(low, [src.at[w.g]] + [parts.at[d] for d in range(w.n_groups - 1)])
    stays = w.home_source() == w.g * w.n_plane + w.j
    copy = pltpu.make_async_remote_copy(
        src_ref=low,
        dst_ref=home,
        send_sem=w.send.at[w.used],
        recv_sem=w.recv.at[w.used],
        device_id=w.at_device(w.n_groups * w.j + w.g),
        device_id_type=MESH,
    )
    w.used += 1

    @pl.when(jnp.logical_not(stays))
    def _():
        copy.start()

    @pl.when(stays)
    def _():
        home[...] = low[...]

    yield

    @pl.when(jnp.logical_not(stays))
    def _():
        copy.wait()

    out[...] = home[...].astype(F32)
    wait_sent(copies)


def plane_sum_shift(w, src, out, from_core, pairs, from_chips, low, later):
    rows = out.shape[0]
    yield from plane_sum(w, src, low, from_core, pairs, from_chips)
    copy = w.start(
        low.at[pl.ds(0, rows)], later, w.at_group(lax.rem(w.g + w.n_groups - 1, w.n_groups))
    )
    yield
    copy.wait()
    keep = jnp.where(w.g == w.n_groups - 1, 0.0, 1.0)
    out[...] = low[rows:, :].astype(F32) + later[...].astype(F32) * keep


def group_sum(w, src, out, parts):
    copies = []
    for d in range(1, w.n_groups):
        to = w.group_peer(d)
        copies.append(w.start(src.at[to], parts.at[d - 1], w.at_group(to)))
    yield
    wait_received(copies)
    sum_rows(out, [src.at[w.g]] + [parts.at[d] for d in range(w.n_groups - 1)])
    wait_sent(copies)


def group_sum_swap(w, src, out, total, parts):
    copies = []
    for d in range(1, w.n_groups):
        to = w.group_peer(d)
        copies.append(w.start(src.at[to], parts.at[d - 1], w.at_group(to)))
    yield from pause(4)
    wait_received(copies)

    def step(i, carry):
        sum_rows(total.at[i], [src.at[w.g, i]] + [parts.at[d, i] for d in range(w.n_groups - 1)])
        return carry

    lax.fori_loop(0, w.n_plane, step, 0)
    second = []
    for d in range(1, w.n_plane):
        to = w.plane_peer(d)
        second.append(w.start(total.at[to], out.at[w.j], w.at_plane(to)))
    out[w.j] = total[w.j]
    yield
    wait_sent(copies)
    wait_all(second)


ROUTINES = {
    "plane_gather": plane_gather,
    "shift_gather": shift_gather,
    "whole_gather": whole_gather,
    "far_gather": far_gather,
    "plane_swap_gather": plane_swap_gather,
    "plane_swap": plane_swap,
    "plane_sum": plane_sum,
    "plane_sum_shift": plane_sum_shift,
    "head_rows": head_rows,
    "group_sum": group_sum,
    "whole_sum": whole_sum,
    "whole_swap": whole_swap,
    "group_sum_home": group_sum_home,
    "group_sum_swap": group_sum_swap,
}


def exchange_kernel(n_groups, n_plane, kinds, extra, *refs):
    count = len(kinds)
    sources, outs = refs[:count], refs[count : 2 * count]
    scratch = list(refs[2 * count : -2])
    w = Wires(n_groups, n_plane, refs[-2], refs[-1])
    w.meet("head_rows" in kinds, "group_sum_home" in kinds)
    running = []
    for kind, source, out, number in zip(kinds, sources, outs, extra):
        mine, scratch = scratch[:number], scratch[number:]
        if kind == "shift_gather":
            running.append(shift_gather(w, source, mine[0], out))
        else:
            running.append(ROUTINES[kind](w, source, out, *mine))
    while running:
        still = []
        for routine in running:
            try:
                next(routine)
                still.append(routine)
            except StopIteration:
                pass
        running = still


def exchange(n_groups, n_plane, number, *items):
    kinds = [kind for kind, _ in items]
    arrays = [array for _, array in items]
    shapes, scratch, extra = [], [], []
    chips = n_plane // 2
    for kind, array in items:
        shape, dtype = array.shape, array.dtype
        own = []
        if kind in ("plane_gather", "shift_gather"):
            out = (n_plane,) + shape
            if kind == "shift_gather":
                own = [shape]
        elif kind in ("whole_gather", "far_gather"):
            out = (n_groups, n_plane) + shape
        elif kind == "plane_swap_gather":
            out = (n_groups,) + shape
        elif kind == "plane_swap":
            out = shape
        elif kind == "head_rows":
            out = (n_groups,) + shape
        elif kind == "plane_sum_shift":
            pair = shape[1:]
            out = (shape[1] // 2, shape[2])
            half = (pair[0] // 2, pair[1])
            own = [(chips,) + pair, (chips,) + pair, (6,) + half, pair, out]
        elif kind == "plane_sum":
            out = shape[1:]
            own = [(chips,) + out, (chips,) + out, (6, out[0] // 2, out[1])]
        elif kind == "group_sum_home":
            out = shape[1:]
            own = [(n_groups - 1,) + out, out, out]
        elif kind == "group_sum":
            out = shape[1:]
            own = [(n_groups - 1,) + out]
        elif kind == "whole_swap":
            out = shape
            own = [shape]
        elif kind == "whole_sum":
            out = shape[2:]
            full = (n_groups,) + out
            own = [(chips,) + full, (chips,) + full, (chips - 1,) + full, full]
            own = own + [(n_groups - 1,) + out]
        elif kind == "group_sum_swap":
            out = shape[1:]
            own = [out, (n_groups - 1,) + out]
        if kind in ("plane_sum", "plane_sum_shift", "group_sum", "group_sum_home", "whole_sum"):
            shapes.append(jax.ShapeDtypeStruct(out, F32))
        else:
            shapes.append(jax.ShapeDtypeStruct(out, dtype))
        scratch += [pltpu.VMEM(s, dtype) for s in own]
        if kind == "far_gather":
            own = [None]
            scratch.append(pltpu.SemaphoreType.DMA)
        extra.append(len(own))
    copies = 64 + 32 * len(items)
    vmem = pl.BlockSpec(memory_space=pltpu.VMEM)
    return pl.pallas_call(
        functools.partial(exchange_kernel, n_groups, n_plane, kinds, extra),
        out_shape=shapes,
        in_specs=[vmem] * len(items),
        out_specs=[
            pl.BlockSpec(memory_space=pl.ANY) if kind == "far_gather" else vmem for kind in kinds
        ],
        scratch_shapes=scratch
        + [pltpu.SemaphoreType.DMA((copies,)), pltpu.SemaphoreType.DMA((copies,))],
        compiler_params=pltpu.CompilerParams(
            collective_id=number,
            has_side_effects=True,
            vmem_limit_bytes=60 * 1024 * 1024,
        ),
        name="exchange_%d" % number,
    )(*arrays)


def gather_all(x):
    return lax.all_gather(x, ALL, axis=0, tiled=True)


class StreamSum:
    def __init__(self, w, steps, stage, from_core, pairs, from_chips, totals, parts, sems, credit):
        self.w, self.steps = w, steps
        self.stage, self.from_core, self.pairs = stage, from_core, pairs
        self.from_chips, self.totals, self.parts = from_chips, totals, parts
        self.core_sems, self.chip_sems, self.chip_recv, self.group_sems = sems
        self.credit = credit

    @staticmethod
    def chips(w, step):
        half = lax.rem(step, 2)
        beside = w.p + 1 - 2 * lax.rem(w.p, 2)
        above = w.p + 2 - 4 * (w.p // 2)
        return beside + half * (above - beside), 3 - w.p + half * (2 * w.p - 3)

    def core_copy(self, step, i):
        slot = lax.rem(step, 2)
        return pltpu.make_async_remote_copy(
            src_ref=self.stage.at[slot, 2 * i + 1 - self.w.c],
            dst_ref=self.from_core.at[slot, i],
            send_sem=self.core_sems.at[0, slot, i],
            recv_sem=self.core_sems.at[1, slot, i],
            device_id=self.w.partner(),
            device_id_type=MESH,
        )

    def part(self, ref, upper):
        rows = ref.shape[0] // 2
        return ref.at[pl.ds(rows, rows)] if upper else ref.at[pl.ds(0, rows)]

    def chip_copy(self, group_at, which):
        slot, i, upper, up = (
            (0, 0, False, False),
            (0, 1, False, False),
            (0, 1, True, True),
            (1, 0, True, True),
            (1, 0, False, True),
            (0, 0, True, False),
        )[which]
        p = self.w.p
        to = p + 2 - 4 * (p // 2) if up else p + 1 - 2 * lax.rem(p, 2)
        return pltpu.make_async_remote_copy(
            src_ref=self.part(self.pairs.at[slot, i], upper),
            dst_ref=self.from_chips.at[group_at, which],
            send_sem=self.chip_sems.at[which],
            recv_sem=self.chip_recv.at[group_at, which],
            device_id=self.w.at_chip(to),
            device_id_type=MESH,
        )

    def group_copy(self, group_at):
        return pltpu.make_async_remote_copy(
            src_ref=self.totals.at[group_at],
            dst_ref=self.parts.at[group_at],
            send_sem=self.group_sems.at[0, group_at],
            recv_sem=self.group_sems.at[1, group_at],
            device_id=self.w.at_group(self.w.group_peer(group_at + 1)),
            device_id_type=MESH,
        )

    def open_stage(self, step):
        @pl.when(step >= 2)
        def _():
            for i in range(2):
                self.core_copy(step, i).wait_send()

    def push(self, step):
        @pl.when(step >= 2)
        def _():
            pl.semaphore_wait(self.credit, 1)

        for i in range(2):
            self.core_copy(step, i).start()

    def merge(self, step):
        slot, group_at = lax.rem(step, 2), step // 2
        for half, sends in ((0, (0, 1, 2, 5)), (1, (3, 4))):

            @pl.when((slot == half) & (step >= 2))
            def _():
                for which in sends:
                    self.chip_copy(group_at, which).wait_send()

        for i in range(2):
            self.core_copy(step, i).wait_recv()
            sum_rows(
                self.pairs.at[slot, i],
                [self.stage.at[slot, 2 * i + self.w.c], self.from_core.at[slot, i]],
            )

        @pl.when(step + 2 < self.steps)
        def _():
            pl.semaphore_signal(
                self.credit, inc=1, device_id=self.w.partner(), device_id_type=MESH
            )

        @pl.when(slot == 0)
        def _():
            for which in (0, 1, 2):
                self.chip_copy(group_at, which).start()

        @pl.when(slot == 1)
        def _():
            self.chip_copy(group_at, 3).start()
            for source, i, upper, which in ((1, (1, 0), False, 4), (2, (0, 0), True, 5)):
                self.chip_copy(group_at, source).wait_recv()
                target = self.part(self.pairs.at[i], upper)
                sum_rows(target, [target, self.from_chips.at[group_at, source]])
                self.chip_copy(group_at, which).start()

    def plane_total(self, group_at):
        for which in (0, 3, 4, 5):
            self.chip_copy(group_at, which).wait_recv()
        return [
            [self.part(self.pairs.at[1, 1], upper)]
            + [self.from_chips.at[group_at, which] for which in arrived]
            for upper, arrived in ((False, (0, 4)), (True, (3, 5)))
        ]

    def advance(self, step):
        @pl.when(step >= 1)
        def _():
            last = step - 1

            @pl.when((lax.rem(last, 2) == 0) & (last >= 2))
            def _():
                group_at = last // 2 - 1
                for upper, sources in enumerate(self.plane_total(group_at)):
                    sum_rows(self.part(self.totals.at[group_at], upper), sources)
                self.group_copy(group_at).start()

            self.merge(last)

    def finish(self, out):
        steps = self.steps
        self.merge(steps - 1)
        groups = steps // 2 - 1
        halves = self.plane_total(groups)
        for d in range(groups):
            self.group_copy(d).wait_recv()
        for upper, sources in enumerate(halves):
            parts = [self.part(self.parts.at[d], upper) for d in range(groups)]
            sum_rows(self.part(out, upper), sources + parts)
        for d in range(groups):
            self.group_copy(d).wait_send()
        for i in range(2):
            self.core_copy(steps - 2, i).wait_send()
            self.core_copy(steps - 1, i).wait_send()
        for which in range(6):
            self.chip_copy(groups, which).wait_send()

    @staticmethod
    def scratch(n_groups, rows, width):
        dma = pltpu.SemaphoreType.DMA
        return [
            pltpu.VMEM((2, 4, rows, width), BF),
            pltpu.VMEM((2, 2, rows, width), BF),
            pltpu.VMEM((2, 2, rows, width), BF),
            pltpu.VMEM((n_groups, 6, rows // 2, width), BF),
            pltpu.VMEM((n_groups - 1, rows, width), BF),
            pltpu.VMEM((n_groups - 1, rows, width), BF),
            dma((2, 2, 2)),
            dma((6,)),
            dma((n_groups, 6)),
            dma((2, n_groups - 1)),
            pltpu.SemaphoreType.REGULAR,
        ]


def swiglu_both(gate, up, grad):
    sigmoid = 1.0 / (1.0 + jnp.exp(-gate))
    silu = gate * sigmoid
    return silu * up, grad * up * (sigmoid * (1.0 + gate * (1.0 - sigmoid))), grad * silu


def step_chips(w, step):
    group = lax.rem(w.g + 1 + step // 2, w.n_groups)
    return [group * 4 + chip for chip in StreamSum.chips(w, step)]


def hot_rows(place, rows, core, slot_count):
    mine = place[:, core * rows : (core + 1) * rows]
    return lax.broadcasted_iota(jnp.int32, (slot_count, rows), 0) == mine


def moe_kernel(
    n_groups, experts, first_logit, slot_count,
    h2_hbm, cot_hbm, place_ref, wg_ref, wu_ref, wd_ref, sc_ref, sd_ref,
    sum_ref, rows_ref, gin_ref, act_ref, gg_ref, gu_ref, rw_ref, sact_ref, dboth_ref, dsd_ref,
    tok_ref,
    h2_buf, cot_buf, load_sems, *comm,
):
    rows = sum_ref.shape[0]
    step, steps = pl.program_id(0), 2 * n_groups
    w = Wires(n_groups, 8, None, None)
    stream = StreamSum(w, steps, *comm[:6], comm[6:10], comm[10])
    expert_id = w.g * 4 + w.p
    half = sc_ref.shape[1] // 2

    def loads(at):
        slot = lax.rem(at, 2)
        for i, chip in enumerate(step_chips(w, at)):
            source = pl.ds(pl.multiple_of(chip * 2 * rows, 2 * rows), 2 * rows)
            target = pl.ds(i * 2 * rows, 2 * rows)
            for k, (hbm, buf) in enumerate(((h2_hbm, h2_buf), (cot_hbm, cot_buf))):
                yield pltpu.make_async_copy(
                    hbm.at[source], buf.at[slot, target], load_sems.at[slot, i, k]
                )

    @pl.when(step == 0)
    def _():
        for copy in loads(step):
            copy.start()
        w.meet()
        for ref in (dboth_ref, dsd_ref):
            ref[...] = jnp.zeros_like(ref)

    @pl.when(step + 1 < steps)
    def _():
        for copy in loads(step + 1):
            copy.start()

    for copy in loads(step):
        copy.wait()
    slot = lax.rem(step, 2)
    h2, cot = h2_buf[slot], cot_buf[slot]
    chips = step_chips(w, step)

    pre = jnp.dot(h2, sc_ref[...], preferred_element_type=F32)
    back = dot_nt(cot, sd_ref[...])
    gate, up = pre[:, :half], pre[:, half:]
    lane = lax.broadcasted_iota(jnp.int32, gate.shape, 1)
    logits = jnp.where((lane >= first_logit) & (lane < first_logit + experts), gate, -1e30)
    exps = jnp.exp(logits - jnp.max(logits, axis=1, keepdims=True))
    chosen = jnp.where(lane == first_logit + expert_id, exps, 0.0)
    weight = jnp.sum(chosen, axis=1, keepdims=True) / jnp.sum(exps, axis=1, keepdims=True)
    act, grad_gate, grad_up = swiglu_both(gate, up, back)
    shared_act = act.astype(BF)
    shared_grad = jnp.concatenate([grad_gate.astype(BF), grad_up.astype(BF)], axis=1)
    for i, chip in enumerate(chips):
        at = pl.ds(pl.multiple_of(chip * 2 * rows, 2 * rows), 2 * rows)
        sact_ref[at, :] = shared_act[i * 2 * rows : (i + 1) * 2 * rows]

    hots, weights = [], []
    for q in range(4):
        place = place_ref[pl.ds(chips[q // 2], 1), :]
        hot = hot_rows(place, rows, q % 2, slot_count).astype(F32)
        hots.append(hot)
        tokens = slice(q * rows, (q + 1) * rows)
        slots = slice(q * slot_count, (q + 1) * slot_count)
        low = hot.astype(BF)
        rows_ref[slots, :] = jnp.dot(low, h2[tokens], preferred_element_type=F32).astype(BF)
        gin_ref[slots, :] = jnp.dot(low, cot[tokens], preferred_element_type=F32).astype(BF)
        spread = jnp.broadcast_to(weight[tokens], (rows, 128))
        weights.append(
            jnp.dot(hot, spread, preferred_element_type=F32, precision=lax.Precision.HIGHEST)[:, :1]
        )
    row_weight = jnp.concatenate(weights, axis=0)
    rw_ref[...] = row_weight
    expert_rows = rows_ref[...]
    picked_cot = gin_ref[...]
    back = dot_nt(picked_cot, wd_ref[...])
    gin_ref[...] = (picked_cot.astype(F32) * row_weight).astype(BF)
    gate = dot_nt(expert_rows, wg_ref[...])
    up = dot_nt(expert_rows, wu_ref[...])
    act, grad_gate, grad_up = swiglu_both(gate, up, back * row_weight)
    act_low, grad_gate, grad_up = act.astype(BF), grad_gate.astype(BF), grad_up.astype(BF)
    act_ref[...] = act_low
    gg_ref[...] = grad_gate
    gu_ref[...] = grad_up
    picked = jnp.sum(act_low.astype(F32) * back, axis=1, keepdims=True)
    grad_rows = jnp.dot(grad_gate, wg_ref[...], preferred_element_type=F32)
    grad_rows = grad_rows + jnp.dot(grad_up, wu_ref[...], preferred_element_type=F32)
    grad_rows = grad_rows.astype(BF)
    stream.open_stage(step)
    for q in range(4):
        tokens = slice(q * rows, (q + 1) * rows)
        slots = slice(q * slot_count, (q + 1) * slot_count)
        tok_ref[pl.ds(chips[q // 2] * 2 + q % 2, 1), :] = jnp.sum(
            hots[q] * picked[slots], axis=0, keepdims=True
        )
        total = dot_tn(hots[q].astype(BF), grad_rows[slots]) + dot_nt(
            shared_grad[tokens], sc_ref[...]
        )
        stream.stage[slot, q] = total.astype(BF)
    stream.push(step)

    piece = h2.shape[1] // 4
    turned, turned_act = shared_grad.T, shared_act.T
    for k in range(4):
        cols = slice(k * piece, (k + 1) * piece)
        dboth_ref[:, cols] += jnp.dot(turned, h2[:, cols], preferred_element_type=F32)
        dsd_ref[:, cols] += jnp.dot(turned_act, cot[:, cols], preferred_element_type=F32)
    stream.advance(step)

    @pl.when(step == steps - 1)
    def _():
        stream.finish(sum_ref)


def out_kernel(
    n_groups, slot_count,
    act_ref, rw_ref, rows_ref, gin_ref, gg_ref, gu_ref, place_ref, sact_ref, wd_ref, sd_ref,
    sum_ref, dg_ref, du_ref, dd_ref, *comm,
):
    rows = sum_ref.shape[0]
    step, steps = pl.program_id(0), 2 * n_groups
    w = Wires(n_groups, 8, None, None)
    stream = StreamSum(w, steps, *comm[:6], comm[6:10], comm[10])

    @pl.when(step == 0)
    def _():
        w.meet()
        for ref in (dg_ref, du_ref, dd_ref):
            ref[...] = jnp.zeros_like(ref)

    slot = lax.rem(step, 2)
    chips = step_chips(w, step)
    out_rows = jnp.dot(act_ref[...], wd_ref[...], preferred_element_type=F32) * rw_ref[...]
    out_rows = out_rows.astype(BF)
    stream.open_stage(step)
    for q in range(4):
        chip = chips[q // 2]
        place = place_ref[pl.ds(chip, 1), :]
        low = hot_rows(place, rows, q % 2, slot_count).astype(F32).astype(BF)
        slots = slice(q * slot_count, (q + 1) * slot_count)
        shared = sact_ref[pl.ds(pl.multiple_of((chip * 2 + q % 2) * rows, rows), rows), :]
        total = dot_tn(low, out_rows[slots]) + jnp.dot(
            shared, sd_ref[...], preferred_element_type=F32
        )
        stream.stage[slot, q] = total.astype(BF)
    stream.push(step)
    stream.advance(step)

    width = rows_ref.shape[1]
    piece = width // 4
    for left_ref, right_ref, total_ref in (
        (gg_ref, rows_ref, dg_ref),
        (gu_ref, rows_ref, du_ref),
        (act_ref, gin_ref, dd_ref),
    ):
        turned = left_ref[...].T
        for k in range(4):
            cols = slice(k * piece, (k + 1) * piece)
            total_ref[:, cols] += jnp.dot(
                turned, right_ref[:, cols], preferred_element_type=F32
            )

    @pl.when(step == steps - 1)
    def _():
        stream.finish(sum_ref)


def experts_sums(
    n_groups, rows, h2, cot, place, slot_count, expert_w, shared_w, router_weight, first_id
):
    w_gate, w_up, w_down = expert_w
    s_both, s_down = shared_w
    tokens, width = h2.shape
    hidden, hidden_s = w_down.shape[0], s_down.shape[0]
    experts = router_weight.shape[1]
    steps = 2 * n_groups
    devices = tokens // rows
    step_slots = slot_count * 4
    all_slots = step_slots * steps
    half = 128
    s_cat = jnp.concatenate(
        [
            s_both[:, :hidden_s],
            router_weight,
            jnp.zeros((width, half - hidden_s - experts), BF),
            s_both[:, hidden_s:],
            jnp.zeros((width, half - hidden_s), BF),
        ],
        axis=1,
    )
    s_tall = jnp.pad(s_down, ((0, half - hidden_s), (0, 0)))

    def whole(array):
        return pl.BlockSpec(array.shape, lambda i: (0, 0), pipeline_mode=pl.Buffered(1))

    def blocked(rows, cols):
        return pl.BlockSpec((rows, cols), lambda i: (i, 0))

    shape = jax.ShapeDtypeStruct
    flops = 2 * all_slots * width * hidden * 5 + 2 * tokens * width * (4 * half + 3 * slot_count)
    shapes = [
        shape((rows, width), F32),
        shape((all_slots, width), BF),
        shape((all_slots, width), BF),
        shape((all_slots, hidden), BF),
        shape((all_slots, hidden), BF),
        shape((all_slots, hidden), BF),
        shape((all_slots, 1), F32),
        shape((tokens, half), BF),
        shape((2 * half, width), F32),
        shape((half, width), F32),
        shape((devices, rows), F32),
    ]
    specs = [
        blocked(step_slots, s.shape[1]) if s.shape[0] == all_slots else whole(s) for s in shapes
    ]
    hbm = pl.BlockSpec(memory_space=pl.ANY)
    grad_h2, rows_in, grad_in, act, grad_gate, grad_up, row_weight, s_act, *d_shared, token_grad = (
        pl.pallas_call(
            functools.partial(moe_kernel, n_groups, experts, hidden_s, slot_count),
            grid=(steps,),
            in_specs=[
                hbm,
                hbm,
                whole(place),
                whole(w_gate),
                whole(w_up),
                whole(w_down),
                whole(s_cat),
                whole(s_tall),
            ],
            out_specs=specs,
            out_shape=shapes,
            scratch_shapes=[
                pltpu.VMEM((2, 4 * rows, width), BF),
                pltpu.VMEM((2, 4 * rows, width), BF),
                pltpu.SemaphoreType.DMA((2, 2, 2)),
            ]
            + StreamSum.scratch(n_groups, rows, width),
            cost_estimate=pl.CostEstimate(
                flops=flops, bytes_accessed=12 * tokens * width, transcendentals=tokens * 1024
            ),
            compiler_params=pltpu.CompilerParams(
                collective_id=first_id,
                has_side_effects=True,
                vmem_limit_bytes=67043328,
            ),
            name="experts",
        )(h2, cot, place, w_gate, w_up, w_down, s_cat, s_tall)
    )
    shapes = [grad_h2] + [shape(x.shape, F32) for x in expert_w]
    out, d_gate, d_up, d_down = pl.pallas_call(
        functools.partial(out_kernel, n_groups, slot_count),
        grid=(steps,),
        in_specs=[
            blocked(step_slots, hidden),
            blocked(step_slots, 1),
            blocked(step_slots, width),
            blocked(step_slots, width),
            blocked(step_slots, hidden),
            blocked(step_slots, hidden),
            whole(place),
            whole(s_act),
            whole(w_down),
            whole(s_tall),
        ],
        out_specs=[whole(x) for x in shapes],
        out_shape=[shape(x.shape, F32) for x in shapes],
        scratch_shapes=StreamSum.scratch(n_groups, rows, width),
        cost_estimate=pl.CostEstimate(
            flops=2 * width * (4 * all_slots * hidden + tokens * (half + slot_count)),
            bytes_accessed=4 * tokens * width,
            transcendentals=0,
        ),
        compiler_params=pltpu.CompilerParams(
            collective_id=first_id + 1,
            has_side_effects=True,
            vmem_limit_bytes=67043328,
        ),
        name="expert_out",
    )(act, row_weight, rows_in, grad_in, grad_gate, grad_up, place, s_act, w_down, s_tall)
    d_both, d_tall = d_shared
    d_both = jnp.concatenate([d_both[:hidden_s], d_both[half : half + hidden_s]], axis=0)
    grads = (d_gate, d_up, d_down, d_both.T, d_tall[:hidden_s])
    return out, grad_h2, token_grad, grads


def body(
    n_groups, n_plane, layer_input, attn_gain, w_query, w_latent, kv_gain, w_expand, w_output,
    ffn_gain, w_router, shared_gate, shared_up, shared_down, expert_gate, expert_up,
    expert_down, routes, segments, cotangent,
):
    tok, width = layer_input.shape
    devices = n_groups * n_plane
    experts = w_router.shape[1]
    local_heads = HEADS // n_plane
    scale = (NOPE + ROPE) ** (-0.5)
    group = lax.axis_index("g")
    place_in = lax.axis_index(PLANE)
    me = lax.axis_index(ALL)
    expert_id = lax.axis_index(("g", "p"))
    plane_tok = n_plane * tok
    plane_start = group * plane_tok

    rows_w = w_router.shape[0]
    kv_n = kv_gain.shape[0]
    small = jnp.concatenate(
        [
            attn_gain,
            ffn_gain,
            kv_gain,
            w_router.reshape(-1),
            routes.reshape(-1).astype(BF),
            segments.astype(BF),
        ]
    )
    small = jnp.pad(small, (0, -small.shape[0] % 4096)).reshape(-1, 128)
    head_cols = local_heads * (NOPE + ROPE)
    kv_cols = local_heads * (NOPE + VDIM)
    fold = kv_n * kv_cols // rows_w
    pair = jnp.concatenate(
        [
            w_query.reshape(rows_w, n_plane, head_cols).transpose(1, 0, 2),
            w_expand.reshape(kv_n, n_plane, kv_cols // fold, fold)
            .transpose(1, 0, 2, 3)
            .reshape(n_plane, rows_w, fold),
        ],
        axis=2,
    )
    swap = functools.partial(exchange, n_groups, n_plane)
    pair, latent_weight, small, x_plane = swap(
        0,
        ("plane_swap_gather", pair),
        ("whole_gather", w_latent),
        ("whole_gather", small),
        ("plane_gather", layer_input),
    )
    x_plane = x_plane.reshape(plane_tok, width).astype(F32)
    latent_weight = latent_weight.reshape(width, RANK + ROPE)
    pair = pair.reshape(width, head_cols + fold)
    small = small.reshape(devices, -1)
    cuts = [rows_w, 2 * rows_w, 2 * rows_w + kv_n, 2 * rows_w + kv_n + rows_w * experts]
    cuts = cuts + [cuts[-1] + tok * TOP, cuts[-1] + tok * TOP + tok]
    gain_one = small[:, : cuts[0]].reshape(-1).astype(F32)
    gain_two = small[:, cuts[0] : cuts[1]].reshape(-1).astype(F32)
    gain_kv = small[:, cuts[1] : cuts[2]].reshape(-1).astype(F32)
    router_weight = small[:, cuts[2] : cuts[3]].reshape(width, experts)
    routes_all = small[:, cuts[3] : cuts[4]].astype(jnp.int32).reshape(devices, tok, TOP)
    segments_all = small[:, cuts[4] : cuts[5]].astype(jnp.int32).reshape(-1)

    query_weight = pair[:, :head_cols].reshape(width, local_heads, NOPE + ROPE)
    wq_nope = query_weight[:, :, :NOPE].reshape(width, local_heads * NOPE)
    wq_rope = query_weight[:, :, NOPE:].reshape(width, local_heads * ROPE)
    expand_weight = pair[:, head_cols:].reshape(RANK, kv_cols)
    cotangent_later = jnp.where(x_plane[0, 0] < 1e6, cotangent, jnp.zeros_like(cotangent))

    shared_n = shared_down.shape[0]
    s_both = jnp.concatenate(
        [
            shared_gate.reshape(rows_w, devices, shared_n),
            shared_up.reshape(rows_w, devices, shared_n),
        ],
        axis=2,
    )
    s_both = s_both.transpose(1, 0, 2).reshape(n_groups, n_plane, rows_w, 2 * shared_n)

    hidden = rms_norm(x_plane, gain_one).astype(BF)
    rope_half = ROPE // 2
    positions = plane_start + jnp.arange(plane_tok, dtype=jnp.int32)
    frequency = 10000.0 ** (-jnp.arange(rope_half, dtype=F32) / rope_half)
    angles = positions.astype(F32)[:, None] * frequency[None, :]
    cosine = jnp.cos(angles)
    sine_part = jnp.sin(angles)
    cos_h, sin_h = cosine[:, None, :], sine_part[:, None, :]
    latent = matmul(hidden, latent_weight)
    compressed_own = rms_norm(latent[:, :RANK], gain_kv).astype(BF)
    key_rope_own = rotate(latent[:, RANK:], cosine, sine_part).astype(BF)

    def own_rows(table):
        return lax.dynamic_slice_in_dim(table, place_in * tok, tok, 0)

    piece = own_rows(jnp.concatenate([compressed_own, key_rope_own], axis=1))
    before, own_output = swap(1, ("shift_gather", piece), ("head_rows", w_output))
    before = before.reshape(plane_tok, RANK + ROPE)
    own_output = own_output.reshape(local_heads * VDIM, width)
    compressed = jnp.concatenate([before[:, :RANK], compressed_own], axis=0)
    key_rope = jnp.concatenate([before[:, RANK:], key_rope_own], axis=0)
    q_nope = matmul(hidden, wq_nope).astype(BF)
    q_rope = rotate(
        matmul(hidden, wq_rope).reshape(plane_tok, local_heads, ROPE), cos_h, sin_h
    ).reshape(plane_tok, local_heads * ROPE).astype(BF)
    expanded = matmul(compressed, expand_weight).astype(BF)
    plane_segments = lax.dynamic_slice_in_dim(segments_all, plane_start, plane_tok, 0)
    doc_start = jnp.sum(
        (segments_all[None, :] < plane_segments[:, None]).astype(jnp.int32), axis=1, keepdims=True
    )
    low_bound = doc_start - plane_start + DOC_MAX
    mixed_heads, lse = attend(low_bound, q_nope, q_rope, expanded, key_rope, scale)
    attn_out = matmul(mixed_heads, own_output).astype(BF)
    attn_out = swap(2, ("plane_sum", attn_out.reshape(n_plane, tok, width)))[0]
    input_float = layer_input.astype(F32)
    residual_one = input_float + attn_out
    h_two_f, norm_two_back = jax.vjp(rms_norm, residual_one, gain_two)
    h_two = h_two_f.astype(BF)
    router_probs = softmax_rows(matmul(h_two, router_weight))

    expert_w = (expert_gate[0].T, expert_up[0].T, expert_down[0])
    parts = max(1, devices * tok // 4096)
    if parts == 1:
        h2_all, s_both = swap(5, ("far_gather", h_two), ("whole_swap", s_both))
    else:
        s_both = swap(7, ("whole_swap", s_both))[0]
    shared_w = (s_both.reshape(width, 2 * shared_n), shared_down)
    slot_limit = 2 * tok * TOP // experts

    def on_rows(h2, h2_all, cot_gathered, routes_here):
        rows = h2.shape[0]
        slot_count = min(slot_limit, rows)
        member = jnp.any(routes_here == expert_id, axis=2)
        member_int = member.astype(jnp.int32)
        rank = jnp.cumsum(member_int, axis=1) - member_int
        place = jnp.where(member, rank, -1).reshape(devices // 2, 2 * rows)
        out, grad_h2, token_grad, grads = experts_sums(
            n_groups,
            rows,
            h2_all,
            cot_gathered,
            place,
            slot_count,
            expert_w,
            shared_w,
            router_weight,
            8,
        )
        picked = lax.all_to_all(token_grad, ALL, split_axis=0, concat_axis=0, tiled=True)
        picked = jnp.sum(picked.reshape(experts, devices // experts, rows), axis=1).T
        return out, grad_h2, picked, grads

    if parts == 1:
        cot_all = gather_all(cotangent_later)
        out_own, grad_h2_own, grad_router_probs, grads = on_rows(
            h_two, h2_all.reshape(-1, width), cot_all, routes_all
        )
    else:
        rows = tok // parts

        def step(total, inputs):
            h2, cot, routes_here = inputs
            cot_part = gather_all(cot)
            out, grad_h2, picked, grads = on_rows(h2, gather_all(h2), cot_part, routes_here)
            grads = lax.optimization_barrier(grads)
            total = tuple(a + b for a, b in zip(total, grads))
            return total, (out, grad_h2, picked)

        shapes = expert_w + shared_w
        grads, (out_own, grad_h2_own, grad_router_probs) = lax.scan(
            step,
            tuple(jnp.zeros(s.shape, F32) for s in shapes),
            (
                h_two.reshape(parts, rows, width),
                cotangent.reshape(parts, rows, width),
                routes_all.reshape(devices, parts, rows, TOP).transpose(1, 0, 2, 3),
            ),
        )
        out_own = out_own.reshape(tok, width)
        grad_h2_own = grad_h2_own.reshape(tok, width)
        grad_router_probs = grad_router_probs.reshape(tok, experts)
    g_gate, g_up, g_down, g_both, g_sdown = grads
    grad_logits = router_probs * (
        grad_router_probs - jnp.sum(router_probs * grad_router_probs, axis=1, keepdims=True)
    )
    grad_logits = grad_logits.astype(BF)
    grad_router = dot_tn(h_two, grad_logits)
    grad_h_two = grad_h2_own + dot_nt(grad_logits, router_weight)
    output = residual_one + out_own

    grad_x_one, grad_gain_two = norm_two_back(grad_h_two)
    grad_x_one = grad_x_one + cotangent.astype(F32)
    grad_attn_out = grad_x_one.astype(BF)
    g_shared, plane_grad = swap(
        3,
        ("whole_swap", g_both.astype(BF).reshape(n_groups, n_plane, rows_w, 2 * shared_n)),
        ("plane_gather", grad_attn_out),
    )
    plane_grad = plane_grad.reshape(plane_tok, width)
    grad_mixed = dot_nt(plane_grad, own_output).astype(BF)
    dqn, dqr, dex, dkr = attend_back(
        low_bound, q_nope, q_rope, expanded, key_rope, lse, grad_mixed, scale
    )

    g_output = dot_tn(mixed_heads, plane_grad).astype(BF).reshape(n_groups, rows_w, width)

    grad_expanded = dex.astype(BF)
    grad_expand = dot_tn(compressed, grad_expanded)
    grad_comp = dot_nt(grad_expanded, expand_weight)
    key_grads = jnp.concatenate([grad_comp, dkr], axis=1).astype(BF)
    key_grads = (
        key_grads.reshape(2, n_plane, tok, RANK + ROPE)
        .transpose(1, 0, 2, 3)
        .reshape(n_plane, 2 * tok, RANK + ROPE)
    )

    gq_nope = dqn.astype(BF)
    gq_rope = (
        unrotate(dqr.reshape(plane_tok, local_heads, ROPE), cos_h, sin_h)
        .reshape(plane_tok, local_heads * ROPE)
        .astype(BF)
    )
    grad_hidden = (dot_nt(gq_nope, wq_nope) + dot_nt(gq_rope, wq_rope)).astype(BF)
    gw_nope = dot_tn(hidden, gq_nope).astype(BF).reshape(n_groups, n_plane, rows_w, -1)
    gw_rope = dot_tn(hidden, gq_rope).astype(BF).reshape(n_groups, n_plane, rows_w, -1)
    g_expand = grad_expand.astype(BF).reshape(n_groups, n_plane, kv_n, kv_cols)
    key_grad, grad_hidden, gw_nope, gw_rope, g_expand = swap(
        4,
        ("plane_sum_shift", key_grads),
        ("plane_sum", grad_hidden.reshape(n_plane, tok, width)),
        ("group_sum_swap", gw_nope),
        ("group_sum_swap", gw_rope),
        ("group_sum_swap", g_expand),
    )
    latent_own = own_rows(latent)
    kv_norm_back = jax.vjp(rms_norm, latent_own[:, :RANK], gain_kv)[1]
    grad_comp_in, grad_gain_kv = kv_norm_back(key_grad[:, :RANK])
    grad_rope_in = unrotate(key_grad[:, RANK:], own_rows(cosine), own_rows(sine_part))
    grad_latent = jnp.concatenate([grad_comp_in, grad_rope_in], axis=1).astype(BF)

    def per_head(table, cols):
        return table.transpose(1, 0, 2).reshape(rows_w, HEADS, cols)

    grad_query_weight = jnp.concatenate(
        [per_head(gw_nope, NOPE), per_head(gw_rope, ROPE)], axis=2
    ).reshape(rows_w, -1).astype(F32)
    grad_expand_weight = g_expand.transpose(1, 0, 2).reshape(kv_n, -1).astype(F32)

    g_latent = dot_tn(own_rows(hidden), grad_latent).astype(BF)
    g_latent = g_latent.reshape(n_groups, n_plane, rows_w, RANK + ROPE)
    grad_hidden = grad_hidden + dot_nt(grad_latent, latent_weight)
    norm_one_back = jax.vjp(rms_norm, input_float, gain_one)[1]
    grad_x_norm, grad_gain_one = norm_one_back(grad_hidden)
    grad_input = grad_x_one + grad_x_norm

    small_grads = jnp.concatenate(
        [
            p.reshape(devices, -1)
            for p in (grad_gain_one, grad_gain_two, grad_gain_kv, grad_router)
        ],
        axis=1,
    )
    small_grads = jnp.pad(small_grads, ((0, 0), (0, -small_grads.shape[1] % 1024)))
    grad_latent_weight, grad_output_weight, small_grads = swap(
        6,
        ("whole_sum", g_latent),
        ("group_sum_home", g_output),
        ("whole_sum", small_grads.reshape(n_groups, n_plane, -1, 128)),
    )
    small_grads = small_grads.reshape(-1)
    g_shared = g_shared.transpose(2, 0, 1, 3).reshape(rows_w, devices, 2 * shared_n).astype(F32)
    grad_shared_gate = g_shared[:, :, :shared_n].reshape(rows_w, devices * shared_n)
    grad_shared_up = g_shared[:, :, shared_n:].reshape(rows_w, devices * shared_n)
    return (
        output,
        grad_input,
        small_grads[: cuts[0]],
        grad_query_weight,
        grad_latent_weight,
        small_grads[cuts[1] : cuts[2]],
        grad_expand_weight,
        grad_output_weight,
        small_grads[cuts[0] : cuts[1]],
        small_grads[cuts[2] : cuts[3]].reshape(rows_w, experts),
        grad_shared_gate,
        grad_shared_up,
        g_sdown,
        g_gate.T[None],
        g_up.T[None],
        g_down[None],
    )


def solution(mesh):
    n_expert, n_shard = mesh.shape["expert"], mesh.shape["wshard"]
    devices = n_expert * n_shard

    def program(*args):
        tok = args[0].shape[0] // devices
        n_plane = DOC_MAX // tok
        n_groups = devices // n_plane
        inner = Mesh(mesh.devices.reshape(n_groups, n_plane // n_shard, n_shard), ALL)
        rows, vector = P(ALL, None), P(ALL)
        wide, tall = P(("g", "p"), None, "c"), P(("g", "p"), "c", None)
        step = jax.shard_map(
            functools.partial(body, n_groups, n_plane),
            mesh=inner,
            in_specs=(
                rows, vector, rows, rows, vector, rows, rows, vector, rows, rows, rows, rows,
                wide, wide, tall, rows, vector, rows,
            ),
            out_specs=(
                rows, rows, vector, rows, rows, vector, rows, rows, vector, rows, rows, rows,
                rows, wide, wide, tall,
            ),
            check_vma=False,
        )
        return step(*args)

    return program
```

```python
import functools

import jax
import jax.numpy as jnp
from jax import lax
from jax.experimental import pallas as pl
from jax.experimental.pallas import tpu as pltpu
from jax.sharding import Mesh, PartitionSpec as P

HEADS = 16
NOPE = 128
ROPE = 64
VDIM = 128
RANK = 512
TOP = 6
DOC_MAX = 1024
QUERY_BLOCK = 256

BF = jnp.bfloat16
F32 = jnp.float32
ALL = ("g", "p", "c")
PLANE = ("p", "c")

epsilon = 1e-06


def rms_norm(vector, scaling):
    return vector * lax.rsqrt(jnp.mean(vector * vector, axis=-1, keepdims=True) + epsilon) * scaling


def rotate(vector, cosine, sine_part):
    half_width = vector.shape[-1] // 2
    front_half = vector[..., :half_width]
    back_half = vector[..., half_width:]
    return jnp.concatenate(
        [front_half * cosine - back_half * sine_part, back_half * cosine + front_half * sine_part],
        axis=-1,
    )


def unrotate(vector, cosine, sine_part):
    return rotate(vector, cosine, -sine_part)


def matmul(left, right):
    return jnp.dot(left, right, preferred_element_type=F32)


def dot_nt(left, right):
    return lax.dot_general(left, right, (((1,), (1,)), ((), ())), preferred_element_type=F32)


def dot_tn(left, right):
    return lax.dot_general(left, right, (((0,), (0,)), ((), ())), preferred_element_type=F32)


def swiglu(gate_pre, up_pre):
    return jax.nn.silu(gate_pre) * up_pre


def softmax_rows(scores):
    row_top = jnp.max(scores, axis=-1, keepdims=True)
    exp_scores = jnp.exp(scores - row_top)
    return exp_scores / jnp.sum(exp_scores, axis=-1, keepdims=True)


def masked_scores(base, low_bound, q_nope, q_rope, k_nope, k_rope, scale):
    rows, span = q_nope.shape[0], k_nope.shape[0]
    key_at = lax.broadcasted_iota(jnp.int32, (rows, span), 1) + base
    query_at = lax.broadcasted_iota(jnp.int32, (rows, span), 0) + (base + DOC_MAX)
    allowed = (key_at >= low_bound) & (key_at <= query_at)
    scores = (dot_nt(q_nope, k_nope) + dot_nt(q_rope, k_rope)) * scale
    return jnp.where(allowed, scores, -1e30)


def attend_kernel(heads, scale, low_ref, qn_ref, qr_ref, ex_ref, kr_ref, out_ref, lse_ref):
    rows = qn_ref.shape[0]
    base = pl.multiple_of(pl.program_id(0) * rows, rows)
    window = pl.ds(base, rows + DOC_MAX)
    k_rope = kr_ref[window, :]
    low_bound = low_ref[...]
    for h in range(heads):
        at = h * (NOPE + VDIM)
        k_nope = ex_ref[window, at : at + NOPE]
        value = ex_ref[window, at + NOPE : at + NOPE + VDIM]
        scores = masked_scores(
            base,
            low_bound,
            qn_ref[:, h * NOPE : (h + 1) * NOPE],
            qr_ref[:, h * ROPE : (h + 1) * ROPE],
            k_nope,
            k_rope,
            scale,
        )
        top = jnp.max(scores, axis=-1, keepdims=True)
        exps = jnp.exp(scores - top)
        total = jnp.sum(exps, axis=-1, keepdims=True)
        probs = (exps / total).astype(BF)
        out_ref[:, h * VDIM : (h + 1) * VDIM] = jnp.dot(
            probs, value, preferred_element_type=F32
        ).astype(BF)
        lse_ref[:, h : h + 1] = top + jnp.log(total)


def attend(low_bound, q_nope, q_rope, expanded, key_rope, scale):
    queries = q_nope.shape[0]
    heads = q_nope.shape[1] // NOPE
    rows = QUERY_BLOCK

    def whole(array):
        return pl.BlockSpec(array.shape, lambda i: (0, 0))

    def blocked(width):
        return pl.BlockSpec((rows, width), lambda i: (i, 0))

    flops = 2 * heads * queries * (rows + DOC_MAX) * (NOPE + ROPE + VDIM)
    return pl.pallas_call(
        functools.partial(attend_kernel, heads, scale),
        grid=(queries // rows,),
        in_specs=[
            blocked(1),
            blocked(heads * NOPE),
            blocked(heads * ROPE),
            whole(expanded),
            whole(key_rope),
        ],
        out_specs=[blocked(heads * VDIM), blocked(heads)],
        out_shape=[
            jax.ShapeDtypeStruct((queries, heads * VDIM), BF),
            jax.ShapeDtypeStruct((queries, heads), F32),
        ],
        cost_estimate=pl.CostEstimate(
            flops=flops, bytes_accessed=4 * expanded.size, transcendentals=flops // 640
        ),
        compiler_params=pltpu.CompilerParams(vmem_limit_bytes=50 * 1024 * 1024),
        name="attend",
    )(low_bound, q_nope, q_rope, expanded, key_rope)


def attend_back_kernel(
    heads, scale, low_ref, qn_ref, qr_ref, ex_ref, kr_ref, lse_ref, gm_ref,
    dqn_ref, dqr_ref, dex_ref, dkr_ref,
):
    rows = qn_ref.shape[0]
    step = pl.program_id(0)
    base = pl.multiple_of(step * rows, rows)
    window = pl.ds(base, rows + DOC_MAX)

    @pl.when(step == 0)
    def _():
        dex_ref[...] = jnp.zeros_like(dex_ref)
        dkr_ref[...] = jnp.zeros_like(dkr_ref)

    k_rope = kr_ref[window, :]
    low_bound = low_ref[...]
    for h in range(heads):
        at = h * (NOPE + VDIM)
        k_nope = ex_ref[window, at : at + NOPE]
        value = ex_ref[window, at + NOPE : at + NOPE + VDIM]
        q_nope = qn_ref[:, h * NOPE : (h + 1) * NOPE]
        q_rope = qr_ref[:, h * ROPE : (h + 1) * ROPE]
        grad_out = gm_ref[:, h * VDIM : (h + 1) * VDIM]
        scores = masked_scores(base, low_bound, q_nope, q_rope, k_nope, k_rope, scale)
        probs = jnp.exp(scores - lse_ref[:, h : h + 1])
        grad_probs = dot_nt(grad_out, value)
        mean_grad = jnp.sum(probs * grad_probs, axis=-1, keepdims=True)
        grad_scores = (probs * (grad_probs - mean_grad) * scale).astype(BF)
        probs_low = probs.astype(BF)
        dqn_ref[:, h * NOPE : (h + 1) * NOPE] = jnp.dot(
            grad_scores, k_nope, preferred_element_type=F32
        )
        dqr_ref[:, h * ROPE : (h + 1) * ROPE] = jnp.dot(
            grad_scores, k_rope, preferred_element_type=F32
        )
        dex_ref[window, at : at + NOPE] += dot_tn(grad_scores, q_nope)
        dex_ref[window, at + NOPE : at + NOPE + VDIM] += dot_tn(probs_low, grad_out)
        dkr_ref[window, :] += dot_tn(grad_scores, q_rope)


def attend_back(low_bound, q_nope, q_rope, expanded, key_rope, lse, grad_mixed, scale):
    queries = q_nope.shape[0]
    heads = q_nope.shape[1] // NOPE
    rows = QUERY_BLOCK

    def whole(shape):
        return pl.BlockSpec(shape, lambda i: (0, 0))

    def blocked(width):
        return pl.BlockSpec((rows, width), lambda i: (i, 0))

    flops = 2 * heads * queries * (rows + DOC_MAX) * (3 * NOPE + 3 * ROPE + 2 * VDIM)
    return pl.pallas_call(
        functools.partial(attend_back_kernel, heads, scale),
        grid=(queries // rows,),
        in_specs=[
            blocked(1),
            blocked(heads * NOPE),
            blocked(heads * ROPE),
            whole(expanded.shape),
            whole(key_rope.shape),
            blocked(heads),
            blocked(heads * VDIM),
        ],
        out_specs=[
            blocked(heads * NOPE),
            blocked(heads * ROPE),
            whole(expanded.shape),
            whole(key_rope.shape),
        ],
        out_shape=[
            jax.ShapeDtypeStruct(q_nope.shape, F32),
            jax.ShapeDtypeStruct(q_rope.shape, F32),
            jax.ShapeDtypeStruct(expanded.shape, F32),
            jax.ShapeDtypeStruct(key_rope.shape, F32),
        ],
        cost_estimate=pl.CostEstimate(
            flops=flops, bytes_accessed=8 * expanded.size, transcendentals=flops // 1664
        ),
        compiler_params=pltpu.CompilerParams(vmem_limit_bytes=56 * 1024 * 1024),
        name="attend_back",
    )(low_bound, q_nope, q_rope, expanded, key_rope, lse, grad_mixed)


MESH = pl.DeviceIdType.MESH


def pause(rounds):
    for _ in range(rounds):
        yield


class Wires:
    def __init__(self, n_groups, n_plane, send, recv):
        self.n_groups, self.n_plane, self.send, self.recv = n_groups, n_plane, send, recv
        self.cores = 2
        self.g, self.p, self.c = lax.axis_index("g"), lax.axis_index("p"), lax.axis_index("c")
        self.j = self.p * self.cores + self.c
        self.used = 0

    def at_plane(self, j):
        return {"g": self.g, "p": j // self.cores, "c": j % self.cores}

    def at_chip(self, p):
        return {"g": self.g, "p": p, "c": self.c}

    def at_group(self, g):
        return {"g": g, "p": self.p, "c": self.c}

    def partner(self):
        return {"g": self.g, "p": self.p, "c": 1 - self.c}

    def beside(self):
        return self.p + 1 - 2 * lax.rem(self.p, 2)

    def above(self):
        return self.p + 2 - 4 * (self.p // 2)

    def core_of(self, p):
        return p * self.cores + self.c

    def plane_peer(self, d):
        return lax.rem(self.j + d, self.n_plane)

    def group_peer(self, d):
        return lax.rem(self.g + d, self.n_groups)

    def start(self, src, dst, device):
        copy = pltpu.make_async_remote_copy(
            src_ref=src,
            dst_ref=dst,
            send_sem=self.send.at[self.used],
            recv_sem=self.recv.at[self.used],
            device_id=device,
            device_id_type=MESH,
        )
        self.used += 1
        copy.start()
        return copy

    def at_device(self, index):
        return {"g": index // self.n_plane, **self.on_plane(lax.rem(index, self.n_plane))}

    def on_plane(self, j):
        return {"p": j // self.cores, "c": j % self.cores}

    def meet(self, heads=False, home=False):
        barrier = pltpu.get_barrier_semaphore()
        waits = self.n_plane - 1 + self.n_groups - 1
        if heads:
            mine = self.head_owner() == self.j
            part = lax.rem(self.g * self.n_plane + self.j, self.n_groups)
            for r in range(self.n_groups):

                @pl.when(jnp.logical_not(mine) | (part != r))
                def _():
                    source = self.at_device(self.n_groups * self.j + r)
                    pl.semaphore_signal(barrier, inc=1, device_id=source, device_id_type=MESH)

            waits = waits + jnp.where(mine, self.n_groups - 1, self.n_groups)
        if home:
            source = self.home_source()
            stays = source == self.g * self.n_plane + self.j

            @pl.when(jnp.logical_not(stays))
            def _():
                pl.semaphore_signal(
                    barrier, inc=1, device_id=self.at_device(source), device_id_type=MESH
                )

            waits = waits + jnp.where(stays, 0, 1)
        for d in range(1, self.n_plane):
            pl.semaphore_signal(
                barrier, inc=1, device_id=self.at_plane(self.plane_peer(d)), device_id_type=MESH
            )
        for d in range(1, self.n_groups):
            pl.semaphore_signal(
                barrier, inc=1, device_id=self.at_group(self.group_peer(d)), device_id_type=MESH
            )
        pl.semaphore_wait(barrier, waits)

    def home_source(self):
        index = self.g * self.n_plane + self.j
        return lax.rem(index, self.n_groups) * self.n_plane + index // self.n_groups

    def head_owner(self):
        return (self.g * self.n_plane + self.j) // self.n_groups


def sum_rows(dst, sources):
    rows = dst.shape[0]
    tile = 32 if rows % 32 == 0 else rows

    def step(i, carry):
        at = pl.ds(pl.multiple_of(i * tile, tile), tile)
        if len(sources) == 2 and all(r.dtype == BF for r in [dst] + sources):
            dst[at, :] = sources[0][at, :] + sources[1][at, :]
        else:
            total = sources[0][at, :].astype(F32)
            for source in sources[1:]:
                total = total + source[at, :].astype(F32)
            dst[at, :] = total.astype(dst.dtype)
        return carry

    lax.fori_loop(0, rows // tile, step, 0)


def wait_all(copies):
    for copy in copies:
        copy.wait()


def wait_received(copies):
    for copy in copies:
        copy.wait_recv()


def wait_sent(copies):
    for copy in copies:
        copy.wait_send()


def part_of(ref, upper):
    rows = ref.shape[0] // 2
    return ref.at[pl.ds(rows, rows)] if upper else ref.at[pl.ds(0, rows)]


def spread(w, own, at):
    beside, above = w.at_chip(w.beside()), w.at_chip(w.above())
    mine = at(w.j)
    halves = [(part_of(own, u), part_of(mine, u)) for u in (0, 1)]
    lower = w.start(*halves[0], beside)
    upper = w.start(*halves[1], above)
    rest = [w.start(*halves[1], beside), w.start(*halves[0], above)]
    on_chip = [w.start(own, mine, w.partner())]
    yield
    lower.wait_recv()
    block = part_of(at(w.core_of(w.beside())), 0)
    rest.append(w.start(block, block, above))
    upper.wait_recv()
    block = part_of(at(w.core_of(w.above())), 1)
    rest.append(w.start(block, block, beside))
    yield
    wait_received(rest)
    for p in (w.beside(), w.above(), 3 - w.p):
        block = at(w.core_of(p))
        on_chip.append(w.start(block, block, w.partner()))
    yield
    wait_sent([lower, upper] + rest)
    wait_all(on_chip)


def plane_gather(w, src, out):
    out[w.j] = src[...]
    yield from spread(w, src, lambda j: out.at[j])


def far_gather(w, src, out, sem):
    mine = out.at[w.g, w.j]
    away = [w.start(src, mine, w.at_group(w.group_peer(d))) for d in range(1, w.n_groups)]
    local = pltpu.make_async_copy(src, mine, sem)
    local.start()
    running = [spread(w, src, lambda j: out.at[w.g, j])]
    next(running[0])
    for d in range(1, w.n_groups):
        away[d - 1].wait_recv()
        g = w.group_peer(w.n_groups - d)
        running.append(spread(w, out.at[g, w.j], lambda j, g=g: out.at[g, j]))
        next(running[d])
    for _ in range(3):
        for routine in running:
            next(routine, None)
        yield
    local.wait()
    wait_sent(away)


def shift_gather(w, src, mid, out):
    copy = w.start(src, mid, w.at_group(lax.rem(w.g + 1, w.n_groups)))
    yield
    copy.wait()
    yield from plane_gather(w, mid, out)


def whole_gather(w, src, out):
    chips = w.n_plane // w.cores
    first = [
        w.start(src, out.at[w.g, w.j], w.at_group(w.group_peer(d))) for d in range(1, w.n_groups)
    ]
    out[w.g, w.j] = src[...]
    yield
    wait_received(first)
    mine = out.at[:, w.j]
    second = [w.start(mine, mine, w.at_chip(lax.rem(w.p + d, chips))) for d in range(1, chips)]
    third = [w.start(mine, mine, w.partner())]
    yield
    for d in range(1, chips):
        second[d - 1].wait_recv()
        block = out.at[:, w.core_of(lax.rem(w.p + chips - d, chips))]
        third.append(w.start(block, block, w.partner()))
    yield
    wait_sent(first)
    wait_sent(second)
    wait_all(third)


def plane_swap_gather(w, src, out):
    first = []
    for d in range(1, w.n_plane):
        to = w.plane_peer(d)
        first.append(w.start(src.at[to], out.at[w.g, w.j], w.at_plane(to)))
    out[w.g, w.j] = src[w.j]
    yield
    wait_received(first)
    second = [
        w.start(out.at[w.g], out.at[w.g], w.at_group(w.group_peer(d)))
        for d in range(1, w.n_groups)
    ]
    yield from pause(4)
    wait_sent(first)
    wait_all(second)


def head_rows(w, src, out):
    index = w.g * w.n_plane + w.j
    owner, part = w.head_owner(), lax.rem(index, w.n_groups)
    mine = owner == w.j

    def to(d):
        return pltpu.make_async_remote_copy(
            src_ref=src,
            dst_ref=out.at[part],
            send_sem=w.send.at[base + d],
            recv_sem=w.recv.at[base + part],
            device_id={"g": w.group_peer(d), **w.on_plane(owner)},
            device_id_type=MESH,
        )

    def arrival(r):
        return pltpu.make_async_remote_copy(
            src_ref=src,
            dst_ref=out.at[r],
            send_sem=w.send.at[base],
            recv_sem=w.recv.at[base + r],
            device_id=w.at_device(w.n_groups * w.j + r),
            device_id_type=MESH,
        )

    yield from pause(3)
    base = w.used
    w.used += w.n_groups
    for d in range(w.n_groups):

        @pl.when((d > 0) | jnp.logical_not(mine))
        def _():
            to(d).start()

    @pl.when(mine)
    def _():
        out[part] = src[...]

    yield from pause(2)
    for r in range(w.n_groups):

        @pl.when(jnp.logical_not(mine) | (part != r))
        def _():
            arrival(r).wait_recv()

    for d in range(w.n_groups):

        @pl.when((d > 0) | jnp.logical_not(mine))
        def _():
            to(d).wait_send()


def plane_swap(w, src, out):
    copies = []
    for d in range(1, w.n_plane):
        to = w.plane_peer(d)
        copies.append(w.start(src.at[to], out.at[w.j], w.at_plane(to)))
    out[w.j] = src[w.j]
    yield
    wait_all(copies)


def plane_sum(w, src, out, from_core, pairs, from_chips):
    to = (w.beside(), 3 - w.p, w.above(), w.p)
    beside, above = w.at_chip(w.beside()), w.at_chip(w.above())
    first = [
        w.start(src.at[p * w.cores + 1 - w.c], from_core.at[i], w.partner())
        for i, p in enumerate(to)
    ]
    yield
    sent = []

    def send(i, upper, slot, device):
        sent.append(w.start(part_of(pairs.at[i], upper), from_chips.at[slot], device))

    for i, p in enumerate(to):
        first[i].wait_recv()
        sum_rows(pairs.at[i], [src.at[w.core_of(p)], from_core.at[i]])
        if i < 2:
            send(i, 0, i, beside)
        if i == 1:
            send(1, 1, 2, above)
        if i == 2:
            send(2, 1, 3, above)
    yield
    for wire, i, upper, slot, device in ((1, 2, 0, 4, above), (2, 0, 1, 5, beside)):
        sent[wire].wait_recv()
        target = part_of(pairs.at[i], upper)
        sum_rows(target, [target, from_chips.at[wire]])
        send(i, upper, slot, device)
    yield
    for wire in (0, 3, 4, 5):
        sent[wire].wait_recv()
    for upper, arrived in ((0, (0, 4)), (1, (3, 5))):
        sum_rows(
            part_of(out, upper),
            [part_of(pairs.at[3], upper)] + [from_chips.at[slot] for slot in arrived],
        )
    wait_sent(first)
    wait_sent(sent)


def whole_sum(w, src, out, from_core, pairs, from_chips, total, parts):
    chips = w.n_plane // w.cores
    to = [lax.rem(w.p + d, chips) for d in range(chips)]
    first = [
        w.start(src.at[:, p * w.cores + 1 - w.c], from_core.at[d], w.partner())
        for d, p in enumerate(to)
    ]
    yield
    second = []
    for d in list(range(1, chips)) + [0]:
        first[d].wait_recv()

        def step(i, carry):
            sum_rows(pairs.at[d, i], [src.at[i, w.core_of(to[d])], from_core.at[d, i]])
            return carry

        lax.fori_loop(0, w.n_groups, step, 0)
        if d:
            second.append(w.start(pairs.at[d], from_chips.at[d - 1], w.at_chip(to[d])))
    yield
    wait_received(second)

    def step(i, carry):
        sum_rows(total.at[i], [pairs.at[0, i]] + [from_chips.at[d, i] for d in range(chips - 1)])
        return carry

    lax.fori_loop(0, w.n_groups, step, 0)
    wait_sent(first)
    wait_sent(second)
    yield from group_sum(w, total, out, parts)


def whole_swap(w, src, out, mid):
    first = []
    for d in range(1, w.n_groups):
        to = w.group_peer(d)
        first.append(w.start(src.at[to], mid.at[w.g], w.at_group(to)))
    mid[w.g] = src[w.g]
    yield from pause(3)
    wait_received(first)
    second = []
    for d in range(1, w.n_plane):
        to = w.plane_peer(d)
        second.append(w.start(mid.at[:, to], out.at[:, w.j], w.at_plane(to)))
    out[:, w.j] = mid[:, w.j]
    yield
    wait_sent(first)
    wait_all(second)


def group_sum_home(w, src, out, parts, low, home):
    copies = []
    for d in range(1, w.n_groups):
        to = w.group_peer(d)
        copies.append(w.start(src.at[to], parts.at[d - 1], w.at_group(to)))
    yield from pause(3)
    wait_received(copies)
    sum_rows(low, [src.at[w.g]] + [parts.at[d] for d in range(w.n_groups - 1)])
    stays = w.home_source() == w.g * w.n_plane + w.j
    copy = pltpu.make_async_remote_copy(
        src_ref=low,
        dst_ref=home,
        send_sem=w.send.at[w.used],
        recv_sem=w.recv.at[w.used],
        device_id=w.at_device(w.n_groups * w.j + w.g),
        device_id_type=MESH,
    )
    w.used += 1

    @pl.when(jnp.logical_not(stays))
    def _():
        copy.start()

    @pl.when(stays)
    def _():
        home[...] = low[...]

    yield

    @pl.when(jnp.logical_not(stays))
    def _():
        copy.wait()

    out[...] = home[...].astype(F32)
    wait_sent(copies)


def plane_sum_shift(w, src, out, from_core, pairs, from_chips, low, later):
    rows = out.shape[0]
    yield from plane_sum(w, src, low, from_core, pairs, from_chips)
    copy = w.start(
        low.at[pl.ds(0, rows)], later, w.at_group(lax.rem(w.g + w.n_groups - 1, w.n_groups))
    )
    yield
    copy.wait()
    keep = jnp.where(w.g == w.n_groups - 1, 0.0, 1.0)
    out[...] = low[rows:, :].astype(F32) + later[...].astype(F32) * keep


def group_sum(w, src, out, parts):
    copies = []
    for d in range(1, w.n_groups):
        to = w.group_peer(d)
        copies.append(w.start(src.at[to], parts.at[d - 1], w.at_group(to)))
    yield
    wait_received(copies)
    sum_rows(out, [src.at[w.g]] + [parts.at[d] for d in range(w.n_groups - 1)])
    wait_sent(copies)


def group_sum_swap(w, src, out, total, parts):
    copies = []
    for d in range(1, w.n_groups):
        to = w.group_peer(d)
        copies.append(w.start(src.at[to], parts.at[d - 1], w.at_group(to)))
    yield from pause(4)
    wait_received(copies)

    def step(i, carry):
        sum_rows(total.at[i], [src.at[w.g, i]] + [parts.at[d, i] for d in range(w.n_groups - 1)])
        return carry

    lax.fori_loop(0, w.n_plane, step, 0)
    second = []
    for d in range(1, w.n_plane):
        to = w.plane_peer(d)
        second.append(w.start(total.at[to], out.at[w.j], w.at_plane(to)))
    out[w.j] = total[w.j]
    yield
    wait_sent(copies)
    wait_all(second)


ROUTINES = {
    "plane_gather": plane_gather,
    "shift_gather": shift_gather,
    "whole_gather": whole_gather,
    "far_gather": far_gather,
    "plane_swap_gather": plane_swap_gather,
    "plane_swap": plane_swap,
    "plane_sum": plane_sum,
    "plane_sum_shift": plane_sum_shift,
    "head_rows": head_rows,
    "group_sum": group_sum,
    "whole_sum": whole_sum,
    "whole_swap": whole_swap,
    "group_sum_home": group_sum_home,
    "group_sum_swap": group_sum_swap,
}


def exchange_kernel(n_groups, n_plane, kinds, extra, *refs):
    count = len(kinds)
    sources, outs = refs[:count], refs[count : 2 * count]
    scratch = list(refs[2 * count : -2])
    w = Wires(n_groups, n_plane, refs[-2], refs[-1])
    w.meet("head_rows" in kinds, "group_sum_home" in kinds)
    running = []
    for kind, source, out, number in zip(kinds, sources, outs, extra):
        mine, scratch = scratch[:number], scratch[number:]
        if kind == "shift_gather":
            running.append(shift_gather(w, source, mine[0], out))
        else:
            running.append(ROUTINES[kind](w, source, out, *mine))
    while running:
        still = []
        for routine in running:
            try:
                next(routine)
                still.append(routine)
            except StopIteration:
                pass
        running = still


def exchange(n_groups, n_plane, number, *items):
    kinds = [kind for kind, _ in items]
    arrays = [array for _, array in items]
    shapes, scratch, extra = [], [], []
    chips = n_plane // 2
    for kind, array in items:
        shape, dtype = array.shape, array.dtype
        own = []
        if kind in ("plane_gather", "shift_gather"):
            out = (n_plane,) + shape
            if kind == "shift_gather":
                own = [shape]
        elif kind in ("whole_gather", "far_gather"):
            out = (n_groups, n_plane) + shape
        elif kind == "plane_swap_gather":
            out = (n_groups,) + shape
        elif kind == "plane_swap":
            out = shape
        elif kind == "head_rows":
            out = (n_groups,) + shape
        elif kind == "plane_sum_shift":
            pair = shape[1:]
            out = (shape[1] // 2, shape[2])
            half = (pair[0] // 2, pair[1])
            own = [(chips,) + pair, (chips,) + pair, (6,) + half, pair, out]
        elif kind == "plane_sum":
            out = shape[1:]
            own = [(chips,) + out, (chips,) + out, (6, out[0] // 2, out[1])]
        elif kind == "group_sum_home":
            out = shape[1:]
            own = [(n_groups - 1,) + out, out, out]
        elif kind == "group_sum":
            out = shape[1:]
            own = [(n_groups - 1,) + out]
        elif kind == "whole_swap":
            out = shape
            own = [shape]
        elif kind == "whole_sum":
            out = shape[2:]
            full = (n_groups,) + out
            own = [(chips,) + full, (chips,) + full, (chips - 1,) + full, full]
            own = own + [(n_groups - 1,) + out]
        elif kind == "group_sum_swap":
            out = shape[1:]
            own = [out, (n_groups - 1,) + out]
        if kind in ("plane_sum", "plane_sum_shift", "group_sum", "group_sum_home", "whole_sum"):
            shapes.append(jax.ShapeDtypeStruct(out, F32))
        else:
            shapes.append(jax.ShapeDtypeStruct(out, dtype))
        scratch += [pltpu.VMEM(s, dtype) for s in own]
        if kind == "far_gather":
            own = [None]
            scratch.append(pltpu.SemaphoreType.DMA)
        extra.append(len(own))
    copies = 64 + 32 * len(items)
    vmem = pl.BlockSpec(memory_space=pltpu.VMEM)
    return pl.pallas_call(
        functools.partial(exchange_kernel, n_groups, n_plane, kinds, extra),
        out_shape=shapes,
        in_specs=[vmem] * len(items),
        out_specs=[
            pl.BlockSpec(memory_space=pl.ANY) if kind == "far_gather" else vmem for kind in kinds
        ],
        scratch_shapes=scratch
        + [pltpu.SemaphoreType.DMA((copies,)), pltpu.SemaphoreType.DMA((copies,))],
        compiler_params=pltpu.CompilerParams(
            collective_id=number,
            has_side_effects=True,
            vmem_limit_bytes=60 * 1024 * 1024,
        ),
        name="exchange_%d" % number,
    )(*arrays)


def gather_all(x):
    return lax.all_gather(x, ALL, axis=0, tiled=True)


class StreamSum:
    def __init__(self, w, steps, stage, from_core, pairs, from_chips, totals, parts, sems, credit):
        self.w, self.steps = w, steps
        self.stage, self.from_core, self.pairs = stage, from_core, pairs
        self.from_chips, self.totals, self.parts = from_chips, totals, parts
        self.core_sems, self.chip_sems, self.chip_recv, self.group_sems = sems
        self.credit = credit

    @staticmethod
    def chips(w, step):
        half = lax.rem(step, 2)
        beside = w.p + 1 - 2 * lax.rem(w.p, 2)
        above = w.p + 2 - 4 * (w.p // 2)
        return beside + half * (above - beside), 3 - w.p + half * (2 * w.p - 3)

    def core_copy(self, step, i):
        slot = lax.rem(step, 2)
        return pltpu.make_async_remote_copy(
            src_ref=self.stage.at[slot, 2 * i + 1 - self.w.c],
            dst_ref=self.from_core.at[slot, i],
            send_sem=self.core_sems.at[0, slot, i],
            recv_sem=self.core_sems.at[1, slot, i],
            device_id=self.w.partner(),
            device_id_type=MESH,
        )

    def part(self, ref, upper):
        rows = ref.shape[0] // 2
        return ref.at[pl.ds(rows, rows)] if upper else ref.at[pl.ds(0, rows)]

    def chip_copy(self, group_at, which):
        slot, i, upper, up = (
            (0, 0, False, False),
            (0, 1, False, False),
            (0, 1, True, True),
            (1, 0, True, True),
            (1, 0, False, True),
            (0, 0, True, False),
        )[which]
        p = self.w.p
        to = p + 2 - 4 * (p // 2) if up else p + 1 - 2 * lax.rem(p, 2)
        return pltpu.make_async_remote_copy(
            src_ref=self.part(self.pairs.at[slot, i], upper),
            dst_ref=self.from_chips.at[group_at, which],
            send_sem=self.chip_sems.at[which],
            recv_sem=self.chip_recv.at[group_at, which],
            device_id=self.w.at_chip(to),
            device_id_type=MESH,
        )

    def group_copy(self, group_at):
        return pltpu.make_async_remote_copy(
            src_ref=self.totals.at[group_at],
            dst_ref=self.parts.at[group_at],
            send_sem=self.group_sems.at[0, group_at],
            recv_sem=self.group_sems.at[1, group_at],
            device_id=self.w.at_group(self.w.group_peer(group_at + 1)),
            device_id_type=MESH,
        )

    def open_stage(self, step):
        @pl.when(step >= 2)
        def _():
            for i in range(2):
                self.core_copy(step, i).wait_send()

    def push(self, step):
        @pl.when(step >= 2)
        def _():
            pl.semaphore_wait(self.credit, 1)

        for i in range(2):
            self.core_copy(step, i).start()

    def merge(self, step):
        slot, group_at = lax.rem(step, 2), step // 2
        for half, sends in ((0, (0, 1, 2, 5)), (1, (3, 4))):

            @pl.when((slot == half) & (step >= 2))
            def _():
                for which in sends:
                    self.chip_copy(group_at, which).wait_send()

        for i in range(2):
            self.core_copy(step, i).wait_recv()
            sum_rows(
                self.pairs.at[slot, i],
                [self.stage.at[slot, 2 * i + self.w.c], self.from_core.at[slot, i]],
            )

        @pl.when(step + 2 < self.steps)
        def _():
            pl.semaphore_signal(
                self.credit, inc=1, device_id=self.w.partner(), device_id_type=MESH
            )

        @pl.when(slot == 0)
        def _():
            for which in (0, 1, 2):
                self.chip_copy(group_at, which).start()

        @pl.when(slot == 1)
        def _():
            self.chip_copy(group_at, 3).start()
            for source, i, upper, which in ((1, (1, 0), False, 4), (2, (0, 0), True, 5)):
                self.chip_copy(group_at, source).wait_recv()
                target = self.part(self.pairs.at[i], upper)
                sum_rows(target, [target, self.from_chips.at[group_at, source]])
                self.chip_copy(group_at, which).start()

    def plane_total(self, group_at):
        for which in (0, 3, 4, 5):
            self.chip_copy(group_at, which).wait_recv()
        return [
            [self.part(self.pairs.at[1, 1], upper)]
            + [self.from_chips.at[group_at, which] for which in arrived]
            for upper, arrived in ((False, (0, 4)), (True, (3, 5)))
        ]

    def advance(self, step):
        @pl.when(step >= 1)
        def _():
            last = step - 1

            @pl.when((lax.rem(last, 2) == 0) & (last >= 2))
            def _():
                group_at = last // 2 - 1
                for upper, sources in enumerate(self.plane_total(group_at)):
                    sum_rows(self.part(self.totals.at[group_at], upper), sources)
                self.group_copy(group_at).start()

            self.merge(last)

    def finish(self, out):
        steps = self.steps
        self.merge(steps - 1)
        groups = steps // 2 - 1
        halves = self.plane_total(groups)
        for d in range(groups):
            self.group_copy(d).wait_recv()
        for upper, sources in enumerate(halves):
            parts = [self.part(self.parts.at[d], upper) for d in range(groups)]
            sum_rows(self.part(out, upper), sources + parts)
        for d in range(groups):
            self.group_copy(d).wait_send()
        for i in range(2):
            self.core_copy(steps - 2, i).wait_send()
            self.core_copy(steps - 1, i).wait_send()
        for which in range(6):
            self.chip_copy(groups, which).wait_send()

    @staticmethod
    def scratch(n_groups, rows, width):
        dma = pltpu.SemaphoreType.DMA
        return [
            pltpu.VMEM((2, 4, rows, width), BF),
            pltpu.VMEM((2, 2, rows, width), BF),
            pltpu.VMEM((2, 2, rows, width), BF),
            pltpu.VMEM((n_groups, 6, rows // 2, width), BF),
            pltpu.VMEM((n_groups - 1, rows, width), BF),
            pltpu.VMEM((n_groups - 1, rows, width), BF),
            dma((2, 2, 2)),
            dma((6,)),
            dma((n_groups, 6)),
            dma((2, n_groups - 1)),
            pltpu.SemaphoreType.REGULAR,
        ]


def swiglu_both(gate, up, grad):
    sigmoid = 1.0 / (1.0 + jnp.exp(-gate))
    silu = gate * sigmoid
    return silu * up, grad * up * (sigmoid * (1.0 + gate * (1.0 - sigmoid))), grad * silu


def step_chips(w, step):
    group = lax.rem(w.g + 1 + step // 2, w.n_groups)
    return [group * 4 + chip for chip in StreamSum.chips(w, step)]


def hot_rows(place, rows, core, slot_count):
    mine = place[:, core * rows : (core + 1) * rows]
    return lax.broadcasted_iota(jnp.int32, (slot_count, rows), 0) == mine


def moe_kernel(
    n_groups, experts, first_logit, slot_count,
    h2_hbm, cot_hbm, place_ref, wg_ref, wu_ref, wd_ref, sc_ref, sd_ref,
    sum_ref, rows_ref, gin_ref, act_ref, gg_ref, gu_ref, rw_ref, sact_ref, dboth_ref, dsd_ref,
    tok_ref,
    h2_buf, cot_buf, load_sems, *comm,
):
    rows = sum_ref.shape[0]
    step, steps = pl.program_id(0), 2 * n_groups
    w = Wires(n_groups, 8, None, None)
    stream = StreamSum(w, steps, *comm[:6], comm[6:10], comm[10])
    expert_id = w.g * 4 + w.p
    half = sc_ref.shape[1] // 2

    def loads(at):
        slot = lax.rem(at, 2)
        for i, chip in enumerate(step_chips(w, at)):
            source = pl.ds(pl.multiple_of(chip * 2 * rows, 2 * rows), 2 * rows)
            target = pl.ds(i * 2 * rows, 2 * rows)
            for k, (hbm, buf) in enumerate(((h2_hbm, h2_buf), (cot_hbm, cot_buf))):
                yield pltpu.make_async_copy(
                    hbm.at[source], buf.at[slot, target], load_sems.at[slot, i, k]
                )

    @pl.when(step == 0)
    def _():
        for copy in loads(step):
            copy.start()
        w.meet()
        for ref in (dboth_ref, dsd_ref):
            ref[...] = jnp.zeros_like(ref)

    @pl.when(step + 1 < steps)
    def _():
        for copy in loads(step + 1):
            copy.start()

    for copy in loads(step):
        copy.wait()
    slot = lax.rem(step, 2)
    h2, cot = h2_buf[slot], cot_buf[slot]
    chips = step_chips(w, step)

    pre = jnp.dot(h2, sc_ref[...], preferred_element_type=F32)
    back = dot_nt(cot, sd_ref[...])
    gate, up = pre[:, :half], pre[:, half:]
    lane = lax.broadcasted_iota(jnp.int32, gate.shape, 1)
    logits = jnp.where((lane >= first_logit) & (lane < first_logit + experts), gate, -1e30)
    exps = jnp.exp(logits - jnp.max(logits, axis=1, keepdims=True))
    chosen = jnp.where(lane == first_logit + expert_id, exps, 0.0)
    weight = jnp.sum(chosen, axis=1, keepdims=True) / jnp.sum(exps, axis=1, keepdims=True)
    act, grad_gate, grad_up = swiglu_both(gate, up, back)
    shared_act = act.astype(BF)
    shared_grad = jnp.concatenate([grad_gate.astype(BF), grad_up.astype(BF)], axis=1)
    for i, chip in enumerate(chips):
        at = pl.ds(pl.multiple_of(chip * 2 * rows, 2 * rows), 2 * rows)
        sact_ref[at, :] = shared_act[i * 2 * rows : (i + 1) * 2 * rows]

    hots, weights = [], []
    for q in range(4):
        place = place_ref[pl.ds(chips[q // 2], 1), :]
        hot = hot_rows(place, rows, q % 2, slot_count).astype(F32)
        hots.append(hot)
        tokens = slice(q * rows, (q + 1) * rows)
        slots = slice(q * slot_count, (q + 1) * slot_count)
        low = hot.astype(BF)
        rows_ref[slots, :] = jnp.dot(low, h2[tokens], preferred_element_type=F32).astype(BF)
        gin_ref[slots, :] = jnp.dot(low, cot[tokens], preferred_element_type=F32).astype(BF)
        spread = jnp.broadcast_to(weight[tokens], (rows, 128))
        weights.append(
            jnp.dot(hot, spread, preferred_element_type=F32, precision=lax.Precision.HIGHEST)[:, :1]
        )
    row_weight = jnp.concatenate(weights, axis=0)
    rw_ref[...] = row_weight
    expert_rows = rows_ref[...]
    picked_cot = gin_ref[...]
    back = dot_nt(picked_cot, wd_ref[...])
    gin_ref[...] = (picked_cot.astype(F32) * row_weight).astype(BF)
    gate = dot_nt(expert_rows, wg_ref[...])
    up = dot_nt(expert_rows, wu_ref[...])
    act, grad_gate, grad_up = swiglu_both(gate, up, back * row_weight)
    act_low, grad_gate, grad_up = act.astype(BF), grad_gate.astype(BF), grad_up.astype(BF)
    act_ref[...] = act_low
    gg_ref[...] = grad_gate
    gu_ref[...] = grad_up
    picked = jnp.sum(act_low.astype(F32) * back, axis=1, keepdims=True)
    grad_rows = jnp.dot(grad_gate, wg_ref[...], preferred_element_type=F32)
    grad_rows = grad_rows + jnp.dot(grad_up, wu_ref[...], preferred_element_type=F32)
    grad_rows = grad_rows.astype(BF)
    stream.open_stage(step)
    for q in range(4):
        tokens = slice(q * rows, (q + 1) * rows)
        slots = slice(q * slot_count, (q + 1) * slot_count)
        tok_ref[pl.ds(chips[q // 2] * 2 + q % 2, 1), :] = jnp.sum(
            hots[q] * picked[slots], axis=0, keepdims=True
        )
        total = dot_tn(hots[q].astype(BF), grad_rows[slots]) + dot_nt(
            shared_grad[tokens], sc_ref[...]
        )
        stream.stage[slot, q] = total.astype(BF)
    stream.push(step)

    piece = h2.shape[1] // 4
    turned, turned_act = shared_grad.T, shared_act.T
    for k in range(4):
        cols = slice(k * piece, (k + 1) * piece)
        dboth_ref[:, cols] += jnp.dot(turned, h2[:, cols], preferred_element_type=F32)
        dsd_ref[:, cols] += jnp.dot(turned_act, cot[:, cols], preferred_element_type=F32)
    stream.advance(step)

    @pl.when(step == steps - 1)
    def _():
        stream.finish(sum_ref)


def out_kernel(
    n_groups, slot_count,
    act_ref, rw_ref, rows_ref, gin_ref, gg_ref, gu_ref, place_ref, sact_ref, wd_ref, sd_ref,
    sum_ref, dg_ref, du_ref, dd_ref, *comm,
):
    rows = sum_ref.shape[0]
    step, steps = pl.program_id(0), 2 * n_groups
    w = Wires(n_groups, 8, None, None)
    stream = StreamSum(w, steps, *comm[:6], comm[6:10], comm[10])

    @pl.when(step == 0)
    def _():
        w.meet()
        for ref in (dg_ref, du_ref, dd_ref):
            ref[...] = jnp.zeros_like(ref)

    slot = lax.rem(step, 2)
    chips = step_chips(w, step)
    out_rows = jnp.dot(act_ref[...], wd_ref[...], preferred_element_type=F32) * rw_ref[...]
    out_rows = out_rows.astype(BF)
    stream.open_stage(step)
    for q in range(4):
        chip = chips[q // 2]
        place = place_ref[pl.ds(chip, 1), :]
        low = hot_rows(place, rows, q % 2, slot_count).astype(F32).astype(BF)
        slots = slice(q * slot_count, (q + 1) * slot_count)
        shared = sact_ref[pl.ds(pl.multiple_of((chip * 2 + q % 2) * rows, rows), rows), :]
        total = dot_tn(low, out_rows[slots]) + jnp.dot(
            shared, sd_ref[...], preferred_element_type=F32
        )
        stream.stage[slot, q] = total.astype(BF)
    stream.push(step)
    stream.advance(step)

    width = rows_ref.shape[1]
    piece = width // 4
    for left_ref, right_ref, total_ref in (
        (gg_ref, rows_ref, dg_ref),
        (gu_ref, rows_ref, du_ref),
        (act_ref, gin_ref, dd_ref),
    ):
        turned = left_ref[...].T
        for k in range(4):
            cols = slice(k * piece, (k + 1) * piece)
            total_ref[:, cols] += jnp.dot(
                turned, right_ref[:, cols], preferred_element_type=F32
            )

    @pl.when(step == steps - 1)
    def _():
        stream.finish(sum_ref)


def experts_sums(
    n_groups, rows, h2, cot, place, slot_count, expert_w, shared_w, router_weight, first_id
):
    w_gate, w_up, w_down = expert_w
    s_both, s_down = shared_w
    tokens, width = h2.shape
    hidden, hidden_s = w_down.shape[0], s_down.shape[0]
    experts = router_weight.shape[1]
    steps = 2 * n_groups
    devices = tokens // rows
    step_slots = slot_count * 4
    all_slots = step_slots * steps
    half = 128
    s_cat = jnp.concatenate(
        [
            s_both[:, :hidden_s],
            router_weight,
            jnp.zeros((width, half - hidden_s - experts), BF),
            s_both[:, hidden_s:],
            jnp.zeros((width, half - hidden_s), BF),
        ],
        axis=1,
    )
    s_tall = jnp.pad(s_down, ((0, half - hidden_s), (0, 0)))

    def whole(array):
        return pl.BlockSpec(array.shape, lambda i: (0, 0), pipeline_mode=pl.Buffered(1))

    def blocked(rows, cols):
        return pl.BlockSpec((rows, cols), lambda i: (i, 0))

    shape = jax.ShapeDtypeStruct
    flops = 2 * all_slots * width * hidden * 5 + 2 * tokens * width * (4 * half + 3 * slot_count)
    shapes = [
        shape((rows, width), F32),
        shape((all_slots, width), BF),
        shape((all_slots, width), BF),
        shape((all_slots, hidden), BF),
        shape((all_slots, hidden), BF),
        shape((all_slots, hidden), BF),
        shape((all_slots, 1), F32),
        shape((tokens, half), BF),
        shape((2 * half, width), F32),
        shape((half, width), F32),
        shape((devices, rows), F32),
    ]
    specs = [
        blocked(step_slots, s.shape[1]) if s.shape[0] == all_slots else whole(s) for s in shapes
    ]
    hbm = pl.BlockSpec(memory_space=pl.ANY)
    grad_h2, rows_in, grad_in, act, grad_gate, grad_up, row_weight, s_act, *d_shared, token_grad = (
        pl.pallas_call(
            functools.partial(moe_kernel, n_groups, experts, hidden_s, slot_count),
            grid=(steps,),
            in_specs=[
                hbm,
                hbm,
                whole(place),
                whole(w_gate),
                whole(w_up),
                whole(w_down),
                whole(s_cat),
                whole(s_tall),
            ],
            out_specs=specs,
            out_shape=shapes,
            scratch_shapes=[
                pltpu.VMEM((2, 4 * rows, width), BF),
                pltpu.VMEM((2, 4 * rows, width), BF),
                pltpu.SemaphoreType.DMA((2, 2, 2)),
            ]
            + StreamSum.scratch(n_groups, rows, width),
            cost_estimate=pl.CostEstimate(
                flops=flops, bytes_accessed=12 * tokens * width, transcendentals=tokens * 1024
            ),
            compiler_params=pltpu.CompilerParams(
                collective_id=first_id,
                has_side_effects=True,
                vmem_limit_bytes=67043328,
            ),
            name="experts",
        )(h2, cot, place, w_gate, w_up, w_down, s_cat, s_tall)
    )
    shapes = [grad_h2] + [shape(x.shape, F32) for x in expert_w]
    out, d_gate, d_up, d_down = pl.pallas_call(
        functools.partial(out_kernel, n_groups, slot_count),
        grid=(steps,),
        in_specs=[
            blocked(step_slots, hidden),
            blocked(step_slots, 1),
            blocked(step_slots, width),
            blocked(step_slots, width),
            blocked(step_slots, hidden),
            blocked(step_slots, hidden),
            whole(place),
            whole(s_act),
            whole(w_down),
            whole(s_tall),
        ],
        out_specs=[whole(x) for x in shapes],
        out_shape=[shape(x.shape, F32) for x in shapes],
        scratch_shapes=StreamSum.scratch(n_groups, rows, width),
        cost_estimate=pl.CostEstimate(
            flops=2 * width * (4 * all_slots * hidden + tokens * (half + slot_count)),
            bytes_accessed=4 * tokens * width,
            transcendentals=0,
        ),
        compiler_params=pltpu.CompilerParams(
            collective_id=first_id + 1,
            has_side_effects=True,
            vmem_limit_bytes=67043328,
        ),
        name="expert_out",
    )(act, row_weight, rows_in, grad_in, grad_gate, grad_up, place, s_act, w_down, s_tall)
    d_both, d_tall = d_shared
    d_both = jnp.concatenate([d_both[:hidden_s], d_both[half : half + hidden_s]], axis=0)
    grads = (d_gate, d_up, d_down, d_both.T, d_tall[:hidden_s])
    return out, grad_h2, token_grad, grads


def body(
    n_groups, n_plane, layer_input, attn_gain, w_query, w_latent, kv_gain, w_expand, w_output,
    ffn_gain, w_router, shared_gate, shared_up, shared_down, expert_gate, expert_up,
    expert_down, routes, segments, cotangent,
):
    tok, width = layer_input.shape
    devices = n_groups * n_plane
    experts = w_router.shape[1]
    local_heads = HEADS // n_plane
    scale = (NOPE + ROPE) ** (-0.5)
    group = lax.axis_index("g")
    place_in = lax.axis_index(PLANE)
    me = lax.axis_index(ALL)
    expert_id = lax.axis_index(("g", "p"))
    plane_tok = n_plane * tok
    plane_start = group * plane_tok

    rows_w = w_router.shape[0]
    kv_n = kv_gain.shape[0]
    small = jnp.concatenate(
        [
            attn_gain,
            ffn_gain,
            kv_gain,
            w_router.reshape(-1),
            routes.reshape(-1).astype(BF),
            segments.astype(BF),
        ]
    )
    small = jnp.pad(small, (0, -small.shape[0] % 4096)).reshape(-1, 128)
    kv_cols = local_heads * (NOPE + VDIM)
    fold = kv_n * kv_cols // rows_w
    by_head = w_query.reshape(rows_w, n_plane, local_heads, NOPE + ROPE).transpose(1, 0, 2, 3)
    folded = (
        w_expand.reshape(kv_n, n_plane, kv_cols // fold, fold)
        .transpose(1, 0, 2, 3)
        .reshape(n_plane, rows_w, fold)
    )
    swap = functools.partial(exchange, n_groups, n_plane)
    wq_nope, wq_rope, expand_weight, latent_weight, small, x_plane = swap(
        0,
        ("plane_swap_gather", by_head[..., :NOPE].reshape(n_plane, rows_w, local_heads * NOPE)),
        ("plane_swap_gather", by_head[..., NOPE:].reshape(n_plane, rows_w, local_heads * ROPE)),
        ("plane_swap_gather", folded),
        ("whole_gather", w_latent),
        ("whole_gather", small),
        ("plane_gather", layer_input),
    )
    x_plane = x_plane.reshape(plane_tok, width).astype(F32)
    latent_weight = latent_weight.reshape(width, RANK + ROPE)
    wq_nope = wq_nope.reshape(width, local_heads * NOPE)
    wq_rope = wq_rope.reshape(width, local_heads * ROPE)
    expand_weight = expand_weight.reshape(RANK, kv_cols)
    small = small.reshape(devices, -1)
    cuts = [rows_w, 2 * rows_w, 2 * rows_w + kv_n, 2 * rows_w + kv_n + rows_w * experts]
    cuts = cuts + [cuts[-1] + tok * TOP, cuts[-1] + tok * TOP + tok]
    gain_one = small[:, : cuts[0]].reshape(-1).astype(F32)
    gain_two = small[:, cuts[0] : cuts[1]].reshape(-1).astype(F32)
    gain_kv = small[:, cuts[1] : cuts[2]].reshape(-1).astype(F32)
    router_weight = small[:, cuts[2] : cuts[3]].reshape(width, experts)
    routes_all = small[:, cuts[3] : cuts[4]].astype(jnp.int32).reshape(devices, tok, TOP)
    segments_all = small[:, cuts[4] : cuts[5]].astype(jnp.int32).reshape(-1)

    cotangent_later = jnp.where(x_plane[0, 0] < 1e6, cotangent, jnp.zeros_like(cotangent))

    shared_n = shared_down.shape[0]
    s_both = jnp.concatenate(
        [
            shared_gate.reshape(rows_w, devices, shared_n),
            shared_up.reshape(rows_w, devices, shared_n),
        ],
        axis=2,
    )
    s_both = s_both.transpose(1, 0, 2).reshape(n_groups, n_plane, rows_w, 2 * shared_n)

    hidden = rms_norm(x_plane, gain_one).astype(BF)
    rope_half = ROPE // 2
    positions = plane_start + jnp.arange(plane_tok, dtype=jnp.int32)
    frequency = 10000.0 ** (-jnp.arange(rope_half, dtype=F32) / rope_half)
    angles = positions.astype(F32)[:, None] * frequency[None, :]
    cosine = jnp.cos(angles)
    sine_part = jnp.sin(angles)
    cos_h = jnp.tile(cosine, (1, 2 * local_heads))
    sin_h = jnp.tile(jnp.concatenate([-sine_part, sine_part], axis=1), (1, local_heads))

    def turn(rows, direction):
        pieces = []
        for h in range(local_heads):
            at = h * ROPE
            pieces += [rows[:, at + rope_half : at + ROPE], rows[:, at : at + rope_half]]
        return rows * cos_h + jnp.concatenate(pieces, axis=1) * (direction * sin_h)

    latent = matmul(hidden, latent_weight)
    compressed_own = rms_norm(latent[:, :RANK], gain_kv).astype(BF)
    key_rope_own = rotate(latent[:, RANK:], cosine, sine_part).astype(BF)

    def own_rows(table):
        return lax.dynamic_slice_in_dim(table, place_in * tok, tok, 0)

    piece = own_rows(jnp.concatenate([compressed_own, key_rope_own], axis=1))
    before, own_output = swap(1, ("shift_gather", piece), ("head_rows", w_output))
    before = before.reshape(plane_tok, RANK + ROPE)
    own_output = own_output.reshape(local_heads * VDIM, width)
    compressed = jnp.concatenate([before[:, :RANK], compressed_own], axis=0)
    key_rope = jnp.concatenate([before[:, RANK:], key_rope_own], axis=0)
    q_nope = matmul(hidden, wq_nope).astype(BF)
    q_rope = turn(matmul(hidden, wq_rope), 1.0).astype(BF)
    expanded = matmul(compressed, expand_weight).astype(BF)
    plane_segments = lax.dynamic_slice_in_dim(segments_all, plane_start, plane_tok, 0)
    doc_start = jnp.sum(
        (segments_all[None, :] < plane_segments[:, None]).astype(jnp.int32), axis=1, keepdims=True
    )
    low_bound = doc_start - plane_start + DOC_MAX
    mixed_heads, lse = attend(low_bound, q_nope, q_rope, expanded, key_rope, scale)
    attn_out = matmul(mixed_heads, own_output).astype(BF)
    attn_out = swap(2, ("plane_sum", attn_out.reshape(n_plane, tok, width)))[0]
    input_float = layer_input.astype(F32)
    residual_one = input_float + attn_out
    h_two_f, norm_two_back = jax.vjp(rms_norm, residual_one, gain_two)
    h_two = h_two_f.astype(BF)
    router_probs = softmax_rows(matmul(h_two, router_weight))

    expert_w = (expert_gate[0].T, expert_up[0].T, expert_down[0])
    parts = max(1, devices * tok // 4096)
    if parts == 1:
        h2_all, s_both = swap(5, ("far_gather", h_two), ("whole_swap", s_both))
    else:
        s_both = swap(7, ("whole_swap", s_both))[0]
    shared_w = (s_both.reshape(width, 2 * shared_n), shared_down)
    slot_limit = 2 * tok * TOP // experts

    def on_rows(h2, h2_all, cot_gathered, routes_here):
        rows = h2.shape[0]
        slot_count = min(slot_limit, rows)
        member = jnp.any(routes_here == expert_id, axis=2)
        before_it = jnp.arange(rows)[:, None] < jnp.arange(rows)[None, :]
        rank = matmul(member.astype(BF), before_it.astype(BF)).astype(jnp.int32)
        place = jnp.where(member, rank, -1).reshape(devices // 2, 2 * rows)
        out, grad_h2, token_grad, grads = experts_sums(
            n_groups,
            rows,
            h2_all,
            cot_gathered,
            place,
            slot_count,
            expert_w,
            shared_w,
            router_weight,
            8,
        )
        picked = lax.all_to_all(token_grad, ALL, split_axis=0, concat_axis=0, tiled=True)
        picked = jnp.sum(picked.reshape(experts, devices // experts, rows), axis=1).T
        return out, grad_h2, picked, grads

    if parts == 1:
        cot_all = gather_all(cotangent_later)
        out_own, grad_h2_own, grad_router_probs, grads = on_rows(
            h_two, h2_all.reshape(-1, width), cot_all, routes_all
        )
    else:
        rows = tok // parts

        def step(total, inputs):
            h2, cot, routes_here = inputs
            cot_part = gather_all(cot)
            out, grad_h2, picked, grads = on_rows(h2, gather_all(h2), cot_part, routes_here)
            grads = lax.optimization_barrier(grads)
            total = tuple(a + b for a, b in zip(total, grads))
            return total, (out, grad_h2, picked)

        shapes = expert_w + shared_w
        grads, (out_own, grad_h2_own, grad_router_probs) = lax.scan(
            step,
            tuple(jnp.zeros(s.shape, F32) for s in shapes),
            (
                h_two.reshape(parts, rows, width),
                cotangent.reshape(parts, rows, width),
                routes_all.reshape(devices, parts, rows, TOP).transpose(1, 0, 2, 3),
            ),
        )
        out_own = out_own.reshape(tok, width)
        grad_h2_own = grad_h2_own.reshape(tok, width)
        grad_router_probs = grad_router_probs.reshape(tok, experts)
    g_gate, g_up, g_down, g_both, g_sdown = grads
    grad_logits = router_probs * (
        grad_router_probs - jnp.sum(router_probs * grad_router_probs, axis=1, keepdims=True)
    )
    grad_logits = grad_logits.astype(BF)
    grad_router = dot_tn(h_two, grad_logits)
    grad_h_two = grad_h2_own + dot_nt(grad_logits, router_weight)
    output = residual_one + out_own

    grad_x_one, grad_gain_two = norm_two_back(grad_h_two)
    grad_x_one = grad_x_one + cotangent.astype(F32)
    grad_attn_out = grad_x_one.astype(BF)
    g_shared, plane_grad = swap(
        3,
        ("whole_swap", g_both.astype(BF).reshape(n_groups, n_plane, rows_w, 2 * shared_n)),
        ("plane_gather", grad_attn_out),
    )
    plane_grad = plane_grad.reshape(plane_tok, width)
    grad_mixed = dot_nt(plane_grad, own_output).astype(BF)
    dqn, dqr, dex, dkr = attend_back(
        low_bound, q_nope, q_rope, expanded, key_rope, lse, grad_mixed, scale
    )

    g_output = dot_tn(mixed_heads, plane_grad).astype(BF).reshape(n_groups, rows_w, width)

    grad_expanded = dex.astype(BF)
    grad_expand = dot_tn(compressed, grad_expanded)
    grad_comp = dot_nt(grad_expanded, expand_weight)
    key_grads = jnp.concatenate([grad_comp, dkr], axis=1).astype(BF)
    key_grads = (
        key_grads.reshape(2, n_plane, tok, RANK + ROPE)
        .transpose(1, 0, 2, 3)
        .reshape(n_plane, 2 * tok, RANK + ROPE)
    )

    gq_nope = dqn.astype(BF)
    gq_rope = turn(dqr, -1.0).astype(BF)
    grad_hidden = (dot_nt(gq_nope, wq_nope) + dot_nt(gq_rope, wq_rope)).astype(BF)
    gw_nope = dot_tn(hidden, gq_nope).astype(BF).reshape(n_groups, n_plane, rows_w, -1)
    gw_rope = dot_tn(hidden, gq_rope).astype(BF).reshape(n_groups, n_plane, rows_w, -1)
    g_expand = grad_expand.astype(BF).reshape(n_groups, n_plane, kv_n, kv_cols)
    key_grad, grad_hidden, gw_nope, gw_rope, g_expand = swap(
        4,
        ("plane_sum_shift", key_grads),
        ("plane_sum", grad_hidden.reshape(n_plane, tok, width)),
        ("group_sum_swap", gw_nope),
        ("group_sum_swap", gw_rope),
        ("group_sum_swap", g_expand),
    )
    latent_own = own_rows(latent)
    kv_norm_back = jax.vjp(rms_norm, latent_own[:, :RANK], gain_kv)[1]
    grad_comp_in, grad_gain_kv = kv_norm_back(key_grad[:, :RANK])
    grad_rope_in = unrotate(key_grad[:, RANK:], own_rows(cosine), own_rows(sine_part))
    grad_latent = jnp.concatenate([grad_comp_in, grad_rope_in], axis=1).astype(BF)

    def per_head(table, cols):
        return table.transpose(1, 0, 2).reshape(rows_w, HEADS, cols)

    grad_query_weight = jnp.concatenate(
        [per_head(gw_nope, NOPE), per_head(gw_rope, ROPE)], axis=2
    ).reshape(rows_w, -1).astype(F32)
    grad_expand_weight = g_expand.transpose(1, 0, 2).reshape(kv_n, -1).astype(F32)

    g_latent = dot_tn(own_rows(hidden), grad_latent).astype(BF)
    g_latent = g_latent.reshape(n_groups, n_plane, rows_w, RANK + ROPE)
    grad_hidden = grad_hidden + dot_nt(grad_latent, latent_weight)
    norm_one_back = jax.vjp(rms_norm, input_float, gain_one)[1]
    grad_x_norm, grad_gain_one = norm_one_back(grad_hidden)
    grad_input = grad_x_one + grad_x_norm

    small_grads = jnp.concatenate(
        [
            p.reshape(devices, -1)
            for p in (grad_gain_one, grad_gain_two, grad_gain_kv, grad_router)
        ],
        axis=1,
    )
    small_grads = jnp.pad(small_grads, ((0, 0), (0, -small_grads.shape[1] % 1024)))
    grad_latent_weight, grad_output_weight, small_grads = swap(
        6,
        ("whole_sum", g_latent),
        ("group_sum_home", g_output),
        ("whole_sum", small_grads.reshape(n_groups, n_plane, -1, 128)),
    )
    small_grads = small_grads.reshape(-1)
    g_shared = g_shared.transpose(2, 0, 1, 3).reshape(rows_w, devices, 2 * shared_n).astype(F32)
    grad_shared_gate = g_shared[:, :, :shared_n].reshape(rows_w, devices * shared_n)
    grad_shared_up = g_shared[:, :, shared_n:].reshape(rows_w, devices * shared_n)
    return (
        output,
        grad_input,
        small_grads[: cuts[0]],
        grad_query_weight,
        grad_latent_weight,
        small_grads[cuts[1] : cuts[2]],
        grad_expand_weight,
        grad_output_weight,
        small_grads[cuts[0] : cuts[1]],
        small_grads[cuts[2] : cuts[3]].reshape(rows_w, experts),
        grad_shared_gate,
        grad_shared_up,
        g_sdown,
        g_gate.T[None],
        g_up.T[None],
        g_down[None],
    )


def solution(mesh):
    n_expert, n_shard = mesh.shape["expert"], mesh.shape["wshard"]
    devices = n_expert * n_shard

    def program(*args):
        tok = args[0].shape[0] // devices
        n_plane = DOC_MAX // tok
        n_groups = devices // n_plane
        inner = Mesh(mesh.devices.reshape(n_groups, n_plane // n_shard, n_shard), ALL)
        rows, vector = P(ALL, None), P(ALL)
        wide, tall = P(("g", "p"), None, "c"), P(("g", "p"), "c", None)
        step = jax.shard_map(
            functools.partial(body, n_groups, n_plane),
            mesh=inner,
            in_specs=(
                rows, vector, rows, rows, vector, rows, rows, vector, rows, rows, rows, rows,
                wide, wide, tall, rows, vector, rows,
            ),
            out_specs=(
                rows, rows, vector, rows, rows, vector, rows, rows, vector, rows, rows, rows,
                rows, wide, wide, tall,
            ),
            check_vma=False,
        )
        return step(*args)

    return program
```

```python
import functools

import jax
import jax.numpy as jnp
from jax import lax
from jax.experimental import pallas as pl
from jax.experimental.pallas import tpu as pltpu
from jax.sharding import Mesh, PartitionSpec as P

HEADS = 16
NOPE = 128
ROPE = 64
VDIM = 128
RANK = 512
TOP = 6
DOC_MAX = 1024
QUERY_BLOCK = 256

BF = jnp.bfloat16
F32 = jnp.float32
ALL = ("g", "p", "c")
PLANE = ("p", "c")

epsilon = 1e-06


def rms_norm(vector, scaling):
    return vector * lax.rsqrt(jnp.mean(vector * vector, axis=-1, keepdims=True) + epsilon) * scaling


def rotate(vector, cosine, sine_part):
    half_width = vector.shape[-1] // 2
    front_half = vector[..., :half_width]
    back_half = vector[..., half_width:]
    return jnp.concatenate(
        [front_half * cosine - back_half * sine_part, back_half * cosine + front_half * sine_part],
        axis=-1,
    )


def unrotate(vector, cosine, sine_part):
    return rotate(vector, cosine, -sine_part)


def matmul(left, right):
    return jnp.dot(left, right, preferred_element_type=F32)


def dot_nt(left, right):
    return lax.dot_general(left, right, (((1,), (1,)), ((), ())), preferred_element_type=F32)


def dot_tn(left, right):
    return lax.dot_general(left, right, (((0,), (0,)), ((), ())), preferred_element_type=F32)


def swiglu(gate_pre, up_pre):
    return jax.nn.silu(gate_pre) * up_pre


def softmax_rows(scores):
    row_top = jnp.max(scores, axis=-1, keepdims=True)
    exp_scores = jnp.exp(scores - row_top)
    return exp_scores / jnp.sum(exp_scores, axis=-1, keepdims=True)


def masked_scores(base, low_bound, q_nope, q_rope, k_nope, k_rope, scale):
    rows, span = q_nope.shape[0], k_nope.shape[0]
    key_at = lax.broadcasted_iota(jnp.int32, (rows, span), 1) + base
    query_at = lax.broadcasted_iota(jnp.int32, (rows, span), 0) + (base + DOC_MAX)
    allowed = (key_at >= low_bound) & (key_at <= query_at)
    scores = (dot_nt(q_nope, k_nope) + dot_nt(q_rope, k_rope)) * scale
    return jnp.where(allowed, scores, -1e30)


def attend_kernel(heads, scale, low_ref, qn_ref, qr_ref, ex_ref, kr_ref, out_ref, lse_ref):
    rows = qn_ref.shape[0]
    base = pl.multiple_of(pl.program_id(0) * rows, rows)
    window = pl.ds(base, rows + DOC_MAX)
    k_rope = kr_ref[window, :]
    low_bound = low_ref[...]
    for h in range(heads):
        at = h * (NOPE + VDIM)
        k_nope = ex_ref[window, at : at + NOPE]
        value = ex_ref[window, at + NOPE : at + NOPE + VDIM]
        scores = masked_scores(
            base,
            low_bound,
            qn_ref[:, h * NOPE : (h + 1) * NOPE],
            qr_ref[:, h * ROPE : (h + 1) * ROPE],
            k_nope,
            k_rope,
            scale,
        )
        top = jnp.max(scores, axis=-1, keepdims=True)
        exps = jnp.exp(scores - top)
        total = jnp.sum(exps, axis=-1, keepdims=True)
        probs = (exps / total).astype(BF)
        out_ref[:, h * VDIM : (h + 1) * VDIM] = jnp.dot(
            probs, value, preferred_element_type=F32
        ).astype(BF)
        lse_ref[:, h : h + 1] = top + jnp.log(total)


def attend(low_bound, q_nope, q_rope, expanded, key_rope, scale):
    queries = q_nope.shape[0]
    heads = q_nope.shape[1] // NOPE
    rows = QUERY_BLOCK

    def whole(array):
        return pl.BlockSpec(array.shape, lambda i: (0, 0))

    def blocked(width):
        return pl.BlockSpec((rows, width), lambda i: (i, 0))

    flops = 2 * heads * queries * (rows + DOC_MAX) * (NOPE + ROPE + VDIM)
    return pl.pallas_call(
        functools.partial(attend_kernel, heads, scale),
        grid=(queries // rows,),
        in_specs=[
            blocked(1),
            blocked(heads * NOPE),
            blocked(heads * ROPE),
            whole(expanded),
            whole(key_rope),
        ],
        out_specs=[blocked(heads * VDIM), blocked(heads)],
        out_shape=[
            jax.ShapeDtypeStruct((queries, heads * VDIM), BF),
            jax.ShapeDtypeStruct((queries, heads), F32),
        ],
        cost_estimate=pl.CostEstimate(
            flops=flops, bytes_accessed=4 * expanded.size, transcendentals=flops // 640
        ),
        compiler_params=pltpu.CompilerParams(vmem_limit_bytes=50 * 1024 * 1024),
        name="attend",
    )(low_bound, q_nope, q_rope, expanded, key_rope)


def attend_back_kernel(
    heads, scale, low_ref, qn_ref, qr_ref, ex_ref, kr_ref, lse_ref, gm_ref,
    dqn_ref, dqr_ref, dex_ref, dkr_ref,
):
    rows = qn_ref.shape[0]
    step = pl.program_id(0)
    base = pl.multiple_of(step * rows, rows)
    window = pl.ds(base, rows + DOC_MAX)

    @pl.when(step == 0)
    def _():
        dex_ref[...] = jnp.zeros_like(dex_ref)
        dkr_ref[...] = jnp.zeros_like(dkr_ref)

    k_rope = kr_ref[window, :]
    low_bound = low_ref[...]
    for h in range(heads):
        at = h * (NOPE + VDIM)
        k_nope = ex_ref[window, at : at + NOPE]
        value = ex_ref[window, at + NOPE : at + NOPE + VDIM]
        q_nope = qn_ref[:, h * NOPE : (h + 1) * NOPE]
        q_rope = qr_ref[:, h * ROPE : (h + 1) * ROPE]
        grad_out = gm_ref[:, h * VDIM : (h + 1) * VDIM]
        scores = masked_scores(base, low_bound, q_nope, q_rope, k_nope, k_rope, scale)
        probs = jnp.exp(scores - lse_ref[:, h : h + 1])
        grad_probs = dot_nt(grad_out, value)
        mean_grad = jnp.sum(probs * grad_probs, axis=-1, keepdims=True)
        grad_scores = (probs * (grad_probs - mean_grad) * scale).astype(BF)
        probs_low = probs.astype(BF)
        dqn_ref[:, h * NOPE : (h + 1) * NOPE] = jnp.dot(
            grad_scores, k_nope, preferred_element_type=F32
        )
        dqr_ref[:, h * ROPE : (h + 1) * ROPE] = jnp.dot(
            grad_scores, k_rope, preferred_element_type=F32
        )
        dex_ref[window, at : at + NOPE] += dot_tn(grad_scores, q_nope)
        dex_ref[window, at + NOPE : at + NOPE + VDIM] += dot_tn(probs_low, grad_out)
        dkr_ref[window, :] += dot_tn(grad_scores, q_rope)


def attend_back(low_bound, q_nope, q_rope, expanded, key_rope, lse, grad_mixed, scale):
    queries = q_nope.shape[0]
    heads = q_nope.shape[1] // NOPE
    rows = QUERY_BLOCK

    def whole(shape):
        return pl.BlockSpec(shape, lambda i: (0, 0))

    def blocked(width):
        return pl.BlockSpec((rows, width), lambda i: (i, 0))

    flops = 2 * heads * queries * (rows + DOC_MAX) * (3 * NOPE + 3 * ROPE + 2 * VDIM)
    return pl.pallas_call(
        functools.partial(attend_back_kernel, heads, scale),
        grid=(queries // rows,),
        in_specs=[
            blocked(1),
            blocked(heads * NOPE),
            blocked(heads * ROPE),
            whole(expanded.shape),
            whole(key_rope.shape),
            blocked(heads),
            blocked(heads * VDIM),
        ],
        out_specs=[
            blocked(heads * NOPE),
            blocked(heads * ROPE),
            whole(expanded.shape),
            whole(key_rope.shape),
        ],
        out_shape=[
            jax.ShapeDtypeStruct(q_nope.shape, F32),
            jax.ShapeDtypeStruct(q_rope.shape, F32),
            jax.ShapeDtypeStruct(expanded.shape, F32),
            jax.ShapeDtypeStruct(key_rope.shape, F32),
        ],
        cost_estimate=pl.CostEstimate(
            flops=flops, bytes_accessed=8 * expanded.size, transcendentals=flops // 1664
        ),
        compiler_params=pltpu.CompilerParams(vmem_limit_bytes=56 * 1024 * 1024),
        name="attend_back",
    )(low_bound, q_nope, q_rope, expanded, key_rope, lse, grad_mixed)


MESH = pl.DeviceIdType.MESH


def pause(rounds):
    for _ in range(rounds):
        yield


class Wires:
    def __init__(self, n_groups, n_plane, send, recv):
        self.n_groups, self.n_plane, self.send, self.recv = n_groups, n_plane, send, recv
        self.cores = 2
        self.g, self.p, self.c = lax.axis_index("g"), lax.axis_index("p"), lax.axis_index("c")
        self.j = self.p * self.cores + self.c
        self.used = 0

    def at_plane(self, j):
        return {"g": self.g, "p": j // self.cores, "c": j % self.cores}

    def at_chip(self, p):
        return {"g": self.g, "p": p, "c": self.c}

    def at_group(self, g):
        return {"g": g, "p": self.p, "c": self.c}

    def partner(self):
        return {"g": self.g, "p": self.p, "c": 1 - self.c}

    def beside(self):
        return self.p + 1 - 2 * lax.rem(self.p, 2)

    def above(self):
        return self.p + 2 - 4 * (self.p // 2)

    def core_of(self, p):
        return p * self.cores + self.c

    def plane_peer(self, d):
        return lax.rem(self.j + d, self.n_plane)

    def group_peer(self, d):
        return lax.rem(self.g + d, self.n_groups)

    def start(self, src, dst, device):
        copy = pltpu.make_async_remote_copy(
            src_ref=src,
            dst_ref=dst,
            send_sem=self.send.at[self.used],
            recv_sem=self.recv.at[self.used],
            device_id=device,
            device_id_type=MESH,
        )
        self.used += 1
        copy.start()
        return copy

    def at_device(self, index):
        return {"g": index // self.n_plane, **self.on_plane(lax.rem(index, self.n_plane))}

    def on_plane(self, j):
        return {"p": j // self.cores, "c": j % self.cores}

    def meet(self, heads=False, home=False):
        barrier = pltpu.get_barrier_semaphore()
        waits = self.n_plane - 1 + self.n_groups - 1
        if heads:
            mine = self.head_owner() == self.j
            part = lax.rem(self.g * self.n_plane + self.j, self.n_groups)
            for r in range(self.n_groups):

                @pl.when(jnp.logical_not(mine) | (part != r))
                def _():
                    source = self.at_device(self.n_groups * self.j + r)
                    pl.semaphore_signal(barrier, inc=1, device_id=source, device_id_type=MESH)

            waits = waits + jnp.where(mine, self.n_groups - 1, self.n_groups)
        if home:
            source = self.home_source()
            stays = source == self.g * self.n_plane + self.j

            @pl.when(jnp.logical_not(stays))
            def _():
                pl.semaphore_signal(
                    barrier, inc=1, device_id=self.at_device(source), device_id_type=MESH
                )

            waits = waits + jnp.where(stays, 0, 1)
        for d in range(1, self.n_plane):
            pl.semaphore_signal(
                barrier, inc=1, device_id=self.at_plane(self.plane_peer(d)), device_id_type=MESH
            )
        for d in range(1, self.n_groups):
            pl.semaphore_signal(
                barrier, inc=1, device_id=self.at_group(self.group_peer(d)), device_id_type=MESH
            )
        pl.semaphore_wait(barrier, waits)

    def home_source(self):
        index = self.g * self.n_plane + self.j
        return lax.rem(index, self.n_groups) * self.n_plane + index // self.n_groups

    def head_owner(self):
        return (self.g * self.n_plane + self.j) // self.n_groups


def sum_rows(dst, sources):
    rows = dst.shape[0]
    tile = 32 if rows % 32 == 0 else rows

    def step(i, carry):
        at = pl.ds(pl.multiple_of(i * tile, tile), tile)
        if len(sources) == 2 and all(r.dtype == BF for r in [dst] + sources):
            dst[at, :] = sources[0][at, :] + sources[1][at, :]
        else:
            total = sources[0][at, :].astype(F32)
            for source in sources[1:]:
                total = total + source[at, :].astype(F32)
            dst[at, :] = total.astype(dst.dtype)
        return carry

    lax.fori_loop(0, rows // tile, step, 0)


def wait_all(copies):
    for copy in copies:
        copy.wait()


def wait_received(copies):
    for copy in copies:
        copy.wait_recv()


def wait_sent(copies):
    for copy in copies:
        copy.wait_send()


def part_of(ref, upper):
    rows = ref.shape[0] // 2
    return ref.at[pl.ds(rows, rows)] if upper else ref.at[pl.ds(0, rows)]


def spread(w, own, at):
    beside, above = w.at_chip(w.beside()), w.at_chip(w.above())
    mine = at(w.j)
    halves = [(part_of(own, u), part_of(mine, u)) for u in (0, 1)]
    lower = w.start(*halves[0], beside)
    upper = w.start(*halves[1], above)
    rest = [w.start(*halves[1], beside), w.start(*halves[0], above)]
    on_chip = [w.start(own, mine, w.partner())]
    yield
    lower.wait_recv()
    block = part_of(at(w.core_of(w.beside())), 0)
    rest.append(w.start(block, block, above))
    upper.wait_recv()
    block = part_of(at(w.core_of(w.above())), 1)
    rest.append(w.start(block, block, beside))
    yield
    wait_received(rest)
    for p in (w.beside(), w.above(), 3 - w.p):
        block = at(w.core_of(p))
        on_chip.append(w.start(block, block, w.partner()))
    yield
    wait_sent([lower, upper] + rest)
    wait_all(on_chip)


def plane_gather(w, src, out):
    out[w.j] = src[...]
    yield from spread(w, src, lambda j: out.at[j])


def far_gather(w, src, out, sem):
    mine = out.at[w.g, w.j]
    away = [w.start(src, mine, w.at_group(w.group_peer(d))) for d in range(1, w.n_groups)]
    local = pltpu.make_async_copy(src, mine, sem)
    local.start()
    running = [spread(w, src, lambda j: out.at[w.g, j])]
    next(running[0])
    for d in range(1, w.n_groups):
        away[d - 1].wait_recv()
        g = w.group_peer(w.n_groups - d)
        running.append(spread(w, out.at[g, w.j], lambda j, g=g: out.at[g, j]))
        next(running[d])
    for _ in range(3):
        for routine in running:
            next(routine, None)
        yield
    local.wait()
    wait_sent(away)


def shift_gather(w, src, mid, out):
    copy = w.start(src, mid, w.at_group(lax.rem(w.g + 1, w.n_groups)))
    yield
    copy.wait()
    yield from plane_gather(w, mid, out)


def whole_gather(w, src, out):
    chips = w.n_plane // w.cores
    first = [
        w.start(src, out.at[w.g, w.j], w.at_group(w.group_peer(d))) for d in range(1, w.n_groups)
    ]
    out[w.g, w.j] = src[...]
    yield
    wait_received(first)
    mine = out.at[:, w.j]
    second = [w.start(mine, mine, w.at_chip(lax.rem(w.p + d, chips))) for d in range(1, chips)]
    third = [w.start(mine, mine, w.partner())]
    yield
    for d in range(1, chips):
        second[d - 1].wait_recv()
        block = out.at[:, w.core_of(lax.rem(w.p + chips - d, chips))]
        third.append(w.start(block, block, w.partner()))
    yield
    wait_sent(first)
    wait_sent(second)
    wait_all(third)


def plane_swap_gather(w, src, out):
    first = []
    for d in range(1, w.n_plane):
        to = w.plane_peer(d)
        first.append(w.start(src.at[to], out.at[w.g, w.j], w.at_plane(to)))
    out[w.g, w.j] = src[w.j]
    yield
    wait_received(first)
    second = [
        w.start(out.at[w.g], out.at[w.g], w.at_group(w.group_peer(d)))
        for d in range(1, w.n_groups)
    ]
    yield from pause(4)
    wait_sent(first)
    wait_all(second)


def head_rows(w, src, out):
    index = w.g * w.n_plane + w.j
    owner, part = w.head_owner(), lax.rem(index, w.n_groups)
    mine = owner == w.j

    def to(d):
        return pltpu.make_async_remote_copy(
            src_ref=src,
            dst_ref=out.at[part],
            send_sem=w.send.at[base + d],
            recv_sem=w.recv.at[base + part],
            device_id={"g": w.group_peer(d), **w.on_plane(owner)},
            device_id_type=MESH,
        )

    def arrival(r):
        return pltpu.make_async_remote_copy(
            src_ref=src,
            dst_ref=out.at[r],
            send_sem=w.send.at[base],
            recv_sem=w.recv.at[base + r],
            device_id=w.at_device(w.n_groups * w.j + r),
            device_id_type=MESH,
        )

    yield from pause(3)
    base = w.used
    w.used += w.n_groups
    for d in range(w.n_groups):

        @pl.when((d > 0) | jnp.logical_not(mine))
        def _():
            to(d).start()

    @pl.when(mine)
    def _():
        out[part] = src[...]

    yield from pause(2)
    for r in range(w.n_groups):

        @pl.when(jnp.logical_not(mine) | (part != r))
        def _():
            arrival(r).wait_recv()

    for d in range(w.n_groups):

        @pl.when((d > 0) | jnp.logical_not(mine))
        def _():
            to(d).wait_send()


def plane_swap(w, src, out):
    copies = []
    for d in range(1, w.n_plane):
        to = w.plane_peer(d)
        copies.append(w.start(src.at[to], out.at[w.j], w.at_plane(to)))
    out[w.j] = src[w.j]
    yield
    wait_all(copies)


def plane_sum(w, src, out, from_core, pairs, from_chips):
    to = (w.beside(), 3 - w.p, w.above(), w.p)
    beside, above = w.at_chip(w.beside()), w.at_chip(w.above())
    first = [
        w.start(src.at[p * w.cores + 1 - w.c], from_core.at[i], w.partner())
        for i, p in enumerate(to)
    ]
    yield
    sent = []

    def send(i, upper, slot, device):
        sent.append(w.start(part_of(pairs.at[i], upper), from_chips.at[slot], device))

    for i, p in enumerate(to):
        first[i].wait_recv()
        sum_rows(pairs.at[i], [src.at[w.core_of(p)], from_core.at[i]])
        if i < 2:
            send(i, 0, i, beside)
        if i == 1:
            send(1, 1, 2, above)
        if i == 2:
            send(2, 1, 3, above)
    yield
    for wire, i, upper, slot, device in ((1, 2, 0, 4, above), (2, 0, 1, 5, beside)):
        sent[wire].wait_recv()
        target = part_of(pairs.at[i], upper)
        sum_rows(target, [target, from_chips.at[wire]])
        send(i, upper, slot, device)
    yield
    for wire in (0, 3, 4, 5):
        sent[wire].wait_recv()
    for upper, arrived in ((0, (0, 4)), (1, (3, 5))):
        sum_rows(
            part_of(out, upper),
            [part_of(pairs.at[3], upper)] + [from_chips.at[slot] for slot in arrived],
        )
    wait_sent(first)
    wait_sent(sent)


def whole_sum(w, src, out, from_core, pairs, from_chips, total, parts):
    chips = w.n_plane // w.cores
    to = [lax.rem(w.p + d, chips) for d in range(chips)]
    first = [
        w.start(src.at[:, p * w.cores + 1 - w.c], from_core.at[d], w.partner())
        for d, p in enumerate(to)
    ]
    yield
    second = []
    for d in list(range(1, chips)) + [0]:
        first[d].wait_recv()

        def step(i, carry):
            sum_rows(pairs.at[d, i], [src.at[i, w.core_of(to[d])], from_core.at[d, i]])
            return carry

        lax.fori_loop(0, w.n_groups, step, 0)
        if d:
            second.append(w.start(pairs.at[d], from_chips.at[d - 1], w.at_chip(to[d])))
    yield
    wait_received(second)

    def step(i, carry):
        sum_rows(total.at[i], [pairs.at[0, i]] + [from_chips.at[d, i] for d in range(chips - 1)])
        return carry

    lax.fori_loop(0, w.n_groups, step, 0)
    wait_sent(first)
    wait_sent(second)
    yield from group_sum(w, total, out, parts)


def whole_swap(w, src, out, mid):
    first = []
    for d in range(1, w.n_groups):
        to = w.group_peer(d)
        first.append(w.start(src.at[to], mid.at[w.g], w.at_group(to)))
    mid[w.g] = src[w.g]
    yield from pause(3)
    wait_received(first)
    second = []
    for d in range(1, w.n_plane):
        to = w.plane_peer(d)
        second.append(w.start(mid.at[:, to], out.at[:, w.j], w.at_plane(to)))
    out[:, w.j] = mid[:, w.j]
    yield
    wait_sent(first)
    wait_all(second)


def group_sum_home(w, src, out, parts, low, home):
    copies = []
    for d in range(1, w.n_groups):
        to = w.group_peer(d)
        copies.append(w.start(src.at[to], parts.at[d - 1], w.at_group(to)))
    yield from pause(3)
    wait_received(copies)
    sum_rows(low, [src.at[w.g]] + [parts.at[d] for d in range(w.n_groups - 1)])
    stays = w.home_source() == w.g * w.n_plane + w.j
    copy = pltpu.make_async_remote_copy(
        src_ref=low,
        dst_ref=home,
        send_sem=w.send.at[w.used],
        recv_sem=w.recv.at[w.used],
        device_id=w.at_device(w.n_groups * w.j + w.g),
        device_id_type=MESH,
    )
    w.used += 1

    @pl.when(jnp.logical_not(stays))
    def _():
        copy.start()

    @pl.when(stays)
    def _():
        home[...] = low[...]

    yield

    @pl.when(jnp.logical_not(stays))
    def _():
        copy.wait()

    out[...] = home[...].astype(F32)
    wait_sent(copies)


def plane_sum_shift(w, src, out, from_core, pairs, from_chips, low, later):
    rows = out.shape[0]
    yield from plane_sum(w, src, low, from_core, pairs, from_chips)
    copy = w.start(
        low.at[pl.ds(0, rows)], later, w.at_group(lax.rem(w.g + w.n_groups - 1, w.n_groups))
    )
    yield
    copy.wait()
    keep = jnp.where(w.g == w.n_groups - 1, 0.0, 1.0)
    out[...] = low[rows:, :].astype(F32) + later[...].astype(F32) * keep


def group_sum(w, src, out, parts):
    copies = []
    for d in range(1, w.n_groups):
        to = w.group_peer(d)
        copies.append(w.start(src.at[to], parts.at[d - 1], w.at_group(to)))
    yield
    wait_received(copies)
    sum_rows(out, [src.at[w.g]] + [parts.at[d] for d in range(w.n_groups - 1)])
    wait_sent(copies)


def group_sum_swap(w, src, out, total, parts):
    copies = []
    for d in range(1, w.n_groups):
        to = w.group_peer(d)
        copies.append(w.start(src.at[to], parts.at[d - 1], w.at_group(to)))
    yield from pause(4)
    wait_received(copies)

    def step(i, carry):
        sum_rows(total.at[i], [src.at[w.g, i]] + [parts.at[d, i] for d in range(w.n_groups - 1)])
        return carry

    lax.fori_loop(0, w.n_plane, step, 0)
    second = []
    for d in range(1, w.n_plane):
        to = w.plane_peer(d)
        second.append(w.start(total.at[to], out.at[w.j], w.at_plane(to)))
    out[w.j] = total[w.j]
    yield
    wait_sent(copies)
    wait_all(second)


ROUTINES = {
    "plane_gather": plane_gather,
    "shift_gather": shift_gather,
    "whole_gather": whole_gather,
    "far_gather": far_gather,
    "plane_swap_gather": plane_swap_gather,
    "plane_swap": plane_swap,
    "plane_sum": plane_sum,
    "plane_sum_shift": plane_sum_shift,
    "head_rows": head_rows,
    "group_sum": group_sum,
    "whole_sum": whole_sum,
    "whole_swap": whole_swap,
    "group_sum_home": group_sum_home,
    "group_sum_swap": group_sum_swap,
}


def exchange_kernel(n_groups, n_plane, kinds, extra, *refs):
    count = len(kinds)
    sources, outs = refs[:count], refs[count : 2 * count]
    scratch = list(refs[2 * count : -2])
    w = Wires(n_groups, n_plane, refs[-2], refs[-1])
    w.meet("head_rows" in kinds, "group_sum_home" in kinds)
    running = []
    for kind, source, out, number in zip(kinds, sources, outs, extra):
        mine, scratch = scratch[:number], scratch[number:]
        if kind == "shift_gather":
            running.append(shift_gather(w, source, mine[0], out))
        else:
            running.append(ROUTINES[kind](w, source, out, *mine))
    while running:
        still = []
        for routine in running:
            try:
                next(routine)
                still.append(routine)
            except StopIteration:
                pass
        running = still


def exchange(n_groups, n_plane, number, *items):
    kinds = [kind for kind, _ in items]
    arrays = [array for _, array in items]
    shapes, scratch, extra = [], [], []
    chips = n_plane // 2
    for kind, array in items:
        shape, dtype = array.shape, array.dtype
        own = []
        if kind in ("plane_gather", "shift_gather"):
            out = (n_plane,) + shape
            if kind == "shift_gather":
                own = [shape]
        elif kind in ("whole_gather", "far_gather"):
            out = (n_groups, n_plane) + shape
        elif kind == "plane_swap_gather":
            out = (n_groups,) + shape
        elif kind == "plane_swap":
            out = shape
        elif kind == "head_rows":
            out = (n_groups,) + shape
        elif kind == "plane_sum_shift":
            pair = shape[1:]
            out = (shape[1] // 2, shape[2])
            half = (pair[0] // 2, pair[1])
            own = [(chips,) + pair, (chips,) + pair, (6,) + half, pair, out]
        elif kind == "plane_sum":
            out = shape[1:]
            own = [(chips,) + out, (chips,) + out, (6, out[0] // 2, out[1])]
        elif kind == "group_sum_home":
            out = shape[1:]
            own = [(n_groups - 1,) + out, out, out]
        elif kind == "group_sum":
            out = shape[1:]
            own = [(n_groups - 1,) + out]
        elif kind == "whole_swap":
            out = shape
            own = [shape]
        elif kind == "whole_sum":
            out = shape[2:]
            full = (n_groups,) + out
            own = [(chips,) + full, (chips,) + full, (chips - 1,) + full, full]
            own = own + [(n_groups - 1,) + out]
        elif kind == "group_sum_swap":
            out = shape[1:]
            own = [out, (n_groups - 1,) + out]
        if kind in ("plane_sum", "plane_sum_shift", "group_sum", "group_sum_home", "whole_sum"):
            shapes.append(jax.ShapeDtypeStruct(out, F32))
        else:
            shapes.append(jax.ShapeDtypeStruct(out, dtype))
        scratch += [pltpu.VMEM(s, dtype) for s in own]
        if kind == "far_gather":
            own = [None]
            scratch.append(pltpu.SemaphoreType.DMA)
        extra.append(len(own))
    copies = 64 + 32 * len(items)
    vmem = pl.BlockSpec(memory_space=pltpu.VMEM)
    return pl.pallas_call(
        functools.partial(exchange_kernel, n_groups, n_plane, kinds, extra),
        out_shape=shapes,
        in_specs=[vmem] * len(items),
        out_specs=[
            pl.BlockSpec(memory_space=pl.ANY) if kind == "far_gather" else vmem for kind in kinds
        ],
        scratch_shapes=scratch
        + [pltpu.SemaphoreType.DMA((copies,)), pltpu.SemaphoreType.DMA((copies,))],
        compiler_params=pltpu.CompilerParams(
            collective_id=number,
            has_side_effects=True,
            vmem_limit_bytes=60 * 1024 * 1024,
        ),
        name="exchange_%d" % number,
    )(*arrays)


def gather_all(x):
    return lax.all_gather(x, ALL, axis=0, tiled=True)


class StreamSum:
    def __init__(self, w, steps, stage, from_core, pairs, from_chips, totals, parts, sems, credit):
        self.w, self.steps = w, steps
        self.stage, self.from_core, self.pairs = stage, from_core, pairs
        self.from_chips, self.totals, self.parts = from_chips, totals, parts
        self.core_sems, self.chip_sems, self.chip_recv, self.group_sems = sems
        self.credit = credit

    @staticmethod
    def chips(w, step):
        half = lax.rem(step, 2)
        beside = w.p + 1 - 2 * lax.rem(w.p, 2)
        above = w.p + 2 - 4 * (w.p // 2)
        return beside + half * (above - beside), 3 - w.p + half * (2 * w.p - 3)

    def core_copy(self, step, i):
        slot = lax.rem(step, 2)
        return pltpu.make_async_remote_copy(
            src_ref=self.stage.at[slot, 2 * i + 1 - self.w.c],
            dst_ref=self.from_core.at[slot, i],
            send_sem=self.core_sems.at[0, slot, i],
            recv_sem=self.core_sems.at[1, slot, i],
            device_id=self.w.partner(),
            device_id_type=MESH,
        )

    def part(self, ref, upper):
        rows = ref.shape[0] // 2
        return ref.at[pl.ds(rows, rows)] if upper else ref.at[pl.ds(0, rows)]

    def chip_copy(self, group_at, which):
        slot, i, upper, up = (
            (0, 0, False, False),
            (0, 1, False, False),
            (0, 1, True, True),
            (1, 0, True, True),
            (1, 0, False, True),
            (0, 0, True, False),
        )[which]
        p = self.w.p
        to = p + 2 - 4 * (p // 2) if up else p + 1 - 2 * lax.rem(p, 2)
        return pltpu.make_async_remote_copy(
            src_ref=self.part(self.pairs.at[slot, i], upper),
            dst_ref=self.from_chips.at[group_at, which],
            send_sem=self.chip_sems.at[which],
            recv_sem=self.chip_recv.at[group_at, which],
            device_id=self.w.at_chip(to),
            device_id_type=MESH,
        )

    def group_copy(self, group_at):
        return pltpu.make_async_remote_copy(
            src_ref=self.totals.at[group_at],
            dst_ref=self.parts.at[group_at],
            send_sem=self.group_sems.at[0, group_at],
            recv_sem=self.group_sems.at[1, group_at],
            device_id=self.w.at_group(self.w.group_peer(group_at + 1)),
            device_id_type=MESH,
        )

    def open_stage(self, step):
        @pl.when(step >= 2)
        def _():
            for i in range(2):
                self.core_copy(step, i).wait_send()

    def push(self, step):
        @pl.when(step >= 2)
        def _():
            pl.semaphore_wait(self.credit, 1)

        for i in range(2):
            self.core_copy(step, i).start()

    def merge(self, step):
        slot, group_at = lax.rem(step, 2), step // 2
        for half, sends in ((0, (0, 1, 2, 5)), (1, (3, 4))):

            @pl.when((slot == half) & (step >= 2))
            def _():
                for which in sends:
                    self.chip_copy(group_at, which).wait_send()

        for i in range(2):
            self.core_copy(step, i).wait_recv()
            sum_rows(
                self.pairs.at[slot, i],
                [self.stage.at[slot, 2 * i + self.w.c], self.from_core.at[slot, i]],
            )

        @pl.when(step + 2 < self.steps)
        def _():
            pl.semaphore_signal(
                self.credit, inc=1, device_id=self.w.partner(), device_id_type=MESH
            )

        @pl.when(slot == 0)
        def _():
            for which in (0, 1, 2):
                self.chip_copy(group_at, which).start()

        @pl.when(slot == 1)
        def _():
            self.chip_copy(group_at, 3).start()
            for source, i, upper, which in ((1, (1, 0), False, 4), (2, (0, 0), True, 5)):
                self.chip_copy(group_at, source).wait_recv()
                target = self.part(self.pairs.at[i], upper)
                sum_rows(target, [target, self.from_chips.at[group_at, source]])
                self.chip_copy(group_at, which).start()

    def plane_total(self, group_at):
        for which in (0, 3, 4, 5):
            self.chip_copy(group_at, which).wait_recv()
        return [
            [self.part(self.pairs.at[1, 1], upper)]
            + [self.from_chips.at[group_at, which] for which in arrived]
            for upper, arrived in ((False, (0, 4)), (True, (3, 5)))
        ]

    def advance(self, step):
        @pl.when(step >= 1)
        def _():
            last = step - 1

            @pl.when((lax.rem(last, 2) == 0) & (last >= 2))
            def _():
                group_at = last // 2 - 1
                for upper, sources in enumerate(self.plane_total(group_at)):
                    sum_rows(self.part(self.totals.at[group_at], upper), sources)
                self.group_copy(group_at).start()

            self.merge(last)

    def finish(self, out):
        steps = self.steps
        self.merge(steps - 1)
        groups = steps // 2 - 1
        halves = self.plane_total(groups)
        for d in range(groups):
            self.group_copy(d).wait_recv()
        for upper, sources in enumerate(halves):
            parts = [self.part(self.parts.at[d], upper) for d in range(groups)]
            sum_rows(self.part(out, upper), sources + parts)
        for d in range(groups):
            self.group_copy(d).wait_send()
        for i in range(2):
            self.core_copy(steps - 2, i).wait_send()
            self.core_copy(steps - 1, i).wait_send()
        for which in range(6):
            self.chip_copy(groups, which).wait_send()

    @staticmethod
    def scratch(n_groups, rows, width):
        dma = pltpu.SemaphoreType.DMA
        return [
            pltpu.VMEM((2, 4, rows, width), BF),
            pltpu.VMEM((2, 2, rows, width), BF),
            pltpu.VMEM((2, 2, rows, width), BF),
            pltpu.VMEM((n_groups, 6, rows // 2, width), BF),
            pltpu.VMEM((n_groups - 1, rows, width), BF),
            pltpu.VMEM((n_groups - 1, rows, width), BF),
            dma((2, 2, 2)),
            dma((6,)),
            dma((n_groups, 6)),
            dma((2, n_groups - 1)),
            pltpu.SemaphoreType.REGULAR,
        ]


def swiglu_both(gate, up, grad):
    sigmoid = 1.0 / (1.0 + jnp.exp(-gate))
    silu = gate * sigmoid
    return silu * up, grad * up * (sigmoid * (1.0 + gate * (1.0 - sigmoid))), grad * silu


def step_chips(w, step):
    group = lax.rem(w.g + 1 + step // 2, w.n_groups)
    return [group * 4 + chip for chip in StreamSum.chips(w, step)]


def hot_rows(place, rows, core, slot_count):
    mine = place[:, core * rows : (core + 1) * rows]
    return lax.broadcasted_iota(jnp.int32, (slot_count, rows), 0) == mine


def moe_kernel(
    n_groups, experts, first_logit, slot_count,
    h2_hbm, cot_hbm, place_ref, wg_ref, wu_ref, wd_ref, sc_ref, sd_ref,
    sum_ref, rows_ref, gin_ref, act_ref, gg_ref, gu_ref, rw_ref, sact_ref, dboth_ref, dsd_ref,
    tok_ref,
    h2_buf, cot_buf, load_sems, *comm,
):
    rows = sum_ref.shape[0]
    step, steps = pl.program_id(0), 2 * n_groups
    w = Wires(n_groups, 8, None, None)
    stream = StreamSum(w, steps, *comm[:6], comm[6:10], comm[10])
    expert_id = w.g * 4 + w.p
    half = sc_ref.shape[1] // 2

    def loads(at):
        slot = lax.rem(at, 2)
        for i, chip in enumerate(step_chips(w, at)):
            source = pl.ds(pl.multiple_of(chip * 2 * rows, 2 * rows), 2 * rows)
            target = pl.ds(i * 2 * rows, 2 * rows)
            for k, (hbm, buf) in enumerate(((h2_hbm, h2_buf), (cot_hbm, cot_buf))):
                yield pltpu.make_async_copy(
                    hbm.at[source], buf.at[slot, target], load_sems.at[slot, i, k]
                )

    @pl.when(step == 0)
    def _():
        for copy in loads(step):
            copy.start()
        w.meet()
        for ref in (dboth_ref, dsd_ref):
            ref[...] = jnp.zeros_like(ref)

    @pl.when(step + 1 < steps)
    def _():
        for copy in loads(step + 1):
            copy.start()

    for copy in loads(step):
        copy.wait()
    slot = lax.rem(step, 2)
    h2, cot = h2_buf[slot], cot_buf[slot]
    chips = step_chips(w, step)

    pre = jnp.dot(h2, sc_ref[...], preferred_element_type=F32)
    back = dot_nt(cot, sd_ref[...])
    gate, up = pre[:, :half], pre[:, half:]
    lane = lax.broadcasted_iota(jnp.int32, gate.shape, 1)
    logits = jnp.where((lane >= first_logit) & (lane < first_logit + experts), gate, -1e30)
    exps = jnp.exp(logits - jnp.max(logits, axis=1, keepdims=True))
    chosen = jnp.where(lane == first_logit + expert_id, exps, 0.0)
    weight = jnp.sum(chosen, axis=1, keepdims=True) / jnp.sum(exps, axis=1, keepdims=True)
    act, grad_gate, grad_up = swiglu_both(gate, up, back)
    shared_act = act.astype(BF)
    shared_grad = jnp.concatenate([grad_gate.astype(BF), grad_up.astype(BF)], axis=1)
    for i, chip in enumerate(chips):
        at = pl.ds(pl.multiple_of(chip * 2 * rows, 2 * rows), 2 * rows)
        sact_ref[at, :] = shared_act[i * 2 * rows : (i + 1) * 2 * rows]

    hots, weights = [], []
    for q in range(4):
        place = place_ref[pl.ds(chips[q // 2], 1), :]
        hot = hot_rows(place, rows, q % 2, slot_count).astype(F32)
        hots.append(hot)
        tokens = slice(q * rows, (q + 1) * rows)
        slots = slice(q * slot_count, (q + 1) * slot_count)
        low = hot.astype(BF)
        rows_ref[slots, :] = jnp.dot(low, h2[tokens], preferred_element_type=F32).astype(BF)
        gin_ref[slots, :] = jnp.dot(low, cot[tokens], preferred_element_type=F32).astype(BF)
        spread = jnp.broadcast_to(weight[tokens], (rows, 128))
        weights.append(
            jnp.dot(hot, spread, preferred_element_type=F32, precision=lax.Precision.HIGHEST)[:, :1]
        )
    row_weight = jnp.concatenate(weights, axis=0)
    rw_ref[...] = row_weight
    expert_rows = rows_ref[...]
    picked_cot = gin_ref[...]
    back = dot_nt(picked_cot, wd_ref[...])
    gin_ref[...] = (picked_cot.astype(F32) * row_weight).astype(BF)
    gate = dot_nt(expert_rows, wg_ref[...])
    up = dot_nt(expert_rows, wu_ref[...])
    act, grad_gate, grad_up = swiglu_both(gate, up, back * row_weight)
    act_low, grad_gate, grad_up = act.astype(BF), grad_gate.astype(BF), grad_up.astype(BF)
    act_ref[...] = act_low
    gg_ref[...] = grad_gate
    gu_ref[...] = grad_up
    picked = jnp.sum(act_low.astype(F32) * back, axis=1, keepdims=True)
    grad_rows = jnp.dot(grad_gate, wg_ref[...], preferred_element_type=F32)
    grad_rows = grad_rows + jnp.dot(grad_up, wu_ref[...], preferred_element_type=F32)
    grad_rows = grad_rows.astype(BF)
    stream.open_stage(step)
    for q in range(4):
        tokens = slice(q * rows, (q + 1) * rows)
        slots = slice(q * slot_count, (q + 1) * slot_count)
        tok_ref[pl.ds(chips[q // 2] * 2 + q % 2, 1), :] = jnp.sum(
            hots[q] * picked[slots], axis=0, keepdims=True
        )
        total = dot_tn(hots[q].astype(BF), grad_rows[slots]) + dot_nt(
            shared_grad[tokens], sc_ref[...]
        )
        stream.stage[slot, q] = total.astype(BF)
    stream.push(step)
    stream.advance(step)

    piece = h2.shape[1] // 4
    turned, turned_act = shared_grad.T, shared_act.T
    for k in range(4):
        cols = slice(k * piece, (k + 1) * piece)
        dboth_ref[:, cols] += jnp.dot(turned, h2[:, cols], preferred_element_type=F32)
        dsd_ref[:, cols] += jnp.dot(turned_act, cot[:, cols], preferred_element_type=F32)

    @pl.when(step == steps - 1)
    def _():
        stream.finish(sum_ref)


def out_kernel(
    n_groups, slot_count,
    act_ref, rw_ref, rows_ref, gin_ref, gg_ref, gu_ref, place_ref, sact_ref, wd_ref, sd_ref,
    sum_ref, dg_ref, du_ref, dd_ref, *comm,
):
    rows = sum_ref.shape[0]
    step, steps = pl.program_id(0), 2 * n_groups
    w = Wires(n_groups, 8, None, None)
    stream = StreamSum(w, steps, *comm[:6], comm[6:10], comm[10])

    @pl.when(step == 0)
    def _():
        w.meet()
        for ref in (dg_ref, du_ref, dd_ref):
            ref[...] = jnp.zeros_like(ref)

    slot = lax.rem(step, 2)
    chips = step_chips(w, step)
    out_rows = jnp.dot(act_ref[...], wd_ref[...], preferred_element_type=F32) * rw_ref[...]
    out_rows = out_rows.astype(BF)
    stream.open_stage(step)
    for q in range(4):
        chip = chips[q // 2]
        place = place_ref[pl.ds(chip, 1), :]
        low = hot_rows(place, rows, q % 2, slot_count).astype(F32).astype(BF)
        slots = slice(q * slot_count, (q + 1) * slot_count)
        shared = sact_ref[pl.ds(pl.multiple_of((chip * 2 + q % 2) * rows, rows), rows), :]
        total = dot_tn(low, out_rows[slots]) + jnp.dot(
            shared, sd_ref[...], preferred_element_type=F32
        )
        stream.stage[slot, q] = total.astype(BF)
    stream.push(step)
    stream.advance(step)

    width = rows_ref.shape[1]
    piece = width // 4
    for left_ref, right_ref, total_ref in (
        (gg_ref, rows_ref, dg_ref),
        (gu_ref, rows_ref, du_ref),
        (act_ref, gin_ref, dd_ref),
    ):
        turned = left_ref[...].T
        for k in range(4):
            cols = slice(k * piece, (k + 1) * piece)
            total_ref[:, cols] += jnp.dot(
                turned, right_ref[:, cols], preferred_element_type=F32
            )

    @pl.when(step == steps - 1)
    def _():
        stream.finish(sum_ref)


def experts_sums(
    n_groups, rows, h2, cot, place, slot_count, expert_w, shared_w, router_weight, first_id
):
    w_gate, w_up, w_down = expert_w
    s_both, s_down = shared_w
    tokens, width = h2.shape
    hidden, hidden_s = w_down.shape[0], s_down.shape[0]
    experts = router_weight.shape[1]
    steps = 2 * n_groups
    devices = tokens // rows
    step_slots = slot_count * 4
    all_slots = step_slots * steps
    half = 128
    s_cat = jnp.concatenate(
        [
            s_both[:, :hidden_s],
            router_weight,
            jnp.zeros((width, half - hidden_s - experts), BF),
            s_both[:, hidden_s:],
            jnp.zeros((width, half - hidden_s), BF),
        ],
        axis=1,
    )
    s_tall = jnp.pad(s_down, ((0, half - hidden_s), (0, 0)))

    def whole(array):
        return pl.BlockSpec(array.shape, lambda i: (0, 0), pipeline_mode=pl.Buffered(1))

    def blocked(rows, cols):
        return pl.BlockSpec((rows, cols), lambda i: (i, 0))

    shape = jax.ShapeDtypeStruct
    flops = 2 * all_slots * width * hidden * 5 + 2 * tokens * width * (4 * half + 3 * slot_count)
    shapes = [
        shape((rows, width), F32),
        shape((all_slots, width), BF),
        shape((all_slots, width), BF),
        shape((all_slots, hidden), BF),
        shape((all_slots, hidden), BF),
        shape((all_slots, hidden), BF),
        shape((all_slots, 1), F32),
        shape((tokens, half), BF),
        shape((2 * half, width), F32),
        shape((half, width), F32),
        shape((devices, rows), F32),
    ]
    specs = [
        blocked(step_slots, s.shape[1]) if s.shape[0] == all_slots else whole(s) for s in shapes
    ]
    hbm = pl.BlockSpec(memory_space=pl.ANY)
    grad_h2, rows_in, grad_in, act, grad_gate, grad_up, row_weight, s_act, *d_shared, token_grad = (
        pl.pallas_call(
            functools.partial(moe_kernel, n_groups, experts, hidden_s, slot_count),
            grid=(steps,),
            in_specs=[
                hbm,
                hbm,
                whole(place),
                whole(w_gate),
                whole(w_up),
                whole(w_down),
                whole(s_cat),
                whole(s_tall),
            ],
            out_specs=specs,
            out_shape=shapes,
            scratch_shapes=[
                pltpu.VMEM((2, 4 * rows, width), BF),
                pltpu.VMEM((2, 4 * rows, width), BF),
                pltpu.SemaphoreType.DMA((2, 2, 2)),
            ]
            + StreamSum.scratch(n_groups, rows, width),
            cost_estimate=pl.CostEstimate(
                flops=flops, bytes_accessed=12 * tokens * width, transcendentals=tokens * 1024
            ),
            compiler_params=pltpu.CompilerParams(
                collective_id=first_id,
                has_side_effects=True,
                vmem_limit_bytes=67043328,
            ),
            name="experts",
        )(h2, cot, place, w_gate, w_up, w_down, s_cat, s_tall)
    )
    shapes = [grad_h2] + [shape(x.shape, F32) for x in expert_w]
    out, d_gate, d_up, d_down = pl.pallas_call(
        functools.partial(out_kernel, n_groups, slot_count),
        grid=(steps,),
        in_specs=[
            blocked(step_slots, hidden),
            blocked(step_slots, 1),
            blocked(step_slots, width),
            blocked(step_slots, width),
            blocked(step_slots, hidden),
            blocked(step_slots, hidden),
            whole(place),
            whole(s_act),
            whole(w_down),
            whole(s_tall),
        ],
        out_specs=[whole(x) for x in shapes],
        out_shape=[shape(x.shape, F32) for x in shapes],
        scratch_shapes=StreamSum.scratch(n_groups, rows, width),
        cost_estimate=pl.CostEstimate(
            flops=2 * width * (4 * all_slots * hidden + tokens * (half + slot_count)),
            bytes_accessed=4 * tokens * width,
            transcendentals=0,
        ),
        compiler_params=pltpu.CompilerParams(
            collective_id=first_id + 1,
            has_side_effects=True,
            vmem_limit_bytes=67043328,
        ),
        name="expert_out",
    )(act, row_weight, rows_in, grad_in, grad_gate, grad_up, place, s_act, w_down, s_tall)
    d_both, d_tall = d_shared
    d_both = jnp.concatenate([d_both[:hidden_s], d_both[half : half + hidden_s]], axis=0)
    grads = (d_gate, d_up, d_down, d_both.T, d_tall[:hidden_s])
    return out, grad_h2, token_grad, grads


def body(
    n_groups, n_plane, layer_input, attn_gain, w_query, w_latent, kv_gain, w_expand, w_output,
    ffn_gain, w_router, shared_gate, shared_up, shared_down, expert_gate, expert_up,
    expert_down, routes, segments, cotangent,
):
    tok, width = layer_input.shape
    devices = n_groups * n_plane
    experts = w_router.shape[1]
    local_heads = HEADS // n_plane
    scale = (NOPE + ROPE) ** (-0.5)
    group = lax.axis_index("g")
    place_in = lax.axis_index(PLANE)
    me = lax.axis_index(ALL)
    expert_id = lax.axis_index(("g", "p"))
    plane_tok = n_plane * tok
    plane_start = group * plane_tok

    rows_w = w_router.shape[0]
    kv_n = kv_gain.shape[0]
    small = jnp.concatenate(
        [
            attn_gain,
            ffn_gain,
            kv_gain,
            w_router.reshape(-1),
            routes.reshape(-1).astype(BF),
            segments.astype(BF),
        ]
    )
    small = jnp.pad(small, (0, -small.shape[0] % 4096)).reshape(-1, 128)
    kv_cols = local_heads * (NOPE + VDIM)
    fold = kv_n * kv_cols // rows_w
    by_head = w_query.reshape(rows_w, n_plane, local_heads, NOPE + ROPE).transpose(1, 0, 2, 3)
    folded = (
        w_expand.reshape(kv_n, n_plane, kv_cols // fold, fold)
        .transpose(1, 0, 2, 3)
        .reshape(n_plane, rows_w, fold)
    )
    swap = functools.partial(exchange, n_groups, n_plane)
    wq_nope, wq_rope, expand_weight, latent_weight, small, x_plane = swap(
        0,
        ("plane_swap_gather", by_head[..., :NOPE].reshape(n_plane, rows_w, local_heads * NOPE)),
        ("plane_swap_gather", by_head[..., NOPE:].reshape(n_plane, rows_w, local_heads * ROPE)),
        ("plane_swap_gather", folded),
        ("whole_gather", w_latent),
        ("whole_gather", small),
        ("plane_gather", layer_input),
    )
    x_plane = x_plane.reshape(plane_tok, width).astype(F32)
    latent_weight = latent_weight.reshape(width, RANK + ROPE)
    wq_nope = wq_nope.reshape(width, local_heads * NOPE)
    wq_rope = wq_rope.reshape(width, local_heads * ROPE)
    expand_weight = expand_weight.reshape(RANK, kv_cols)
    small = small.reshape(devices, -1)
    cuts = [rows_w, 2 * rows_w, 2 * rows_w + kv_n, 2 * rows_w + kv_n + rows_w * experts]
    cuts = cuts + [cuts[-1] + tok * TOP, cuts[-1] + tok * TOP + tok]
    gain_one = small[:, : cuts[0]].reshape(-1).astype(F32)
    gain_two = small[:, cuts[0] : cuts[1]].reshape(-1).astype(F32)
    gain_kv = small[:, cuts[1] : cuts[2]].reshape(-1).astype(F32)
    router_weight = small[:, cuts[2] : cuts[3]].reshape(width, experts)
    routes_all = small[:, cuts[3] : cuts[4]].astype(jnp.int32).reshape(devices, tok, TOP)
    segments_all = small[:, cuts[4] : cuts[5]].astype(jnp.int32).reshape(-1)

    cotangent_later = jnp.where(x_plane[0, 0] < 1e6, cotangent, jnp.zeros_like(cotangent))

    shared_n = shared_down.shape[0]
    s_both = jnp.concatenate(
        [
            shared_gate.reshape(rows_w, devices, shared_n),
            shared_up.reshape(rows_w, devices, shared_n),
        ],
        axis=2,
    )
    s_both = s_both.transpose(1, 0, 2).reshape(n_groups, n_plane, rows_w, 2 * shared_n)

    hidden = lax.optimization_barrier(rms_norm(x_plane, gain_one).astype(BF))
    rope_half = ROPE // 2
    positions = plane_start + jnp.arange(plane_tok, dtype=jnp.int32)
    frequency = 10000.0 ** (-jnp.arange(rope_half, dtype=F32) / rope_half)
    angles = positions.astype(F32)[:, None] * frequency[None, :]
    cosine = jnp.cos(angles)
    sine_part = jnp.sin(angles)
    cos_h = jnp.tile(cosine, (1, 2 * local_heads))
    sin_h = jnp.tile(jnp.concatenate([-sine_part, sine_part], axis=1), (1, local_heads))

    def turn(rows, direction):
        pieces = []
        for h in range(local_heads):
            at = h * ROPE
            pieces += [rows[:, at + rope_half : at + ROPE], rows[:, at : at + rope_half]]
        return rows * cos_h + jnp.concatenate(pieces, axis=1) * (direction * sin_h)

    latent = matmul(hidden, latent_weight)
    compressed_own = rms_norm(latent[:, :RANK], gain_kv).astype(BF)
    key_rope_own = rotate(latent[:, RANK:], cosine, sine_part).astype(BF)

    def own_rows(table):
        return lax.dynamic_slice_in_dim(table, place_in * tok, tok, 0)

    piece = own_rows(jnp.concatenate([compressed_own, key_rope_own], axis=1))
    before, own_output = swap(1, ("shift_gather", piece), ("head_rows", w_output))
    before = before.reshape(plane_tok, RANK + ROPE)
    own_output = own_output.reshape(local_heads * VDIM, width)
    compressed = jnp.concatenate([before[:, :RANK], compressed_own], axis=0)
    key_rope = jnp.concatenate([before[:, RANK:], key_rope_own], axis=0)
    q_nope = matmul(hidden, wq_nope).astype(BF)
    q_rope = turn(matmul(hidden, wq_rope), 1.0).astype(BF)
    expanded = matmul(compressed, expand_weight).astype(BF)
    plane_segments = lax.dynamic_slice_in_dim(segments_all, plane_start, plane_tok, 0)
    doc_start = jnp.sum(
        (segments_all[None, :] < plane_segments[:, None]).astype(jnp.int32), axis=1, keepdims=True
    )
    low_bound = doc_start - plane_start + DOC_MAX
    mixed_heads, lse = attend(low_bound, q_nope, q_rope, expanded, key_rope, scale)
    attn_out = matmul(mixed_heads, own_output).astype(BF)
    parts = max(1, devices * tok // 4096)
    attn_out, s_both = swap(
        2,
        ("plane_sum", attn_out.reshape(n_plane, tok, width)),
        ("whole_swap", s_both),
    )
    input_float = layer_input.astype(F32)
    residual_one = input_float + attn_out
    h_two_f, norm_two_back = jax.vjp(rms_norm, residual_one, gain_two)
    h_two = h_two_f.astype(BF)
    router_probs = softmax_rows(matmul(h_two, router_weight))

    expert_w = (expert_gate[0].T, expert_up[0].T, expert_down[0])
    if parts == 1:
        h2_all = swap(5, ("far_gather", h_two))[0]
    shared_w = (s_both.reshape(width, 2 * shared_n), shared_down)
    slot_limit = 2 * tok * TOP // experts

    def on_rows(h2, h2_all, cot_gathered, routes_here):
        rows = h2.shape[0]
        slot_count = min(slot_limit, rows)
        member = jnp.any(routes_here == expert_id, axis=2)
        before_it = jnp.arange(rows)[:, None] < jnp.arange(rows)[None, :]
        rank = matmul(member.astype(BF), before_it.astype(BF)).astype(jnp.int32)
        place = jnp.where(member, rank, -1).reshape(devices // 2, 2 * rows)
        out, grad_h2, token_grad, grads = experts_sums(
            n_groups,
            rows,
            h2_all,
            cot_gathered,
            place,
            slot_count,
            expert_w,
            shared_w,
            router_weight,
            8,
        )
        picked = lax.all_to_all(token_grad, ALL, split_axis=0, concat_axis=0, tiled=True)
        picked = jnp.sum(picked.reshape(experts, devices // experts, rows), axis=1).T
        return out, grad_h2, picked, grads

    if parts == 1:
        cot_all = gather_all(cotangent_later)
        out_own, grad_h2_own, grad_router_probs, grads = on_rows(
            h_two, h2_all.reshape(-1, width), cot_all, routes_all
        )
    else:
        rows = tok // parts

        def step(total, inputs):
            h2, cot, routes_here = inputs
            cot_part = gather_all(cot)
            out, grad_h2, picked, grads = on_rows(h2, gather_all(h2), cot_part, routes_here)
            grads = lax.optimization_barrier(grads)
            total = tuple(a + b for a, b in zip(total, grads))
            return total, (out, grad_h2, picked)

        shapes = expert_w + shared_w
        grads, (out_own, grad_h2_own, grad_router_probs) = lax.scan(
            step,
            tuple(jnp.zeros(s.shape, F32) for s in shapes),
            (
                h_two.reshape(parts, rows, width),
                cotangent.reshape(parts, rows, width),
                routes_all.reshape(devices, parts, rows, TOP).transpose(1, 0, 2, 3),
            ),
        )
        out_own = out_own.reshape(tok, width)
        grad_h2_own = grad_h2_own.reshape(tok, width)
        grad_router_probs = grad_router_probs.reshape(tok, experts)
    g_gate, g_up, g_down, g_both, g_sdown = grads
    grad_logits = router_probs * (
        grad_router_probs - jnp.sum(router_probs * grad_router_probs, axis=1, keepdims=True)
    )
    grad_logits = grad_logits.astype(BF)
    grad_router = dot_tn(h_two, grad_logits)
    grad_h_two = grad_h2_own + dot_nt(grad_logits, router_weight)
    output = residual_one + out_own

    grad_x_one, grad_gain_two = norm_two_back(grad_h_two)
    grad_x_one = grad_x_one + cotangent.astype(F32)
    grad_attn_out = grad_x_one.astype(BF)
    g_shared, plane_grad = swap(
        3,
        ("whole_swap", g_both.astype(BF).reshape(n_groups, n_plane, rows_w, 2 * shared_n)),
        ("plane_gather", grad_attn_out),
    )
    plane_grad = plane_grad.reshape(plane_tok, width)
    grad_mixed = dot_nt(plane_grad, own_output).astype(BF)
    dqn, dqr, dex, dkr = attend_back(
        low_bound, q_nope, q_rope, expanded, key_rope, lse, grad_mixed, scale
    )

    g_output = dot_tn(mixed_heads, plane_grad).astype(BF).reshape(n_groups, rows_w, width)

    grad_expanded = dex.astype(BF)
    grad_expand = dot_tn(compressed, grad_expanded)
    grad_comp = dot_nt(grad_expanded, expand_weight)
    key_grads = jnp.concatenate([grad_comp, dkr], axis=1).astype(BF)
    key_grads = (
        key_grads.reshape(2, n_plane, tok, RANK + ROPE)
        .transpose(1, 0, 2, 3)
        .reshape(n_plane, 2 * tok, RANK + ROPE)
    )

    gq_nope = dqn.astype(BF)
    gq_rope = turn(dqr, -1.0).astype(BF)
    grad_hidden = (dot_nt(gq_nope, wq_nope) + dot_nt(gq_rope, wq_rope)).astype(BF)
    gw_nope = dot_tn(hidden, gq_nope).astype(BF).reshape(n_groups, n_plane, rows_w, -1)
    gw_rope = dot_tn(hidden, gq_rope).astype(BF).reshape(n_groups, n_plane, rows_w, -1)
    g_expand = grad_expand.astype(BF).reshape(n_groups, n_plane, kv_n, kv_cols)
    key_grad, grad_hidden, gw_nope, gw_rope, g_expand = swap(
        4,
        ("plane_sum_shift", key_grads),
        ("plane_sum", grad_hidden.reshape(n_plane, tok, width)),
        ("group_sum_swap", gw_nope),
        ("group_sum_swap", gw_rope),
        ("group_sum_swap", g_expand),
    )
    latent_own = own_rows(latent)
    kv_norm_back = jax.vjp(rms_norm, latent_own[:, :RANK], gain_kv)[1]
    grad_comp_in, grad_gain_kv = kv_norm_back(key_grad[:, :RANK])
    grad_rope_in = unrotate(key_grad[:, RANK:], own_rows(cosine), own_rows(sine_part))
    grad_latent = jnp.concatenate([grad_comp_in, grad_rope_in], axis=1).astype(BF)

    def per_head(table, cols):
        return table.transpose(1, 0, 2).reshape(rows_w, HEADS, cols)

    grad_query_weight = jnp.concatenate(
        [per_head(gw_nope, NOPE), per_head(gw_rope, ROPE)], axis=2
    ).reshape(rows_w, -1).astype(F32)
    grad_expand_weight = g_expand.transpose(1, 0, 2).reshape(kv_n, -1).astype(F32)

    g_latent = dot_tn(own_rows(hidden), grad_latent).astype(BF)
    g_latent = g_latent.reshape(n_groups, n_plane, rows_w, RANK + ROPE)
    grad_hidden = grad_hidden + dot_nt(grad_latent, latent_weight)
    norm_one_back = jax.vjp(rms_norm, input_float, gain_one)[1]
    grad_x_norm, grad_gain_one = norm_one_back(grad_hidden)
    grad_input = grad_x_one + grad_x_norm

    small_grads = jnp.concatenate(
        [
            p.reshape(devices, -1)
            for p in (grad_gain_one, grad_gain_two, grad_gain_kv, grad_router)
        ],
        axis=1,
    )
    small_grads = jnp.pad(small_grads, ((0, 0), (0, -small_grads.shape[1] % 1024)))
    grad_latent_weight, grad_output_weight, small_grads = swap(
        6,
        ("whole_sum", g_latent),
        ("group_sum_home", g_output),
        ("whole_sum", small_grads.reshape(n_groups, n_plane, -1, 128)),
    )
    small_grads = small_grads.reshape(-1)
    g_shared = g_shared.transpose(2, 0, 1, 3).reshape(rows_w, devices, 2 * shared_n).astype(F32)
    grad_shared_gate = g_shared[:, :, :shared_n].reshape(rows_w, devices * shared_n)
    grad_shared_up = g_shared[:, :, shared_n:].reshape(rows_w, devices * shared_n)
    return (
        output,
        grad_input,
        small_grads[: cuts[0]],
        grad_query_weight,
        grad_latent_weight,
        small_grads[cuts[1] : cuts[2]],
        grad_expand_weight,
        grad_output_weight,
        small_grads[cuts[0] : cuts[1]],
        small_grads[cuts[2] : cuts[3]].reshape(rows_w, experts),
        grad_shared_gate,
        grad_shared_up,
        g_sdown,
        g_gate.T[None],
        g_up.T[None],
        g_down[None],
    )


def solution(mesh):
    n_expert, n_shard = mesh.shape["expert"], mesh.shape["wshard"]
    devices = n_expert * n_shard

    def program(*args):
        tok = args[0].shape[0] // devices
        n_plane = DOC_MAX // tok
        n_groups = devices // n_plane
        inner = Mesh(mesh.devices.reshape(n_groups, n_plane // n_shard, n_shard), ALL)
        rows, vector = P(ALL, None), P(ALL)
        wide, tall = P(("g", "p"), None, "c"), P(("g", "p"), "c", None)
        step = jax.shard_map(
            functools.partial(body, n_groups, n_plane),
            mesh=inner,
            in_specs=(
                rows, vector, rows, rows, vector, rows, rows, vector, rows, rows, rows, rows,
                wide, wide, tall, rows, vector, rows,
            ),
            out_specs=(
                rows, rows, vector, rows, rows, vector, rows, rows, vector, rows, rows, rows,
                rows, wide, wide, tall,
            ),
            check_vma=False,
        )
        return step(*args)

    return program
```

```python
import functools

import jax
import jax.numpy as jnp
from jax import lax
from jax.experimental import pallas as pl
from jax.experimental.pallas import tpu as pltpu
from jax.sharding import Mesh, PartitionSpec as P

HEADS = 16
NOPE = 128
ROPE = 64
VDIM = 128
RANK = 512
TOP = 6
DOC_MAX = 1024
QUERY_BLOCK = 256

BF = jnp.bfloat16
F32 = jnp.float32
ALL = ("g", "p", "c")
PLANE = ("p", "c")

epsilon = 1e-06


def rms_norm(vector, scaling):
    return vector * lax.rsqrt(jnp.mean(vector * vector, axis=-1, keepdims=True) + epsilon) * scaling


def rotate(vector, cosine, sine_part):
    half_width = vector.shape[-1] // 2
    front_half = vector[..., :half_width]
    back_half = vector[..., half_width:]
    return jnp.concatenate(
        [front_half * cosine - back_half * sine_part, back_half * cosine + front_half * sine_part],
        axis=-1,
    )


def unrotate(vector, cosine, sine_part):
    return rotate(vector, cosine, -sine_part)


def matmul(left, right):
    return jnp.dot(left, right, preferred_element_type=F32)


def dot_nt(left, right):
    return lax.dot_general(left, right, (((1,), (1,)), ((), ())), preferred_element_type=F32)


def dot_tn(left, right):
    return lax.dot_general(left, right, (((0,), (0,)), ((), ())), preferred_element_type=F32)


def swiglu(gate_pre, up_pre):
    return jax.nn.silu(gate_pre) * up_pre


def softmax_rows(scores):
    row_top = jnp.max(scores, axis=-1, keepdims=True)
    exp_scores = jnp.exp(scores - row_top)
    return exp_scores / jnp.sum(exp_scores, axis=-1, keepdims=True)


def masked_scores(base, low_bound, q_nope, q_rope, k_nope, k_rope, scale):
    rows, span = q_nope.shape[0], k_nope.shape[0]
    key_at = lax.broadcasted_iota(jnp.int32, (rows, span), 1) + base
    query_at = lax.broadcasted_iota(jnp.int32, (rows, span), 0) + (base + DOC_MAX)
    allowed = (key_at >= low_bound) & (key_at <= query_at)
    scores = (dot_nt(q_nope, k_nope) + dot_nt(q_rope, k_rope)) * scale
    return jnp.where(allowed, scores, -1e30)


def attend_kernel(heads, scale, low_ref, qn_ref, qr_ref, ex_ref, kr_ref, out_ref, lse_ref):
    rows = qn_ref.shape[0]
    base = pl.multiple_of(pl.program_id(0) * rows, rows)
    window = pl.ds(base, rows + DOC_MAX)
    k_rope = kr_ref[window, :]
    low_bound = low_ref[...]
    for h in range(heads):
        at = h * (NOPE + VDIM)
        k_nope = ex_ref[window, at : at + NOPE]
        value = ex_ref[window, at + NOPE : at + NOPE + VDIM]
        scores = masked_scores(
            base,
            low_bound,
            qn_ref[:, h * NOPE : (h + 1) * NOPE],
            qr_ref[:, h * ROPE : (h + 1) * ROPE],
            k_nope,
            k_rope,
            scale,
        )
        top = jnp.max(scores, axis=-1, keepdims=True)
        exps = jnp.exp(scores - top)
        total = jnp.sum(exps, axis=-1, keepdims=True)
        probs = (exps / total).astype(BF)
        out_ref[:, h * VDIM : (h + 1) * VDIM] = jnp.dot(
            probs, value, preferred_element_type=F32
        ).astype(BF)
        lse_ref[:, h : h + 1] = top + jnp.log(total)


def attend(low_bound, q_nope, q_rope, expanded, key_rope, scale):
    queries = q_nope.shape[0]
    heads = q_nope.shape[1] // NOPE
    rows = QUERY_BLOCK

    def whole(array):
        return pl.BlockSpec(array.shape, lambda i: (0, 0))

    def blocked(width):
        return pl.BlockSpec((rows, width), lambda i: (i, 0))

    flops = 2 * heads * queries * (rows + DOC_MAX) * (NOPE + ROPE + VDIM)
    return pl.pallas_call(
        functools.partial(attend_kernel, heads, scale),
        grid=(queries // rows,),
        in_specs=[
            blocked(1),
            blocked(heads * NOPE),
            blocked(heads * ROPE),
            whole(expanded),
            whole(key_rope),
        ],
        out_specs=[blocked(heads * VDIM), blocked(heads)],
        out_shape=[
            jax.ShapeDtypeStruct((queries, heads * VDIM), BF),
            jax.ShapeDtypeStruct((queries, heads), F32),
        ],
        cost_estimate=pl.CostEstimate(
            flops=flops, bytes_accessed=4 * expanded.size, transcendentals=flops // 640
        ),
        compiler_params=pltpu.CompilerParams(vmem_limit_bytes=50 * 1024 * 1024),
        name="attend",
    )(low_bound, q_nope, q_rope, expanded, key_rope)


def attend_back_kernel(
    heads, scale, low_ref, qn_ref, qr_ref, ex_ref, kr_ref, lse_ref, gm_ref,
    dqn_ref, dqr_ref, dex_ref, dkr_ref,
):
    rows = qn_ref.shape[0]
    step = pl.program_id(0)
    base = pl.multiple_of(step * rows, rows)
    window = pl.ds(base, rows + DOC_MAX)

    @pl.when(step == 0)
    def _():
        dex_ref[...] = jnp.zeros_like(dex_ref)
        dkr_ref[...] = jnp.zeros_like(dkr_ref)

    k_rope = kr_ref[window, :]
    low_bound = low_ref[...]
    for h in range(heads):
        at = h * (NOPE + VDIM)
        k_nope = ex_ref[window, at : at + NOPE]
        value = ex_ref[window, at + NOPE : at + NOPE + VDIM]
        q_nope = qn_ref[:, h * NOPE : (h + 1) * NOPE]
        q_rope = qr_ref[:, h * ROPE : (h + 1) * ROPE]
        grad_out = gm_ref[:, h * VDIM : (h + 1) * VDIM]
        scores = masked_scores(base, low_bound, q_nope, q_rope, k_nope, k_rope, scale)
        probs = jnp.exp(scores - lse_ref[:, h : h + 1])
        grad_probs = dot_nt(grad_out, value)
        mean_grad = jnp.sum(probs * grad_probs, axis=-1, keepdims=True)
        grad_scores = (probs * (grad_probs - mean_grad) * scale).astype(BF)
        probs_low = probs.astype(BF)
        dqn_ref[:, h * NOPE : (h + 1) * NOPE] = jnp.dot(
            grad_scores, k_nope, preferred_element_type=F32
        )
        dqr_ref[:, h * ROPE : (h + 1) * ROPE] = jnp.dot(
            grad_scores, k_rope, preferred_element_type=F32
        )
        dex_ref[window, at : at + NOPE] += dot_tn(grad_scores, q_nope)
        dex_ref[window, at + NOPE : at + NOPE + VDIM] += dot_tn(probs_low, grad_out)
        dkr_ref[window, :] += dot_tn(grad_scores, q_rope)


def attend_back(low_bound, q_nope, q_rope, expanded, key_rope, lse, grad_mixed, scale):
    queries = q_nope.shape[0]
    heads = q_nope.shape[1] // NOPE
    rows = QUERY_BLOCK

    def whole(shape):
        return pl.BlockSpec(shape, lambda i: (0, 0))

    def blocked(width):
        return pl.BlockSpec((rows, width), lambda i: (i, 0))

    flops = 2 * heads * queries * (rows + DOC_MAX) * (3 * NOPE + 3 * ROPE + 2 * VDIM)
    return pl.pallas_call(
        functools.partial(attend_back_kernel, heads, scale),
        grid=(queries // rows,),
        in_specs=[
            blocked(1),
            blocked(heads * NOPE),
            blocked(heads * ROPE),
            whole(expanded.shape),
            whole(key_rope.shape),
            blocked(heads),
            blocked(heads * VDIM),
        ],
        out_specs=[
            blocked(heads * NOPE),
            blocked(heads * ROPE),
            whole(expanded.shape),
            whole(key_rope.shape),
        ],
        out_shape=[
            jax.ShapeDtypeStruct(q_nope.shape, F32),
            jax.ShapeDtypeStruct(q_rope.shape, F32),
            jax.ShapeDtypeStruct(expanded.shape, F32),
            jax.ShapeDtypeStruct(key_rope.shape, F32),
        ],
        cost_estimate=pl.CostEstimate(
            flops=flops, bytes_accessed=8 * expanded.size, transcendentals=flops // 1664
        ),
        compiler_params=pltpu.CompilerParams(vmem_limit_bytes=56 * 1024 * 1024),
        name="attend_back",
    )(low_bound, q_nope, q_rope, expanded, key_rope, lse, grad_mixed)


MESH = pl.DeviceIdType.MESH


def pause(rounds):
    for _ in range(rounds):
        yield


class Wires:
    def __init__(self, n_groups, n_plane, send, recv):
        self.n_groups, self.n_plane, self.send, self.recv = n_groups, n_plane, send, recv
        self.cores = 2
        self.g, self.p, self.c = lax.axis_index("g"), lax.axis_index("p"), lax.axis_index("c")
        self.j = self.p * self.cores + self.c
        self.used = 0

    def at_plane(self, j):
        return {"g": self.g, "p": j // self.cores, "c": j % self.cores}

    def at_chip(self, p):
        return {"g": self.g, "p": p, "c": self.c}

    def at_group(self, g):
        return {"g": g, "p": self.p, "c": self.c}

    def partner(self):
        return {"g": self.g, "p": self.p, "c": 1 - self.c}

    def beside(self):
        return self.p + 1 - 2 * lax.rem(self.p, 2)

    def above(self):
        return self.p + 2 - 4 * (self.p // 2)

    def core_of(self, p):
        return p * self.cores + self.c

    def plane_peer(self, d):
        return lax.rem(self.j + d, self.n_plane)

    def group_peer(self, d):
        return lax.rem(self.g + d, self.n_groups)

    def start(self, src, dst, device):
        copy = pltpu.make_async_remote_copy(
            src_ref=src,
            dst_ref=dst,
            send_sem=self.send.at[self.used],
            recv_sem=self.recv.at[self.used],
            device_id=device,
            device_id_type=MESH,
        )
        self.used += 1
        copy.start()
        return copy

    def at_device(self, index):
        return {"g": index // self.n_plane, **self.on_plane(lax.rem(index, self.n_plane))}

    def on_plane(self, j):
        return {"p": j // self.cores, "c": j % self.cores}

    def meet(self, heads=False, home=False):
        barrier = pltpu.get_barrier_semaphore()
        waits = self.n_plane - 1 + self.n_groups - 1
        if heads:
            mine = self.head_owner() == self.j
            part = lax.rem(self.g * self.n_plane + self.j, self.n_groups)
            for r in range(self.n_groups):

                @pl.when(jnp.logical_not(mine) | (part != r))
                def _():
                    source = self.at_device(self.n_groups * self.j + r)
                    pl.semaphore_signal(barrier, inc=1, device_id=source, device_id_type=MESH)

            waits = waits + jnp.where(mine, self.n_groups - 1, self.n_groups)
        if home:
            source = self.home_source()
            stays = source == self.g * self.n_plane + self.j

            @pl.when(jnp.logical_not(stays))
            def _():
                pl.semaphore_signal(
                    barrier, inc=1, device_id=self.at_device(source), device_id_type=MESH
                )

            waits = waits + jnp.where(stays, 0, 1)
        for d in range(1, self.n_plane):
            pl.semaphore_signal(
                barrier, inc=1, device_id=self.at_plane(self.plane_peer(d)), device_id_type=MESH
            )
        for d in range(1, self.n_groups):
            pl.semaphore_signal(
                barrier, inc=1, device_id=self.at_group(self.group_peer(d)), device_id_type=MESH
            )
        pl.semaphore_wait(barrier, waits)

    def home_source(self):
        index = self.g * self.n_plane + self.j
        return lax.rem(index, self.n_groups) * self.n_plane + index // self.n_groups

    def head_owner(self):
        return (self.g * self.n_plane + self.j) // self.n_groups


def sum_rows(dst, sources):
    rows = dst.shape[0]
    tile = 32 if rows % 32 == 0 else rows

    def step(i, carry):
        at = pl.ds(pl.multiple_of(i * tile, tile), tile)
        if len(sources) == 2 and all(r.dtype == BF for r in [dst] + sources):
            dst[at, :] = sources[0][at, :] + sources[1][at, :]
        else:
            total = sources[0][at, :].astype(F32)
            for source in sources[1:]:
                total = total + source[at, :].astype(F32)
            dst[at, :] = total.astype(dst.dtype)
        return carry

    lax.fori_loop(0, rows // tile, step, 0)


def wait_all(copies):
    for copy in copies:
        copy.wait()


def wait_received(copies):
    for copy in copies:
        copy.wait_recv()


def wait_sent(copies):
    for copy in copies:
        copy.wait_send()


def part_of(ref, upper):
    rows = ref.shape[0] // 2
    return ref.at[pl.ds(rows, rows)] if upper else ref.at[pl.ds(0, rows)]


def spread(w, own, at):
    beside, above = w.at_chip(w.beside()), w.at_chip(w.above())
    mine = at(w.j)
    halves = [(part_of(own, u), part_of(mine, u)) for u in (0, 1)]
    lower = w.start(*halves[0], beside)
    upper = w.start(*halves[1], above)
    rest = [w.start(*halves[1], beside), w.start(*halves[0], above)]
    on_chip = [w.start(own, mine, w.partner())]
    yield
    lower.wait_recv()
    block = part_of(at(w.core_of(w.beside())), 0)
    rest.append(w.start(block, block, above))
    upper.wait_recv()
    block = part_of(at(w.core_of(w.above())), 1)
    rest.append(w.start(block, block, beside))
    yield
    wait_received(rest)
    for p in (w.beside(), w.above(), 3 - w.p):
        block = at(w.core_of(p))
        on_chip.append(w.start(block, block, w.partner()))
    yield
    wait_sent([lower, upper] + rest)
    wait_all(on_chip)


def plane_gather(w, src, out):
    out[w.j] = src[...]
    yield from spread(w, src, lambda j: out.at[j])


def far_gather(w, src, out, sem):
    mine = out.at[w.g, w.j]
    away = [w.start(src, mine, w.at_group(w.group_peer(d))) for d in range(1, w.n_groups)]
    local = pltpu.make_async_copy(src, mine, sem)
    local.start()
    running = [spread(w, src, lambda j: out.at[w.g, j])]
    next(running[0])
    for d in range(1, w.n_groups):
        away[d - 1].wait_recv()
        g = w.group_peer(w.n_groups - d)
        running.append(spread(w, out.at[g, w.j], lambda j, g=g: out.at[g, j]))
        next(running[d])
    for _ in range(3):
        for routine in running:
            next(routine, None)
        yield
    local.wait()
    wait_sent(away)


def shift_gather(w, src, mid, out):
    copy = w.start(src, mid, w.at_group(lax.rem(w.g + 1, w.n_groups)))
    yield
    copy.wait()
    yield from plane_gather(w, mid, out)


def whole_gather(w, src, out):
    chips = w.n_plane // w.cores
    first = [
        w.start(src, out.at[w.g, w.j], w.at_group(w.group_peer(d))) for d in range(1, w.n_groups)
    ]
    out[w.g, w.j] = src[...]
    yield
    wait_received(first)
    mine = out.at[:, w.j]
    second = [w.start(mine, mine, w.at_chip(lax.rem(w.p + d, chips))) for d in range(1, chips)]
    third = [w.start(mine, mine, w.partner())]
    yield
    for d in range(1, chips):
        second[d - 1].wait_recv()
        block = out.at[:, w.core_of(lax.rem(w.p + chips - d, chips))]
        third.append(w.start(block, block, w.partner()))
    yield
    wait_sent(first)
    wait_sent(second)
    wait_all(third)


def plane_swap_gather(w, src, out):
    first = []
    for d in range(1, w.n_plane):
        to = w.plane_peer(d)
        first.append(w.start(src.at[to], out.at[w.g, w.j], w.at_plane(to)))
    out[w.g, w.j] = src[w.j]
    yield
    wait_received(first)
    second = [
        w.start(out.at[w.g], out.at[w.g], w.at_group(w.group_peer(d)))
        for d in range(1, w.n_groups)
    ]
    yield from pause(4)
    wait_sent(first)
    wait_all(second)


def head_rows(w, src, out):
    index = w.g * w.n_plane + w.j
    owner, part = w.head_owner(), lax.rem(index, w.n_groups)
    mine = owner == w.j

    def to(d):
        return pltpu.make_async_remote_copy(
            src_ref=src,
            dst_ref=out.at[part],
            send_sem=w.send.at[base + d],
            recv_sem=w.recv.at[base + part],
            device_id={"g": w.group_peer(d), **w.on_plane(owner)},
            device_id_type=MESH,
        )

    def arrival(r):
        return pltpu.make_async_remote_copy(
            src_ref=src,
            dst_ref=out.at[r],
            send_sem=w.send.at[base],
            recv_sem=w.recv.at[base + r],
            device_id=w.at_device(w.n_groups * w.j + r),
            device_id_type=MESH,
        )

    yield from pause(3)
    base = w.used
    w.used += w.n_groups
    for d in range(w.n_groups):

        @pl.when((d > 0) | jnp.logical_not(mine))
        def _():
            to(d).start()

    @pl.when(mine)
    def _():
        out[part] = src[...]

    yield from pause(2)
    for r in range(w.n_groups):

        @pl.when(jnp.logical_not(mine) | (part != r))
        def _():
            arrival(r).wait_recv()

    for d in range(w.n_groups):

        @pl.when((d > 0) | jnp.logical_not(mine))
        def _():
            to(d).wait_send()


def plane_swap(w, src, out):
    copies = []
    for d in range(1, w.n_plane):
        to = w.plane_peer(d)
        copies.append(w.start(src.at[to], out.at[w.j], w.at_plane(to)))
    out[w.j] = src[w.j]
    yield
    wait_all(copies)


def plane_sum(w, src, out, from_core, pairs, from_chips):
    to = (w.beside(), 3 - w.p, w.above(), w.p)
    beside, above = w.at_chip(w.beside()), w.at_chip(w.above())
    first = [
        w.start(src.at[p * w.cores + 1 - w.c], from_core.at[i], w.partner())
        for i, p in enumerate(to)
    ]
    yield
    sent = []

    def send(i, upper, slot, device):
        sent.append(w.start(part_of(pairs.at[i], upper), from_chips.at[slot], device))

    for i, p in enumerate(to):
        first[i].wait_recv()
        sum_rows(pairs.at[i], [src.at[w.core_of(p)], from_core.at[i]])
        if i < 2:
            send(i, 0, i, beside)
        if i == 1:
            send(1, 1, 2, above)
        if i == 2:
            send(2, 1, 3, above)
    yield
    for wire, i, upper, slot, device in ((1, 2, 0, 4, above), (2, 0, 1, 5, beside)):
        sent[wire].wait_recv()
        target = part_of(pairs.at[i], upper)
        sum_rows(target, [target, from_chips.at[wire]])
        send(i, upper, slot, device)
    yield
    for wire in (0, 3, 4, 5):
        sent[wire].wait_recv()
    for upper, arrived in ((0, (0, 4)), (1, (3, 5))):
        sum_rows(
            part_of(out, upper),
            [part_of(pairs.at[3], upper)] + [from_chips.at[slot] for slot in arrived],
        )
    wait_sent(first)
    wait_sent(sent)


def whole_sum(w, src, out, from_core, pairs, from_chips, total, parts):
    chips = w.n_plane // w.cores
    to = [lax.rem(w.p + d, chips) for d in range(chips)]
    first = [
        w.start(src.at[:, p * w.cores + 1 - w.c], from_core.at[d], w.partner())
        for d, p in enumerate(to)
    ]
    yield
    second = []
    for d in list(range(1, chips)) + [0]:
        first[d].wait_recv()

        def step(i, carry):
            sum_rows(pairs.at[d, i], [src.at[i, w.core_of(to[d])], from_core.at[d, i]])
            return carry

        lax.fori_loop(0, w.n_groups, step, 0)
        if d:
            second.append(w.start(pairs.at[d], from_chips.at[d - 1], w.at_chip(to[d])))
    yield
    wait_received(second)

    def step(i, carry):
        sum_rows(total.at[i], [pairs.at[0, i]] + [from_chips.at[d, i] for d in range(chips - 1)])
        return carry

    lax.fori_loop(0, w.n_groups, step, 0)
    wait_sent(first)
    wait_sent(second)
    yield from group_sum(w, total, out, parts)


def whole_swap(w, src, out, mid):
    first = []
    for d in range(1, w.n_groups):
        to = w.group_peer(d)
        first.append(w.start(src.at[to], mid.at[w.g], w.at_group(to)))
    mid[w.g] = src[w.g]
    yield from pause(3)
    wait_received(first)
    second = []
    for d in range(1, w.n_plane):
        to = w.plane_peer(d)
        second.append(w.start(mid.at[:, to], out.at[:, w.j], w.at_plane(to)))
    out[:, w.j] = mid[:, w.j]
    yield
    wait_sent(first)
    wait_all(second)


def group_sum_home(w, src, out, parts, low, home):
    copies = []
    for d in range(1, w.n_groups):
        to = w.group_peer(d)
        copies.append(w.start(src.at[to], parts.at[d - 1], w.at_group(to)))
    yield from pause(3)
    wait_received(copies)
    sum_rows(low, [src.at[w.g]] + [parts.at[d] for d in range(w.n_groups - 1)])
    stays = w.home_source() == w.g * w.n_plane + w.j
    copy = pltpu.make_async_remote_copy(
        src_ref=low,
        dst_ref=home,
        send_sem=w.send.at[w.used],
        recv_sem=w.recv.at[w.used],
        device_id=w.at_device(w.n_groups * w.j + w.g),
        device_id_type=MESH,
    )
    w.used += 1

    @pl.when(jnp.logical_not(stays))
    def _():
        copy.start()

    @pl.when(stays)
    def _():
        home[...] = low[...]

    yield

    @pl.when(jnp.logical_not(stays))
    def _():
        copy.wait()

    out[...] = home[...].astype(F32)
    wait_sent(copies)


def plane_sum_shift(w, src, out, from_core, pairs, from_chips, low, later):
    rows = out.shape[0]
    yield from plane_sum(w, src, low, from_core, pairs, from_chips)
    copy = w.start(
        low.at[pl.ds(0, rows)], later, w.at_group(lax.rem(w.g + w.n_groups - 1, w.n_groups))
    )
    yield
    copy.wait()
    keep = jnp.where(w.g == w.n_groups - 1, 0.0, 1.0)
    out[...] = low[rows:, :].astype(F32) + later[...].astype(F32) * keep


def group_sum(w, src, out, parts):
    copies = []
    for d in range(1, w.n_groups):
        to = w.group_peer(d)
        copies.append(w.start(src.at[to], parts.at[d - 1], w.at_group(to)))
    yield
    wait_received(copies)
    sum_rows(out, [src.at[w.g]] + [parts.at[d] for d in range(w.n_groups - 1)])
    wait_sent(copies)


def group_sum_swap(w, src, out, total, parts):
    copies = []
    for d in range(1, w.n_groups):
        to = w.group_peer(d)
        copies.append(w.start(src.at[to], parts.at[d - 1], w.at_group(to)))
    yield from pause(4)
    wait_received(copies)

    def step(i, carry):
        sum_rows(total.at[i], [src.at[w.g, i]] + [parts.at[d, i] for d in range(w.n_groups - 1)])
        return carry

    lax.fori_loop(0, w.n_plane, step, 0)
    second = []
    for d in range(1, w.n_plane):
        to = w.plane_peer(d)
        second.append(w.start(total.at[to], out.at[w.j], w.at_plane(to)))
    out[w.j] = total[w.j]
    yield
    wait_sent(copies)
    wait_all(second)


ROUTINES = {
    "plane_gather": plane_gather,
    "shift_gather": shift_gather,
    "whole_gather": whole_gather,
    "far_gather": far_gather,
    "plane_swap_gather": plane_swap_gather,
    "plane_swap": plane_swap,
    "plane_sum": plane_sum,
    "plane_sum_shift": plane_sum_shift,
    "head_rows": head_rows,
    "group_sum": group_sum,
    "whole_sum": whole_sum,
    "whole_swap": whole_swap,
    "group_sum_home": group_sum_home,
    "group_sum_swap": group_sum_swap,
}


def exchange_kernel(n_groups, n_plane, kinds, extra, *refs):
    count = len(kinds)
    sources, outs = refs[:count], refs[count : 2 * count]
    scratch = list(refs[2 * count : -2])
    w = Wires(n_groups, n_plane, refs[-2], refs[-1])
    w.meet("head_rows" in kinds, "group_sum_home" in kinds)
    running = []
    for kind, source, out, number in zip(kinds, sources, outs, extra):
        mine, scratch = scratch[:number], scratch[number:]
        if kind == "shift_gather":
            running.append(shift_gather(w, source, mine[0], out))
        else:
            running.append(ROUTINES[kind](w, source, out, *mine))
    while running:
        still = []
        for routine in running:
            try:
                next(routine)
                still.append(routine)
            except StopIteration:
                pass
        running = still


def exchange(n_groups, n_plane, number, *items):
    kinds = [kind for kind, _ in items]
    arrays = [array for _, array in items]
    shapes, scratch, extra = [], [], []
    chips = n_plane // 2
    for kind, array in items:
        shape, dtype = array.shape, array.dtype
        own = []
        if kind in ("plane_gather", "shift_gather"):
            out = (n_plane,) + shape
            if kind == "shift_gather":
                own = [shape]
        elif kind in ("whole_gather", "far_gather"):
            out = (n_groups, n_plane) + shape
        elif kind == "plane_swap_gather":
            out = (n_groups,) + shape
        elif kind == "plane_swap":
            out = shape
        elif kind == "head_rows":
            out = (n_groups,) + shape
        elif kind == "plane_sum_shift":
            pair = shape[1:]
            out = (shape[1] // 2, shape[2])
            half = (pair[0] // 2, pair[1])
            own = [(chips,) + pair, (chips,) + pair, (6,) + half, pair, out]
        elif kind == "plane_sum":
            out = shape[1:]
            own = [(chips,) + out, (chips,) + out, (6, out[0] // 2, out[1])]
        elif kind == "group_sum_home":
            out = shape[1:]
            own = [(n_groups - 1,) + out, out, out]
        elif kind == "group_sum":
            out = shape[1:]
            own = [(n_groups - 1,) + out]
        elif kind == "whole_swap":
            out = shape
            own = [shape]
        elif kind == "whole_sum":
            out = shape[2:]
            full = (n_groups,) + out
            own = [(chips,) + full, (chips,) + full, (chips - 1,) + full, full]
            own = own + [(n_groups - 1,) + out]
        elif kind == "group_sum_swap":
            out = shape[1:]
            own = [out, (n_groups - 1,) + out]
        if kind in ("plane_sum", "plane_sum_shift", "group_sum", "group_sum_home", "whole_sum"):
            shapes.append(jax.ShapeDtypeStruct(out, F32))
        else:
            shapes.append(jax.ShapeDtypeStruct(out, dtype))
        scratch += [pltpu.VMEM(s, dtype) for s in own]
        if kind == "far_gather":
            own = [None]
            scratch.append(pltpu.SemaphoreType.DMA)
        extra.append(len(own))
    copies = 64 + 32 * len(items)
    vmem = pl.BlockSpec(memory_space=pltpu.VMEM)
    return pl.pallas_call(
        functools.partial(exchange_kernel, n_groups, n_plane, kinds, extra),
        out_shape=shapes,
        in_specs=[vmem] * len(items),
        out_specs=[
            pl.BlockSpec(memory_space=pl.ANY) if kind == "far_gather" else vmem for kind in kinds
        ],
        scratch_shapes=scratch
        + [pltpu.SemaphoreType.DMA((copies,)), pltpu.SemaphoreType.DMA((copies,))],
        compiler_params=pltpu.CompilerParams(
            collective_id=number,
            has_side_effects=True,
            vmem_limit_bytes=60 * 1024 * 1024,
        ),
        name="exchange_%d" % number,
    )(*arrays)


def gather_all(x):
    return lax.all_gather(x, ALL, axis=0, tiled=True)


class StreamSum:
    def __init__(self, w, steps, stage, from_core, pairs, from_chips, totals, parts, sems, credit):
        self.w, self.steps = w, steps
        self.stage, self.from_core, self.pairs = stage, from_core, pairs
        self.from_chips, self.totals, self.parts = from_chips, totals, parts
        self.core_sems, self.chip_sems, self.chip_recv, self.group_sems = sems
        self.credit = credit

    @staticmethod
    def chips(w, step):
        half = lax.rem(step, 2)
        beside = w.p + 1 - 2 * lax.rem(w.p, 2)
        above = w.p + 2 - 4 * (w.p // 2)
        return beside + half * (above - beside), 3 - w.p + half * (2 * w.p - 3)

    def core_copy(self, step, i):
        slot = lax.rem(step, 2)
        return pltpu.make_async_remote_copy(
            src_ref=self.stage.at[slot, 2 * i + 1 - self.w.c],
            dst_ref=self.from_core.at[slot, i],
            send_sem=self.core_sems.at[0, slot, i],
            recv_sem=self.core_sems.at[1, slot, i],
            device_id=self.w.partner(),
            device_id_type=MESH,
        )

    def part(self, ref, upper):
        rows = ref.shape[0] // 2
        return ref.at[pl.ds(rows, rows)] if upper else ref.at[pl.ds(0, rows)]

    def chip_copy(self, group_at, which):
        slot, i, upper, up = (
            (0, 0, False, False),
            (0, 1, False, False),
            (0, 1, True, True),
            (1, 0, True, True),
            (1, 0, False, True),
            (0, 0, True, False),
        )[which]
        p = self.w.p
        to = p + 2 - 4 * (p // 2) if up else p + 1 - 2 * lax.rem(p, 2)
        return pltpu.make_async_remote_copy(
            src_ref=self.part(self.pairs.at[slot, i], upper),
            dst_ref=self.from_chips.at[group_at, which],
            send_sem=self.chip_sems.at[which],
            recv_sem=self.chip_recv.at[group_at, which],
            device_id=self.w.at_chip(to),
            device_id_type=MESH,
        )

    def group_copy(self, group_at):
        return pltpu.make_async_remote_copy(
            src_ref=self.totals.at[group_at],
            dst_ref=self.parts.at[group_at],
            send_sem=self.group_sems.at[0, group_at],
            recv_sem=self.group_sems.at[1, group_at],
            device_id=self.w.at_group(self.w.group_peer(group_at + 1)),
            device_id_type=MESH,
        )

    def open_stage(self, step):
        @pl.when(step >= 2)
        def _():
            for i in range(2):
                self.core_copy(step, i).wait_send()

    def push(self, step):
        @pl.when(step >= 2)
        def _():
            pl.semaphore_wait(self.credit, 1)

        for i in range(2):
            self.core_copy(step, i).start()

    def merge(self, step):
        slot, group_at = lax.rem(step, 2), step // 2
        for half, sends in ((0, (0, 1, 2, 5)), (1, (3, 4))):

            @pl.when((slot == half) & (step >= 2))
            def _():
                for which in sends:
                    self.chip_copy(group_at, which).wait_send()

        for i in range(2):
            self.core_copy(step, i).wait_recv()
            sum_rows(
                self.pairs.at[slot, i],
                [self.stage.at[slot, 2 * i + self.w.c], self.from_core.at[slot, i]],
            )

        @pl.when(step + 2 < self.steps)
        def _():
            pl.semaphore_signal(
                self.credit, inc=1, device_id=self.w.partner(), device_id_type=MESH
            )

        @pl.when(slot == 0)
        def _():
            for which in (0, 1, 2):
                self.chip_copy(group_at, which).start()

        @pl.when(slot == 1)
        def _():
            self.chip_copy(group_at, 3).start()
            for source, i, upper, which in ((1, (1, 0), False, 4), (2, (0, 0), True, 5)):
                self.chip_copy(group_at, source).wait_recv()
                target = self.part(self.pairs.at[i], upper)
                sum_rows(target, [target, self.from_chips.at[group_at, source]])
                self.chip_copy(group_at, which).start()

    def plane_total(self, group_at):
        for which in (0, 3, 4, 5):
            self.chip_copy(group_at, which).wait_recv()
        return [
            [self.part(self.pairs.at[1, 1], upper)]
            + [self.from_chips.at[group_at, which] for which in arrived]
            for upper, arrived in ((False, (0, 4)), (True, (3, 5)))
        ]

    def advance(self, step):
        @pl.when(step >= 1)
        def _():
            last = step - 1

            @pl.when((lax.rem(last, 2) == 0) & (last >= 2))
            def _():
                group_at = last // 2 - 1
                for upper, sources in enumerate(self.plane_total(group_at)):
                    sum_rows(self.part(self.totals.at[group_at], upper), sources)
                self.group_copy(group_at).start()

            self.merge(last)

    def finish(self, out):
        steps = self.steps
        self.merge(steps - 1)
        groups = steps // 2 - 1
        halves = self.plane_total(groups)
        for d in range(groups):
            self.group_copy(d).wait_recv()
        for upper, sources in enumerate(halves):
            parts = [self.part(self.parts.at[d], upper) for d in range(groups)]
            sum_rows(self.part(out, upper), sources + parts)
        for d in range(groups):
            self.group_copy(d).wait_send()
        for i in range(2):
            self.core_copy(steps - 2, i).wait_send()
            self.core_copy(steps - 1, i).wait_send()
        for which in range(6):
            self.chip_copy(groups, which).wait_send()

    @staticmethod
    def scratch(n_groups, rows, width):
        dma = pltpu.SemaphoreType.DMA
        return [
            pltpu.VMEM((2, 4, rows, width), BF),
            pltpu.VMEM((2, 2, rows, width), BF),
            pltpu.VMEM((2, 2, rows, width), BF),
            pltpu.VMEM((n_groups, 6, rows // 2, width), BF),
            pltpu.VMEM((n_groups - 1, rows, width), BF),
            pltpu.VMEM((n_groups - 1, rows, width), BF),
            dma((2, 2, 2)),
            dma((6,)),
            dma((n_groups, 6)),
            dma((2, n_groups - 1)),
            pltpu.SemaphoreType.REGULAR,
        ]


def swiglu_both(gate, up, grad):
    sigmoid = 1.0 / (1.0 + jnp.exp(-gate))
    silu = gate * sigmoid
    return silu * up, grad * up * (sigmoid * (1.0 + gate * (1.0 - sigmoid))), grad * silu


def step_chips(w, step):
    group = lax.rem(w.g + 1 + step // 2, w.n_groups)
    return [group * 4 + chip for chip in StreamSum.chips(w, step)]


def hot_rows(place, rows, core, slot_count):
    mine = place[:, core * rows : (core + 1) * rows]
    return lax.broadcasted_iota(jnp.int32, (slot_count, rows), 0) == mine


def moe_kernel(
    n_groups, experts, first_logit, slot_count,
    h2_hbm, cot_hbm, place_ref, wg_ref, wu_ref, wd_ref, sc_ref, sd_ref,
    sum_ref, rows_ref, gin_ref, act_ref, gg_ref, gu_ref, rw_ref, sact_ref, dboth_ref, dsd_ref,
    tok_ref,
    h2_buf, cot_buf, load_sems, *comm,
):
    rows = sum_ref.shape[0]
    step, steps = pl.program_id(0), 2 * n_groups
    w = Wires(n_groups, 8, None, None)
    stream = StreamSum(w, steps, *comm[:6], comm[6:10], comm[10])
    expert_id = w.g * 4 + w.p
    half = sc_ref.shape[1] // 2

    def loads(at):
        slot = lax.rem(at, 2)
        for i, chip in enumerate(step_chips(w, at)):
            source = pl.ds(pl.multiple_of(chip * 2 * rows, 2 * rows), 2 * rows)
            target = pl.ds(i * 2 * rows, 2 * rows)
            for k, (hbm, buf) in enumerate(((h2_hbm, h2_buf), (cot_hbm, cot_buf))):
                yield pltpu.make_async_copy(
                    hbm.at[source], buf.at[slot, target], load_sems.at[slot, i, k]
                )

    @pl.when(step == 0)
    def _():
        for copy in loads(step):
            copy.start()
        w.meet()
        for ref in (dboth_ref, dsd_ref):
            ref[...] = jnp.zeros_like(ref)

    @pl.when(step + 1 < steps)
    def _():
        for copy in loads(step + 1):
            copy.start()

    for copy in loads(step):
        copy.wait()
    slot = lax.rem(step, 2)
    h2, cot = h2_buf[slot], cot_buf[slot]
    chips = step_chips(w, step)

    pre = jnp.dot(h2, sc_ref[...], preferred_element_type=F32)
    back = dot_nt(cot, sd_ref[...])
    gate, up = pre[:, :half], pre[:, half:]
    lane = lax.broadcasted_iota(jnp.int32, gate.shape, 1)
    logits = jnp.where((lane >= first_logit) & (lane < first_logit + experts), gate, -1e30)
    exps = jnp.exp(logits - jnp.max(logits, axis=1, keepdims=True))
    chosen = jnp.where(lane == first_logit + expert_id, exps, 0.0)
    weight = jnp.sum(chosen, axis=1, keepdims=True) / jnp.sum(exps, axis=1, keepdims=True)
    act, grad_gate, grad_up = swiglu_both(gate, up, back)
    shared_act = act.astype(BF)
    shared_grad = jnp.concatenate([grad_gate.astype(BF), grad_up.astype(BF)], axis=1)
    for i, chip in enumerate(chips):
        at = pl.ds(pl.multiple_of(chip * 2 * rows, 2 * rows), 2 * rows)
        sact_ref[at, :] = shared_act[i * 2 * rows : (i + 1) * 2 * rows]

    hots, weights = [], []
    for q in range(4):
        place = place_ref[pl.ds(chips[q // 2], 1), :]
        hot = hot_rows(place, rows, q % 2, slot_count).astype(F32)
        hots.append(hot)
        tokens = slice(q * rows, (q + 1) * rows)
        slots = slice(q * slot_count, (q + 1) * slot_count)
        low = hot.astype(BF)
        rows_ref[slots, :] = jnp.dot(low, h2[tokens], preferred_element_type=F32).astype(BF)
        gin_ref[slots, :] = jnp.dot(low, cot[tokens], preferred_element_type=F32).astype(BF)
        spread = jnp.broadcast_to(weight[tokens], (rows, 128))
        weights.append(
            jnp.dot(hot, spread, preferred_element_type=F32, precision=lax.Precision.HIGHEST)[:, :1]
        )
    row_weight = jnp.concatenate(weights, axis=0)
    rw_ref[...] = row_weight
    expert_rows = rows_ref[...]
    picked_cot = gin_ref[...]
    back = dot_nt(picked_cot, wd_ref[...])
    gin_ref[...] = (picked_cot.astype(F32) * row_weight).astype(BF)
    gate = dot_nt(expert_rows, wg_ref[...])
    up = dot_nt(expert_rows, wu_ref[...])
    act, grad_gate, grad_up = swiglu_both(gate, up, back * row_weight)
    act_low, grad_gate, grad_up = act.astype(BF), grad_gate.astype(BF), grad_up.astype(BF)
    act_ref[...] = act_low
    gg_ref[...] = grad_gate
    gu_ref[...] = grad_up
    picked = jnp.sum(act_low.astype(F32) * back, axis=1, keepdims=True)
    grad_rows = jnp.dot(grad_gate, wg_ref[...], preferred_element_type=F32)
    grad_rows = grad_rows + jnp.dot(grad_up, wu_ref[...], preferred_element_type=F32)
    grad_rows = grad_rows.astype(BF)
    stream.open_stage(step)
    for q in range(4):
        tokens = slice(q * rows, (q + 1) * rows)
        slots = slice(q * slot_count, (q + 1) * slot_count)
        tok_ref[pl.ds(chips[q // 2] * 2 + q % 2, 1), :] = jnp.sum(
            hots[q] * picked[slots], axis=0, keepdims=True
        )
        total = dot_tn(hots[q].astype(BF), grad_rows[slots]) + dot_nt(
            shared_grad[tokens], sc_ref[...]
        )
        stream.stage[slot, q] = total.astype(BF)
    stream.push(step)
    stream.advance(step)

    piece = h2.shape[1] // 4
    turned, turned_act = shared_grad.T, shared_act.T
    for k in range(4):
        cols = slice(k * piece, (k + 1) * piece)
        dboth_ref[:, cols] += jnp.dot(turned, h2[:, cols], preferred_element_type=F32)
        dsd_ref[:, cols] += jnp.dot(turned_act, cot[:, cols], preferred_element_type=F32)

    @pl.when(step == steps - 1)
    def _():
        stream.finish(sum_ref)


def out_kernel(
    n_groups, slot_count,
    act_ref, rw_ref, rows_ref, gin_ref, gg_ref, gu_ref, place_ref, sact_ref, wd_ref, sd_ref,
    sum_ref, dg_ref, du_ref, dd_ref, *comm,
):
    rows = sum_ref.shape[0]
    step, steps = pl.program_id(0), 2 * n_groups
    w = Wires(n_groups, 8, None, None)
    stream = StreamSum(w, steps, *comm[:6], comm[6:10], comm[10])

    @pl.when(step == 0)
    def _():
        w.meet()
        for ref in (dg_ref, du_ref, dd_ref):
            ref[...] = jnp.zeros_like(ref)

    slot = lax.rem(step, 2)
    chips = step_chips(w, step)
    out_rows = jnp.dot(act_ref[...], wd_ref[...], preferred_element_type=F32) * rw_ref[...]
    out_rows = out_rows.astype(BF)
    stream.open_stage(step)
    for q in range(4):
        chip = chips[q // 2]
        place = place_ref[pl.ds(chip, 1), :]
        low = hot_rows(place, rows, q % 2, slot_count).astype(F32).astype(BF)
        slots = slice(q * slot_count, (q + 1) * slot_count)
        shared = sact_ref[pl.ds(pl.multiple_of((chip * 2 + q % 2) * rows, rows), rows), :]
        total = dot_tn(low, out_rows[slots]) + jnp.dot(
            shared, sd_ref[...], preferred_element_type=F32
        )
        stream.stage[slot, q] = total.astype(BF)
    stream.push(step)
    stream.advance(step)

    width = rows_ref.shape[1]
    piece = width // 4
    for left_ref, right_ref, total_ref in (
        (gg_ref, rows_ref, dg_ref),
        (gu_ref, rows_ref, du_ref),
        (act_ref, gin_ref, dd_ref),
    ):
        turned = left_ref[...].T
        for k in range(4):
            cols = slice(k * piece, (k + 1) * piece)
            total_ref[:, cols] += jnp.dot(
                turned, right_ref[:, cols], preferred_element_type=F32
            )

    @pl.when(step == steps - 1)
    def _():
        stream.finish(sum_ref)


def experts_sums(
    n_groups, rows, h2, cot, place, slot_count, expert_w, shared_w, router_weight, first_id
):
    w_gate, w_up, w_down = expert_w
    s_both, s_down = shared_w
    tokens, width = h2.shape
    hidden, hidden_s = w_down.shape[0], s_down.shape[0]
    experts = router_weight.shape[1]
    steps = 2 * n_groups
    devices = tokens // rows
    step_slots = slot_count * 4
    all_slots = step_slots * steps
    half = 128
    s_cat = jnp.concatenate(
        [
            s_both[:, :hidden_s],
            router_weight,
            jnp.zeros((width, half - hidden_s - experts), BF),
            s_both[:, hidden_s:],
            jnp.zeros((width, half - hidden_s), BF),
        ],
        axis=1,
    )
    s_tall = jnp.pad(s_down, ((0, half - hidden_s), (0, 0)))

    def whole(array):
        return pl.BlockSpec(array.shape, lambda i: (0, 0), pipeline_mode=pl.Buffered(1))

    def blocked(rows, cols):
        return pl.BlockSpec((rows, cols), lambda i: (i, 0))

    shape = jax.ShapeDtypeStruct
    flops = 2 * all_slots * width * hidden * 5 + 2 * tokens * width * (4 * half + 3 * slot_count)
    shapes = [
        shape((rows, width), F32),
        shape((all_slots, width), BF),
        shape((all_slots, width), BF),
        shape((all_slots, hidden), BF),
        shape((all_slots, hidden), BF),
        shape((all_slots, hidden), BF),
        shape((all_slots, 1), F32),
        shape((tokens, half), BF),
        shape((2 * half, width), F32),
        shape((half, width), F32),
        shape((devices, rows), F32),
    ]
    specs = [
        blocked(step_slots, s.shape[1]) if s.shape[0] == all_slots else whole(s) for s in shapes
    ]
    hbm = pl.BlockSpec(memory_space=pl.ANY)
    grad_h2, rows_in, grad_in, act, grad_gate, grad_up, row_weight, s_act, *d_shared, token_grad = (
        pl.pallas_call(
            functools.partial(moe_kernel, n_groups, experts, hidden_s, slot_count),
            grid=(steps,),
            in_specs=[
                hbm,
                hbm,
                whole(place),
                whole(w_gate),
                whole(w_up),
                whole(w_down),
                whole(s_cat),
                whole(s_tall),
            ],
            out_specs=specs,
            out_shape=shapes,
            scratch_shapes=[
                pltpu.VMEM((2, 4 * rows, width), BF),
                pltpu.VMEM((2, 4 * rows, width), BF),
                pltpu.SemaphoreType.DMA((2, 2, 2)),
            ]
            + StreamSum.scratch(n_groups, rows, width),
            cost_estimate=pl.CostEstimate(
                flops=flops, bytes_accessed=12 * tokens * width, transcendentals=tokens * 1024
            ),
            compiler_params=pltpu.CompilerParams(
                collective_id=first_id,
                has_side_effects=True,
                vmem_limit_bytes=67043328,
            ),
            name="experts",
        )(h2, cot, place, w_gate, w_up, w_down, s_cat, s_tall)
    )
    shapes = [grad_h2] + [shape(x.shape, F32) for x in expert_w]
    out, d_gate, d_up, d_down = pl.pallas_call(
        functools.partial(out_kernel, n_groups, slot_count),
        grid=(steps,),
        in_specs=[
            blocked(step_slots, hidden),
            blocked(step_slots, 1),
            blocked(step_slots, width),
            blocked(step_slots, width),
            blocked(step_slots, hidden),
            blocked(step_slots, hidden),
            whole(place),
            whole(s_act),
            whole(w_down),
            whole(s_tall),
        ],
        out_specs=[whole(x) for x in shapes],
        out_shape=[shape(x.shape, F32) for x in shapes],
        scratch_shapes=StreamSum.scratch(n_groups, rows, width),
        cost_estimate=pl.CostEstimate(
            flops=2 * width * (4 * all_slots * hidden + tokens * (half + slot_count)),
            bytes_accessed=4 * tokens * width,
            transcendentals=0,
        ),
        compiler_params=pltpu.CompilerParams(
            collective_id=first_id + 1,
            has_side_effects=True,
            vmem_limit_bytes=67043328,
        ),
        name="expert_out",
    )(act, row_weight, rows_in, grad_in, grad_gate, grad_up, place, s_act, w_down, s_tall)
    d_both, d_tall = d_shared
    d_both = jnp.concatenate([d_both[:hidden_s], d_both[half : half + hidden_s]], axis=0)
    grads = (d_gate, d_up, d_down, d_both.T, d_tall[:hidden_s])
    return out, grad_h2, token_grad, grads


def body(
    n_groups, n_plane, layer_input, attn_gain, w_query, w_latent, kv_gain, w_expand, w_output,
    ffn_gain, w_router, shared_gate, shared_up, shared_down, expert_gate, expert_up,
    expert_down, routes, segments, cotangent,
):
    tok, width = layer_input.shape
    devices = n_groups * n_plane
    experts = w_router.shape[1]
    local_heads = HEADS // n_plane
    scale = (NOPE + ROPE) ** (-0.5)
    group = lax.axis_index("g")
    place_in = lax.axis_index(PLANE)
    me = lax.axis_index(ALL)
    expert_id = lax.axis_index(("g", "p"))
    plane_tok = n_plane * tok
    plane_start = group * plane_tok

    rows_w = w_router.shape[0]
    kv_n = kv_gain.shape[0]
    small = jnp.concatenate(
        [
            attn_gain,
            ffn_gain,
            kv_gain,
            w_router.reshape(-1),
            routes.reshape(-1).astype(BF),
            segments.astype(BF),
        ]
    )
    small = jnp.pad(small, (0, -small.shape[0] % 4096)).reshape(-1, 128)
    kv_cols = local_heads * (NOPE + VDIM)
    fold = kv_n * kv_cols // rows_w
    by_head = w_query.reshape(rows_w, n_plane, local_heads, NOPE + ROPE).transpose(1, 0, 2, 3)
    folded = (
        w_expand.reshape(kv_n, n_plane, kv_cols // fold, fold)
        .transpose(1, 0, 2, 3)
        .reshape(n_plane, rows_w, fold)
    )
    swap = functools.partial(exchange, n_groups, n_plane)
    wq_nope, wq_rope, expand_weight, latent_weight, small, x_plane = swap(
        0,
        ("plane_swap_gather", by_head[..., :NOPE].reshape(n_plane, rows_w, local_heads * NOPE)),
        ("plane_swap_gather", by_head[..., NOPE:].reshape(n_plane, rows_w, local_heads * ROPE)),
        ("plane_swap_gather", folded),
        ("whole_gather", w_latent),
        ("whole_gather", small),
        ("plane_gather", layer_input),
    )
    x_plane = x_plane.reshape(plane_tok, width).astype(F32)
    latent_weight = latent_weight.reshape(width, RANK + ROPE)
    wq_nope = wq_nope.reshape(width, local_heads * NOPE)
    wq_rope = wq_rope.reshape(width, local_heads * ROPE)
    expand_weight = expand_weight.reshape(RANK, kv_cols)
    small = small.reshape(devices, -1)
    cuts = [rows_w, 2 * rows_w, 2 * rows_w + kv_n, 2 * rows_w + kv_n + rows_w * experts]
    cuts = cuts + [cuts[-1] + tok * TOP, cuts[-1] + tok * TOP + tok]
    gain_one = small[:, : cuts[0]].reshape(-1).astype(F32)
    gain_two = small[:, cuts[0] : cuts[1]].reshape(-1).astype(F32)
    gain_kv = small[:, cuts[1] : cuts[2]].reshape(-1).astype(F32)
    router_weight = small[:, cuts[2] : cuts[3]].reshape(width, experts)
    routes_all = small[:, cuts[3] : cuts[4]].astype(jnp.int32).reshape(devices, tok, TOP)
    segments_all = small[:, cuts[4] : cuts[5]].astype(jnp.int32).reshape(-1)

    cotangent_later = jnp.where(x_plane[0, 0] < 1e6, cotangent, jnp.zeros_like(cotangent))

    shared_n = shared_down.shape[0]
    s_both = jnp.concatenate(
        [
            shared_gate.reshape(rows_w, devices, shared_n),
            shared_up.reshape(rows_w, devices, shared_n),
        ],
        axis=2,
    )
    s_both = s_both.transpose(1, 0, 2).reshape(n_groups, n_plane, rows_w, 2 * shared_n)

    hidden = rms_norm(x_plane, gain_one).astype(BF)
    rope_half = ROPE // 2
    positions = plane_start + jnp.arange(plane_tok, dtype=jnp.int32)
    frequency = 10000.0 ** (-jnp.arange(rope_half, dtype=F32) / rope_half)
    angles = positions.astype(F32)[:, None] * frequency[None, :]
    cosine = jnp.cos(angles)
    sine_part = jnp.sin(angles)
    cos_h = jnp.tile(cosine, (1, 2 * local_heads))
    sin_h = jnp.tile(jnp.concatenate([-sine_part, sine_part], axis=1), (1, local_heads))

    def turn(rows, direction):
        pieces = []
        for h in range(local_heads):
            at = h * ROPE
            pieces += [rows[:, at + rope_half : at + ROPE], rows[:, at : at + rope_half]]
        return rows * cos_h + jnp.concatenate(pieces, axis=1) * (direction * sin_h)

    latent = matmul(hidden, latent_weight)
    compressed_own = rms_norm(latent[:, :RANK], gain_kv).astype(BF)
    key_rope_own = rotate(latent[:, RANK:], cosine, sine_part).astype(BF)

    def own_rows(table):
        return lax.dynamic_slice_in_dim(table, place_in * tok, tok, 0)

    piece = own_rows(jnp.concatenate([compressed_own, key_rope_own], axis=1))
    before, own_output = swap(1, ("shift_gather", piece), ("head_rows", w_output))
    before = before.reshape(plane_tok, RANK + ROPE)
    own_output = own_output.reshape(local_heads * VDIM, width)
    compressed = jnp.concatenate([before[:, :RANK], compressed_own], axis=0)
    key_rope = jnp.concatenate([before[:, RANK:], key_rope_own], axis=0)
    q_nope = matmul(hidden, wq_nope).astype(BF)
    q_rope = turn(matmul(hidden, wq_rope), 1.0).astype(BF)
    expanded = matmul(compressed, expand_weight).astype(BF)
    plane_segments = lax.dynamic_slice_in_dim(segments_all, plane_start, plane_tok, 0)
    doc_start = jnp.sum(
        (segments_all[None, :] < plane_segments[:, None]).astype(jnp.int32), axis=1, keepdims=True
    )
    low_bound = doc_start - plane_start + DOC_MAX
    mixed_heads, lse = attend(low_bound, q_nope, q_rope, expanded, key_rope, scale)
    attn_out = matmul(mixed_heads, own_output).astype(BF)
    attn_out = swap(2, ("plane_sum", attn_out.reshape(n_plane, tok, width)))[0]
    input_float = layer_input.astype(F32)
    residual_one = input_float + attn_out
    h_two_f, norm_two_back = jax.vjp(rms_norm, residual_one, gain_two)
    h_two = h_two_f.astype(BF)
    router_probs = softmax_rows(matmul(h_two, router_weight))

    expert_w = (expert_gate[0].T, expert_up[0].T, expert_down[0])
    parts = max(1, devices * tok // 4096)
    if parts == 1:
        h2_all, s_both = swap(5, ("far_gather", h_two), ("whole_swap", s_both))
    else:
        s_both = swap(7, ("whole_swap", s_both))[0]
    shared_w = (s_both.reshape(width, 2 * shared_n), shared_down)
    slot_limit = 2 * tok * TOP // experts

    def on_rows(h2, h2_all, cot_gathered, routes_here):
        rows = h2.shape[0]
        slot_count = min(slot_limit, rows)
        member = jnp.any(routes_here == expert_id, axis=2)
        before_it = jnp.arange(rows)[:, None] < jnp.arange(rows)[None, :]
        rank = matmul(member.astype(BF), before_it.astype(BF)).astype(jnp.int32)
        place = jnp.where(member, rank, -1).reshape(devices // 2, 2 * rows)
        out, grad_h2, token_grad, grads = experts_sums(
            n_groups,
            rows,
            h2_all,
            cot_gathered,
            place,
            slot_count,
            expert_w,
            shared_w,
            router_weight,
            8,
        )
        picked = lax.all_to_all(token_grad, ALL, split_axis=0, concat_axis=0, tiled=True)
        picked = jnp.sum(picked.reshape(experts, devices // experts, rows), axis=1).T
        return out, grad_h2, picked, grads

    if parts == 1:
        cot_all = gather_all(cotangent_later)
        out_own, grad_h2_own, grad_router_probs, grads = on_rows(
            h_two, h2_all.reshape(-1, width), cot_all, routes_all
        )
    else:
        rows = tok // parts

        def step(total, inputs):
            h2, cot, routes_here = inputs
            cot_part = gather_all(cot)
            out, grad_h2, picked, grads = on_rows(h2, gather_all(h2), cot_part, routes_here)
            grads = lax.optimization_barrier(grads)
            total = tuple(a + b for a, b in zip(total, grads))
            return total, (out, grad_h2, picked)

        shapes = expert_w + shared_w
        grads, (out_own, grad_h2_own, grad_router_probs) = lax.scan(
            step,
            tuple(jnp.zeros(s.shape, F32) for s in shapes),
            (
                h_two.reshape(parts, rows, width),
                cotangent.reshape(parts, rows, width),
                routes_all.reshape(devices, parts, rows, TOP).transpose(1, 0, 2, 3),
            ),
        )
        out_own = out_own.reshape(tok, width)
        grad_h2_own = grad_h2_own.reshape(tok, width)
        grad_router_probs = grad_router_probs.reshape(tok, experts)
    g_gate, g_up, g_down, g_both, g_sdown = grads
    grad_logits = router_probs * (
        grad_router_probs - jnp.sum(router_probs * grad_router_probs, axis=1, keepdims=True)
    )
    grad_logits = grad_logits.astype(BF)
    grad_router = dot_tn(h_two, grad_logits)
    grad_h_two = grad_h2_own + dot_nt(grad_logits, router_weight)
    output = residual_one + out_own

    grad_x_one, grad_gain_two = norm_two_back(grad_h_two)
    grad_x_one = grad_x_one + cotangent.astype(F32)
    grad_attn_out = grad_x_one.astype(BF)
    g_shared, plane_grad = swap(
        3,
        ("whole_swap", g_both.astype(BF).reshape(n_groups, n_plane, rows_w, 2 * shared_n)),
        ("plane_gather", grad_attn_out),
    )
    plane_grad = plane_grad.reshape(plane_tok, width)
    grad_mixed = dot_nt(plane_grad, own_output).astype(BF)
    dqn, dqr, dex, dkr = attend_back(
        low_bound, q_nope, q_rope, expanded, key_rope, lse, grad_mixed, scale
    )

    g_output = dot_tn(mixed_heads, plane_grad).astype(BF).reshape(n_groups, rows_w, width)

    grad_expanded = dex.astype(BF)
    grad_expand = dot_tn(compressed, grad_expanded)
    grad_comp = dot_nt(grad_expanded, expand_weight)
    key_grads = jnp.concatenate([grad_comp, dkr], axis=1).astype(BF)
    key_grads = (
        key_grads.reshape(2, n_plane, tok, RANK + ROPE)
        .transpose(1, 0, 2, 3)
        .reshape(n_plane, 2 * tok, RANK + ROPE)
    )

    gq_nope = dqn.astype(BF)
    gq_rope = turn(dqr, -1.0).astype(BF)
    grad_hidden = (dot_nt(gq_nope, wq_nope) + dot_nt(gq_rope, wq_rope)).astype(BF)
    gw_nope = dot_tn(hidden, gq_nope).astype(BF).reshape(n_groups, n_plane, rows_w, -1)
    gw_rope = dot_tn(hidden, gq_rope).astype(BF).reshape(n_groups, n_plane, rows_w, -1)
    g_expand = grad_expand.astype(BF).reshape(n_groups, n_plane, kv_n, kv_cols)
    key_grad, grad_hidden, gw_nope, gw_rope, g_expand = swap(
        4,
        ("plane_sum_shift", key_grads),
        ("plane_sum", grad_hidden.reshape(n_plane, tok, width)),
        ("group_sum_swap", gw_nope),
        ("group_sum_swap", gw_rope),
        ("group_sum_swap", g_expand),
    )
    latent_own = own_rows(latent)
    kv_norm_back = jax.vjp(rms_norm, latent_own[:, :RANK], gain_kv)[1]
    grad_comp_in, grad_gain_kv = kv_norm_back(key_grad[:, :RANK])
    grad_rope_in = unrotate(key_grad[:, RANK:], own_rows(cosine), own_rows(sine_part))
    grad_latent = jnp.concatenate([grad_comp_in, grad_rope_in], axis=1).astype(BF)

    def per_head(table, cols):
        return table.transpose(1, 0, 2).reshape(rows_w, HEADS, cols)

    grad_query_weight = jnp.concatenate(
        [per_head(gw_nope, NOPE), per_head(gw_rope, ROPE)], axis=2
    ).reshape(rows_w, -1).astype(F32)
    grad_expand_weight = g_expand.transpose(1, 0, 2).reshape(kv_n, -1).astype(F32)

    g_latent = dot_tn(own_rows(hidden), grad_latent).astype(BF)
    g_latent = g_latent.reshape(n_groups, n_plane, rows_w, RANK + ROPE)
    grad_hidden = grad_hidden + dot_nt(grad_latent, latent_weight)
    norm_one_back = jax.vjp(rms_norm, input_float, gain_one)[1]
    grad_x_norm, grad_gain_one = norm_one_back(grad_hidden)
    grad_input = grad_x_one + grad_x_norm

    small_grads = jnp.concatenate(
        [
            p.reshape(devices, -1)
            for p in (grad_gain_one, grad_gain_two, grad_gain_kv, grad_router)
        ],
        axis=1,
    )
    small_grads = jnp.pad(small_grads, ((0, 0), (0, -small_grads.shape[1] % 1024)))
    grad_latent_weight, grad_output_weight, small_grads = swap(
        6,
        ("whole_sum", g_latent),
        ("group_sum_home", g_output),
        ("whole_sum", small_grads.reshape(n_groups, n_plane, -1, 128)),
    )
    small_grads = small_grads.reshape(-1)
    g_shared = g_shared.transpose(2, 0, 1, 3).reshape(rows_w, devices, 2 * shared_n).astype(F32)
    grad_shared_gate = g_shared[:, :, :shared_n].reshape(rows_w, devices * shared_n)
    grad_shared_up = g_shared[:, :, shared_n:].reshape(rows_w, devices * shared_n)
    return (
        output,
        grad_input,
        small_grads[: cuts[0]],
        grad_query_weight,
        grad_latent_weight,
        small_grads[cuts[1] : cuts[2]],
        grad_expand_weight,
        grad_output_weight,
        small_grads[cuts[0] : cuts[1]],
        small_grads[cuts[2] : cuts[3]].reshape(rows_w, experts),
        grad_shared_gate,
        grad_shared_up,
        g_sdown,
        g_gate.T[None],
        g_up.T[None],
        g_down[None],
    )


def solution(mesh):
    n_expert, n_shard = mesh.shape["expert"], mesh.shape["wshard"]
    devices = n_expert * n_shard

    def program(*args):
        tok = args[0].shape[0] // devices
        n_plane = DOC_MAX // tok
        n_groups = devices // n_plane
        inner = Mesh(mesh.devices.reshape(n_groups, n_plane // n_shard, n_shard), ALL)
        rows, vector = P(ALL, None), P(ALL)
        wide, tall = P(("g", "p"), None, "c"), P(("g", "p"), "c", None)
        step = jax.shard_map(
            functools.partial(body, n_groups, n_plane),
            mesh=inner,
            in_specs=(
                rows, vector, rows, rows, vector, rows, rows, vector, rows, rows, rows, rows,
                wide, wide, tall, rows, vector, rows,
            ),
            out_specs=(
                rows, rows, vector, rows, rows, vector, rows, rows, vector, rows, rows, rows,
                rows, wide, wide, tall,
            ),
            check_vma=False,
        )
        return step(*args)

    return program
```
